128 devices in a mesh: rep: 1, dp: 128 (over x, y, z, core).
Axes of the slice: x: 4, y: 4, z: 4, core: 2. Of those that a mesh axis runs over, the one named last changes fastest.
Arguments:
- x: bfloat16 [128, 1024, 1536], P(('rep', 'dp'))
- dy: bfloat16 [128, 1024, 1536], P(('rep', 'dp'))
- w_gate: bfloat16 [2, 1536, 4224], replicated
- w_up: bfloat16 [2, 1536, 4224], replicated
- w_down: bfloat16 [2, 4224, 1536], replicated
- m_w_gate: float32 [2, 1536, 4224], P(None, 'dp')
- m_w_up: float32 [2, 1536, 4224], P(None, 'dp')
- m_w_down: float32 [2, 4224, 1536], P(None, 'dp')
- v_w_gate: float32 [2, 1536, 4224], P(None, 'dp')
- v_w_up: float32 [2, 1536, 4224], P(None, 'dp')
- v_w_down: float32 [2, 4224, 1536], P(None, 'dp')
Outputs:
- output 1: bfloat16 [2, 1536, 4224], P('rep')
- output 2: bfloat16 [2, 1536, 4224], P('rep')
- output 3: bfloat16 [2, 4224, 1536], P('rep')
- output 4: float32 [2, 1536, 4224], P('rep', 'dp')
- output 5: float32 [2, 1536, 4224], P('rep', 'dp')
- output 6: float32 [2, 4224, 1536], P('rep', 'dp')
- output 7: float32 [2, 1536, 4224], P('rep', 'dp')
- output 8: float32 [2, 1536, 4224], P('rep', 'dp')
- output 9: float32 [2, 4224, 1536], P('rep', 'dp')
All inputs are finite; a program needn't handle non-finite values.
Results may differ from the reference program's by a relative error of at most 0.022.
Values are sent between devices in bfloat16 or wider.
A program may use at most 1.5 GiB of HBM per device.

```python
import jax
import jax.numpy as jnp
from jax import lax

SEQUENCES = 128
TOKENS = 1024
D = 1536
FF = 4224
LAYERS = 2
NAMES = ("w_gate", "w_up", "w_down")
SHAPES = {"w_gate": (LAYERS, D, FF), "w_up": (LAYERS, D, FF), "w_down": (LAYERS, FF, D)}


def bump(key, n, height):
    away = (jnp.arange(n, dtype=jnp.int32) - jax.random.randint(key, (), 0, n, jnp.int32)) % n
    return jnp.where(away < n // 8, height, 1.0)


def together(key, own, strength):
    shared = jax.random.normal(key, own.shape[1:], jnp.float32)
    return (own + strength * shared) * lax.rsqrt(1 + strength * strength)


def setup_inputs(seed: int = 0, part: int = 0) -> dict:
    kx, kdy, ka, kb, kz, kf, kh, kl, *keys = jax.random.split(jax.random.key(seed), 8 + 3 * len(NAMES))
    kx, kdy, ka, kb = (jax.random.fold_in(k, part) for k in (kx, kdy, ka, kb))
    kw, km, kv = (keys[i::3] for i in range(3))
    shape = (SEQUENCES, TOKENS, D)
    much_x, much_dy = jax.random.uniform(kz, (2,), jnp.float32, 0.0, 1.0)
    loud = 2.0 ** jax.random.uniform(jax.random.fold_in(kz, 1), (), jnp.float32, -1.0, 2.0)
    layers = 2.0 ** jax.random.uniform(kl, (LAYERS, 1, 1), jnp.float32, -1.0, 1.0)
    x = together(ka, jax.random.normal(kx, shape, jnp.float32), much_x) * bump(kf, D, 4.0)
    dy = together(kb, jax.random.normal(kdy, shape, jnp.float32), much_dy)
    drawn = {"x": x.astype(jnp.bfloat16), "dy": (loud * dy * (SEQUENCES * TOKENS) ** -0.5).astype(jnp.bfloat16)}
    for key, name in zip(kw, NAMES, strict=True):
        w = jax.random.normal(key, SHAPES[name], jnp.float32) * SHAPES[name][1] ** -0.5
        drawn[name] = (w * {"w_gate": 1.0, "w_up": bump(kh, FF, 4.0), "w_down": layers}[name]).astype(jnp.bfloat16)
    for key, name in zip(km, NAMES, strict=True):
        drawn[f"m_{name}"] = 0.1 * jax.random.normal(key, SHAPES[name], jnp.float32)
    for key, name in zip(kv, NAMES, strict=True):
        drawn[f"v_{name}"] = jax.random.uniform(key, SHAPES[name], jnp.float32, 0.005, 0.015)
    return drawn


def matmul(a, w):
    return jnp.dot(a, w, preferred_element_type=jnp.float32).astype(jnp.bfloat16)


def normed(h):
    wide = h.astype(jnp.float32)
    scale = lax.rsqrt(jnp.mean(wide**2, -1, keepdims=True) + 1e-6)
    return (wide * scale).astype(jnp.bfloat16)


def layer(h, w):
    a = normed(h)
    gate = jnp.dot(a, w["w_gate"], preferred_element_type=jnp.float32)
    up = jnp.dot(a, w["w_up"], preferred_element_type=jnp.float32)
    return h + matmul((jax.nn.silu(gate) * up).astype(jnp.bfloat16), w["w_down"])


def adamw(w, m, v, g):
    m = 0.9 * m + 0.1 * g
    v = 0.95 * v + 0.05 * g * g
    step = m * lax.rsqrt(v + 1e-8) + 0.1 * w
    return (w - 0.02 * step).astype(jnp.bfloat16), m, v


def clipped(gradients, sum_of_squares, count):
    factor = jnp.minimum(1.0, 0.5 * lax.rsqrt(sum_of_squares / count + 1e-30))
    return [g * factor for g in gradients]


def stack(weights, h):
    return lax.scan(lambda h, w: (layer(h, w), None), h, weights)[0]


def reference(x, dy, w_gate, w_up, w_down, m_w_gate, m_w_up, m_w_down, v_w_gate, v_w_up, v_w_down):
    weights = dict(zip(NAMES, (w_gate, w_up, w_down), strict=True))

    def take(so_far, sequence):
        h, by_y = sequence
        _, back = jax.vjp(lambda w: stack(w, h), weights)
        return jax.tree.map(lambda total, term: total + term.astype(jnp.float32), so_far, back(by_y)[0]), None

    none_yet = {name: jnp.zeros(w.shape, jnp.float32) for name, w in weights.items()}
    by_weights, _ = lax.scan(take, none_yet, (x, dy))
    gradients = [by_weights[name].astype(jnp.bfloat16).astype(jnp.float32) for name in NAMES]
    gradients = clipped(gradients, sum(jnp.sum(g * g) for g in gradients), sum(g.size for g in gradients))
    new = [
        adamw(w.astype(jnp.float32), m, v, g)
        for w, m, v, g in zip((w_gate, w_up, w_down), (m_w_gate, m_w_up, m_w_down), (v_w_gate, v_w_up, v_w_down), gradients, strict=True)
    ]
    return tuple(one[which] for which in range(3) for one in new)
```

```python
import jax
import jax.numpy as jnp
from jax import lax
from jax.sharding import PartitionSpec as P

F32, BF16 = jnp.float32, jnp.bfloat16
CLIP_EPS = 1e-30


def dot(a, b, dims):
    return lax.dot_general(a, b, (dims, ((), ())), preferred_element_type=F32)


def norm_scale(h):
    wide = h.astype(F32)
    return wide, lax.rsqrt(jnp.mean(wide * wide, -1, keepdims=True) + 1e-6)


def normed(h):
    wide, scale = norm_scale(h)
    return (wide * scale).astype(BF16)


def hidden_back(gate, up, dp):
    dp = dp.astype(F32)
    s = jax.nn.sigmoid(gate)
    act = gate * s
    return (dp * up * (s + act * (1.0 - s))).astype(BF16), (dp * act).astype(BF16)


def norm_back(h, da):
    wide, scale = norm_scale(h)
    da = da.astype(F32)
    return (scale * da - wide * (scale * scale * scale * jnp.mean(da * wide, -1, keepdims=True))).astype(BF16)


def adamw(w, m, v, g):
    w = w.astype(F32)
    m = 0.9 * m + 0.1 * g
    v = 0.95 * v + 0.05 * g * g
    step = m * lax.rsqrt(v + 1e-8) + 0.1 * w
    return (w - 0.02 * step).astype(BF16), m, v


def solution(mesh):
    n = mesh.shape["dp"]

    pairs = [[2 * i, 2 * i + 1] for i in range(n // 2)]
    alike = [list(range(c, n, 2)) for c in range(2)]

    def body(x, dy, wg, wu, wd, mg, mu, md, vg, vu, vd):
        x, dy = x[0], dy[0]
        d, ff = wg.shape[1:]
        half = d // 2

        def summed(two, rows):
            mine = lax.psum_scatter(two, "dp", scatter_dimension=0, axis_index_groups=pairs)
            mine = mine.reshape(n // 2, rows, mine.shape[-1])
            return lax.psum_scatter(mine, "dp", scatter_dimension=0, axis_index_groups=alike)

        def down_sum(p, dy):
            two = [dot(p, dy[:, i * half : (i + 1) * half], ((0,), (0,))).astype(BF16) for i in range(2)]
            return summed(jnp.stack(two), 2 * ff // n)

        def gate_up_sum(a, dg, du):
            two = [dot(a, t, ((0,), (0,))).astype(BF16) for t in (dg, du)]
            return summed(jnp.stack(two), 2 * d // n)

        a0 = normed(x)
        gate0, up0 = dot(a0, wg[0], ((1,), (0,))), dot(a0, wu[0], ((1,), (0,)))
        p0 = (jax.nn.silu(gate0) * up0).astype(BF16)
        h1 = x + dot(p0, wd[0], ((1,), (0,))).astype(BF16)
        a1 = normed(h1)
        gate1, up1 = dot(a1, wg[1], ((1,), (0,))), dot(a1, wu[1], ((1,), (0,)))
        p1 = (jax.nn.silu(gate1) * up1).astype(BF16)
        sd1 = down_sum(p1, dy)
        dp1 = dot(dy, wd[1], ((1,), (1,))).astype(BF16)
        dg1, du1 = hidden_back(gate1, up1, dp1)
        sgu1 = gate_up_sum(a1, dg1, du1)
        da1 = dot(dg1, wg[1], ((1,), (1,))).astype(BF16) + dot(du1, wu[1], ((1,), (1,))).astype(BF16)
        dh1 = dy + norm_back(h1, da1)
        dp0 = dot(dh1, wd[0], ((1,), (1,))).astype(BF16)
        dg0, du0 = hidden_back(gate0, up0, dp0)
        sd0 = down_sum(p0, dh1)
        sgu0 = gate_up_sum(a0, dg0, du0)

        count = 3 * 2 * d * ff
        squares = sum(jnp.sum(g.astype(F32) ** 2) for g in (sd1, sgu1, sd0, sgu0))
        total = lax.psum(squares, "dp")
        factor = jnp.minimum(1.0, 0.5 * lax.rsqrt(total / count + CLIP_EPS))
        core = lax.axis_index("dp") % 2

        def own_rows(s):
            both = lax.all_gather(s, "dp", axis_index_groups=pairs)
            rows = s.shape[0] // 2
            return lax.dynamic_slice_in_dim(both, core * rows, rows, 1).astype(F32)

        gu = [own_rows(s) for s in (sgu0, sgu1)]
        down = [own_rows(s) for s in (sd0, sd1)]
        grads = [[t[0] for t in gu], [t[1] for t in gu], [jnp.concatenate([t[0], t[1]], -1) for t in down]]
        me = lax.axis_index("dp")
        ws, ms, vs = [], [], []
        for pair, w, m, v in zip(grads, (wg, wu, wd), (mg, mu, md), (vg, vu, vd), strict=True):
            rows = m.shape[1]
            own = lax.dynamic_slice_in_dim(w, me * rows, rows, 1)
            new = [adamw(own[i], m[i], v[i], pair[i] * factor) for i in range(2)]
            ws.append(jnp.stack([lax.all_gather(new[i][0], "dp", axis=0, tiled=True) for i in range(2)]))
            ms.append(jnp.stack([new[i][1] for i in range(2)]))
            vs.append(jnp.stack([new[i][2] for i in range(2)]))
        return (*ws, *ms, *vs)

    shard = P(None, "dp", None)
    return jax.shard_map(
        body,
        mesh=mesh,
        in_specs=(P(("rep", "dp")), P(("rep", "dp")), P(), P(), P(), *[shard] * 6),
        out_specs=(P("rep"), P("rep"), P("rep"), *[P("rep", "dp", None)] * 6),
        check_vma=False,
    )
```

```python
import functools

import jax
import jax.numpy as jnp
from jax import lax
from jax.experimental import pallas as pl
from jax.experimental.layout import Layout, with_layout_constraint
from jax.experimental.pallas import tpu as pltpu
from jax.sharding import PartitionSpec as P

F32, BF16 = jnp.float32, jnp.bfloat16
CLIP_EPS = 1e-30
LANES = 128
SIDE = 4
ORDERS = ((0, 1, 2), (1, 2, 0), (2, 0, 1))
VMEM_LIMIT = 63 * 1024 * 1024


class Place:
    def __init__(self):
        me = lax.axis_index("dp")
        self.core = lax.rem(me, 2)
        chip = lax.div(me, 2)
        self.at = (lax.div(chip, SIDE * SIDE), lax.rem(lax.div(chip, SIDE), SIDE), lax.rem(chip, SIDE))

    def device(self, axis=None, off=0, core=None):
        at = list(self.at)
        if axis is not None:
            at[axis] = lax.rem(at[axis] + off, SIDE)
        core = self.core if core is None else core
        return {"dp": ((at[0] * SIDE + at[1]) * SIDE + at[2]) * 2 + core}

    def partner(self):
        return self.device(core=1 - self.core)

    def onward(self, way):
        return 1 + 2 * lax.rem(way + self.core, 2)

    def block(self, axis, way, hops):
        return lax.rem(self.at[axis] + hops * (SIDE - self.onward(way)), SIDE)


def signal_all(devices):
    barrier = pltpu.get_barrier_semaphore()
    for d in devices:
        pl.semaphore_signal(barrier, inc=1, device_id=d, device_id_type=pl.DeviceIdType.MESH)
    pl.semaphore_wait(barrier, len(devices))


def near(place):
    return [place.partner()] + [place.device(axis, off) for axis in range(3) for off in (1, SIDE - 1)]


def put(src, dst, send, recv, device):
    return pltpu.make_async_remote_copy(
        src_ref=src, dst_ref=dst, send_sem=send, recv_sem=recv, device_id=device, device_id_type=pl.DeviceIdType.MESH
    )


def ways_of(cols):
    tiles = cols // LANES
    first = (tiles + 1) // 2 * LANES
    return ((0, first), (first, cols - first))


def index(order, values):
    out = [None] * 3
    for axis, value in zip(order, values, strict=True):
        out[axis] = value
    return tuple(out)


ALL = slice(None)


class Rings:
    def __init__(self, place, rows, cols, slots, sems):
        self.place, self.rows, self.slots, self.sems = place, rows // 3, slots, sems
        self.ways = ways_of(cols)

    def part(self, t, way):
        start, width = self.ways[way]
        return pl.ds(t * self.rows, self.rows), pl.ds(start, width)

    @staticmethod
    def pairs():
        return [(t, way) for t in range(3) for way in range(2)]

    def send(self, axis, way, src, landing, key, sems):
        src = landing if src is None else src
        return put(src, landing, sems[0].at[key], sems[1].at[key], self.place.device(axis, self.place.onward(way)))


class First(Rings):
    @staticmethod
    def scratch(rows, cols):
        third, dma = rows // 3, pltpu.SemaphoreType.DMA
        slots = [pltpu.VMEM((3, 3, SIDE, SIDE, third, width), BF16) for _, width in ways_of(cols)]
        return [pltpu.VMEM((SIDE, SIDE, SIDE, rows, cols), BF16), *slots, dma((3, 2, 3, SIDE)), dma((3, 2, 3, SIDE))]

    @classmethod
    def of(cls, place, rows, cols, refs):
        one = cls(place, rows, cols, refs[1:3], refs[3:5])
        one.held = refs[0]
        return one

    def block(self, t, way, hops, k, c=ALL):
        order = ORDERS[t]
        return self.held.at[(*index(order, (self.place.block(order[0], way, hops), k, c)), *self.part(t, way))]

    def message(self, t, way, n, k, arriving=False):
        src = None
        if not arriving:
            src = self.block(t, way, 1, k) if isinstance(n, int) and n == 0 else self.slots[way].at[t, n - 1, k]
        return self.send(ORDERS[t][0], way, src, self.slots[way].at[t, n, k], (t, way, n, k), self.sems)

    def start(self, k):
        for t, way in self.pairs():
            self.message(t, way, 0, k).start()

    def step(self, n, k):
        for t, way in self.pairs():
            self.message(t, way, n - 1, k, arriving=True).wait_recv()
            slots = self.slots[way]
            for c in range(SIDE):
                own = self.block(t, way, n + 1, k, c)
                slots[t, n - 1, k, c] = (slots[t, n - 1, k, c].astype(F32) + own[...].astype(F32)).astype(BF16)
            pl.when(n < 3)(lambda t=t, way=way: self.message(t, way, n, k).start())

    def tick(self, i):
        pl.when(i < SIDE)(lambda: self.start(i))
        pl.when(i >= SIDE)(lambda: self.step(lax.div(i, SIDE), lax.rem(i, SIDE)))

    def results(self):
        return [slots.at[:, 2] for slots in self.slots]

    def drain(self):
        def sent(k, _):
            for t, way in self.pairs():
                self.message(t, way, 0, k).wait_send()
                lax.fori_loop(1, 3, lambda n, _: (self.message(t, way, n, k).wait_send(), 0)[1], 0)
            return 0

        lax.fori_loop(0, SIDE, sent, 0)


class Rest(Rings):
    @staticmethod
    def scratch(rows, cols):
        third, dma = rows // 3, pltpu.SemaphoreType.DMA
        shapes = [pltpu.VMEM((*lead, third, width), BF16) for lead in ((3, 3, SIDE), (3, 3)) for _, width in ways_of(cols)]
        return shapes + [dma((3, 2, 3))] * 4

    @classmethod
    def of(cls, place, rows, cols, before, refs):
        one = cls(place, rows, cols, refs[:4], refs[4:8])
        one.before = before
        return one

    def message(self, phase, t, way, n, arriving=False):
        slots = self.slots[2 * phase - 2 + way]
        axis = ORDERS[t][phase]
        if arriving:
            src = None
        elif isinstance(n, int) and n == 0:
            v = self.place.block(axis, way, 1)
            src = self.before[way].at[t, v] if phase == 1 else self.slots[way].at[t, 2, v]
        else:
            src = slots.at[t, n - 1]
        return self.send(axis, way, src, slots.at[t, n], (t, way, n), self.sems[2 * phase - 2 : 2 * phase])

    def start(self, phase):
        for t, way in self.pairs():
            self.message(phase, t, way, 0).start()

    def step1(self, n):
        for t, way in self.pairs():
            self.message(1, t, way, n - 1, arriving=True).wait_recv()
            v = self.place.block(ORDERS[t][1], way, n + 1)
            before, slots = self.before[way], self.slots[way]
            for c in range(SIDE):
                slots[t, n - 1, c] = (slots[t, n - 1, c].astype(F32) + before[t, v, c].astype(F32)).astype(BF16)
            pl.when(n < 3)(lambda t=t, way=way: self.message(1, t, way, n).start())

    def step2(self, n):
        for t, way in self.pairs():
            self.message(2, t, way, n - 1, arriving=True).wait_recv()
            v = self.place.block(ORDERS[t][2], way, n + 1)
            before, slots = self.slots[way], self.slots[2 + way]
            slots[t, n - 1] = (slots[t, n - 1].astype(F32) + before[t, 2, v].astype(F32)).astype(BF16)
            pl.when(n < 3)(lambda t=t, way=way: self.message(2, t, way, n).start())

    def tick(self, i):
        pl.when(i == 0)(lambda: self.start(1))
        pl.when((i >= 1) & (i <= 3))(lambda: self.step1(i))
        pl.when(i == 3)(lambda: self.start(2))
        pl.when((i >= 4) & (i <= 6))(lambda: self.step2(i - 3))

    def result(self, out):
        for t, way in self.pairs():
            out[self.part(t, way)] = self.slots[2 + way][t, 2]

    def drain(self):
        for t, way in self.pairs():
            for phase in (1, 2):
                for n in range(3):
                    self.message(phase, t, way, n).wait_send()


def loads_down(source, first, sems):
    return [pltpu.make_async_copy(source.at[:, :, pl.ds(64 * z, 72)], first.held.at[:, :, z], sems.at[z]) for z in range(SIDE)]


def spread(j, steps, count, tick):
    low, high = lax.div(count * j, steps), lax.div(count * (j + 1), steps)
    lax.fori_loop(low, high, lambda i, _: (tick(i), 0)[1], 0)


def copies(sources, targets, sems):
    return [pltpu.make_async_copy(s, t, sems.at[i]) for i, (s, t) in enumerate(zip(sources, targets, strict=True))]


def begin(all_copies):
    for copy in all_copies:
        copy.start()


def end(all_copies):
    for copy in all_copies:
        copy.wait()


def half_sums(rows, cols):
    return [(3, SIDE, SIDE, rows // 3, width) for _, width in ways_of(cols)]


PREV = 6
DOWN_ROWS = 33


class Gather:
    def __init__(self, place, bufs, sems, outs, copy_sems):
        self.place, self.bufs, self.sems, self.outs, self.copy_sems = place, bufs, sems, outs, copy_sems

    @staticmethod
    def scratch(gate_cols, down_cols):
        bufs = [pltpu.VMEM((2, SIDE, SIDE, SIDE, 24, gate_cols), BF16), pltpu.VMEM((2, SIDE, SIDE, SIDE, 72, down_cols), BF16)]
        return bufs + [pltpu.SemaphoreType.DMA((2, 3, 2, 3, 3))] * 4 + [pltpu.SemaphoreType.DMA((2,))] * 3

    def part(self, kind, t, way):
        rows, cols = self.bufs[kind].shape[-2:]
        start, width = ways_of(cols)[way]
        return pl.ds(t * (rows // 3), rows // 3), pl.ds(start, width)

    def message(self, kind, l, t, way, phase, n, hops):
        order, place = ORDERS[t], self.place
        v = place.block(order[phase], way, hops)
        values = [ALL] * phase + [v] + [place.at[axis] for axis in order[phase + 1 :]]
        ref = self.bufs[kind].at[(l, *index(order, values), *self.part(kind, t, way))]
        key = (l, t, way, phase, n)
        axis = order[phase]
        return put(ref, ref, self.sems[2 * kind].at[key], self.sems[2 * kind + 1].at[key], place.device(axis, place.onward(way)))

    def copies(self, kind, l, t, way, v):
        order = ORDERS[t]
        rows, cols = self.part(kind, t, way)
        if kind == 0:
            at = (l, *index(order, (ALL, ALL, v)), rows, cols)
            return [(lambda out, at=at: (self.bufs[0].at[at], out.at[at]))]
        half = self.bufs[1].shape[-1]
        start, width = ways_of(half)[way]
        columns = pl.ds(pl.multiple_of(self.place.core * half + start, LANES), width)

        def pair(out, z, count):
            x, y, _ = index(order, (ALL, ALL, v))
            src = self.bufs[1].at[l, x, y, z, pl.ds(24 * t, count), cols]
            return src, out.at[l, x, y, pl.ds(64 * z + 24 * t, count), columns]

        if order[2] == 2:
            return [lambda out: pair(out, v, 24)]
        return [lambda out, z=z: pair(out, z, 16 if t == 2 and z < SIDE - 1 else 24) for z in range(SIDE)]

    def copy_out(self, kind, l, t, way, v):
        local, send, recv = self.copy_sems

        def both(out):
            for pair in self.copies(kind, l, t, way, v):
                src, dst = pair(out)
                pltpu.make_async_copy(src, dst, local.at[kind]).start()
                put(src, dst, send.at[kind], recv.at[kind], self.place.partner()).start()

        if kind:
            both(self.outs[2])
        else:
            for core in range(2):
                pl.when(self.place.core == core)(lambda core=core: both(self.outs[core]))

    def parts(self):
        return [(kind, t, way) for kind in range(2) for t in range(3) for way in range(2)]

    def own(self, l):
        for kind, t, way in self.parts():
            self.message(kind, l, t, way, 0, 0, 0).start()

    def phase(self, phase):
        def step(i, _):
            n, l = 1 + lax.div(i, 2), lax.rem(i, 2)
            for kind, t, way in self.parts():
                self.message(kind, l, t, way, phase, n - 1, n).wait_recv()
                pl.when(n < 3)(lambda kind=kind, t=t, way=way: self.message(kind, l, t, way, phase, n, n).start())
                if phase < 2:

                    @pl.when(n == 3)
                    def _(kind=kind, t=t, way=way):
                        self.message(kind, l, t, way, phase + 1, 0, 0).start()
                        if phase == 1:
                            self.copy_out(kind, l, t, way, self.place.at[ORDERS[t][2]])

                else:
                    self.copy_out(kind, l, t, way, self.place.block(ORDERS[t][2], way, n))
            return 0

        lax.fori_loop(0, 6, step, 0)

    def drain(self):
        local, send, recv = self.copy_sems
        half = self.bufs[1].shape[-1]
        columns = self.outs[2].at[:, :, :, :, pl.ds(0, half)]
        for kind, whole in ((0, self.outs[0]), (1, columns)):
            pltpu.make_async_copy(whole, whole, local.at[kind]).wait()
            copy = put(whole, whole, send.at[kind], recv.at[kind], self.place.partner())
            copy.wait_send()
            copy.wait_recv()

        def sent(i, _):
            l, n = lax.div(i, 3), lax.rem(i, 3)
            for phase in range(3):
                for kind, t, way in self.parts():
                    self.message(kind, l, t, way, phase, n, n).wait_send()
            return 0

        lax.fori_loop(0, 6, sent, 0)


def finish_kernel(count, *refs):
    sums_gu, sums_d, m_in, v_in, w_in = refs[0:2], refs[2:4], refs[4:7], refs[7:10], refs[10:13]
    w_out, m_out, v_out = refs[13:16], refs[16:19], refs[19:22]
    moments_gu, moments_d, old_gu, old_d, other_d, tiles = refs[22:28]
    load_sem, early_send, early_recv, norm_send, norm_recv, late_local, late_send, late_recv = refs[28:36]
    gather_refs = refs[36:]
    place = Place()
    x, y, z = place.at
    core = place.core
    gather = Gather(place, gather_refs[:2], gather_refs[2:6], w_out, gather_refs[6:9])
    partner = place.partner()
    gate_tiles, down_tiles = sums_gu[0].shape[1] // LANES, sums_d[0].shape[1] // LANES
    gate_stride, down_stride = 2 * gate_tiles, 4 * down_tiles
    gate_size, down_size = 12 * gate_stride, DOWN_ROWS * down_stride

    def blank(i, _):
        for which in range(2):
            moments_d[which, pl.ds(pl.multiple_of(8 * i, 8), 8), :] = jnp.zeros((8, LANES), F32)
        return 0

    lax.fori_loop(0, moments_d.shape[1] // 8, blank, 0)
    following = [place.device(2, 1, core=c) for c in range(2)]
    others = [place.device(axis, 2) for axis in range(3)] + [place.device(2, off, core=1 - core) for off in (1, SIDE - 1)]
    signal_all(near(place) + others)

    def gate_rows(i, which):
        return moments_gu.at[i, pl.ds(pl.multiple_of(which * gate_size, 8), gate_size)]

    def down_rows(i, first, rows):
        return moments_d.at[i, pl.ds(pl.multiple_of(first * down_stride, 8), rows * down_stride)]

    def columns(ref):
        half = down_tiles * LANES
        return ref.at[:, x, y, pl.ds(pl.multiple_of(64 * z, 8), 72), pl.ds(pl.multiple_of(core * half, LANES), half)]

    own_rows = PREV + 2 * z + DOWN_ROWS * core
    loads, sends = [], []
    for i, moment in enumerate((m_in, v_in)):
        for c in range(2):

            @pl.when(core == c)
            def _(i=i, moment=moment, c=c):
                pltpu.make_async_copy(moment[c], gate_rows(i, core), load_sem.at[i]).start()
                put(moment[1 - c], gate_rows(i, core), early_send.at[i], early_recv.at[i], partner).start()

        loads.append(pltpu.make_async_copy(moment[0], gate_rows(i, core), load_sem.at[i]))
        sends.append(put(moment[0], gate_rows(i, core), early_send.at[i], early_recv.at[i], partner))
        loads.append(pltpu.make_async_copy(moment[2], down_rows(i, own_rows, DOWN_ROWS), load_sem.at[2 + i]))
        loads[-1].start()
        sends.append(put(moment[2], down_rows(i, own_rows, DOWN_ROWS), early_send.at[2 + i], early_recv.at[2 + i], partner))
        sends[-1].start()
        last = moment[2].at[pl.ds((DOWN_ROWS - PREV) * down_stride, PREV * down_stride)]
        landing = down_rows(i, 2 * lax.rem(z + 1, SIDE), PREV)

        @pl.when(core == 1)
        def _(i=i, last=last, landing=landing):
            for c in range(2):
                put(last, landing, early_send.at[4 + 2 * i + c], early_recv.at[4 + i], following[c]).start()

    for l in range(2):
        sends.append(put(sums_d[l], other_d.at[l], early_send.at[8 + l], early_recv.at[6 + l], partner))
        sends[-1].start()
    for c in range(2):

        @pl.when(core == c)
        def _(c=c):
            pltpu.make_async_copy(w_in[c].at[:, x, y, z], old_gu, load_sem.at[4]).start()

    loads.append(pltpu.make_async_copy(w_in[0].at[:, x, y, z], old_gu, load_sem.at[4]))
    loads.append(pltpu.make_async_copy(columns(w_in[2]), old_d, load_sem.at[5]))
    loads[-1].start()

    squares = jnp.zeros((8, LANES), F32)
    for l in range(2):

        def of_gate_up(j, total, l=l):
            for t in range(3):
                g = sums_gu[l][pl.ds(8 * t, 8), pl.ds(pl.multiple_of(j * LANES, LANES), LANES)].astype(F32)
                total += g * g
            return total

        squares = lax.fori_loop(0, gate_tiles, of_gate_up, squares)

        def of_down(i, total, l=l):
            row = 8 * i + lax.broadcasted_iota(jnp.int32, (8, LANES), 0)
            mine = (row >= 2 * z) & (row < 2 * z + 2 * DOWN_ROWS)
            for j in range(down_tiles):
                g = sums_d[l][pl.ds(pl.multiple_of(8 * i, 8), 8), pl.ds(j * LANES, LANES)].astype(F32)
                total += jnp.where(mine, g * g, 0.0)
            return total

        squares = lax.fori_loop(0, 9, of_down, squares)
    for stage, (coordinate, size) in enumerate(((core, 2), (x, SIDE), (y, SIDE), (z, SIDE))):
        tiles[stage, coordinate] = squares
        exchanges = []
        for off in range(1, size):
            target = partner if stage == 0 else place.device(stage - 1, off)
            key = 3 * stage + off - 1
            here = tiles.at[stage, coordinate]
            exchanges.append(put(here, here, norm_send.at[key], norm_recv.at[key], target))
            exchanges[-1].start()
        for exchange in exchanges:
            exchange.wait_recv()
        for exchange in exchanges:
            exchange.wait_send()
        squares = tiles[stage, 0]
        for other in range(1, size):
            squares += tiles[stage, other]
    total = jnp.sum(jnp.sum(squares, 0, keepdims=True), 1, keepdims=True)
    factor = jnp.minimum(1.0, 0.5 * lax.rsqrt(total / count + CLIP_EPS))

    for copy in loads:
        copy.wait()
    for copy in sends:
        copy.wait_recv()
    for i in range(2):
        put(down_rows(i, 0, PREV), down_rows(i, 0, PREV), early_send.at[0], early_recv.at[4 + i], partner).wait_recv()

    def moments(ref, start, stride, g):
        rows = pl.ds(start, 8, stride=stride)
        m = 0.9 * ref[0, rows, :] + 0.1 * g
        v = 0.95 * ref[1, rows, :] + 0.05 * g * g
        ref[0, rows, :] = m
        ref[1, rows, :] = v
        return m * lax.rsqrt(v + 1e-8)

    def weight(w, step):
        w = w.astype(F32)
        return (w - 0.02 * (step + 0.1 * w)).astype(BF16)

    for l in range(2):

        def gate_up(j, _, l=l):
            lanes = pl.ds(pl.multiple_of(j * LANES, LANES), LANES)
            for t in range(3):
                rows = pl.ds(8 * t, 8)
                g = sums_gu[l][rows, lanes].astype(F32) * factor
                step = moments(moments_gu, 8 * t * gate_stride + 2 * j + l, gate_stride, g)
                gather.bufs[0][l, x, y, z, rows, lanes] = weight(old_gu[l, rows, lanes], step)
            return 0

        lax.fori_loop(0, gate_tiles, gate_up, 0)

        def down(i, _, l=l):
            rows = pl.ds(pl.multiple_of(8 * i, 8), 8)
            for j in range(down_tiles):
                lanes = pl.ds(j * LANES, LANES)
                start = (PREV + 8 * i) * down_stride + 2 * j + l
                g = sums_d[l][rows, lanes].astype(F32) * factor
                step = moments(moments_d, start + 2 * down_tiles * core, down_stride, g)
                gather.bufs[1][l, x, y, z, rows, lanes] = weight(old_d[l, rows, lanes], step)
                g = other_d[l, rows, lanes].astype(F32) * factor
                moments(moments_d, start + 2 * down_tiles * (1 - core), down_stride, g)
            return 0

        lax.fori_loop(0, 9, down, 0)
        gather.own(l)

    late = []
    for i, out in enumerate((m_out, v_out)):
        for c in range(2):

            @pl.when(core == c)
            def _(i=i, out=out, c=c):
                pltpu.make_async_copy(gate_rows(i, core), out[c], late_local.at[i]).start()
                put(gate_rows(i, 1 - core), out[c], late_send.at[i], late_recv.at[i], partner).start()

        pltpu.make_async_copy(down_rows(i, own_rows, DOWN_ROWS), out[2], late_local.at[2 + i]).start()
    for phase in range(3):
        gather.phase(phase)
    for i, out in enumerate((m_out, v_out)):
        pltpu.make_async_copy(gate_rows(i, core), out[0], late_local.at[i]).wait()
        pltpu.make_async_copy(down_rows(i, own_rows, DOWN_ROWS), out[2], late_local.at[2 + i]).wait()
        copy = put(gate_rows(i, 1 - core), out[0], late_send.at[i], late_recv.at[i], partner)
        copy.wait_recv()
        copy.wait_send()
    for copy in sends:
        copy.wait_send()
    for i in range(2):
        for c in range(2):

            @pl.when(core == 1)
            def _(i=i, c=c):
                rows = down_rows(i, 0, PREV)
                put(rows, rows, early_send.at[4 + 2 * i + c], early_recv.at[4 + i], following[c]).wait_send()

    gather.drain()


def finish_call(count, collective_id, sums_gu, sums_d, m, v, w):
    gate_cols, down_half = sums_gu[0].shape[1], sums_d[0].shape[1]
    operands = [*sums_gu, *sums_d, *m, *v, *w]
    hbm, vmem = pl.BlockSpec(memory_space=pltpu.HBM), pl.BlockSpec(memory_space=pltpu.VMEM)
    dma = pltpu.SemaphoreType.DMA
    gate_stride, down_stride = gate_cols // 64, down_half // 32
    scratch = [
        pltpu.VMEM((2, 24 * gate_stride, LANES), F32),
        pltpu.VMEM((2, (PREV + 72) * down_stride, LANES), F32),
        pltpu.VMEM((2, 24, gate_cols), BF16),
        pltpu.VMEM((2, 72, down_half), BF16),
        pltpu.VMEM((2, 72, down_half), BF16),
        pltpu.VMEM((4, SIDE, 8, LANES), F32),
        dma((6,)), dma((10,)), dma((8,)), dma((12,)), dma((12,)), dma((4,)), dma((2,)), dma((2,)),
    ]
    return pl.pallas_call(
        functools.partial(finish_kernel, count),
        name="finish",
        out_shape=[jax.ShapeDtypeStruct(t.shape, t.dtype) for t in (*w, *m, *v)],
        in_specs=[vmem] * 4 + [hbm] * 9,
        out_specs=[hbm] * 9,
        scratch_shapes=scratch + Gather.scratch(gate_cols, down_half),
        compiler_params=pltpu.CompilerParams(collective_id=collective_id, has_side_effects=True, vmem_limit_bytes=VMEM_LIMIT),
        cost_estimate=pl.CostEstimate(flops=10**9, bytes_accessed=10**8, transcendentals=0),
    )(*operands)


TILE = 384
ROWS = 256
TIGHT = pl.Buffered(buffer_count=1)


def dot(a, b, dims):
    return lax.dot_general(a, b, (dims, ((), ())), preferred_element_type=F32)


NN, NT, TN = ((1,), (0,)), ((1,), (1,)), ((0,), (0,))


def norm_scale(wide):
    return lax.rsqrt(jnp.mean(wide * wide, -1, keepdims=True) + 1e-6)


def in_rows(total, step, body):
    def one(i, _):
        body(pl.ds(pl.multiple_of(i * step, step), step))
        return 0

    lax.fori_loop(0, total // step, one, 0)


def clear(acc):
    def rows(r):
        acc[r, :] = jnp.zeros((8, acc.shape[1]), F32)

    in_rows(acc.shape[0], 8, rows)


def spec(shape, index_map, tight=False):
    return pl.BlockSpec(shape, index_map, pipeline_mode=TIGHT) if tight else pl.BlockSpec(shape, index_map)


def whole(shape, tight=True):
    return spec(shape, lambda j: (0,) * len(shape), tight)


HBM = pl.BlockSpec(memory_space=pltpu.HBM)


def params(collective_id=None, semantics=("arbitrary",)):
    more = {} if collective_id is None else {"collective_id": collective_id, "has_side_effects": True}
    return pltpu.CompilerParams(dimension_semantics=semantics, vmem_limit_bytes=VMEM_LIMIT, **more)


def transpose_piece(j, last, src, dst):
    def piece(i):
        at = pl.ds(pl.multiple_of(i * LANES, LANES), LANES)
        dst[at, :] = src[:, at].T

    piece(j)
    pl.when(j == last)(lambda: piece(last + 1))


def forward_kernel(tiles, x, wg, wu, wd, gate, up, h_out, a_out, at, a, acc):
    j = pl.program_id(0)

    @pl.when(j == 0)
    def _():
        def rows(r):
            wide = x[r, :].astype(F32)
            a[r, :] = (wide * norm_scale(wide)).astype(BF16)

        in_rows(x.shape[0], 128, rows)
        clear(acc)

    transpose_piece(j, tiles - 1, a, at)
    for m in range(x.shape[0] // ROWS):
        r = pl.ds(m * ROWS, ROWS)
        g = dot(a[r, :], wg[0], NN)
        u = dot(a[r, :], wu[0], NN)
        gate[r, :] = g
        up[r, :] = u
        p = (g * lax.logistic(g) * u).astype(BF16)
        acc[r, :] += dot(p, wd[0], NN)

    @pl.when(j == tiles - 1)
    def _():
        def rows(r):
            h = (x[r, :].astype(F32) + acc[r, :].astype(BF16).astype(F32)).astype(BF16)
            h_out[r, :] = h
            wide = h.astype(F32)
            a_out[r, :] = (wide * norm_scale(wide)).astype(BF16)

        in_rows(x.shape[0], 128, rows)


def forward_call(x, wg, wu, wd):
    tokens, d = x.shape
    ff = wg.shape[2]
    tiles = ff // TILE
    w_in = spec((1, d, TILE), lambda j: (0, 0, j))
    return pl.pallas_call(
        functools.partial(forward_kernel, tiles),
        name="forward_0",
        grid=(tiles,),
        in_specs=[whole((tokens, d)), w_in, w_in, spec((1, TILE, d), lambda j: (0, j, 0))],
        out_specs=[spec((tokens, TILE), lambda j: (0, j))] * 2 + [whole((tokens, d))] * 2 + [whole((d, tokens))],
        out_shape=[jax.ShapeDtypeStruct((tokens, ff), F32)] * 2
        + [jax.ShapeDtypeStruct((tokens, d), BF16)] * 2
        + [jax.ShapeDtypeStruct((d, tokens), BF16)],
        scratch_shapes=[pltpu.VMEM((tokens, d), BF16), pltpu.VMEM((tokens, d), F32)],
        compiler_params=params(),
    )(x, wg, wu, wd)


class PairSum:
    def __init__(self, place, tiles, landing, stage, send, recv):
        self.place, self.tiles, self.landing, self.stage, self.send, self.recv = place, tiles, landing, stage, send, recv

    @staticmethod
    def scratch(tiles, rows, cols):
        dma = pltpu.SemaphoreType.DMA
        return [pltpu.VMEM((tiles, rows, cols), BF16), pltpu.VMEM((2, rows, cols), BF16), dma((2,)), dma((tiles,))]

    def copy(self, i):
        slot = lax.rem(i, 2)
        return put(self.stage.at[slot], self.landing.at[i], self.send.at[slot], self.recv.at[i], self.place.partner())

    def reserve(self, i):
        pl.when(i >= 2)(lambda: self.copy(i - 2).wait_send())
        return self.stage.at[lax.rem(i, 2)]

    def drain(self):
        for i in (self.tiles - 2, self.tiles - 1):
            self.copy(i).wait_send()


def hidden_back(gate, up, dp):
    dp = dp.astype(BF16).astype(F32)
    s = lax.logistic(gate)
    act = gate * s
    return (act * up).astype(BF16), (dp * up * (s + act * (1.0 - s))).astype(BF16), (dp * act).astype(BF16)


def down_gradient(j, tiles, pair, p, dy, half, out):
    core = pair.place.core

    def columns(c):
        return pl.ds(pl.multiple_of(c * half, LANES), half)

    @pl.when(j < tiles)
    def _():
        slot = pair.reserve(j)
        slot[...] = dot(p[lax.rem(j, 2)], dy[:, columns(1 - core)], TN).astype(BF16)
        pair.copy(j).start()

    @pl.when(j >= 1)
    def _():
        pair.copy(j - 1).wait_recv()
        own = dot(p[lax.rem(j - 1, 2)], dy[:, columns(core)], TN)
        out[...] = (own + pair.landing[j - 1].astype(F32)).astype(BF16)

    pl.when(j == tiles)(pair.drain)


def layer_kernel(tiles, a, dy, wg, wu, wd, dgu, at, out, p, *rest):
    j = pl.program_id(0)
    place = Place()
    pair = PairSum(place, tiles, *rest)
    pl.when(j == 0)(lambda: signal_all([place.partner()]))

    @pl.when(j < tiles)
    def _():
        transpose_piece(j, tiles - 1, a, at)
        slot = lax.rem(j, 2)
        for m in range(a.shape[0] // ROWS):
            r = pl.ds(m * ROWS, ROWS)
            g = dot(a[r, :], wg[0], NN)
            u = dot(a[r, :], wu[0], NN)
            dp = dot(dy[r, :], wd[0], NT)
            p[slot, r, :], dgu[0, r, :], dgu[1, r, :] = hidden_back(g, u, dp)

    down_gradient(j, tiles, pair, p, dy, dy.shape[1] // 2, out)


def clip(tiles, back=0):
    return lambda j: jnp.clip(j - back, 0, tiles - 1)


def layer_call(collective_id, a, dy, wg, wu, wd):
    tokens, d = a.shape
    ff = wg.shape[2]
    tiles, half = ff // TILE, d // 2
    now, before = clip(tiles), clip(tiles, 1)
    w_in = spec((1, d, TILE), lambda j: (1, 0, now(j)))
    return pl.pallas_call(
        functools.partial(layer_kernel, tiles),
        name="layer_1",
        grid=(tiles + 1,),
        in_specs=[whole((tokens, d))] * 2 + [w_in, w_in, spec((1, TILE, d), lambda j: (1, now(j), 0))],
        out_specs=[spec((2, tokens, TILE), lambda j: (0, 0, now(j))), whole((d, tokens)), spec((TILE, half), lambda j: (before(j), 0))],
        out_shape=[
            jax.ShapeDtypeStruct((2, tokens, ff), BF16),
            jax.ShapeDtypeStruct((d, tokens), BF16),
            jax.ShapeDtypeStruct((ff, half), BF16),
        ],
        scratch_shapes=[pltpu.VMEM((2, tokens, TILE), BF16), *PairSum.scratch(tiles, TILE, half)],
        compiler_params=params(collective_id),
    )(a, dy, wg, wu, wd)


GATE_ROWS, DOWN_WINDOW = 24, 72


def gate_up_kernel(tiles, cols, at, ahead, behind, sum_down, out, half0, half1, *rest):
    j = pl.program_id(0)
    place = Place()
    core = place.core
    pair = PairSum(place, tiles, *rest[:4])
    first = First.of(place, DOWN_WINDOW, cols, rest[4:9])
    load_sem, save_sem = rest[9:11]
    loads = loads_down(sum_down, first, load_sem)

    @pl.when(j == 0)
    def _():
        signal_all(near(place))
        begin(loads)

    @pl.when(j < tiles)
    def _():
        slot = pair.reserve(j)
        other = ahead[1 - core]
        for m in range(at.shape[0] // ROWS):
            r = pl.ds(m * ROWS, ROWS)
            slot[r, :] = dot(at[r, :], other, NN).astype(BF16)
        pair.copy(j).start()

    @pl.when(j >= 1)
    def _():
        pair.copy(j - 1).wait_recv()
        own = behind[core]
        for m in range(at.shape[0] // ROWS):
            r = pl.ds(m * ROWS, ROWS)
            out[r, :] = (dot(at[r, :], own, NN) + pair.landing[j - 1, r, :].astype(F32)).astype(BF16)

    pl.when(j == 0)(lambda: end(loads))
    spread(j, tiles + 1, 16, first.tick)

    @pl.when(j == tiles)
    def _():
        saves = copies(first.results(), (half0, half1), save_sem)
        begin(saves)
        pair.drain()
        first.drain()
        end(saves)


def gate_up_call(name, collective_id, at, dgu, sum_down):
    d, tokens = at.shape
    ff = dgu.shape[2]
    tiles, cols, dma = ff // TILE, sum_down.shape[-1], pltpu.SemaphoreType.DMA
    now, before = clip(tiles), clip(tiles, 1)
    return pl.pallas_call(
        functools.partial(gate_up_kernel, tiles, cols),
        name=name,
        grid=(tiles + 1,),
        in_specs=[
            whole((d, tokens)),
            spec((2, tokens, TILE), lambda j: (0, 0, now(j))),
            spec((2, tokens, TILE), lambda j: (0, 0, before(j))),
            HBM,
        ],
        out_specs=[spec((d, TILE), lambda j: (0, before(j))), HBM, HBM],
        out_shape=[jax.ShapeDtypeStruct((d, ff), BF16)] + [jax.ShapeDtypeStruct(s, BF16) for s in half_sums(DOWN_WINDOW, cols)],
        scratch_shapes=[*PairSum.scratch(tiles, d, TILE), *First.scratch(DOWN_WINDOW, cols), dma((SIDE,)), dma((2,))],
        compiler_params=params(collective_id),
    )(at, dgu, dgu, sum_down)


def middle_kernel(tiles, gate_cols, down_cols, dgu, wg, wu, h, dy, sum_gu, down0, down1, dh, half0, half1, out_down, acc_g, acc_u, *rest):
    j = pl.program_id(0)
    place = Place()
    first = First.of(place, GATE_ROWS, gate_cols, rest[:5])
    before = rest[5:7]
    down = Rest.of(place, DOWN_WINDOW, down_cols, before, rest[7:15])
    load_sem, save_sem = rest[15:17]
    loads = copies((sum_gu, down0, down1), (first.held, *before), load_sem)

    @pl.when(j == 0)
    def _():
        signal_all(near(place))
        begin(loads)
        clear(acc_g)
        clear(acc_u)

    for m in range(h.shape[0] // ROWS):
        r = pl.ds(m * ROWS, ROWS)
        acc_g[r, :] += dot(dgu[0, r, :], wg[0], NT)
        acc_u[r, :] += dot(dgu[1, r, :], wu[0], NT)

    pl.when(j == 0)(lambda: end(loads))
    down.tick(j)
    pl.when(j == 7)(lambda: down.result(out_down))
    spread(j, tiles, 16, first.tick)

    @pl.when(j == tiles - 1)
    def _():
        saves = copies(first.results(), (half0, half1), save_sem)
        begin(saves)

        def rows(r):
            wide = h[r, :].astype(F32)
            scale = norm_scale(wide)
            da = (acc_g[r, :].astype(BF16).astype(F32) + acc_u[r, :].astype(BF16).astype(F32)).astype(BF16).astype(F32)
            back = scale * da - wide * (scale * scale * scale * jnp.mean(da * wide, -1, keepdims=True))
            dh[r, :] = (dy[r, :].astype(F32) + back.astype(BF16).astype(F32)).astype(BF16)

        in_rows(h.shape[0], 64, rows)
        first.drain()
        down.drain()
        end(saves)


def middle_call(collective_id, dgu, wg, wu, h, dy, sum_gu, down_halves):
    tokens, d = h.shape
    ff = dgu.shape[2]
    tiles, dma, down_cols = ff // TILE, pltpu.SemaphoreType.DMA, d // 2
    w_in = spec((1, d, TILE), lambda j: (1, 0, j))
    return pl.pallas_call(
        functools.partial(middle_kernel, tiles, ff, down_cols),
        name="middle",
        grid=(tiles,),
        in_specs=[spec((2, tokens, TILE), lambda j: (0, 0, j)), w_in, w_in, whole((tokens, d)), whole((tokens, d)), HBM, HBM, HBM],
        out_specs=[whole((tokens, d)), HBM, HBM, whole((DOWN_WINDOW, down_cols))],
        out_shape=[jax.ShapeDtypeStruct((tokens, d), BF16)]
        + [jax.ShapeDtypeStruct(s, BF16) for s in half_sums(GATE_ROWS, ff)]
        + [jax.ShapeDtypeStruct((DOWN_WINDOW, down_cols), BF16)],
        scratch_shapes=[pltpu.VMEM((tokens, d), F32)] * 2
        + First.scratch(GATE_ROWS, ff)
        + [pltpu.VMEM(s, BF16) for s in half_sums(DOWN_WINDOW, down_cols)]
        + Rest.scratch(DOWN_WINDOW, down_cols)
        + [dma((3,)), dma((2,))],
        compiler_params=params(collective_id),
    )(dgu, wg, wu, h, dy, sum_gu.reshape(SIDE, SIDE, SIDE, GATE_ROWS, ff), *down_halves)


def back_kernel(tiles, gate_cols, dh, gate, up, wd, gate0, gate1, dgu, out, out_gu, p, *rest):
    j = pl.program_id(0)
    place = Place()
    pair = PairSum(place, tiles, *rest[:4])
    before = rest[4:6]
    sums = Rest.of(place, GATE_ROWS, gate_cols, before, rest[6:14])
    loads = copies((gate0, gate1), before, rest[14])

    @pl.when(j == 0)
    def _():
        signal_all(near(place))
        begin(loads)

    @pl.when(j < tiles)
    def _():
        slot = lax.rem(j, 2)
        for m in range(dh.shape[0] // ROWS):
            r = pl.ds(m * ROWS, ROWS)
            dp = dot(dh[r, :], wd[0], NT)
            p[slot, r, :], dgu[0, r, :], dgu[1, r, :] = hidden_back(gate[r, :], up[r, :], dp)

    down_gradient(j, tiles, pair, p, dh, dh.shape[1] // 2, out)
    pl.when(j == 0)(lambda: end(loads))
    sums.tick(j)
    pl.when(j == 7)(lambda: sums.result(out_gu))
    pl.when(j == tiles)(sums.drain)


def back_call(collective_id, dh, gate, up, wd, gate_halves):
    tokens, d = dh.shape
    ff = gate.shape[1]
    tiles, half, dma = ff // TILE, d // 2, pltpu.SemaphoreType.DMA
    now, before = clip(tiles), clip(tiles, 1)
    tile = spec((tokens, TILE), lambda j: (0, now(j)))
    return pl.pallas_call(
        functools.partial(back_kernel, tiles, ff),
        name="back_0",
        grid=(tiles + 1,),
        in_specs=[whole((tokens, d)), tile, tile, spec((1, TILE, d), lambda j: (0, now(j), 0)), HBM, HBM],
        out_specs=[spec((2, tokens, TILE), lambda j: (0, 0, now(j))), spec((TILE, half), lambda j: (before(j), 0)), whole((GATE_ROWS, ff))],
        out_shape=[
            jax.ShapeDtypeStruct((2, tokens, ff), BF16),
            jax.ShapeDtypeStruct((ff, half), BF16),
            jax.ShapeDtypeStruct((GATE_ROWS, ff), BF16),
        ],
        scratch_shapes=[pltpu.VMEM((2, tokens, TILE), BF16), *PairSum.scratch(tiles, TILE, half)]
        + [pltpu.VMEM(s, BF16) for s in half_sums(GATE_ROWS, ff)]
        + Rest.scratch(GATE_ROWS, ff)
        + [dma((2,))],
        compiler_params=params(collective_id),
    )(dh, gate, up, wd, *gate_halves)


def last_kernel(gate_cols, down_cols, sum_gu, down0, down1, out_gu, out_down, *rest):
    place = Place()
    first = First.of(place, GATE_ROWS, gate_cols, rest[:5])
    gu = Rest.of(place, GATE_ROWS, gate_cols, first.results(), rest[5:13])
    before = rest[13:15]
    down = Rest.of(place, DOWN_WINDOW, down_cols, before, rest[15:23])
    load_sem = rest[23]
    gate_loads = [pltpu.make_async_copy(sum_gu.at[x], first.held.at[x], load_sem.at[x]) for x in range(SIDE)]
    down_loads = [pltpu.make_async_copy(s, t, load_sem.at[SIDE + i]) for i, (s, t) in enumerate(zip((down0, down1), before, strict=True))]
    begin(gate_loads + down_loads)
    signal_all(near(place))
    end(gate_loads)
    for k in range(SIDE):
        first.start(k)
    end(down_loads)
    down.start(1)

    def phase0(n, _):
        lax.fori_loop(0, SIDE, lambda k, _: (first.step(n, k), 0)[1], 0)
        down.step1(n)
        return 0

    lax.fori_loop(1, 4, phase0, 0)
    gu.start(1)
    down.start(2)

    def phase1(n, _):
        gu.step1(n)
        down.step2(n)
        return 0

    lax.fori_loop(1, 4, phase1, 0)
    gu.start(2)
    down.result(out_down)
    lax.fori_loop(1, 4, lambda n, _: (gu.step2(n), 0)[1], 0)
    gu.result(out_gu)
    first.drain()
    gu.drain()
    down.drain()


def last_call(collective_id, sum_gu, down_halves, down_cols):
    ff = sum_gu.shape[1]
    vmem = pl.BlockSpec(memory_space=pltpu.VMEM)
    return pl.pallas_call(
        functools.partial(last_kernel, ff, down_cols),
        name="last_sums",
        in_specs=[HBM] * 3,
        out_specs=[vmem] * 2,
        out_shape=[jax.ShapeDtypeStruct((GATE_ROWS, ff), BF16), jax.ShapeDtypeStruct((DOWN_WINDOW, down_cols), BF16)],
        scratch_shapes=[
            *First.scratch(GATE_ROWS, ff),
            *Rest.scratch(GATE_ROWS, ff),
            *[pltpu.VMEM(s, BF16) for s in half_sums(DOWN_WINDOW, down_cols)],
            *Rest.scratch(DOWN_WINDOW, down_cols),
            pltpu.SemaphoreType.DMA((SIDE + 2,)),
        ],
        compiler_params=pltpu.CompilerParams(collective_id=collective_id, has_side_effects=True, vmem_limit_bytes=VMEM_LIMIT),
    )(sum_gu.reshape(SIDE, SIDE, SIDE, GATE_ROWS, ff), *down_halves)


def flat(m):
    layers, rows, cols = m.shape
    split = m.transpose(1, 0, 2).reshape(rows, layers, cols // LANES, LANES)
    return with_layout_constraint(split, Layout((0, 2, 1, 3))).transpose(0, 2, 1, 3).reshape(-1, LANES)


def unflat(f, shape):
    layers, rows, cols = shape
    split = f.reshape(rows, cols // LANES, layers, LANES).transpose(0, 2, 1, 3)
    return with_layout_constraint(split, Layout((0, 2, 1, 3))).reshape(rows, layers, cols).transpose(1, 0, 2)


def solution(mesh):
    def body(x, dy, wg, wu, wd, mg, mu, md, vg, vu, vd):
        layers, d, ff = wg.shape
        x, dy = x[0], dy[0]
        windows = (SIDE, SIDE, 4 * 66, d // 2)
        gate0, up0, h1, a1, a0t = forward_call(x, wg, wu, wd)
        dgu1, a1t, down1 = layer_call(1, a1, dy, wg, wu, wd)
        gu1, *down1_halves = gate_up_call("gate_up_1", 2, a1t, dgu1, down1.reshape(windows))
        dh1, *rest = middle_call(3, dgu1, wg, wu, h1, dy, gu1, down1_halves)
        gu1_halves, sum_down1 = rest[:2], rest[2]
        dgu0, down0, sum_gu1 = back_call(4, dh1, gate0, up0, wd, gu1_halves)
        gu0, *down0_halves = gate_up_call("gate_up_0", 5, a0t, dgu0, down0.reshape(windows))
        sum_gu0, sum_down0 = last_call(6, gu0, down0_halves, d // 2)

        views = [(2, SIDE, SIDE, SIDE, GATE_ROWS, ff)] * 2 + [(2, SIDE, SIDE, 4 * 66, d)]
        w = [t.reshape(view) for t, view in zip((wg, wu, wd), views, strict=True)]
        m, v = [flat(t) for t in (mg, mu, md)], [flat(t) for t in (vg, vu, vd)]
        out = finish_call(3 * layers * d * ff, 7, [sum_gu0, sum_gu1], [sum_down0, sum_down1], m, v, w)
        new = [t.reshape(like.shape) for t, like in zip(out[:3], (wg, wu, wd), strict=True)]
        return (*new, *[unflat(t, like.shape) for t, like in zip(out[3:], (mg, mu, md, vg, vu, vd), strict=True)])

    shard = P(None, "dp", None)
    return jax.shard_map(
        body,
        mesh=mesh,
        in_specs=(P(("rep", "dp")), P(("rep", "dp")), P(), P(), P(), *[shard] * 6),
        out_specs=(P("rep"), P("rep"), P("rep"), *[P("rep", "dp", None)] * 6),
        check_vma=False,
    )
```

```python
import functools

import jax
import jax.numpy as jnp
from jax import lax
from jax.experimental import pallas as pl
from jax.experimental.layout import Layout, with_layout_constraint
from jax.experimental.pallas import tpu as pltpu
from jax.sharding import PartitionSpec as P

F32, BF16 = jnp.float32, jnp.bfloat16
CLIP_EPS = 1e-30
LANES = 128
SIDE = 4
ORDERS = ((0, 1, 2), (1, 2, 0), (2, 0, 1))
VMEM_LIMIT = 63 * 1024 * 1024


class Place:
    def __init__(self):
        me = lax.axis_index("dp")
        self.core = lax.rem(me, 2)
        chip = lax.div(me, 2)
        self.at = (lax.div(chip, SIDE * SIDE), lax.rem(lax.div(chip, SIDE), SIDE), lax.rem(chip, SIDE))

    def device(self, axis=None, off=0, core=None):
        at = list(self.at)
        if axis is not None:
            at[axis] = lax.rem(at[axis] + off, SIDE)
        core = self.core if core is None else core
        return {"dp": ((at[0] * SIDE + at[1]) * SIDE + at[2]) * 2 + core}

    def partner(self):
        return self.device(core=1 - self.core)

    def onward(self, way):
        return 1 + 2 * lax.rem(way + self.core, 2)

    def block(self, axis, way, hops):
        return lax.rem(self.at[axis] + hops * (SIDE - self.onward(way)), SIDE)


def signal_all(devices):
    barrier = pltpu.get_barrier_semaphore()
    for d in devices:
        pl.semaphore_signal(barrier, inc=1, device_id=d, device_id_type=pl.DeviceIdType.MESH)
    pl.semaphore_wait(barrier, len(devices))


def near(place):
    return [place.partner()] + [place.device(axis, off) for axis in range(3) for off in (1, SIDE - 1)]


def put(src, dst, send, recv, device):
    return pltpu.make_async_remote_copy(
        src_ref=src, dst_ref=dst, send_sem=send, recv_sem=recv, device_id=device, device_id_type=pl.DeviceIdType.MESH
    )


def ways_of(cols):
    tiles = cols // LANES
    first = (tiles + 1) // 2 * LANES
    return ((0, first), (first, cols - first))


def index(order, values):
    out = [None] * 3
    for axis, value in zip(order, values, strict=True):
        out[axis] = value
    return tuple(out)


ALL = slice(None)


class Rings:
    def __init__(self, place, rows, cols, slots, sems):
        self.place, self.rows, self.slots, self.sems = place, rows // 3, slots, sems
        self.ways = ways_of(cols)

    def part(self, t, way):
        start, width = self.ways[way]
        return pl.ds(t * self.rows, self.rows), pl.ds(start, width)

    @staticmethod
    def pairs():
        return [(t, way) for t in range(3) for way in range(2)]

    def send(self, axis, way, src, landing, key, sems):
        src = landing if src is None else src
        return put(src, landing, sems[0].at[key], sems[1].at[key], self.place.device(axis, self.place.onward(way)))


class First(Rings):
    @staticmethod
    def scratch(rows, cols):
        third, dma = rows // 3, pltpu.SemaphoreType.DMA
        slots = [pltpu.VMEM((3, 3, SIDE, SIDE, third, width), BF16) for _, width in ways_of(cols)]
        return [pltpu.VMEM((SIDE, SIDE, SIDE, rows, cols), BF16), *slots, dma((3, 2, 3, SIDE)), dma((3, 2, 3, SIDE))]

    @classmethod
    def of(cls, place, rows, cols, refs):
        one = cls(place, rows, cols, refs[1:3], refs[3:5])
        one.held = refs[0]
        return one

    def block(self, t, way, hops, k, c=ALL):
        order = ORDERS[t]
        return self.held.at[(*index(order, (self.place.block(order[0], way, hops), k, c)), *self.part(t, way))]

    def message(self, t, way, n, k, arriving=False):
        src = None
        if not arriving:
            src = self.block(t, way, 1, k) if isinstance(n, int) and n == 0 else self.slots[way].at[t, n - 1, k]
        return self.send(ORDERS[t][0], way, src, self.slots[way].at[t, n, k], (t, way, n, k), self.sems)

    def start(self, k):
        for t, way in self.pairs():
            self.message(t, way, 0, k).start()

    def step(self, n, k):
        for t, way in self.pairs():
            self.message(t, way, n - 1, k, arriving=True).wait_recv()
            slots = self.slots[way]
            for c in range(SIDE):
                own = self.block(t, way, n + 1, k, c)
                slots[t, n - 1, k, c] = (slots[t, n - 1, k, c].astype(F32) + own[...].astype(F32)).astype(BF16)
            pl.when(n < 3)(lambda t=t, way=way: self.message(t, way, n, k).start())

    def tick(self, i):
        pl.when(i < SIDE)(lambda: self.start(i))
        pl.when(i >= SIDE)(lambda: self.step(lax.div(i, SIDE), lax.rem(i, SIDE)))

    def results(self):
        return [slots.at[:, 2] for slots in self.slots]

    def drain(self):
        def sent(k, _):
            for t, way in self.pairs():
                self.message(t, way, 0, k).wait_send()
                lax.fori_loop(1, 3, lambda n, _: (self.message(t, way, n, k).wait_send(), 0)[1], 0)
            return 0

        lax.fori_loop(0, SIDE, sent, 0)


class Rest(Rings):
    @staticmethod
    def scratch(rows, cols):
        third, dma = rows // 3, pltpu.SemaphoreType.DMA
        shapes = [pltpu.VMEM((*lead, third, width), BF16) for lead in ((3, 3, SIDE), (3, 3)) for _, width in ways_of(cols)]
        return shapes + [dma((3, 2, 3))] * 4

    @classmethod
    def of(cls, place, rows, cols, before, refs):
        one = cls(place, rows, cols, refs[:4], refs[4:8])
        one.before = before
        return one

    def message(self, phase, t, way, n, arriving=False):
        slots = self.slots[2 * phase - 2 + way]
        axis = ORDERS[t][phase]
        if arriving:
            src = None
        elif isinstance(n, int) and n == 0:
            v = self.place.block(axis, way, 1)
            src = self.before[way].at[t, v] if phase == 1 else self.slots[way].at[t, 2, v]
        else:
            src = slots.at[t, n - 1]
        return self.send(axis, way, src, slots.at[t, n], (t, way, n), self.sems[2 * phase - 2 : 2 * phase])

    def start(self, phase):
        for t, way in self.pairs():
            self.message(phase, t, way, 0).start()

    def step1(self, n):
        for t, way in self.pairs():
            self.message(1, t, way, n - 1, arriving=True).wait_recv()
            v = self.place.block(ORDERS[t][1], way, n + 1)
            before, slots = self.before[way], self.slots[way]
            for c in range(SIDE):
                slots[t, n - 1, c] = (slots[t, n - 1, c].astype(F32) + before[t, v, c].astype(F32)).astype(BF16)
            pl.when(n < 3)(lambda t=t, way=way: self.message(1, t, way, n).start())

    def step2(self, n):
        for t, way in self.pairs():
            self.message(2, t, way, n - 1, arriving=True).wait_recv()
            v = self.place.block(ORDERS[t][2], way, n + 1)
            before, slots = self.slots[way], self.slots[2 + way]
            slots[t, n - 1] = (slots[t, n - 1].astype(F32) + before[t, 2, v].astype(F32)).astype(BF16)
            pl.when(n < 3)(lambda t=t, way=way: self.message(2, t, way, n).start())

    def tick(self, i):
        pl.when(i == 0)(lambda: self.start(1))
        pl.when((i >= 1) & (i <= 3))(lambda: self.step1(i))
        pl.when(i == 3)(lambda: self.start(2))
        pl.when((i >= 4) & (i <= 6))(lambda: self.step2(i - 3))

    def result(self, out):
        for t, way in self.pairs():
            out[self.part(t, way)] = self.slots[2 + way][t, 2]

    def drain(self):
        for t, way in self.pairs():
            for phase in (1, 2):
                for n in range(3):
                    self.message(phase, t, way, n).wait_send()


def loads_down(source, first, sems):
    return [pltpu.make_async_copy(source.at[:, :, pl.ds(64 * z, 72)], first.held.at[:, :, z], sems.at[z]) for z in range(SIDE)]


def spread(j, steps, count, tick):
    low, high = lax.div(count * j, steps), lax.div(count * (j + 1), steps)
    lax.fori_loop(low, high, lambda i, _: (tick(i), 0)[1], 0)


def copies(sources, targets, sems):
    return [pltpu.make_async_copy(s, t, sems.at[i]) for i, (s, t) in enumerate(zip(sources, targets, strict=True))]


def begin(all_copies):
    for copy in all_copies:
        copy.start()


def end(all_copies):
    for copy in all_copies:
        copy.wait()


def half_sums(rows, cols):
    return [(3, SIDE, SIDE, rows // 3, width) for _, width in ways_of(cols)]


PREV = 6
DOWN_ROWS = 33


class Gather:
    def __init__(self, place, bufs, sems, outs, copy_sems):
        self.place, self.bufs, self.sems, self.outs, self.copy_sems = place, bufs, sems, outs, copy_sems

    @staticmethod
    def scratch(gate_cols, down_cols):
        bufs = [pltpu.VMEM((2, SIDE, SIDE, SIDE, 24, gate_cols), BF16), pltpu.VMEM((2, SIDE, SIDE, SIDE, 72, down_cols), BF16)]
        return bufs + [pltpu.SemaphoreType.DMA((2, 3, 2, 3, 3))] * 4 + [pltpu.SemaphoreType.DMA((2,))] * 3

    def part(self, kind, t, way):
        rows, cols = self.bufs[kind].shape[-2:]
        start, width = ways_of(cols)[way]
        return pl.ds(t * (rows // 3), rows // 3), pl.ds(start, width)

    def message(self, kind, l, t, way, phase, n, hops):
        order, place = ORDERS[t], self.place
        v = place.block(order[phase], way, hops)
        values = [ALL] * phase + [v] + [place.at[axis] for axis in order[phase + 1 :]]
        ref = self.bufs[kind].at[(l, *index(order, values), *self.part(kind, t, way))]
        key = (l, t, way, phase, n)
        axis = order[phase]
        return put(ref, ref, self.sems[2 * kind].at[key], self.sems[2 * kind + 1].at[key], place.device(axis, place.onward(way)))

    def copies(self, kind, l, t, way, v):
        order = ORDERS[t]
        rows, cols = self.part(kind, t, way)
        if kind == 0:
            at = (l, *index(order, (ALL, ALL, v)), rows, cols)
            return [(lambda out, at=at: (self.bufs[0].at[at], out.at[at]))]
        half = self.bufs[1].shape[-1]
        start, width = ways_of(half)[way]
        columns = pl.ds(pl.multiple_of(self.place.core * half + start, LANES), width)

        def pair(out, z, count):
            x, y, _ = index(order, (ALL, ALL, v))
            src = self.bufs[1].at[l, x, y, z, pl.ds(24 * t, count), cols]
            return src, out.at[l, x, y, pl.ds(64 * z + 24 * t, count), columns]

        if order[2] == 2:
            return [lambda out: pair(out, v, 24)]
        return [lambda out, z=z: pair(out, z, 16 if t == 2 and z < SIDE - 1 else 24) for z in range(SIDE)]

    def copy_out(self, kind, l, t, way, v):
        local, send, recv = self.copy_sems

        def both(out):
            for pair in self.copies(kind, l, t, way, v):
                src, dst = pair(out)
                pltpu.make_async_copy(src, dst, local.at[kind]).start()
                put(src, dst, send.at[kind], recv.at[kind], self.place.partner()).start()

        if kind:
            both(self.outs[2])
        else:
            for core in range(2):
                pl.when(self.place.core == core)(lambda core=core: both(self.outs[core]))

    def parts(self):
        return [(kind, t, way) for kind in range(2) for t in range(3) for way in range(2)]

    def own(self, l):
        for kind, t, way in self.parts():
            self.message(kind, l, t, way, 0, 0, 0).start()

    def phase(self, phase):
        def step(i, _):
            n, l = 1 + lax.div(i, 2), lax.rem(i, 2)
            for kind, t, way in self.parts():
                self.message(kind, l, t, way, phase, n - 1, n).wait_recv()
                pl.when(n < 3)(lambda kind=kind, t=t, way=way: self.message(kind, l, t, way, phase, n, n).start())
                if phase < 2:

                    @pl.when(n == 3)
                    def _(kind=kind, t=t, way=way):
                        self.message(kind, l, t, way, phase + 1, 0, 0).start()
                        if phase == 1:
                            self.copy_out(kind, l, t, way, self.place.at[ORDERS[t][2]])

                else:
                    self.copy_out(kind, l, t, way, self.place.block(ORDERS[t][2], way, n))
            return 0

        lax.fori_loop(0, 6, step, 0)

    def drain(self):
        local, send, recv = self.copy_sems
        half = self.bufs[1].shape[-1]
        columns = self.outs[2].at[:, :, :, :, pl.ds(0, half)]
        for kind, whole in ((0, self.outs[0]), (1, columns)):
            pltpu.make_async_copy(whole, whole, local.at[kind]).wait()
            copy = put(whole, whole, send.at[kind], recv.at[kind], self.place.partner())
            copy.wait_send()
            copy.wait_recv()

        def sent(i, _):
            l, n = lax.div(i, 3), lax.rem(i, 3)
            for phase in range(3):
                for kind, t, way in self.parts():
                    self.message(kind, l, t, way, phase, n, n).wait_send()
            return 0

        lax.fori_loop(0, 6, sent, 0)


def finish_kernel(count, *refs):
    sums_gu, sums_d, m_in, v_in, w_in = refs[0:2], refs[2:4], refs[4:7], refs[7:10], refs[10:13]
    w_out, m_out, v_out = refs[13:16], refs[16:19], refs[19:22]
    moments_gu, moments_d, old_gu, old_d, other_d, tiles = refs[22:28]
    load_sem, early_send, early_recv, norm_send, norm_recv, late_local, late_send, late_recv = refs[28:36]
    gather_refs = refs[36:]
    place = Place()
    x, y, z = place.at
    core = place.core
    gather = Gather(place, gather_refs[:2], gather_refs[2:6], w_out, gather_refs[6:9])
    partner = place.partner()
    gate_tiles, down_tiles = sums_gu[0].shape[1] // LANES, sums_d[0].shape[1] // LANES
    gate_stride, down_stride = 2 * gate_tiles, 4 * down_tiles
    gate_size, down_size = 12 * gate_stride, DOWN_ROWS * down_stride

    def blank(i, _):
        for which in range(2):
            moments_d[which, pl.ds(pl.multiple_of(8 * i, 8), 8), :] = jnp.zeros((8, LANES), F32)
        return 0

    lax.fori_loop(0, moments_d.shape[1] // 8, blank, 0)
    following = [place.device(2, 1, core=c) for c in range(2)]
    others = [place.device(axis, 2) for axis in range(3)] + [place.device(2, off, core=1 - core) for off in (1, SIDE - 1)]
    signal_all(near(place) + others)

    def gate_rows(i, which):
        return moments_gu.at[i, pl.ds(pl.multiple_of(which * gate_size, 8), gate_size)]

    def down_rows(i, first, rows):
        return moments_d.at[i, pl.ds(pl.multiple_of(first * down_stride, 8), rows * down_stride)]

    def columns(ref):
        half = down_tiles * LANES
        return ref.at[:, x, y, pl.ds(pl.multiple_of(64 * z, 8), 72), pl.ds(pl.multiple_of(core * half, LANES), half)]

    own_rows = PREV + 2 * z + DOWN_ROWS * core
    loads, sends = [], []
    for i, moment in enumerate((m_in, v_in)):
        for c in range(2):

            @pl.when(core == c)
            def _(i=i, moment=moment, c=c):
                pltpu.make_async_copy(moment[c], gate_rows(i, core), load_sem.at[i]).start()
                put(moment[1 - c], gate_rows(i, core), early_send.at[i], early_recv.at[i], partner).start()

        loads.append(pltpu.make_async_copy(moment[0], gate_rows(i, core), load_sem.at[i]))
        sends.append(put(moment[0], gate_rows(i, core), early_send.at[i], early_recv.at[i], partner))
        loads.append(pltpu.make_async_copy(moment[2], down_rows(i, own_rows, DOWN_ROWS), load_sem.at[2 + i]))
        loads[-1].start()
        sends.append(put(moment[2], down_rows(i, own_rows, DOWN_ROWS), early_send.at[2 + i], early_recv.at[2 + i], partner))
        sends[-1].start()
        last = moment[2].at[pl.ds((DOWN_ROWS - PREV) * down_stride, PREV * down_stride)]
        landing = down_rows(i, 2 * lax.rem(z + 1, SIDE), PREV)

        @pl.when(core == 1)
        def _(i=i, last=last, landing=landing):
            for c in range(2):
                put(last, landing, early_send.at[4 + 2 * i + c], early_recv.at[4 + i], following[c]).start()

    for l in range(2):
        sends.append(put(sums_d[l], other_d.at[l], early_send.at[8 + l], early_recv.at[6 + l], partner))
        sends[-1].start()
    for c in range(2):

        @pl.when(core == c)
        def _(c=c):
            pltpu.make_async_copy(w_in[c].at[:, x, y, z], old_gu, load_sem.at[4]).start()

    loads.append(pltpu.make_async_copy(w_in[0].at[:, x, y, z], old_gu, load_sem.at[4]))
    loads.append(pltpu.make_async_copy(columns(w_in[2]), old_d, load_sem.at[5]))
    loads[-1].start()

    squares = jnp.zeros((8, LANES), F32)
    for l in range(2):

        def of_gate_up(j, total, l=l):
            for t in range(3):
                g = sums_gu[l][pl.ds(8 * t, 8), pl.ds(pl.multiple_of(j * LANES, LANES), LANES)].astype(F32)
                total += g * g
            return total

        squares = lax.fori_loop(0, gate_tiles, of_gate_up, squares)

        def of_down(i, total, l=l):
            row = 8 * i + lax.broadcasted_iota(jnp.int32, (8, LANES), 0)
            mine = (row >= 2 * z) & (row < 2 * z + 2 * DOWN_ROWS)
            for j in range(down_tiles):
                g = sums_d[l][pl.ds(pl.multiple_of(8 * i, 8), 8), pl.ds(j * LANES, LANES)].astype(F32)
                total += jnp.where(mine, g * g, 0.0)
            return total

        squares = lax.fori_loop(0, 9, of_down, squares)
    for stage, (coordinate, size) in enumerate(((core, 2), (x, SIDE), (y, SIDE), (z, SIDE))):
        tiles[stage, coordinate] = squares
        exchanges = []
        for off in range(1, size):
            target = partner if stage == 0 else place.device(stage - 1, off)
            key = 3 * stage + off - 1
            here = tiles.at[stage, coordinate]
            exchanges.append(put(here, here, norm_send.at[key], norm_recv.at[key], target))
            exchanges[-1].start()
        for exchange in exchanges:
            exchange.wait_recv()
        for exchange in exchanges:
            exchange.wait_send()
        squares = tiles[stage, 0]
        for other in range(1, size):
            squares += tiles[stage, other]
    total = jnp.sum(jnp.sum(squares, 0, keepdims=True), 1, keepdims=True)
    factor = jnp.minimum(1.0, 0.5 * lax.rsqrt(total / count + CLIP_EPS))

    for copy in loads:
        copy.wait()
    for copy in sends:
        copy.wait_recv()
    for i in range(2):
        put(down_rows(i, 0, PREV), down_rows(i, 0, PREV), early_send.at[0], early_recv.at[4 + i], partner).wait_recv()

    def moments(ref, start, stride, g):
        rows = pl.ds(start, 8, stride=stride)
        m = 0.9 * ref[0, rows, :] + 0.1 * g
        v = 0.95 * ref[1, rows, :] + 0.05 * g * g
        ref[0, rows, :] = m
        ref[1, rows, :] = v
        return m * lax.rsqrt(v + 1e-8)

    def weight(w, step):
        w = w.astype(F32)
        return (w - 0.02 * (step + 0.1 * w)).astype(BF16)

    for l in range(2):

        def gate_up(j, _, l=l):
            lanes = pl.ds(pl.multiple_of(j * LANES, LANES), LANES)
            for t in range(3):
                rows = pl.ds(8 * t, 8)
                g = sums_gu[l][rows, lanes].astype(F32) * factor
                step = moments(moments_gu, 8 * t * gate_stride + 2 * j + l, gate_stride, g)
                gather.bufs[0][l, x, y, z, rows, lanes] = weight(old_gu[l, rows, lanes], step)
            return 0

        lax.fori_loop(0, gate_tiles, gate_up, 0)

        def down(i, _, l=l):
            rows = pl.ds(pl.multiple_of(8 * i, 8), 8)
            for j in range(down_tiles):
                lanes = pl.ds(j * LANES, LANES)
                start = (PREV + 8 * i) * down_stride + 2 * j + l
                g = sums_d[l][rows, lanes].astype(F32) * factor
                step = moments(moments_d, start + 2 * down_tiles * core, down_stride, g)
                gather.bufs[1][l, x, y, z, rows, lanes] = weight(old_d[l, rows, lanes], step)
                g = other_d[l, rows, lanes].astype(F32) * factor
                moments(moments_d, start + 2 * down_tiles * (1 - core), down_stride, g)
            return 0

        lax.fori_loop(0, 9, down, 0)
        gather.own(l)

    late = []
    for i, out in enumerate((m_out, v_out)):
        for c in range(2):

            @pl.when(core == c)
            def _(i=i, out=out, c=c):
                pltpu.make_async_copy(gate_rows(i, core), out[c], late_local.at[i]).start()
                put(gate_rows(i, 1 - core), out[c], late_send.at[i], late_recv.at[i], partner).start()

        pltpu.make_async_copy(down_rows(i, own_rows, DOWN_ROWS), out[2], late_local.at[2 + i]).start()
    for phase in range(3):
        gather.phase(phase)
    for i, out in enumerate((m_out, v_out)):
        pltpu.make_async_copy(gate_rows(i, core), out[0], late_local.at[i]).wait()
        pltpu.make_async_copy(down_rows(i, own_rows, DOWN_ROWS), out[2], late_local.at[2 + i]).wait()
        copy = put(gate_rows(i, 1 - core), out[0], late_send.at[i], late_recv.at[i], partner)
        copy.wait_recv()
        copy.wait_send()
    for copy in sends:
        copy.wait_send()
    for i in range(2):
        for c in range(2):

            @pl.when(core == 1)
            def _(i=i, c=c):
                rows = down_rows(i, 0, PREV)
                put(rows, rows, early_send.at[4 + 2 * i + c], early_recv.at[4 + i], following[c]).wait_send()

    gather.drain()


def finish_call(count, collective_id, sums_gu, sums_d, m, v, w):
    gate_cols, down_half = sums_gu[0].shape[1], sums_d[0].shape[1]
    operands = [*sums_gu, *sums_d, *m, *v, *w]
    hbm, vmem = pl.BlockSpec(memory_space=pltpu.HBM), pl.BlockSpec(memory_space=pltpu.VMEM)
    dma = pltpu.SemaphoreType.DMA
    gate_stride, down_stride = gate_cols // 64, down_half // 32
    scratch = [
        pltpu.VMEM((2, 24 * gate_stride, LANES), F32),
        pltpu.VMEM((2, (PREV + 72) * down_stride, LANES), F32),
        pltpu.VMEM((2, 24, gate_cols), BF16),
        pltpu.VMEM((2, 72, down_half), BF16),
        pltpu.VMEM((2, 72, down_half), BF16),
        pltpu.VMEM((4, SIDE, 8, LANES), F32),
        dma((6,)), dma((10,)), dma((8,)), dma((12,)), dma((12,)), dma((4,)), dma((2,)), dma((2,)),
    ]
    return pl.pallas_call(
        functools.partial(finish_kernel, count),
        name="finish",
        out_shape=[jax.ShapeDtypeStruct(t.shape, t.dtype) for t in (*w, *m, *v)],
        in_specs=[vmem] * 4 + [hbm] * 9,
        out_specs=[hbm] * 9,
        scratch_shapes=scratch + Gather.scratch(gate_cols, down_half),
        compiler_params=pltpu.CompilerParams(collective_id=collective_id, has_side_effects=True, vmem_limit_bytes=VMEM_LIMIT),
        cost_estimate=pl.CostEstimate(flops=10**9, bytes_accessed=10**8, transcendentals=0),
    )(*operands)


TILE = 384
ROWS = 256
TIGHT = pl.Buffered(buffer_count=1)


def dot(a, b, dims):
    return lax.dot_general(a, b, (dims, ((), ())), preferred_element_type=F32)


NN, NT, TN = ((1,), (0,)), ((1,), (1,)), ((0,), (0,))


def norm_scale(wide):
    return lax.rsqrt(jnp.mean(wide * wide, -1, keepdims=True) + 1e-6)


def in_rows(total, step, body):
    def one(i, _):
        body(pl.ds(pl.multiple_of(i * step, step), step))
        return 0

    lax.fori_loop(0, total // step, one, 0)


def clear(acc):
    def rows(r):
        acc[r, :] = jnp.zeros((8, acc.shape[1]), F32)

    in_rows(acc.shape[0], 8, rows)


def spec(shape, index_map, tight=False):
    return pl.BlockSpec(shape, index_map, pipeline_mode=TIGHT) if tight else pl.BlockSpec(shape, index_map)


def whole(shape, tight=True):
    return spec(shape, lambda j: (0,) * len(shape), tight)


HBM = pl.BlockSpec(memory_space=pltpu.HBM)


def params(collective_id=None, semantics=("arbitrary",)):
    more = {} if collective_id is None else {"collective_id": collective_id, "has_side_effects": True}
    return pltpu.CompilerParams(dimension_semantics=semantics, vmem_limit_bytes=VMEM_LIMIT, **more)


def transpose_piece(j, last, src, dst):
    def piece(i):
        at = pl.ds(pl.multiple_of(i * LANES, LANES), LANES)
        dst[at, :] = src[:, at].T

    piece(j)
    pl.when(j == last)(lambda: piece(last + 1))


def forward_kernel(tiles, x, wg, wu, wd, gate, up, h_out, a_out, at, a, acc):
    j = pl.program_id(0)

    @pl.when(j == 0)
    def _():
        def rows(r):
            wide = x[r, :].astype(F32)
            a[r, :] = (wide * norm_scale(wide)).astype(BF16)

        in_rows(x.shape[0], 128, rows)
        clear(acc)

    transpose_piece(j, tiles - 1, a, at)
    for m in range(x.shape[0] // ROWS):
        r = pl.ds(m * ROWS, ROWS)
        g = dot(a[r, :], wg[0], NN)
        u = dot(a[r, :], wu[0], NN)
        gate[r, :] = g
        up[r, :] = u
        p = (g * lax.logistic(g) * u).astype(BF16)
        acc[r, :] += dot(p, wd[0], NN)

    @pl.when(j == tiles - 1)
    def _():
        def rows(r):
            h = (x[r, :].astype(F32) + acc[r, :].astype(BF16).astype(F32)).astype(BF16)
            h_out[r, :] = h
            wide = h.astype(F32)
            a_out[r, :] = (wide * norm_scale(wide)).astype(BF16)

        in_rows(x.shape[0], 128, rows)


def forward_call(x, wg, wu, wd):
    tokens, d = x.shape
    ff = wg.shape[2]
    tiles = ff // TILE
    w_in = spec((1, d, TILE), lambda j: (0, 0, j))
    return pl.pallas_call(
        functools.partial(forward_kernel, tiles),
        name="forward_0",
        grid=(tiles,),
        in_specs=[whole((tokens, d)), w_in, w_in, spec((1, TILE, d), lambda j: (0, j, 0))],
        out_specs=[spec((tokens, TILE), lambda j: (0, j))] * 2 + [whole((tokens, d))] * 2 + [whole((d, tokens))],
        out_shape=[jax.ShapeDtypeStruct((tokens, ff), F32)] * 2
        + [jax.ShapeDtypeStruct((tokens, d), BF16)] * 2
        + [jax.ShapeDtypeStruct((d, tokens), BF16)],
        scratch_shapes=[pltpu.VMEM((tokens, d), BF16), pltpu.VMEM((tokens, d), F32)],
        compiler_params=params(),
    )(x, wg, wu, wd)


class PairSum:
    def __init__(self, place, tiles, landing, stage, send, recv):
        self.place, self.tiles, self.landing, self.stage, self.send, self.recv = place, tiles, landing, stage, send, recv

    @staticmethod
    def scratch(tiles, rows, cols):
        dma = pltpu.SemaphoreType.DMA
        return [pltpu.VMEM((tiles, rows, cols), BF16), pltpu.VMEM((2, rows, cols), BF16), dma((2,)), dma((tiles,))]

    def copy(self, i):
        slot = lax.rem(i, 2)
        return put(self.stage.at[slot], self.landing.at[i], self.send.at[slot], self.recv.at[i], self.place.partner())

    def reserve(self, i):
        pl.when(i >= 2)(lambda: self.copy(i - 2).wait_send())
        return self.stage.at[lax.rem(i, 2)]

    def drain(self):
        for i in (self.tiles - 2, self.tiles - 1):
            self.copy(i).wait_send()


def hidden_back(gate, up, dp):
    dp = dp.astype(BF16).astype(F32)
    s = lax.logistic(gate)
    act = gate * s
    return (act * up).astype(BF16), (dp * up * (s + act * (1.0 - s))).astype(BF16), (dp * act).astype(BF16)


def down_gradient(j, tiles, pair, p, dy, half, out):
    core = pair.place.core

    def columns(c):
        return pl.ds(pl.multiple_of(c * half, LANES), half)

    @pl.when(j < tiles)
    def _():
        slot = pair.reserve(j)
        slot[...] = dot(p[lax.rem(j, 2)], dy[:, columns(1 - core)], TN).astype(BF16)
        pair.copy(j).start()

    @pl.when(j >= 1)
    def _():
        pair.copy(j - 1).wait_recv()
        own = dot(p[lax.rem(j - 1, 2)], dy[:, columns(core)], TN)
        out[...] = (own + pair.landing[j - 1].astype(F32)).astype(BF16)

    pl.when(j == tiles)(pair.drain)


def layer_kernel(tiles, a, dy, wg, wu, wd, dgu, at, out, p, *rest):
    j = pl.program_id(0)
    place = Place()
    pair = PairSum(place, tiles, *rest)
    pl.when(j == 0)(lambda: signal_all([place.partner()]))

    @pl.when(j < tiles)
    def _():
        transpose_piece(j, tiles - 1, a, at)
        slot = lax.rem(j, 2)
        for m in range(a.shape[0] // ROWS):
            r = pl.ds(m * ROWS, ROWS)
            g = dot(a[r, :], wg[0], NN)
            u = dot(a[r, :], wu[0], NN)
            dp = dot(dy[r, :], wd[0], NT)
            p[slot, r, :], dgu[0, r, :], dgu[1, r, :] = hidden_back(g, u, dp)

    down_gradient(j, tiles, pair, p, dy, dy.shape[1] // 2, out)


def clip(tiles, back=0):
    return lambda j: jnp.clip(j - back, 0, tiles - 1)


def layer_call(collective_id, a, dy, wg, wu, wd):
    tokens, d = a.shape
    ff = wg.shape[2]
    tiles, half = ff // TILE, d // 2
    now, before = clip(tiles), clip(tiles, 1)
    w_in = spec((1, d, TILE), lambda j: (1, 0, now(j)))
    return pl.pallas_call(
        functools.partial(layer_kernel, tiles),
        name="layer_1",
        grid=(tiles + 1,),
        in_specs=[whole((tokens, d))] * 2 + [w_in, w_in, spec((1, TILE, d), lambda j: (1, now(j), 0))],
        out_specs=[spec((2, tokens, TILE), lambda j: (0, 0, now(j))), whole((d, tokens)), spec((TILE, half), lambda j: (before(j), 0))],
        out_shape=[
            jax.ShapeDtypeStruct((2, tokens, ff), BF16),
            jax.ShapeDtypeStruct((d, tokens), BF16),
            jax.ShapeDtypeStruct((ff, half), BF16),
        ],
        scratch_shapes=[pltpu.VMEM((2, tokens, TILE), BF16), *PairSum.scratch(tiles, TILE, half)],
        compiler_params=params(collective_id),
    )(a, dy, wg, wu, wd)


GATE_ROWS, DOWN_WINDOW = 24, 72
RING = 6


def second(t, v, rest=ALL):
    return (rest, v) if t == 1 else (v, rest)


class Stream:
    def __init__(self, place, tiles, phases, refs):
        self.place, self.tiles, self.phases, self.rows = place, tiles, phases, GATE_ROWS // 3
        self.held, self.slots, self.send, self.recv = refs[0], refs[1 : 1 + 2 * phases], refs[-2], refs[-1]
        self.ways = ways_of(TILE)

    @staticmethod
    def scratch(tiles, phases):
        third, dma = GATE_ROWS // 3, pltpu.SemaphoreType.DMA
        leads = [(3, 3, tiles, SIDE, SIDE), (3, 3, tiles, SIDE), (3, 3, tiles)][:phases]
        slots = [pltpu.VMEM((*lead, third, width), BF16) for lead in leads for _, width in ways_of(TILE)]
        return [pltpu.VMEM((RING, SIDE, SIDE, SIDE, GATE_ROWS, TILE), BF16), *slots, dma((tiles, 3 * phases)), dma((tiles, 3 * phases))]

    def part(self, t, way):
        start, width = self.ways[way]
        return pl.ds(t * self.rows, self.rows), pl.ds(start, width)

    def own(self, c, t, way, hops, b=ALL, d=ALL):
        at = index(ORDERS[t], (self.place.block(ORDERS[t][0], way, hops), ALL, ALL))
        axes = [i for i in range(3) if i != ORDERS[t][0]]
        at = list(at)
        at[axes[0]], at[axes[1]] = b, d
        return self.held.at[(lax.rem(c, RING), *at, *self.part(t, way))]

    def copy(self, phase, t, way, n, c, first=False):
        axis = ORDERS[t][phase]
        slots = self.slots[2 * phase + way]
        if not first:
            src = slots.at[t, n - 1, c]
        elif phase == 0:
            src = self.own(c, t, way, 1)
        else:
            v = self.place.block(axis, way, 1)
            at = second(t, v) if phase == 1 else (v,)
            src = self.slots[2 * phase - 2 + way].at[(t, 2, c, *at)]
        key = (c, 3 * phase + n)
        return put(src, slots.at[t, n, c], self.send.at[key], self.recv.at[key], self.place.device(axis, self.place.onward(way)))

    def pairs(self):
        return [(t, way) for t in range(3) for way in range(2)]

    def all_of(self, phase):
        return self.held.at[(0,) * (phase + 2)]

    def begin(self, phase, c):
        for t, way in self.pairs():
            self.copy(phase, t, way, 0, c, first=True).start()

    def add(self, phase, t, way, n, c):
        slots = self.slots[2 * phase + way]
        v = self.place.block(ORDERS[t][phase], way, n + 1)

        def one(at, other):
            at = (t, n - 1, c, *at)
            slots[at] = (slots[at].astype(F32) + other[...].astype(F32)).astype(BF16)

        if phase == 0:
            for b in range(SIDE):
                for d in range(SIDE):
                    one((b, d), self.own(c, t, way, n + 1, b, d))
        elif phase == 1:
            for d in range(SIDE):
                one((d,), self.slots[way].at[(t, 2, c, *second(t, v, d))])
        else:
            one((), self.slots[2 + way].at[t, 2, c, v])

    def stage(self, s, c, out):
        phase, n = (s - 1) // 3, (s - 1) % 3 + 1
        key = (c, 3 * phase + n - 1)
        whole_stage = self.all_of(phase)
        pltpu.make_async_copy(whole_stage, whole_stage, self.recv.at[key]).wait()
        for t, way in self.pairs():
            self.add(phase, t, way, n, c)
            if n < 3:
                self.copy(phase, t, way, n, c).start()
        if n == 3 and phase + 1 < self.phases:
            self.begin(phase + 1, c)
        if n == 3 and phase == 2:
            for t, way in self.pairs():
                rows, _ = self.part(t, way)
                start, width = self.ways[way]
                out[rows, pl.ds(pl.multiple_of(c * TILE + start, LANES), width)] = self.slots[4 + way][t, 2, c]

    def sent(self, phase, n, c):
        whole_stage = self.all_of(phase)
        pltpu.make_async_copy(whole_stage, whole_stage, self.send.at[c, 3 * phase + n]).wait()

    def keep(self, c):
        pl.when(c >= RING)(lambda: self.sent(0, 0, c - RING))
        return self.held.at[lax.rem(c, RING)]

    def step(self, newest, out=None):
        valid = lambda c: (c >= 0) & (c < self.tiles)
        pl.when(valid(newest))(lambda: self.begin(0, newest))
        for s in range(3 * self.phases, 0, -1):
            pl.when(valid(newest - s))(lambda s=s: self.stage(s, newest - s, out))

    def drain(self):
        def each(c, _):
            pl.when(c >= self.tiles - RING)(lambda: self.sent(0, 0, c))
            for i in range(1, 3 * self.phases):
                self.sent(i // 3, i % 3, c)
            return 0

        lax.fori_loop(0, self.tiles, each, 0)

    def results(self):
        return [self.slots[way].at[:, 2] for way in range(2)]


def stream_halves(tiles):
    return [(3, tiles, SIDE, SIDE, GATE_ROWS // 3, width) for _, width in ways_of(TILE)]


class StreamRest:
    def __init__(self, place, tiles, before, refs):
        self.place, self.tiles, self.before, self.slots, self.sems = place, tiles, before, refs[:4], refs[4:8]
        self.rows, self.ways = GATE_ROWS // 3, ways_of(TILE)

    @staticmethod
    def scratch(tiles):
        third, dma = GATE_ROWS // 3, pltpu.SemaphoreType.DMA
        shapes = [pltpu.VMEM((3, 3, *lead, third, width), BF16) for lead in ((tiles, SIDE), (tiles,)) for _, width in ways_of(TILE)]
        return shapes + [dma((3, 2, 3))] * 4

    def pairs(self):
        return [(t, way) for t in range(3) for way in range(2)]

    def message(self, phase, t, way, n, arriving=False):
        slots = self.slots[2 * phase - 2 + way]
        axis = ORDERS[t][phase]
        if arriving:
            src = slots.at[t, n]
        elif isinstance(n, int) and n == 0:
            v = self.place.block(axis, way, 1)
            src = self.before[way].at[(t, ALL, *second(t, v))] if phase == 1 else self.slots[way].at[t, 2, :, v]
        else:
            src = slots.at[t, n - 1]
        send, recv = self.sems[2 * phase - 2 : 2 * phase]
        key = (t, way, n)
        return put(src, slots.at[t, n], send.at[key], recv.at[key], self.place.device(axis, self.place.onward(way)))

    def start(self, phase):
        for t, way in self.pairs():
            self.message(phase, t, way, 0).start()

    def step(self, phase, n):
        for t, way in self.pairs():
            self.message(phase, t, way, n - 1, arriving=True).wait_recv()
            v = self.place.block(ORDERS[t][phase], way, n + 1)
            slots = self.slots[2 * phase - 2 + way]

            def add(c, _, t=t, way=way, v=v, slots=slots):
                for d in range(SIDE if phase == 1 else 1):
                    at = (t, n - 1, c, d) if phase == 1 else (t, n - 1, c)
                    other = self.before[way].at[(t, c, *second(t, v, d))] if phase == 1 else self.slots[way].at[t, 2, c, v]
                    slots[at] = (slots[at].astype(F32) + other[...].astype(F32)).astype(BF16)
                return 0

            lax.fori_loop(0, self.tiles, add, 0)
            pl.when(n < 3)(lambda t=t, way=way: self.message(phase, t, way, n).start())

    def tick(self, i):
        pl.when(i == 0)(lambda: self.start(1))
        pl.when((i >= 1) & (i <= 3))(lambda: self.step(1, i))
        pl.when(i == 3)(lambda: self.start(2))
        pl.when((i >= 4) & (i <= 6))(lambda: self.step(2, i - 3))

    def result(self, out):
        def one(c, _):
            for t, way in self.pairs():
                start, width = self.ways[way]
                lanes = pl.ds(pl.multiple_of(c * TILE + start, LANES), width)
                out[pl.ds(t * self.rows, self.rows), lanes] = self.slots[2 + way][t, 2, c]
            return 0

        lax.fori_loop(0, self.tiles, one, 0)

    def drain(self):
        for t, way in self.pairs():
            for phase in (1, 2):
                for n in range(3):
                    self.message(phase, t, way, n).wait_send()


BLOCK_ROWS = SIDE * SIDE * GATE_ROWS


def gate_up_kernel(tiles, phases, cols, at, ahead, behind, sum_down, *rest):
    j = pl.program_id(0)
    place = Place()
    core = place.core
    outs, rest = (rest[:4], rest[4:]) if phases == 1 else (rest[:2], rest[2:])
    pair = PairSum(place, tiles, *rest[:4])
    first = First.of(place, DOWN_WINDOW, cols, rest[4:9])
    stream = Stream(place, tiles, phases, rest[9 : 9 + 3 + 2 * phases])
    rest = rest[9 + 3 + 2 * phases :]
    load_sem, save_sem = rest[:2]
    loads = loads_down(sum_down, first, load_sem)
    last = tiles + 3 * phases

    @pl.when(j == 0)
    def _():
        signal_all(near(place))
        begin(loads)

    @pl.when(j < tiles)
    def _():
        slot = pair.reserve(j)
        other = ahead[1 - core]
        for m in range(SIDE):
            r = pl.ds(m * BLOCK_ROWS, BLOCK_ROWS)
            slot[r, :] = dot(at[r, :], other, NN).astype(BF16)
        pair.copy(j).start()

    @pl.when((j >= 1) & (j <= tiles))
    def _():
        pair.copy(j - 1).wait_recv()
        own = behind[core]
        kept = stream.keep(j - 1)
        for m in range(SIDE):
            r = pl.ds(m * BLOCK_ROWS, BLOCK_ROWS)
            total = (dot(at[r, :], own, NN) + pair.landing[j - 1, r, :].astype(F32)).astype(BF16)
            kept[m] = total.reshape(SIDE, SIDE, GATE_ROWS, TILE)

    if phases == 1:
        stream.step(j - 1)
    else:
        stream.step(j - 1, outs[0])
    pl.when(j == 0)(lambda: end(loads))
    if phases == 1:
        pl.when(j <= tiles)(lambda: spread(j, tiles + 1, 16, first.tick))
    else:
        down = Rest.of(place, DOWN_WINDOW, cols, first.results(), rest[2:10])
        pl.when(j < 8)(lambda: spread(j, 8, 16, first.tick))
        pl.when(j >= 8)(lambda: down.tick(j - 8))
        pl.when(j == 15)(lambda: down.result(outs[1]))

    @pl.when(j == last)
    def _():
        pair.drain()
        if phases == 1:
            saves = copies([*first.results(), *stream.results()], outs, save_sem)
            begin(saves)
        first.drain()
        stream.drain()
        if phases == 1:
            end(saves)
        else:
            down.drain()


def gate_up_call(name, collective_id, phases, at, dgu, sum_down):
    d, tokens = at.shape
    ff = dgu.shape[2]
    tiles, cols, dma = ff // TILE, sum_down.shape[-1], pltpu.SemaphoreType.DMA
    now, before = clip(tiles), clip(tiles, 1)
    if phases == 1:
        shapes = [*half_sums(DOWN_WINDOW, cols), *stream_halves(tiles)]
        out_specs, more = [HBM] * 4, []
    else:
        shapes = [(GATE_ROWS, ff), (DOWN_WINDOW, cols)]
        out_specs, more = [whole(s) for s in shapes], Rest.scratch(DOWN_WINDOW, cols)
    return pl.pallas_call(
        functools.partial(gate_up_kernel, tiles, phases, cols),
        name=name,
        grid=(tiles + 3 * phases + 1,),
        in_specs=[
            whole((d, tokens)),
            spec((2, tokens, TILE), lambda j: (0, 0, now(j))),
            spec((2, tokens, TILE), lambda j: (0, 0, before(j))),
            HBM,
        ],
        out_specs=out_specs,
        out_shape=[jax.ShapeDtypeStruct(s, BF16) for s in shapes],
        scratch_shapes=[
            *PairSum.scratch(tiles, d, TILE),
            *First.scratch(DOWN_WINDOW, cols),
            *Stream.scratch(tiles, phases),
            dma((SIDE,)),
            dma((4,)),
            *more,
        ],
        compiler_params=params(collective_id),
    )(at, dgu, dgu, sum_down)


def middle_kernel(tiles, down_cols, dgu, wg, wu, h, dy, down0, down1, gate0, gate1, dh, out_down, out_gu, acc_g, acc_u, *rest):
    j = pl.program_id(0)
    place = Place()
    before = rest[:4]
    down = Rest.of(place, DOWN_WINDOW, down_cols, before[:2], rest[4:12])
    gate = StreamRest(place, gate0.shape[1], before[2:], rest[12:20])
    loads = copies((down0, down1, gate0, gate1), before, rest[20])

    @pl.when(j == 0)
    def _():
        signal_all(near(place))
        begin(loads)
        clear(acc_g)
        clear(acc_u)

    for m in range(h.shape[0] // ROWS):
        r = pl.ds(m * ROWS, ROWS)
        acc_g[r, :] += dot(dgu[0, r, :], wg[0], NT)
        acc_u[r, :] += dot(dgu[1, r, :], wu[0], NT)

    pl.when(j == 0)(lambda: end(loads))
    down.tick(j)
    gate.tick(j)

    @pl.when(j == 7)
    def _():
        down.result(out_down)
        gate.result(out_gu)

    @pl.when(j == tiles - 1)
    def _():
        def rows(r):
            wide = h[r, :].astype(F32)
            scale = norm_scale(wide)
            da = (acc_g[r, :].astype(BF16).astype(F32) + acc_u[r, :].astype(BF16).astype(F32)).astype(BF16).astype(F32)
            back = scale * da - wide * (scale * scale * scale * jnp.mean(da * wide, -1, keepdims=True))
            dh[r, :] = (dy[r, :].astype(F32) + back.astype(BF16).astype(F32)).astype(BF16)

        in_rows(h.shape[0], 64, rows)
        down.drain()
        gate.drain()


def middle_call(collective_id, dgu, wg, wu, h, dy, halves):
    tokens, d = h.shape
    ff = dgu.shape[2]
    tiles, dma, down_cols = ff // TILE, pltpu.SemaphoreType.DMA, d // 2
    w_in = spec((1, d, TILE), lambda j: (1, 0, j))
    sums = [(DOWN_WINDOW, down_cols), (GATE_ROWS, ff)]
    return pl.pallas_call(
        functools.partial(middle_kernel, tiles, down_cols),
        name="middle",
        grid=(tiles,),
        in_specs=[spec((2, tokens, TILE), lambda j: (0, 0, j)), w_in, w_in, whole((tokens, d)), whole((tokens, d))] + [HBM] * 4,
        out_specs=[whole((tokens, d)), *[whole(s) for s in sums]],
        out_shape=[jax.ShapeDtypeStruct(s, BF16) for s in ((tokens, d), *sums)],
        scratch_shapes=[pltpu.VMEM((tokens, d), F32)] * 2
        + [pltpu.VMEM(t.shape, BF16) for t in halves]
        + Rest.scratch(DOWN_WINDOW, down_cols)
        + StreamRest.scratch(tiles)
        + [dma((4,))],
        compiler_params=params(collective_id),
    )(dgu, wg, wu, h, dy, *halves)


def back_kernel(tiles, dh, gate, up, wd, dgu, out, p, *rest):
    j = pl.program_id(0)
    place = Place()
    pair = PairSum(place, tiles, *rest)
    pl.when(j == 0)(lambda: signal_all([place.partner()]))

    @pl.when(j < tiles)
    def _():
        slot = lax.rem(j, 2)
        for m in range(dh.shape[0] // ROWS):
            r = pl.ds(m * ROWS, ROWS)
            dp = dot(dh[r, :], wd[0], NT)
            p[slot, r, :], dgu[0, r, :], dgu[1, r, :] = hidden_back(gate[r, :], up[r, :], dp)

    down_gradient(j, tiles, pair, p, dh, dh.shape[1] // 2, out)


def back_call(collective_id, dh, gate, up, wd):
    tokens, d = dh.shape
    ff = gate.shape[1]
    tiles, half = ff // TILE, d // 2
    now, before = clip(tiles), clip(tiles, 1)
    tile = spec((tokens, TILE), lambda j: (0, now(j)))
    return pl.pallas_call(
        functools.partial(back_kernel, tiles),
        name="back_0",
        grid=(tiles + 1,),
        in_specs=[whole((tokens, d)), tile, tile, spec((1, TILE, d), lambda j: (0, now(j), 0))],
        out_specs=[spec((2, tokens, TILE), lambda j: (0, 0, now(j))), spec((TILE, half), lambda j: (before(j), 0))],
        out_shape=[jax.ShapeDtypeStruct((2, tokens, ff), BF16), jax.ShapeDtypeStruct((ff, half), BF16)],
        scratch_shapes=[pltpu.VMEM((2, tokens, TILE), BF16), *PairSum.scratch(tiles, TILE, half)],
        compiler_params=params(collective_id),
    )(dh, gate, up, wd)


def flat(m):
    layers, rows, cols = m.shape
    split = m.transpose(1, 0, 2).reshape(rows, layers, cols // LANES, LANES)
    return with_layout_constraint(split, Layout((0, 2, 1, 3))).transpose(0, 2, 1, 3).reshape(-1, LANES)


def unflat(f, shape):
    layers, rows, cols = shape
    split = f.reshape(rows, cols // LANES, layers, LANES).transpose(0, 2, 1, 3)
    return with_layout_constraint(split, Layout((0, 2, 1, 3))).reshape(rows, layers, cols).transpose(1, 0, 2)


def solution(mesh):
    def body(x, dy, wg, wu, wd, mg, mu, md, vg, vu, vd):
        layers, d, ff = wg.shape
        x, dy = x[0], dy[0]
        windows = (SIDE, SIDE, 4 * 66, d // 2)
        gate0, up0, h1, a1, a0t = forward_call(x, wg, wu, wd)
        dgu1, a1t, down1 = layer_call(1, a1, dy, wg, wu, wd)
        halves = gate_up_call("gate_up_1", 2, 1, a1t, dgu1, down1.reshape(windows))
        dh1, sum_down1, sum_gu1 = middle_call(3, dgu1, wg, wu, h1, dy, halves)
        dgu0, down0 = back_call(4, dh1, gate0, up0, wd)
        sum_gu0, sum_down0 = gate_up_call("gate_up_0", 5, 3, a0t, dgu0, down0.reshape(windows))

        views = [(2, SIDE, SIDE, SIDE, GATE_ROWS, ff)] * 2 + [(2, SIDE, SIDE, 4 * 66, d)]
        w = [t.reshape(view) for t, view in zip((wg, wu, wd), views, strict=True)]
        m, v = [flat(t) for t in (mg, mu, md)], [flat(t) for t in (vg, vu, vd)]
        out = finish_call(3 * layers * d * ff, 7, [sum_gu0, sum_gu1], [sum_down0, sum_down1], m, v, w)
        new = [t.reshape(like.shape) for t, like in zip(out[:3], (wg, wu, wd), strict=True)]
        return (*new, *[unflat(t, like.shape) for t, like in zip(out[3:], (mg, mu, md, vg, vu, vd), strict=True)])

    shard = P(None, "dp", None)
    return jax.shard_map(
        body,
        mesh=mesh,
        in_specs=(P(("rep", "dp")), P(("rep", "dp")), P(), P(), P(), *[shard] * 6),
        out_specs=(P("rep"), P("rep"), P("rep"), *[P("rep", "dp", None)] * 6),
        check_vma=False,
    )
```

```python
import functools

import jax
import jax.numpy as jnp
from jax import lax
from jax.experimental import pallas as pl
from jax.experimental.layout import Layout, with_layout_constraint
from jax.experimental.pallas import tpu as pltpu
from jax.sharding import PartitionSpec as P

F32, BF16 = jnp.float32, jnp.bfloat16
CLIP_EPS = 1e-30
LANES = 128
SIDE = 4
ORDERS = ((0, 1, 2), (1, 2, 0), (2, 0, 1))
VMEM_LIMIT = 63 * 1024 * 1024


class Place:
    def __init__(self):
        me = lax.axis_index("dp")
        self.core = lax.rem(me, 2)
        chip = lax.div(me, 2)
        self.at = (lax.div(chip, SIDE * SIDE), lax.rem(lax.div(chip, SIDE), SIDE), lax.rem(chip, SIDE))

    def device(self, axis=None, off=0, core=None):
        at = list(self.at)
        if axis is not None:
            at[axis] = lax.rem(at[axis] + off, SIDE)
        core = self.core if core is None else core
        return {"dp": ((at[0] * SIDE + at[1]) * SIDE + at[2]) * 2 + core}

    def partner(self):
        return self.device(core=1 - self.core)

    def onward(self, way):
        return 1 + 2 * lax.rem(way + self.core, 2)

    def block(self, axis, way, hops):
        return lax.rem(self.at[axis] + hops * (SIDE - self.onward(way)), SIDE)


def signal_all(devices):
    barrier = pltpu.get_barrier_semaphore()
    for d in devices:
        pl.semaphore_signal(barrier, inc=1, device_id=d, device_id_type=pl.DeviceIdType.MESH)
    pl.semaphore_wait(barrier, len(devices))


def near(place):
    return [place.partner()] + [place.device(axis, off) for axis in range(3) for off in (1, SIDE - 1)]


def put(src, dst, send, recv, device):
    return pltpu.make_async_remote_copy(
        src_ref=src, dst_ref=dst, send_sem=send, recv_sem=recv, device_id=device, device_id_type=pl.DeviceIdType.MESH
    )


def ways_of(cols):
    tiles = cols // LANES
    first = (tiles + 1) // 2 * LANES
    return ((0, first), (first, cols - first))


def index(order, values):
    out = [None] * 3
    for axis, value in zip(order, values, strict=True):
        out[axis] = value
    return tuple(out)


ALL = slice(None)


class Rings:
    def __init__(self, place, rows, cols, slots, sems):
        self.place, self.rows, self.slots, self.sems = place, rows // 3, slots, sems
        self.ways = ways_of(cols)

    def part(self, t, way):
        start, width = self.ways[way]
        return pl.ds(t * self.rows, self.rows), pl.ds(start, width)

    @staticmethod
    def pairs():
        return [(t, way) for t in range(3) for way in range(2)]

    def send(self, axis, way, src, landing, key, sems):
        src = landing if src is None else src
        return put(src, landing, sems[0].at[key], sems[1].at[key], self.place.device(axis, self.place.onward(way)))


class First(Rings):
    @staticmethod
    def scratch(rows, cols):
        third, dma = rows // 3, pltpu.SemaphoreType.DMA
        slots = [pltpu.VMEM((3, 3, SIDE, SIDE, third, width), BF16) for _, width in ways_of(cols)]
        return [pltpu.VMEM((SIDE, SIDE, SIDE, rows, cols), BF16), *slots, dma((3, 2, 3, SIDE)), dma((3, 2, 3, SIDE))]

    @classmethod
    def of(cls, place, rows, cols, refs):
        one = cls(place, rows, cols, refs[1:3], refs[3:5])
        one.held = refs[0]
        return one

    def block(self, t, way, hops, k, c=ALL):
        order = ORDERS[t]
        return self.held.at[(*index(order, (self.place.block(order[0], way, hops), k, c)), *self.part(t, way))]

    def message(self, t, way, n, k, arriving=False):
        src = None
        if not arriving:
            src = self.block(t, way, 1, k) if isinstance(n, int) and n == 0 else self.slots[way].at[t, n - 1, k]
        return self.send(ORDERS[t][0], way, src, self.slots[way].at[t, n, k], (t, way, n, k), self.sems)

    def start(self, k):
        for t, way in self.pairs():
            self.message(t, way, 0, k).start()

    def step(self, n, k):
        for t, way in self.pairs():
            self.message(t, way, n - 1, k, arriving=True).wait_recv()
            slots = self.slots[way]
            for c in range(SIDE):
                own = self.block(t, way, n + 1, k, c)
                slots[t, n - 1, k, c] = (slots[t, n - 1, k, c].astype(F32) + own[...].astype(F32)).astype(BF16)
            pl.when(n < 3)(lambda t=t, way=way: self.message(t, way, n, k).start())

    def tick(self, i):
        pl.when(i < SIDE)(lambda: self.start(i))
        pl.when(i >= SIDE)(lambda: self.step(lax.div(i, SIDE), lax.rem(i, SIDE)))

    def results(self):
        return [slots.at[:, 2] for slots in self.slots]

    def drain(self):
        def sent(k, _):
            for t, way in self.pairs():
                self.message(t, way, 0, k).wait_send()
                lax.fori_loop(1, 3, lambda n, _: (self.message(t, way, n, k).wait_send(), 0)[1], 0)
            return 0

        lax.fori_loop(0, SIDE, sent, 0)


class Rest(Rings):
    @staticmethod
    def scratch(rows, cols):
        third, dma = rows // 3, pltpu.SemaphoreType.DMA
        shapes = [pltpu.VMEM((*lead, third, width), BF16) for lead in ((3, 3, SIDE), (3, 3)) for _, width in ways_of(cols)]
        return shapes + [dma((3, 2, 3))] * 4

    @classmethod
    def of(cls, place, rows, cols, before, refs):
        one = cls(place, rows, cols, refs[:4], refs[4:8])
        one.before = before
        return one

    def message(self, phase, t, way, n, arriving=False):
        slots = self.slots[2 * phase - 2 + way]
        axis = ORDERS[t][phase]
        if arriving:
            src = None
        elif isinstance(n, int) and n == 0:
            v = self.place.block(axis, way, 1)
            src = self.before[way].at[t, v] if phase == 1 else self.slots[way].at[t, 2, v]
        else:
            src = slots.at[t, n - 1]
        return self.send(axis, way, src, slots.at[t, n], (t, way, n), self.sems[2 * phase - 2 : 2 * phase])

    def start(self, phase):
        for t, way in self.pairs():
            self.message(phase, t, way, 0).start()

    def step1(self, n):
        for t, way in self.pairs():
            self.message(1, t, way, n - 1, arriving=True).wait_recv()
            v = self.place.block(ORDERS[t][1], way, n + 1)
            before, slots = self.before[way], self.slots[way]
            for c in range(SIDE):
                slots[t, n - 1, c] = (slots[t, n - 1, c].astype(F32) + before[t, v, c].astype(F32)).astype(BF16)
            pl.when(n < 3)(lambda t=t, way=way: self.message(1, t, way, n).start())

    def step2(self, n):
        for t, way in self.pairs():
            self.message(2, t, way, n - 1, arriving=True).wait_recv()
            v = self.place.block(ORDERS[t][2], way, n + 1)
            before, slots = self.slots[way], self.slots[2 + way]
            slots[t, n - 1] = (slots[t, n - 1].astype(F32) + before[t, 2, v].astype(F32)).astype(BF16)
            pl.when(n < 3)(lambda t=t, way=way: self.message(2, t, way, n).start())

    def tick(self, i):
        pl.when(i == 0)(lambda: self.start(1))
        pl.when((i >= 1) & (i <= 3))(lambda: self.step1(i))
        pl.when(i == 3)(lambda: self.start(2))
        pl.when((i >= 4) & (i <= 6))(lambda: self.step2(i - 3))

    def result(self, out):
        for t, way in self.pairs():
            out[self.part(t, way)] = self.slots[2 + way][t, 2]

    def drain(self):
        for t, way in self.pairs():
            for phase in (1, 2):
                for n in range(3):
                    self.message(phase, t, way, n).wait_send()


def loads_down(source, first, sems):
    return [pltpu.make_async_copy(source.at[:, :, pl.ds(64 * z, 72)], first.held.at[:, :, z], sems.at[z]) for z in range(SIDE)]


def spread(j, steps, count, tick):
    low, high = lax.div(count * j, steps), lax.div(count * (j + 1), steps)
    lax.fori_loop(low, high, lambda i, _: (tick(i), 0)[1], 0)


def copies(sources, targets, sems):
    return [pltpu.make_async_copy(s, t, sems.at[i]) for i, (s, t) in enumerate(zip(sources, targets, strict=True))]


def begin(all_copies):
    for copy in all_copies:
        copy.start()


def end(all_copies):
    for copy in all_copies:
        copy.wait()


def half_sums(rows, cols):
    return [(3, SIDE, SIDE, rows // 3, width) for _, width in ways_of(cols)]


PREV = 6
DOWN_ROWS = 33


class Gather:
    def __init__(self, place, bufs, sems, outs, copy_sems):
        self.place, self.bufs, self.sems, self.outs, self.copy_sems = place, bufs, sems, outs, copy_sems

    @staticmethod
    def scratch(gate_cols, down_cols):
        bufs = [pltpu.VMEM((2, SIDE, SIDE, SIDE, 24, gate_cols), BF16), pltpu.VMEM((2, SIDE, SIDE, SIDE, 72, down_cols), BF16)]
        return bufs + [pltpu.SemaphoreType.DMA((2, 3, 2, 6, 3))] * 4 + [pltpu.SemaphoreType.DMA((2,))] * 3

    def part(self, kind, t, way):
        rows, cols = self.bufs[kind].shape[-2:]
        start, width = ways_of(cols)[way]
        return pl.ds(t * (rows // 3), rows // 3), pl.ds(start, width)

    def behind(self, t, way, axis, hops):
        return self.place.block(ORDERS[t][axis], way, hops)

    def message(self, kind, l, t, way, line, n, hops):
        order, place = ORDERS[t], self.place
        if isinstance(line, int) and line == 0:
            axis, values = order[0], [self.behind(t, way, 0, hops), place.at[order[1]], place.at[order[2]]]
        elif isinstance(line, int) and line == 1:
            axis, values = order[1], [ALL, self.behind(t, way, 1, hops), place.at[order[2]]]
        else:
            axis, values = order[2], [ALL, self.behind(t, way, 1, line - 2), self.behind(t, way, 2, hops)]
        ref = self.bufs[kind].at[(l, *index(order, values), *self.part(kind, t, way))]
        key = (l, t, way, line, n)
        return put(ref, ref, self.sems[2 * kind].at[key], self.sems[2 * kind + 1].at[key], place.device(axis, place.onward(way)))

    def copies(self, kind, l, t, way, b, c):
        order = ORDERS[t]
        rows, cols = self.part(kind, t, way)
        at = index(order, (ALL, b, c))
        if kind == 0:
            return [lambda out: (self.bufs[0].at[(l, *at, rows, cols)], out.at[(l, *at, rows, cols)])]
        half = self.bufs[1].shape[-1]
        start, width = ways_of(half)[way]
        columns = pl.ds(pl.multiple_of(self.place.core * half + start, LANES), width)
        x, y, z = at

        def pair(out, z, count):
            src = self.bufs[1].at[l, x, y, z, pl.ds(24 * t, count), cols]
            return src, out.at[l, x, y, pl.ds(pl.multiple_of(64 * z + 24 * t, 8), count), columns]

        if t < 2:
            return [lambda out: pair(out, z, 24)]
        return [lambda out, z=z: pair(out, z, 16 if z < SIDE - 1 else 24) for z in range(SIDE)]

    def copy_out(self, kind, l, t, way, b, c):
        local, send, recv = self.copy_sems

        def both(out):
            for pair in self.copies(kind, l, t, way, b, c):
                src, dst = pair(out)
                pltpu.make_async_copy(src, dst, local.at[kind]).start()
                put(src, dst, send.at[kind], recv.at[kind], self.place.partner()).start()

        if kind:
            both(self.outs[2])
        else:
            for core in range(2):
                pl.when(self.place.core == core)(lambda core=core: both(self.outs[core]))

    def parts(self):
        return [(kind, t, way) for kind in range(2) for t in range(3) for way in range(2)]

    def own(self, l):
        for kind, t, way in self.parts():
            self.message(kind, l, t, way, 0, 0, 0).start()

    def start_third(self, kind, l, t, way, m):
        self.message(kind, l, t, way, 2 + m, 0, 0).start()
        self.copy_out(kind, l, t, way, self.behind(t, way, 1, m), self.place.at[ORDERS[t][2]])

    def first_axis(self):
        def step(i, _):
            n, l = 1 + lax.div(i, 2), lax.rem(i, 2)
            for kind, t, way in self.parts():
                self.message(kind, l, t, way, 0, n - 1, n).wait_recv()
                pl.when(n < 3)(lambda kind=kind, t=t, way=way: self.message(kind, l, t, way, 0, n, n).start())

                @pl.when(n == 3)
                def _(kind=kind, t=t, way=way):
                    self.message(kind, l, t, way, 1, 0, 0).start()
                    self.start_third(kind, l, t, way, 0)

            return 0

        lax.fori_loop(0, 6, step, 0)

    def other_axes(self):
        def step(i, _):
            r, l = 1 + lax.div(i, 2), lax.rem(i, 2)
            for kind, t, way in self.parts():

                @pl.when(r <= 3)
                def _(kind=kind, t=t, way=way):
                    self.message(kind, l, t, way, 1, r - 1, r).wait_recv()
                    pl.when(r < 3)(lambda: self.message(kind, l, t, way, 1, r, r).start())
                    self.start_third(kind, l, t, way, r)

                def third(m, _, kind=kind, t=t, way=way):
                    n = r - m
                    self.message(kind, l, t, way, 2 + m, n - 1, n).wait_recv()
                    pl.when(n < 3)(lambda: self.message(kind, l, t, way, 2 + m, n, n).start())
                    self.copy_out(kind, l, t, way, self.behind(t, way, 1, m), self.behind(t, way, 2, n))
                    return 0

                lax.fori_loop(jnp.maximum(r - 3, 0), jnp.minimum(r, SIDE), third, 0)
            return 0

        lax.fori_loop(0, 12, step, 0)

    def drain(self):
        local, send, recv = self.copy_sems
        half = self.bufs[1].shape[-1]
        columns = self.outs[2].at[:, :, :, :, pl.ds(0, half)]
        for kind, whole in ((0, self.outs[0]), (1, columns)):
            pltpu.make_async_copy(whole, whole, local.at[kind]).wait()
            copy = put(whole, whole, send.at[kind], recv.at[kind], self.place.partner())
            copy.wait_send()
            copy.wait_recv()

        def sent(i, _):
            l, n = lax.div(i, 3), lax.rem(i, 3)
            for kind, t, way in self.parts():
                for line in range(2):
                    self.message(kind, l, t, way, line, n, n).wait_send()
                lax.fori_loop(2, 6, lambda line, _: (self.message(kind, l, t, way, line, n, n).wait_send(), 0)[1], 0)
            return 0

        lax.fori_loop(0, 6, sent, 0)


def finish_kernel(count, *refs):
    sums_gu, sums_d, m_in, v_in, w_in = refs[0:2], refs[2:4], refs[4:7], refs[7:10], refs[10:13]
    w_out, m_out, v_out = refs[13:16], refs[16:19], refs[19:22]
    moments_gu, moments_d, old_gu, old_d, other_d, tiles = refs[22:28]
    load_sem, early_send, early_recv, norm_send, norm_recv, late_local, late_send, late_recv = refs[28:36]
    gather_refs = refs[36:]
    place = Place()
    x, y, z = place.at
    core = place.core
    gather = Gather(place, gather_refs[:2], gather_refs[2:6], w_out, gather_refs[6:9])
    partner = place.partner()
    gate_tiles, down_tiles = sums_gu[0].shape[1] // LANES, sums_d[0].shape[1] // LANES
    gate_stride, down_stride = 2 * gate_tiles, 4 * down_tiles
    gate_size, down_size = 12 * gate_stride, DOWN_ROWS * down_stride

    def blank(i, _):
        for which in range(2):
            moments_d[which, pl.ds(pl.multiple_of(8 * i, 8), 8), :] = jnp.zeros((8, LANES), F32)
        return 0

    lax.fori_loop(0, moments_d.shape[1] // 8, blank, 0)
    following = [place.device(2, 1, core=c) for c in range(2)]
    others = [place.device(axis, 2) for axis in range(3)] + [place.device(2, off, core=1 - core) for off in (1, SIDE - 1)]
    signal_all(near(place) + others)

    def gate_rows(i, which):
        return moments_gu.at[i, pl.ds(pl.multiple_of(which * gate_size, 8), gate_size)]

    def down_rows(i, first, rows):
        return moments_d.at[i, pl.ds(pl.multiple_of(first * down_stride, 8), rows * down_stride)]

    def columns(ref):
        half = down_tiles * LANES
        return ref.at[:, x, y, pl.ds(pl.multiple_of(64 * z, 8), 72), pl.ds(pl.multiple_of(core * half, LANES), half)]

    own_rows = PREV + 2 * z + DOWN_ROWS * core
    loads, sends = [], []
    for i, moment in enumerate((m_in, v_in)):
        for c in range(2):

            @pl.when(core == c)
            def _(i=i, moment=moment, c=c):
                pltpu.make_async_copy(moment[c], gate_rows(i, core), load_sem.at[i]).start()
                put(moment[1 - c], gate_rows(i, core), early_send.at[i], early_recv.at[i], partner).start()

        loads.append(pltpu.make_async_copy(moment[0], gate_rows(i, core), load_sem.at[i]))
        sends.append(put(moment[0], gate_rows(i, core), early_send.at[i], early_recv.at[i], partner))
        loads.append(pltpu.make_async_copy(moment[2], down_rows(i, own_rows, DOWN_ROWS), load_sem.at[2 + i]))
        loads[-1].start()
        sends.append(put(moment[2], down_rows(i, own_rows, DOWN_ROWS), early_send.at[2 + i], early_recv.at[2 + i], partner))
        sends[-1].start()
        last = moment[2].at[pl.ds((DOWN_ROWS - PREV) * down_stride, PREV * down_stride)]
        landing = down_rows(i, 2 * lax.rem(z + 1, SIDE), PREV)

        @pl.when(core == 1)
        def _(i=i, last=last, landing=landing):
            for c in range(2):
                put(last, landing, early_send.at[4 + 2 * i + c], early_recv.at[4 + i], following[c]).start()

    for l in range(2):
        sends.append(put(sums_d[l], other_d.at[l], early_send.at[8 + l], early_recv.at[6 + l], partner))
        sends[-1].start()
    for c in range(2):

        @pl.when(core == c)
        def _(c=c):
            pltpu.make_async_copy(w_in[c].at[:, x, y, z], old_gu, load_sem.at[4]).start()

    loads.append(pltpu.make_async_copy(w_in[0].at[:, x, y, z], old_gu, load_sem.at[4]))
    loads.append(pltpu.make_async_copy(columns(w_in[2]), old_d, load_sem.at[5]))
    loads[-1].start()

    squares = jnp.zeros((8, LANES), F32)
    for l in range(2):

        def of_gate_up(j, total, l=l):
            for t in range(3):
                g = sums_gu[l][pl.ds(8 * t, 8), pl.ds(pl.multiple_of(j * LANES, LANES), LANES)].astype(F32)
                total += g * g
            return total

        squares = lax.fori_loop(0, gate_tiles, of_gate_up, squares)

        def of_down(i, total, l=l):
            row = 8 * i + lax.broadcasted_iota(jnp.int32, (8, LANES), 0)
            mine = (row >= 2 * z) & (row < 2 * z + 2 * DOWN_ROWS)
            for j in range(down_tiles):
                g = sums_d[l][pl.ds(pl.multiple_of(8 * i, 8), 8), pl.ds(j * LANES, LANES)].astype(F32)
                total += jnp.where(mine, g * g, 0.0)
            return total

        squares = lax.fori_loop(0, 9, of_down, squares)
    for stage, (coordinate, size) in enumerate(((core, 2), (x, SIDE), (y, SIDE), (z, SIDE))):
        tiles[stage, coordinate] = squares
        exchanges = []
        for off in range(1, size):
            target = partner if stage == 0 else place.device(stage - 1, off)
            key = 3 * stage + off - 1
            here = tiles.at[stage, coordinate]
            exchanges.append(put(here, here, norm_send.at[key], norm_recv.at[key], target))
            exchanges[-1].start()
        for exchange in exchanges:
            exchange.wait_recv()
        for exchange in exchanges:
            exchange.wait_send()
        squares = tiles[stage, 0]
        for other in range(1, size):
            squares += tiles[stage, other]
    total = jnp.sum(jnp.sum(squares, 0, keepdims=True), 1, keepdims=True)
    factor = jnp.minimum(1.0, 0.5 * lax.rsqrt(total / count + CLIP_EPS))

    for copy in loads:
        copy.wait()
    for copy in sends:
        copy.wait_recv()
    for i in range(2):
        put(down_rows(i, 0, PREV), down_rows(i, 0, PREV), early_send.at[0], early_recv.at[4 + i], partner).wait_recv()

    def moments(ref, start, stride, g):
        rows = pl.ds(start, 8, stride=stride)
        m = 0.9 * ref[0, rows, :] + 0.1 * g
        v = 0.95 * ref[1, rows, :] + 0.05 * g * g
        ref[0, rows, :] = m
        ref[1, rows, :] = v
        return m * lax.rsqrt(v + 1e-8)

    def weight(w, step):
        w = w.astype(F32)
        return (w - 0.02 * (step + 0.1 * w)).astype(BF16)

    for l in range(2):

        def gate_up(j, _, l=l):
            lanes = pl.ds(pl.multiple_of(j * LANES, LANES), LANES)
            for t in range(3):
                rows = pl.ds(8 * t, 8)
                g = sums_gu[l][rows, lanes].astype(F32) * factor
                step = moments(moments_gu, 8 * t * gate_stride + 2 * j + l, gate_stride, g)
                gather.bufs[0][l, x, y, z, rows, lanes] = weight(old_gu[l, rows, lanes], step)
            return 0

        lax.fori_loop(0, gate_tiles, gate_up, 0, unroll=3)

        def down(i, _, l=l):
            rows = pl.ds(pl.multiple_of(8 * i, 8), 8)
            for j in range(down_tiles):
                lanes = pl.ds(j * LANES, LANES)
                start = (PREV + 8 * i) * down_stride + 2 * j + l
                g = sums_d[l][rows, lanes].astype(F32) * factor
                step = moments(moments_d, start + 2 * down_tiles * core, down_stride, g)
                gather.bufs[1][l, x, y, z, rows, lanes] = weight(old_d[l, rows, lanes], step)
            return 0

        lax.fori_loop(0, 9, down, 0)
        gather.own(l)
    for l in range(2):

        def down_other(i, _, l=l):
            rows = pl.ds(pl.multiple_of(8 * i, 8), 8)
            for j in range(down_tiles):
                start = (PREV + 8 * i) * down_stride + 2 * j + l
                g = other_d[l, rows, pl.ds(j * LANES, LANES)].astype(F32) * factor
                moments(moments_d, start + 2 * down_tiles * (1 - core), down_stride, g)
            return 0

        lax.fori_loop(0, 9, down_other, 0)

    late = []
    for i, out in enumerate((m_out, v_out)):
        for c in range(2):

            @pl.when(core == c)
            def _(i=i, out=out, c=c):
                pltpu.make_async_copy(gate_rows(i, core), out[c], late_local.at[i]).start()
                put(gate_rows(i, 1 - core), out[c], late_send.at[i], late_recv.at[i], partner).start()

        pltpu.make_async_copy(down_rows(i, own_rows, DOWN_ROWS), out[2], late_local.at[2 + i]).start()
    gather.first_axis()
    gather.other_axes()
    for i, out in enumerate((m_out, v_out)):
        pltpu.make_async_copy(gate_rows(i, core), out[0], late_local.at[i]).wait()
        pltpu.make_async_copy(down_rows(i, own_rows, DOWN_ROWS), out[2], late_local.at[2 + i]).wait()
        copy = put(gate_rows(i, 1 - core), out[0], late_send.at[i], late_recv.at[i], partner)
        copy.wait_recv()
        copy.wait_send()
    for copy in sends:
        copy.wait_send()
    for i in range(2):
        for c in range(2):

            @pl.when(core == 1)
            def _(i=i, c=c):
                rows = down_rows(i, 0, PREV)
                put(rows, rows, early_send.at[4 + 2 * i + c], early_recv.at[4 + i], following[c]).wait_send()

    gather.drain()


def finish_call(count, collective_id, sums_gu, sums_d, m, v, w):
    gate_cols, down_half = sums_gu[0].shape[1], sums_d[0].shape[1]
    operands = [*sums_gu, *sums_d, *m, *v, *w]
    hbm, vmem = pl.BlockSpec(memory_space=pltpu.HBM), pl.BlockSpec(memory_space=pltpu.VMEM)
    dma = pltpu.SemaphoreType.DMA
    gate_stride, down_stride = gate_cols // 64, down_half // 32
    scratch = [
        pltpu.VMEM((2, 24 * gate_stride, LANES), F32),
        pltpu.VMEM((2, (PREV + 72) * down_stride, LANES), F32),
        pltpu.VMEM((2, 24, gate_cols), BF16),
        pltpu.VMEM((2, 72, down_half), BF16),
        pltpu.VMEM((2, 72, down_half), BF16),
        pltpu.VMEM((4, SIDE, 8, LANES), F32),
        dma((6,)), dma((10,)), dma((8,)), dma((12,)), dma((12,)), dma((4,)), dma((2,)), dma((2,)),
    ]
    return pl.pallas_call(
        functools.partial(finish_kernel, count),
        name="finish",
        out_shape=[jax.ShapeDtypeStruct(t.shape, t.dtype) for t in (*w, *m, *v)],
        in_specs=[vmem] * 4 + [hbm] * 9,
        out_specs=[hbm] * 9,
        scratch_shapes=scratch + Gather.scratch(gate_cols, down_half),
        compiler_params=pltpu.CompilerParams(collective_id=collective_id, has_side_effects=True, vmem_limit_bytes=VMEM_LIMIT),
        cost_estimate=pl.CostEstimate(flops=10**9, bytes_accessed=10**8, transcendentals=0),
    )(*operands)


TILE = 384
ROWS = 256
TIGHT = pl.Buffered(buffer_count=1)


def dot(a, b, dims):
    return lax.dot_general(a, b, (dims, ((), ())), preferred_element_type=F32)


NN, NT, TN = ((1,), (0,)), ((1,), (1,)), ((0,), (0,))


def norm_scale(wide):
    return lax.rsqrt(jnp.mean(wide * wide, -1, keepdims=True) + 1e-6)


def in_rows(total, step, body):
    def one(i, _):
        body(pl.ds(pl.multiple_of(i * step, step), step))
        return 0

    lax.fori_loop(0, total // step, one, 0)


def clear(acc):
    def rows(r):
        acc[r, :] = jnp.zeros((8, acc.shape[1]), F32)

    in_rows(acc.shape[0], 8, rows)


def spec(shape, index_map, tight=False):
    return pl.BlockSpec(shape, index_map, pipeline_mode=TIGHT) if tight else pl.BlockSpec(shape, index_map)


def whole(shape, tight=True):
    return spec(shape, lambda j: (0,) * len(shape), tight)


HBM = pl.BlockSpec(memory_space=pltpu.HBM)


def params(collective_id=None, semantics=("arbitrary",)):
    more = {} if collective_id is None else {"collective_id": collective_id, "has_side_effects": True}
    return pltpu.CompilerParams(dimension_semantics=semantics, vmem_limit_bytes=VMEM_LIMIT, **more)


def transpose_piece(j, last, src, dst):
    def piece(i):
        at = pl.ds(pl.multiple_of(i * LANES, LANES), LANES)
        dst[at, :] = src[:, at].T

    piece(j)
    pl.when(j == last)(lambda: piece(last + 1))


def forward_kernel(tiles, x, wg, wu, wd, gate, up, h_out, a_out, at, a, acc):
    j = pl.program_id(0)

    @pl.when(j == 0)
    def _():
        def rows(r):
            wide = x[r, :].astype(F32)
            a[r, :] = (wide * norm_scale(wide)).astype(BF16)

        in_rows(x.shape[0], 128, rows)
        clear(acc)

    transpose_piece(j, tiles - 1, a, at)
    for m in range(x.shape[0] // ROWS):
        r = pl.ds(m * ROWS, ROWS)
        g = dot(a[r, :], wg[0], NN)
        u = dot(a[r, :], wu[0], NN)
        gate[r, :] = g
        up[r, :] = u
        p = (g * lax.logistic(g) * u).astype(BF16)
        acc[r, :] += dot(p, wd[0], NN)

    @pl.when(j == tiles - 1)
    def _():
        def rows(r):
            h = (x[r, :].astype(F32) + acc[r, :].astype(BF16).astype(F32)).astype(BF16)
            h_out[r, :] = h
            wide = h.astype(F32)
            a_out[r, :] = (wide * norm_scale(wide)).astype(BF16)

        in_rows(x.shape[0], 128, rows)


def forward_call(x, wg, wu, wd):
    tokens, d = x.shape
    ff = wg.shape[2]
    tiles = ff // TILE
    w_in = spec((1, d, TILE), lambda j: (0, 0, j))
    return pl.pallas_call(
        functools.partial(forward_kernel, tiles),
        name="forward_0",
        grid=(tiles,),
        in_specs=[whole((tokens, d)), w_in, w_in, spec((1, TILE, d), lambda j: (0, j, 0))],
        out_specs=[spec((tokens, TILE), lambda j: (0, j))] * 2 + [whole((tokens, d))] * 2 + [whole((d, tokens))],
        out_shape=[jax.ShapeDtypeStruct((tokens, ff), F32)] * 2
        + [jax.ShapeDtypeStruct((tokens, d), BF16)] * 2
        + [jax.ShapeDtypeStruct((d, tokens), BF16)],
        scratch_shapes=[pltpu.VMEM((tokens, d), BF16), pltpu.VMEM((tokens, d), F32)],
        compiler_params=params(),
    )(x, wg, wu, wd)


class PairSum:
    def __init__(self, place, tiles, landing, stage, send, recv):
        self.place, self.tiles, self.landing, self.stage, self.send, self.recv = place, tiles, landing, stage, send, recv

    @staticmethod
    def scratch(tiles, rows, cols):
        dma = pltpu.SemaphoreType.DMA
        return [pltpu.VMEM((tiles, rows, cols), BF16), pltpu.VMEM((2, rows, cols), BF16), dma((2,)), dma((tiles,))]

    def copy(self, i):
        slot = lax.rem(i, 2)
        return put(self.stage.at[slot], self.landing.at[i], self.send.at[slot], self.recv.at[i], self.place.partner())

    def reserve(self, i):
        pl.when(i >= 2)(lambda: self.copy(i - 2).wait_send())
        return self.stage.at[lax.rem(i, 2)]

    def drain(self):
        for i in (self.tiles - 2, self.tiles - 1):
            self.copy(i).wait_send()


def hidden_back(gate, up, dp):
    dp = dp.astype(BF16).astype(F32)
    s = lax.logistic(gate)
    act = gate * s
    return (act * up).astype(BF16), (dp * up * (s + act * (1.0 - s))).astype(BF16), (dp * act).astype(BF16)


def down_gradient(j, tiles, pair, p, dy, half, out):
    core = pair.place.core

    def columns(c):
        return pl.ds(pl.multiple_of(c * half, LANES), half)

    @pl.when(j < tiles)
    def _():
        slot = pair.reserve(j)
        slot[...] = dot(p[lax.rem(j, 2)], dy[:, columns(1 - core)], TN).astype(BF16)
        pair.copy(j).start()

    @pl.when(j >= 1)
    def _():
        pair.copy(j - 1).wait_recv()
        own = dot(p[lax.rem(j - 1, 2)], dy[:, columns(core)], TN)
        out[...] = (own + pair.landing[j - 1].astype(F32)).astype(BF16)

    pl.when(j == tiles)(pair.drain)


def layer_kernel(tiles, a, dy, wg, wu, wd, dgu, at, out, p, *rest):
    j = pl.program_id(0)
    place = Place()
    pair = PairSum(place, tiles, *rest)
    pl.when(j == 0)(lambda: signal_all([place.partner()]))

    @pl.when(j < tiles)
    def _():
        transpose_piece(j, tiles - 1, a, at)
        slot = lax.rem(j, 2)
        for m in range(a.shape[0] // ROWS):
            r = pl.ds(m * ROWS, ROWS)
            g = dot(a[r, :], wg[0], NN)
            u = dot(a[r, :], wu[0], NN)
            dp = dot(dy[r, :], wd[0], NT)
            p[slot, r, :], dgu[0, r, :], dgu[1, r, :] = hidden_back(g, u, dp)

    down_gradient(j, tiles, pair, p, dy, dy.shape[1] // 2, out)


def clip(tiles, back=0):
    return lambda j: jnp.clip(j - back, 0, tiles - 1)


def layer_call(collective_id, a, dy, wg, wu, wd):
    tokens, d = a.shape
    ff = wg.shape[2]
    tiles, half = ff // TILE, d // 2
    now, before = clip(tiles), clip(tiles, 1)
    w_in = spec((1, d, TILE), lambda j: (1, 0, now(j)))
    return pl.pallas_call(
        functools.partial(layer_kernel, tiles),
        name="layer_1",
        grid=(tiles + 1,),
        in_specs=[whole((tokens, d))] * 2 + [w_in, w_in, spec((1, TILE, d), lambda j: (1, now(j), 0))],
        out_specs=[spec((2, tokens, TILE), lambda j: (0, 0, now(j))), whole((d, tokens)), spec((TILE, half), lambda j: (before(j), 0))],
        out_shape=[
            jax.ShapeDtypeStruct((2, tokens, ff), BF16),
            jax.ShapeDtypeStruct((d, tokens), BF16),
            jax.ShapeDtypeStruct((ff, half), BF16),
        ],
        scratch_shapes=[pltpu.VMEM((2, tokens, TILE), BF16), *PairSum.scratch(tiles, TILE, half)],
        compiler_params=params(collective_id),
    )(a, dy, wg, wu, wd)


GATE_ROWS, DOWN_WINDOW = 24, 72
RING = 6


def second(t, v, rest=ALL):
    return (rest, v) if t == 1 else (v, rest)


class Stream:
    def __init__(self, place, tiles, phases, refs):
        self.place, self.tiles, self.phases, self.rows = place, tiles, phases, GATE_ROWS // 3
        self.held, self.slots, self.send, self.recv = refs[0], refs[1 : 1 + 2 * phases], refs[-2], refs[-1]
        self.ways = ways_of(TILE)

    @staticmethod
    def scratch(tiles, phases):
        third, dma = GATE_ROWS // 3, pltpu.SemaphoreType.DMA
        leads = [(3, 3, tiles, SIDE, SIDE), (3, 3, tiles, SIDE), (3, 3, tiles)][:phases]
        slots = [pltpu.VMEM((*lead, third, width), BF16) for lead in leads for _, width in ways_of(TILE)]
        return [pltpu.VMEM((RING, SIDE, SIDE, SIDE, GATE_ROWS, TILE), BF16), *slots, dma((tiles, 7)), dma((tiles, 7))]

    def part(self, t, way):
        start, width = self.ways[way]
        return pl.ds(t * self.rows, self.rows), pl.ds(start, width)

    def own(self, c, t, way, hops, b=ALL, d=ALL):
        at = index(ORDERS[t], (self.place.block(ORDERS[t][0], way, hops), ALL, ALL))
        axes = [i for i in range(3) if i != ORDERS[t][0]]
        at = list(at)
        at[axes[0]], at[axes[1]] = b, d
        return self.held.at[(lax.rem(c, RING), *at, *self.part(t, way))]

    def copy(self, phase, t, way, n, c, first=False):
        axis = ORDERS[t][phase]
        slots = self.slots[2 * phase + way]
        if not first:
            src = slots.at[t, n - 1, c]
        elif phase == 0:
            src = self.own(c, t, way, 1)
        else:
            src = self.slots[way].at[(t, 2, c, *second(t, self.place.block(axis, way, 1)))]
        key = (c, 3 * phase + n)
        return put(src, slots.at[t, n, c], self.send.at[key], self.recv.at[key], self.place.device(axis, self.place.onward(way)))

    def direct(self, t, way, off, c):
        axis = ORDERS[t][2]
        v = lax.rem(self.place.at[axis] + off, SIDE)
        src, dst = self.slots[2 + way].at[t, 2, c, v], self.slots[4 + way].at[t, off - 1, c]
        return put(src, dst, self.send.at[c, 6], self.recv.at[c, 6], self.place.device(axis, off))

    def pairs(self):
        return [(t, way) for t in range(3) for way in range(2)]

    def all_of(self, phase):
        return self.held.at[(0,) * (phase + 2)] if phase < 2 else self.held.at[0, 0, 0, pl.ds(0, 3)]

    def begin(self, phase, c):
        for t, way in self.pairs():
            if phase < 2:
                self.copy(phase, t, way, 0, c, first=True).start()
            else:
                for off in range(1, SIDE):
                    self.direct(t, way, off, c).start()

    def add(self, phase, t, way, n, c):
        slots = self.slots[2 * phase + way]
        v = self.place.block(ORDERS[t][phase], way, n + 1)

        def one(at, other):
            at = (t, n - 1, c, *at)
            slots[at] = (slots[at].astype(F32) + other[...].astype(F32)).astype(BF16)

        if phase == 0:
            for b in range(SIDE):
                for d in range(SIDE):
                    one((b, d), self.own(c, t, way, n + 1, b, d))
        else:
            for d in range(SIDE):
                one((d,), self.slots[way].at[(t, 2, c, *second(t, v, d))])

    def stage(self, s, c, out):
        phase, n = (s - 1) // 3, (s - 1) % 3 + 1
        whole_stage = self.all_of(phase)
        pltpu.make_async_copy(whole_stage, whole_stage, self.recv.at[c, s - 1]).wait()
        if phase == 2:
            for t, way in self.pairs():
                total = self.slots[2 + way][t, 2, c, self.place.at[ORDERS[t][2]]].astype(F32)
                for i in range(3):
                    total += self.slots[4 + way][t, i, c].astype(F32)
                rows, _ = self.part(t, way)
                start, width = self.ways[way]
                out[rows, pl.ds(pl.multiple_of(c * TILE + start, LANES), width)] = total.astype(BF16)
            return
        for t, way in self.pairs():
            self.add(phase, t, way, n, c)
            if n < 3:
                self.copy(phase, t, way, n, c).start()
        if n == 3 and phase + 1 < self.phases:
            self.begin(phase + 1, c)

    def sent(self, phase, n, c):
        whole_stage = self.all_of(phase)
        pltpu.make_async_copy(whole_stage, whole_stage, self.send.at[c, 3 * phase + n]).wait()

    def count(self):
        return 3 if self.phases == 1 else 7

    def keep(self, c):
        pl.when(c >= RING)(lambda: self.sent(0, 0, c - RING))
        return self.held.at[lax.rem(c, RING)]

    def run(self, s, c, out):
        act = (lambda: self.begin(0, c)) if s == 0 else (lambda: self.stage(s, c, out))
        pl.when((c >= 0) & (c < self.tiles))(act)

    def early(self, j, out=None):
        for s in range(self.count(), 1, -1):
            self.run(s, j - 2 - s, out)

    def late(self, j, out=None):
        self.run(0, j - 1, out)
        self.run(1, j - 2, out)

    def last_step(self):
        return self.tiles - 1 + 2 + self.count()

    def drain(self):
        def each(c, _):
            pl.when(c >= self.tiles - RING)(lambda: self.sent(0, 0, c))
            for i in range(1, self.count()):
                self.sent(i // 3, i % 3, c)
            return 0

        lax.fori_loop(0, self.tiles, each, 0)

    def results(self):
        return [self.slots[way].at[:, 2] for way in range(2)]


def stream_halves(tiles):
    return [(3, tiles, SIDE, SIDE, GATE_ROWS // 3, width) for _, width in ways_of(TILE)]


class StreamRest:
    def __init__(self, place, tiles, before, refs):
        self.place, self.tiles, self.before, self.slots, self.sems = place, tiles, before, refs[:4], refs[4:8]
        self.rows, self.ways = GATE_ROWS // 3, ways_of(TILE)

    @staticmethod
    def scratch(tiles):
        third, dma = GATE_ROWS // 3, pltpu.SemaphoreType.DMA
        shapes = [pltpu.VMEM((3, 3, *lead, third, width), BF16) for lead in ((tiles, SIDE), (tiles,)) for _, width in ways_of(TILE)]
        return shapes + [dma((3, 2, 3))] * 4

    def pairs(self):
        return [(t, way) for t in range(3) for way in range(2)]

    def message(self, phase, t, way, n, arriving=False):
        slots = self.slots[2 * phase - 2 + way]
        axis = ORDERS[t][phase]
        if arriving:
            src = slots.at[t, n]
        elif isinstance(n, int) and n == 0:
            v = self.place.block(axis, way, 1)
            src = self.before[way].at[(t, ALL, *second(t, v))] if phase == 1 else self.slots[way].at[t, 2, :, v]
        else:
            src = slots.at[t, n - 1]
        send, recv = self.sems[2 * phase - 2 : 2 * phase]
        key = (t, way, n)
        return put(src, slots.at[t, n], send.at[key], recv.at[key], self.place.device(axis, self.place.onward(way)))

    def start(self, phase):
        for t, way in self.pairs():
            self.message(phase, t, way, 0).start()

    def step(self, phase, n):
        for t, way in self.pairs():
            self.message(phase, t, way, n - 1, arriving=True).wait_recv()
            v = self.place.block(ORDERS[t][phase], way, n + 1)
            slots = self.slots[2 * phase - 2 + way]

            def add(c, _, t=t, way=way, v=v, slots=slots):
                for d in range(SIDE if phase == 1 else 1):
                    at = (t, n - 1, c, d) if phase == 1 else (t, n - 1, c)
                    other = self.before[way].at[(t, c, *second(t, v, d))] if phase == 1 else self.slots[way].at[t, 2, c, v]
                    slots[at] = (slots[at].astype(F32) + other[...].astype(F32)).astype(BF16)
                return 0

            lax.fori_loop(0, self.tiles, add, 0)
            pl.when(n < 3)(lambda t=t, way=way: self.message(phase, t, way, n).start())

    def tick(self, j):
        i = jnp.where(j <= 8, jnp.where(lax.rem(j, 2) == 0, lax.div(j, 2), -1), j - 4)
        pl.when(i == 0)(lambda: self.start(1))
        pl.when((i >= 1) & (i <= 3))(lambda: self.step(1, i))
        pl.when(i == 3)(lambda: self.start(2))
        pl.when((i >= 4) & (i <= 6))(lambda: self.step(2, i - 3))

    def result(self, out):
        def one(c, _):
            for t, way in self.pairs():
                start, width = self.ways[way]
                lanes = pl.ds(pl.multiple_of(c * TILE + start, LANES), width)
                out[pl.ds(t * self.rows, self.rows), lanes] = self.slots[2 + way][t, 2, c]
            return 0

        lax.fori_loop(0, self.tiles, one, 0)

    def drain(self):
        for t, way in self.pairs():
            for phase in (1, 2):
                for n in range(3):
                    self.message(phase, t, way, n).wait_send()


BLOCK_ROWS = SIDE * SIDE * GATE_ROWS


def gate_up_kernel(tiles, phases, cols, at, ahead, behind, *rest):
    j = pl.program_id(0)
    place = Place()
    core = place.core
    if phases == 1:
        outs, out, rest = rest[:2], None, rest[2:]
    else:
        sum_down, out, out_down, rest = rest[0], rest[1], rest[2], rest[3:]
    pair = PairSum(place, tiles, *rest[:4])
    stream = Stream(place, tiles, phases, rest[4 : 4 + 3 + 2 * phases])
    rest = rest[4 + 3 + 2 * phases :]
    if phases == 3:
        first = First.of(place, DOWN_WINDOW, cols, rest[1:6])
        down = Rest.of(place, DOWN_WINDOW, cols, first.results(), rest[6:14])
        loads = loads_down(sum_down, first, rest[0])

    @pl.when(j == 0)
    def _():
        opposite = [place.device(axis, 2) for axis in range(3)] if phases == 3 else []
        signal_all(near(place) + opposite)
        if phases == 3:
            begin(loads)

    @pl.when(j < tiles)
    def _():
        slot = pair.reserve(j)
        other = ahead[1 - core]
        for m in range(SIDE):
            r = pl.ds(m * BLOCK_ROWS, BLOCK_ROWS)
            slot[r, :] = dot(at[r, :], other, NN).astype(BF16)
        pair.copy(j).start()

    stream.early(j, out)
    if phases == 3:
        pl.when(j == 0)(lambda: end(loads))
        pl.when(j < 8)(lambda: spread(j, 8, 16, first.tick))
        pl.when(j >= 8)(lambda: down.tick(j - 8))
        pl.when(j == 15)(lambda: down.result(out_down))

    @pl.when((j >= 1) & (j <= tiles))
    def _():
        pair.copy(j - 1).wait_recv()
        own = behind[core]
        kept = stream.keep(j - 1)
        for m in range(SIDE):
            r = pl.ds(m * BLOCK_ROWS, BLOCK_ROWS)
            total = (dot(at[r, :], own, NN) + pair.landing[j - 1, r, :].astype(F32)).astype(BF16)
            kept[m] = total.reshape(SIDE, SIDE, GATE_ROWS, TILE)

    stream.late(j, out)

    @pl.when(j == stream.last_step())
    def _():
        pair.drain()
        if phases == 1:
            saves = copies(stream.results(), outs, rest[0])
            begin(saves)
            stream.drain()
            end(saves)
        else:
            stream.drain()
            first.drain()
            down.drain()


def gate_up_call(name, collective_id, phases, at, dgu, *sum_down):
    d, tokens = at.shape
    ff = dgu.shape[2]
    tiles, cols, dma = ff // TILE, d // 2, pltpu.SemaphoreType.DMA
    now, before = clip(tiles), clip(tiles, 1)
    if phases == 1:
        shapes = stream_halves(tiles)
        out_specs, more = [HBM] * 2, [dma((2,))]
    else:
        shapes = [(GATE_ROWS, ff), (DOWN_WINDOW, cols)]
        out_specs = [whole(s) for s in shapes]
        more = [dma((SIDE,)), *First.scratch(DOWN_WINDOW, cols), *Rest.scratch(DOWN_WINDOW, cols)]
    return pl.pallas_call(
        functools.partial(gate_up_kernel, tiles, phases, cols),
        name=name,
        grid=(tiles + (5 if phases == 1 else 9),),
        in_specs=[
            whole((d, tokens)),
            spec((2, tokens, TILE), lambda j: (0, 0, now(j))),
            spec((2, tokens, TILE), lambda j: (0, 0, before(j))),
            *[HBM] * len(sum_down),
        ],
        out_specs=out_specs,
        out_shape=[jax.ShapeDtypeStruct(s, BF16) for s in shapes],
        scratch_shapes=[*PairSum.scratch(tiles, d, TILE), *Stream.scratch(tiles, phases), *more],
        compiler_params=params(collective_id),
    )(at, dgu, dgu, *sum_down)


def middle_kernel(tiles, down_cols, dgu, wg, wu, h, dy, sum_down, gate0, gate1, dh, out_gu, half0, half1, acc_g, acc_u, *rest):
    j = pl.program_id(0)
    place = Place()
    first = First.of(place, DOWN_WINDOW, down_cols, rest[:5])
    gate = StreamRest(place, gate0.shape[1], rest[5:7], rest[7:15])
    load_sem, gate_sem, save_sem = rest[15:18]
    loads = loads_down(sum_down, first, load_sem) + copies((gate0, gate1), rest[5:7], gate_sem)

    @pl.when(j == 0)
    def _():
        signal_all(near(place))
        begin(loads)
        clear(acc_g)
        clear(acc_u)

    for m in range(h.shape[0] // ROWS):
        r = pl.ds(m * ROWS, ROWS)
        acc_g[r, :] += dot(dgu[0, r, :], wg[0], NT)
        acc_u[r, :] += dot(dgu[1, r, :], wu[0], NT)

    pl.when(j == 0)(lambda: end(loads))
    gate.tick(j)
    spread(j, tiles, 16, first.tick)

    @pl.when(j == tiles - 1)
    def _():
        saves = copies(first.results(), (half0, half1), save_sem)
        begin(saves)
        gate.result(out_gu)

        def rows(r):
            wide = h[r, :].astype(F32)
            scale = norm_scale(wide)
            da = (acc_g[r, :].astype(BF16).astype(F32) + acc_u[r, :].astype(BF16).astype(F32)).astype(BF16).astype(F32)
            back = scale * da - wide * (scale * scale * scale * jnp.mean(da * wide, -1, keepdims=True))
            dh[r, :] = (dy[r, :].astype(F32) + back.astype(BF16).astype(F32)).astype(BF16)

        in_rows(h.shape[0], 64, rows)
        first.drain()
        gate.drain()
        end(saves)


def middle_call(collective_id, dgu, wg, wu, h, dy, sum_down, gate_halves):
    tokens, d = h.shape
    ff = dgu.shape[2]
    tiles, dma, down_cols = ff // TILE, pltpu.SemaphoreType.DMA, d // 2
    w_in = spec((1, d, TILE), lambda j: (1, 0, j))
    return pl.pallas_call(
        functools.partial(middle_kernel, tiles, down_cols),
        name="middle",
        grid=(tiles,),
        in_specs=[spec((2, tokens, TILE), lambda j: (0, 0, j)), w_in, w_in, whole((tokens, d)), whole((tokens, d))] + [HBM] * 3,
        out_specs=[whole((tokens, d)), whole((GATE_ROWS, ff)), HBM, HBM],
        out_shape=[jax.ShapeDtypeStruct(s, BF16) for s in ((tokens, d), (GATE_ROWS, ff), *half_sums(DOWN_WINDOW, down_cols))],
        scratch_shapes=[pltpu.VMEM((tokens, d), F32)] * 2
        + First.scratch(DOWN_WINDOW, down_cols)
        + [pltpu.VMEM(t.shape, BF16) for t in gate_halves]
        + StreamRest.scratch(tiles)
        + [dma((SIDE,)), dma((2,)), dma((2,))],
        compiler_params=params(collective_id),
    )(dgu, wg, wu, h, dy, sum_down, *gate_halves)


def back_kernel(tiles, dh, gate, up, wd, down0, down1, dgu, out, out_down, p, *rest):
    j = pl.program_id(0)
    place = Place()
    half = dh.shape[1] // 2
    pair = PairSum(place, tiles, *rest[:4])
    before = rest[4:6]
    down = Rest.of(place, DOWN_WINDOW, half, before, rest[6:14])
    loads = copies((down0, down1), before, rest[14])

    @pl.when(j == 0)
    def _():
        signal_all(near(place))
        begin(loads)

    @pl.when(j < tiles)
    def _():
        slot = lax.rem(j, 2)
        for m in range(dh.shape[0] // ROWS):
            r = pl.ds(m * ROWS, ROWS)
            dp = dot(dh[r, :], wd[0], NT)
            p[slot, r, :], dgu[0, r, :], dgu[1, r, :] = hidden_back(gate[r, :], up[r, :], dp)

    down_gradient(j, tiles, pair, p, dh, half, out)
    pl.when(j == 0)(lambda: end(loads))
    down.tick(j)
    pl.when(j == 7)(lambda: down.result(out_down))
    pl.when(j == tiles)(down.drain)


def back_call(collective_id, dh, gate, up, wd, down_halves):
    tokens, d = dh.shape
    ff = gate.shape[1]
    tiles, half = ff // TILE, d // 2
    now, before = clip(tiles), clip(tiles, 1)
    tile = spec((tokens, TILE), lambda j: (0, now(j)))
    return pl.pallas_call(
        functools.partial(back_kernel, tiles),
        name="back_0",
        grid=(tiles + 1,),
        in_specs=[whole((tokens, d)), tile, tile, spec((1, TILE, d), lambda j: (0, now(j), 0)), HBM, HBM],
        out_specs=[
            spec((2, tokens, TILE), lambda j: (0, 0, now(j))),
            spec((TILE, half), lambda j: (before(j), 0)),
            whole((DOWN_WINDOW, half)),
        ],
        out_shape=[jax.ShapeDtypeStruct(s, BF16) for s in ((2, tokens, ff), (ff, half), (DOWN_WINDOW, half))],
        scratch_shapes=[pltpu.VMEM((2, tokens, TILE), BF16), *PairSum.scratch(tiles, TILE, half)]
        + [pltpu.VMEM(t.shape, BF16) for t in down_halves]
        + Rest.scratch(DOWN_WINDOW, half)
        + [pltpu.SemaphoreType.DMA((2,))],
        compiler_params=params(collective_id),
    )(dh, gate, up, wd, *down_halves)


def flat(m):
    layers, rows, cols = m.shape
    split = m.transpose(1, 0, 2).reshape(rows, layers, cols // LANES, LANES)
    return with_layout_constraint(split, Layout((0, 2, 1, 3))).transpose(0, 2, 1, 3).reshape(-1, LANES)


def unflat(f, shape):
    layers, rows, cols = shape
    split = f.reshape(rows, cols // LANES, layers, LANES).transpose(0, 2, 1, 3)
    return with_layout_constraint(split, Layout((0, 2, 1, 3))).reshape(rows, layers, cols).transpose(1, 0, 2)


def solution(mesh):
    def body(x, dy, wg, wu, wd, mg, mu, md, vg, vu, vd):
        layers, d, ff = wg.shape
        x, dy = x[0], dy[0]
        windows = (SIDE, SIDE, 4 * 66, d // 2)
        gate0, up0, h1, a1, a0t = forward_call(x, wg, wu, wd)
        dgu1, a1t, down1 = layer_call(1, a1, dy, wg, wu, wd)
        down1 = down1.reshape(windows)
        gate_halves = gate_up_call("gate_up_1", 2, 1, a1t, dgu1)
        dh1, sum_gu1, *down_halves = middle_call(3, dgu1, wg, wu, h1, dy, down1, gate_halves)
        dgu0, down0, sum_down1 = back_call(4, dh1, gate0, up0, wd, down_halves)
        sum_gu0, sum_down0 = gate_up_call("gate_up_0", 5, 3, a0t, dgu0, down0.reshape(windows))

        views = [(2, SIDE, SIDE, SIDE, GATE_ROWS, ff)] * 2 + [(2, SIDE, SIDE, 4 * 66, d)]
        w = [t.reshape(view) for t, view in zip((wg, wu, wd), views, strict=True)]
        m, v = [flat(t) for t in (mg, mu, md)], [flat(t) for t in (vg, vu, vd)]
        out = finish_call(3 * layers * d * ff, 7, [sum_gu0, sum_gu1], [sum_down0, sum_down1], m, v, w)
        new = [t.reshape(like.shape) for t, like in zip(out[:3], (wg, wu, wd), strict=True)]
        return (*new, *[unflat(t, like.shape) for t, like in zip(out[3:], (mg, mu, md, vg, vu, vd), strict=True)])

    shard = P(None, "dp", None)
    return jax.shard_map(
        body,
        mesh=mesh,
        in_specs=(P(("rep", "dp")), P(("rep", "dp")), P(), P(), P(), *[shard] * 6),
        out_specs=(P("rep"), P("rep"), P("rep"), *[P("rep", "dp", None)] * 6),
        check_vma=False,
    )
```

```python
import functools

import jax
import jax.numpy as jnp
from jax import lax
from jax.experimental import pallas as pl
from jax.experimental.layout import Layout, with_layout_constraint
from jax.experimental.pallas import tpu as pltpu
from jax.sharding import PartitionSpec as P

F32, BF16 = jnp.float32, jnp.bfloat16
CLIP_EPS = 1e-30
LANES = 128
SIDE = 4
ORDERS = ((0, 1, 2), (1, 2, 0), (2, 0, 1))
VMEM_LIMIT = 63 * 1024 * 1024


class Place:
    def __init__(self):
        me = lax.axis_index("dp")
        self.core = lax.rem(me, 2)
        chip = lax.div(me, 2)
        self.at = (lax.div(chip, SIDE * SIDE), lax.rem(lax.div(chip, SIDE), SIDE), lax.rem(chip, SIDE))

    def device(self, axis=None, off=0, core=None):
        at = list(self.at)
        if axis is not None:
            at[axis] = lax.rem(at[axis] + off, SIDE)
        core = self.core if core is None else core
        return {"dp": ((at[0] * SIDE + at[1]) * SIDE + at[2]) * 2 + core}

    def partner(self):
        return self.device(core=1 - self.core)

    def onward(self, way):
        return 1 + 2 * lax.rem(way + self.core, 2)

    def block(self, axis, way, hops):
        return lax.rem(self.at[axis] + hops * (SIDE - self.onward(way)), SIDE)


def signal_all(devices):
    barrier = pltpu.get_barrier_semaphore()
    for d in devices:
        pl.semaphore_signal(barrier, inc=1, device_id=d, device_id_type=pl.DeviceIdType.MESH)
    pl.semaphore_wait(barrier, len(devices))


def near(place):
    return [place.partner()] + [place.device(axis, off) for axis in range(3) for off in (1, SIDE - 1)]


def put(src, dst, send, recv, device):
    return pltpu.make_async_remote_copy(
        src_ref=src, dst_ref=dst, send_sem=send, recv_sem=recv, device_id=device, device_id_type=pl.DeviceIdType.MESH
    )


def ways_of(cols):
    tiles = cols // LANES
    first = (tiles + 1) // 2 * LANES
    return ((0, first), (first, cols - first))


def index(order, values):
    out = [None] * 3
    for axis, value in zip(order, values, strict=True):
        out[axis] = value
    return tuple(out)


ALL = slice(None)


class Rings:
    def __init__(self, place, rows, cols, slots, sems):
        self.place, self.rows, self.slots, self.sems = place, rows // 3, slots, sems
        self.ways = ways_of(cols)

    def part(self, t, way):
        start, width = self.ways[way]
        return pl.ds(t * self.rows, self.rows), pl.ds(start, width)

    @staticmethod
    def pairs():
        return [(t, way) for t in range(3) for way in range(2)]

    def send(self, axis, way, src, landing, key, sems):
        src = landing if src is None else src
        return put(src, landing, sems[0].at[key], sems[1].at[key], self.place.device(axis, self.place.onward(way)))


class First(Rings):
    @staticmethod
    def scratch(rows, cols):
        third, dma = rows // 3, pltpu.SemaphoreType.DMA
        slots = [pltpu.VMEM((3, 3, SIDE, SIDE, third, width), BF16) for _, width in ways_of(cols)]
        return [pltpu.VMEM((SIDE, SIDE, SIDE, rows, cols), BF16), *slots, dma((3, 2, 3, SIDE)), dma((3, 2, 3, SIDE))]

    @classmethod
    def of(cls, place, rows, cols, refs):
        one = cls(place, rows, cols, refs[1:3], refs[3:5])
        one.held = refs[0]
        return one

    def block(self, t, way, hops, k, c=ALL):
        order = ORDERS[t]
        return self.held.at[(*index(order, (self.place.block(order[0], way, hops), k, c)), *self.part(t, way))]

    def message(self, t, way, n, k, arriving=False):
        src = None
        if not arriving:
            src = self.block(t, way, 1, k) if isinstance(n, int) and n == 0 else self.slots[way].at[t, n - 1, k]
        return self.send(ORDERS[t][0], way, src, self.slots[way].at[t, n, k], (t, way, n, k), self.sems)

    def start(self, k):
        for t, way in self.pairs():
            self.message(t, way, 0, k).start()

    def step(self, n, k):
        for t, way in self.pairs():
            self.message(t, way, n - 1, k, arriving=True).wait_recv()
            slots = self.slots[way]
            for c in range(SIDE):
                own = self.block(t, way, n + 1, k, c)
                slots[t, n - 1, k, c] = (slots[t, n - 1, k, c].astype(F32) + own[...].astype(F32)).astype(BF16)
            pl.when(n < 3)(lambda t=t, way=way: self.message(t, way, n, k).start())

    def tick(self, i):
        pl.when(i < SIDE)(lambda: self.start(i))
        pl.when(i >= SIDE)(lambda: self.step(lax.div(i, SIDE), lax.rem(i, SIDE)))

    def results(self):
        return [slots.at[:, 2] for slots in self.slots]

    def drain(self):
        def sent(k, _):
            for t, way in self.pairs():
                self.message(t, way, 0, k).wait_send()
                lax.fori_loop(1, 3, lambda n, _: (self.message(t, way, n, k).wait_send(), 0)[1], 0)
            return 0

        lax.fori_loop(0, SIDE, sent, 0)


class Rest(Rings):
    @staticmethod
    def scratch(rows, cols):
        third, dma = rows // 3, pltpu.SemaphoreType.DMA
        shapes = [pltpu.VMEM((*lead, third, width), BF16) for lead in ((3, 3, SIDE), (3, 3)) for _, width in ways_of(cols)]
        return shapes + [dma((3, 2, 3))] * 4

    @classmethod
    def of(cls, place, rows, cols, before, refs):
        one = cls(place, rows, cols, refs[:4], refs[4:8])
        one.before = before
        return one

    def message(self, phase, t, way, n, arriving=False):
        slots = self.slots[2 * phase - 2 + way]
        axis = ORDERS[t][phase]
        if arriving:
            src = None
        elif isinstance(n, int) and n == 0:
            v = self.place.block(axis, way, 1)
            src = self.before[way].at[t, v] if phase == 1 else self.slots[way].at[t, 2, v]
        else:
            src = slots.at[t, n - 1]
        return self.send(axis, way, src, slots.at[t, n], (t, way, n), self.sems[2 * phase - 2 : 2 * phase])

    def start(self, phase):
        for t, way in self.pairs():
            self.message(phase, t, way, 0).start()

    def step1(self, n):
        for t, way in self.pairs():
            self.message(1, t, way, n - 1, arriving=True).wait_recv()
            v = self.place.block(ORDERS[t][1], way, n + 1)
            before, slots = self.before[way], self.slots[way]
            for c in range(SIDE):
                slots[t, n - 1, c] = (slots[t, n - 1, c].astype(F32) + before[t, v, c].astype(F32)).astype(BF16)
            pl.when(n < 3)(lambda t=t, way=way: self.message(1, t, way, n).start())

    def step2(self, n):
        for t, way in self.pairs():
            self.message(2, t, way, n - 1, arriving=True).wait_recv()
            v = self.place.block(ORDERS[t][2], way, n + 1)
            before, slots = self.slots[way], self.slots[2 + way]
            slots[t, n - 1] = (slots[t, n - 1].astype(F32) + before[t, 2, v].astype(F32)).astype(BF16)
            pl.when(n < 3)(lambda t=t, way=way: self.message(2, t, way, n).start())

    def tick(self, i):
        pl.when(i == 0)(lambda: self.start(1))
        pl.when((i >= 1) & (i <= 3))(lambda: self.step1(i))
        pl.when(i == 3)(lambda: self.start(2))
        pl.when((i >= 4) & (i <= 6))(lambda: self.step2(i - 3))

    def result(self, out):
        for t, way in self.pairs():
            out[self.part(t, way)] = self.slots[2 + way][t, 2]

    def drain(self):
        for t, way in self.pairs():
            for phase in (1, 2):
                for n in range(3):
                    self.message(phase, t, way, n).wait_send()


def loads_down(source, first, sems):
    return [pltpu.make_async_copy(source.at[:, :, pl.ds(64 * z, 72)], first.held.at[:, :, z], sems.at[z]) for z in range(SIDE)]


def spread(j, steps, count, tick):
    low, high = lax.div(count * j, steps), lax.div(count * (j + 1), steps)
    lax.fori_loop(low, high, lambda i, _: (tick(i), 0)[1], 0)


def copies(sources, targets, sems):
    return [pltpu.make_async_copy(s, t, sems.at[i]) for i, (s, t) in enumerate(zip(sources, targets, strict=True))]


def begin(all_copies):
    for copy in all_copies:
        copy.start()


def end(all_copies):
    for copy in all_copies:
        copy.wait()


def half_sums(rows, cols):
    return [(3, SIDE, SIDE, rows // 3, width) for _, width in ways_of(cols)]


PREV = 6
DOWN_ROWS = 33


class Gather:
    def __init__(self, place, bufs, sems, outs, copy_sems):
        self.place, self.bufs, self.sems, self.outs, self.copy_sems = place, bufs, sems, outs, copy_sems

    @staticmethod
    def scratch(gate_cols, down_cols):
        bufs = [pltpu.VMEM((2, SIDE, SIDE, SIDE, 24, gate_cols), BF16), pltpu.VMEM((2, SIDE, SIDE, SIDE, 72, down_cols), BF16)]
        return bufs + [pltpu.SemaphoreType.DMA((2, 3, 2, 6, 3))] * 4 + [pltpu.SemaphoreType.DMA((2,))] * 3

    def part(self, kind, t, way):
        rows, cols = self.bufs[kind].shape[-2:]
        start, width = ways_of(cols)[way]
        return pl.ds(t * (rows // 3), rows // 3), pl.ds(start, width)

    def behind(self, t, way, axis, hops):
        return self.place.block(ORDERS[t][axis], way, hops)

    def message(self, kind, l, t, way, line, n, hops):
        order, place = ORDERS[t], self.place
        if isinstance(line, int) and line == 0:
            axis, values = order[0], [self.behind(t, way, 0, hops), place.at[order[1]], place.at[order[2]]]
        elif isinstance(line, int) and line == 1:
            axis, values = order[1], [ALL, self.behind(t, way, 1, hops), place.at[order[2]]]
        else:
            axis, values = order[2], [ALL, self.behind(t, way, 1, line - 2), self.behind(t, way, 2, hops)]
        ref = self.bufs[kind].at[(l, *index(order, values), *self.part(kind, t, way))]
        key = (l, t, way, line, n)
        return put(ref, ref, self.sems[2 * kind].at[key], self.sems[2 * kind + 1].at[key], place.device(axis, place.onward(way)))

    def copies(self, kind, l, t, way, b, c):
        order = ORDERS[t]
        rows, cols = self.part(kind, t, way)
        at = index(order, (ALL, b, c))
        if kind == 0:
            return [lambda out: (self.bufs[0].at[(l, *at, rows, cols)], out.at[(l, *at, rows, cols)])]
        half = self.bufs[1].shape[-1]
        start, width = ways_of(half)[way]
        columns = pl.ds(pl.multiple_of(self.place.core * half + start, LANES), width)
        x, y, z = at

        def pair(out, z, count):
            src = self.bufs[1].at[l, x, y, z, pl.ds(24 * t, count), cols]
            return src, out.at[l, x, y, pl.ds(pl.multiple_of(64 * z + 24 * t, 8), count), columns]

        if t < 2:
            return [lambda out: pair(out, z, 24)]
        return [lambda out, z=z: pair(out, z, 16 if z < SIDE - 1 else 24) for z in range(SIDE)]

    def copy_out(self, kind, l, t, way, b, c):
        local, send, recv = self.copy_sems

        def both(out):
            for pair in self.copies(kind, l, t, way, b, c):
                src, dst = pair(out)
                pltpu.make_async_copy(src, dst, local.at[kind]).start()
                put(src, dst, send.at[kind], recv.at[kind], self.place.partner()).start()

        if kind:
            both(self.outs[2])
        else:
            for core in range(2):
                pl.when(self.place.core == core)(lambda core=core: both(self.outs[core]))

    def parts(self):
        return [(kind, t, way) for kind in range(2) for t in range(3) for way in range(2)]

    def own(self, l):
        for kind, t, way in self.parts():
            self.message(kind, l, t, way, 0, 0, 0).start()

    def start_third(self, kind, l, t, way, m):
        self.message(kind, l, t, way, 2 + m, 0, 0).start()
        self.copy_out(kind, l, t, way, self.behind(t, way, 1, m), self.place.at[ORDERS[t][2]])

    def first_axis(self):
        def step(i, _):
            n, l = 1 + lax.div(i, 2), lax.rem(i, 2)
            for kind, t, way in self.parts():
                self.message(kind, l, t, way, 0, n - 1, n).wait_recv()
                pl.when(n < 3)(lambda kind=kind, t=t, way=way: self.message(kind, l, t, way, 0, n, n).start())

                @pl.when(n == 3)
                def _(kind=kind, t=t, way=way):
                    self.message(kind, l, t, way, 1, 0, 0).start()
                    self.start_third(kind, l, t, way, 0)

            return 0

        lax.fori_loop(0, 6, step, 0)

    def other_axes(self):
        def step(i, _):
            r, l = 1 + lax.div(i, 2), lax.rem(i, 2)
            for kind, t, way in self.parts():

                @pl.when(r <= 3)
                def _(kind=kind, t=t, way=way):
                    self.message(kind, l, t, way, 1, r - 1, r).wait_recv()
                    pl.when(r < 3)(lambda: self.message(kind, l, t, way, 1, r, r).start())
                    self.start_third(kind, l, t, way, r)

                def third(m, _, kind=kind, t=t, way=way):
                    n = r - m
                    self.message(kind, l, t, way, 2 + m, n - 1, n).wait_recv()
                    pl.when(n < 3)(lambda: self.message(kind, l, t, way, 2 + m, n, n).start())
                    self.copy_out(kind, l, t, way, self.behind(t, way, 1, m), self.behind(t, way, 2, n))
                    return 0

                lax.fori_loop(jnp.maximum(r - 3, 0), jnp.minimum(r, SIDE), third, 0)
            return 0

        lax.fori_loop(0, 12, step, 0)

    def drain(self):
        local, send, recv = self.copy_sems
        half = self.bufs[1].shape[-1]
        columns = self.outs[2].at[:, :, :, :, pl.ds(0, half)]
        for kind, whole in ((0, self.outs[0]), (1, columns)):
            pltpu.make_async_copy(whole, whole, local.at[kind]).wait()
            copy = put(whole, whole, send.at[kind], recv.at[kind], self.place.partner())
            copy.wait_send()
            copy.wait_recv()

        def sent(i, _):
            l, n = lax.div(i, 3), lax.rem(i, 3)
            for kind, t, way in self.parts():
                for line in range(2):
                    self.message(kind, l, t, way, line, n, n).wait_send()
                lax.fori_loop(2, 6, lambda line, _: (self.message(kind, l, t, way, line, n, n).wait_send(), 0)[1], 0)
            return 0

        lax.fori_loop(0, 6, sent, 0)


def finish_kernel(count, *refs):
    sums_gu, sums_d, m_in, v_in, w_in = refs[0:2], refs[2:4], refs[4:7], refs[7:10], refs[10:13]
    w_out, m_out, v_out = refs[13:16], refs[16:19], refs[19:22]
    moments_gu, moments_d, old_gu, old_d, other_d, tiles = refs[22:28]
    load_sem, early_send, early_recv, norm_send, norm_recv, late_local, late_send, late_recv = refs[28:36]
    gather_refs = refs[36:]
    place = Place()
    x, y, z = place.at
    core = place.core
    gather = Gather(place, gather_refs[:2], gather_refs[2:6], w_out, gather_refs[6:9])
    partner = place.partner()
    gate_tiles, down_tiles = sums_gu[0].shape[1] // LANES, sums_d[0].shape[1] // LANES
    gate_stride, down_stride = 2 * gate_tiles, 4 * down_tiles
    gate_size, down_size = 12 * gate_stride, DOWN_ROWS * down_stride

    def blank(i, _):
        for which in range(2):
            moments_d[which, pl.ds(pl.multiple_of(8 * i, 8), 8), :] = jnp.zeros((8, LANES), F32)
        return 0

    lax.fori_loop(0, moments_d.shape[1] // 8, blank, 0)
    following = [place.device(2, 1, core=c) for c in range(2)]
    others = [place.device(axis, 2) for axis in range(3)] + [place.device(2, off, core=1 - core) for off in (1, SIDE - 1)]
    signal_all(near(place) + others)

    def gate_rows(i, which):
        return moments_gu.at[i, pl.ds(pl.multiple_of(which * gate_size, 8), gate_size)]

    def down_rows(i, first, rows):
        return moments_d.at[i, pl.ds(pl.multiple_of(first * down_stride, 8), rows * down_stride)]

    def columns(ref):
        half = down_tiles * LANES
        return ref.at[:, x, y, pl.ds(pl.multiple_of(64 * z, 8), 72), pl.ds(pl.multiple_of(core * half, LANES), half)]

    own_rows = PREV + 2 * z + DOWN_ROWS * core
    loads, sends = [], []
    for i, moment in enumerate((m_in, v_in)):
        for c in range(2):

            @pl.when(core == c)
            def _(i=i, moment=moment, c=c):
                pltpu.make_async_copy(moment[c], gate_rows(i, core), load_sem.at[i]).start()
                put(moment[1 - c], gate_rows(i, core), early_send.at[i], early_recv.at[i], partner).start()

        loads.append(pltpu.make_async_copy(moment[0], gate_rows(i, core), load_sem.at[i]))
        sends.append(put(moment[0], gate_rows(i, core), early_send.at[i], early_recv.at[i], partner))
        loads.append(pltpu.make_async_copy(moment[2], down_rows(i, own_rows, DOWN_ROWS), load_sem.at[2 + i]))
        loads[-1].start()
        sends.append(put(moment[2], down_rows(i, own_rows, DOWN_ROWS), early_send.at[2 + i], early_recv.at[2 + i], partner))
        sends[-1].start()
        last = moment[2].at[pl.ds((DOWN_ROWS - PREV) * down_stride, PREV * down_stride)]
        landing = down_rows(i, 2 * lax.rem(z + 1, SIDE), PREV)

        @pl.when(core == 1)
        def _(i=i, last=last, landing=landing):
            for c in range(2):
                put(last, landing, early_send.at[4 + 2 * i + c], early_recv.at[4 + i], following[c]).start()

    for l in range(2):
        sends.append(put(sums_d[l], other_d.at[l], early_send.at[8 + l], early_recv.at[6 + l], partner))
        sends[-1].start()
    for c in range(2):

        @pl.when(core == c)
        def _(c=c):
            pltpu.make_async_copy(w_in[c].at[:, x, y, z], old_gu, load_sem.at[4]).start()

    loads.append(pltpu.make_async_copy(w_in[0].at[:, x, y, z], old_gu, load_sem.at[4]))
    loads.append(pltpu.make_async_copy(columns(w_in[2]), old_d, load_sem.at[5]))
    loads[-1].start()

    squares = jnp.zeros((8, LANES), F32)
    for l in range(2):

        def of_gate_up(j, total, l=l):
            for t in range(3):
                g = sums_gu[l][pl.ds(8 * t, 8), pl.ds(pl.multiple_of(j * LANES, LANES), LANES)].astype(F32)
                total += g * g
            return total

        squares = lax.fori_loop(0, gate_tiles, of_gate_up, squares)

        def of_down(i, total, l=l):
            row = 8 * i + lax.broadcasted_iota(jnp.int32, (8, LANES), 0)
            mine = (row >= 2 * z) & (row < 2 * z + 2 * DOWN_ROWS)
            for j in range(down_tiles):
                g = sums_d[l][pl.ds(pl.multiple_of(8 * i, 8), 8), pl.ds(j * LANES, LANES)].astype(F32)
                total += jnp.where(mine, g * g, 0.0)
            return total

        squares = lax.fori_loop(0, 9, of_down, squares)
    for stage, (coordinate, size) in enumerate(((core, 2), (x, SIDE), (y, SIDE), (z, SIDE))):
        tiles[stage, coordinate] = squares
        exchanges = []
        for off in range(1, size):
            target = partner if stage == 0 else place.device(stage - 1, off)
            key = 3 * stage + off - 1
            here = tiles.at[stage, coordinate]
            exchanges.append(put(here, here, norm_send.at[key], norm_recv.at[key], target))
            exchanges[-1].start()
        for exchange in exchanges:
            exchange.wait_recv()
        for exchange in exchanges:
            exchange.wait_send()
        squares = tiles[stage, 0]
        for other in range(1, size):
            squares += tiles[stage, other]
    total = jnp.sum(jnp.sum(squares, 0, keepdims=True), 1, keepdims=True)
    factor = jnp.minimum(1.0, 0.5 * lax.rsqrt(total / count + CLIP_EPS))

    for copy in loads:
        copy.wait()
    for copy in sends:
        copy.wait_recv()
    for i in range(2):
        put(down_rows(i, 0, PREV), down_rows(i, 0, PREV), early_send.at[0], early_recv.at[4 + i], partner).wait_recv()

    def moments(ref, start, stride, g):
        rows = pl.ds(start, 8, stride=stride)
        m = 0.9 * ref[0, rows, :] + 0.1 * g
        v = 0.95 * ref[1, rows, :] + 0.05 * g * g
        ref[0, rows, :] = m
        ref[1, rows, :] = v
        return m * lax.rsqrt(v + 1e-8)

    def weight(w, step):
        w = w.astype(F32)
        return (w - 0.02 * (step + 0.1 * w)).astype(BF16)

    for l in range(2):

        def gate_up(j, _, l=l):
            lanes = pl.ds(pl.multiple_of(j * LANES, LANES), LANES)
            for t in range(3):
                rows = pl.ds(8 * t, 8)
                g = sums_gu[l][rows, lanes].astype(F32) * factor
                step = moments(moments_gu, 8 * t * gate_stride + 2 * j + l, gate_stride, g)
                gather.bufs[0][l, x, y, z, rows, lanes] = weight(old_gu[l, rows, lanes], step)
            return 0

        lax.fori_loop(0, gate_tiles, gate_up, 0, unroll=3)

        def down(i, _, l=l):
            rows = pl.ds(pl.multiple_of(8 * i, 8), 8)
            for j in range(down_tiles):
                lanes = pl.ds(j * LANES, LANES)
                start = (PREV + 8 * i) * down_stride + 2 * j + l
                g = sums_d[l][rows, lanes].astype(F32) * factor
                step = moments(moments_d, start + 2 * down_tiles * core, down_stride, g)
                gather.bufs[1][l, x, y, z, rows, lanes] = weight(old_d[l, rows, lanes], step)
            return 0

        lax.fori_loop(0, 9, down, 0)
        gather.own(l)
    for l in range(2):

        def down_other(i, _, l=l):
            rows = pl.ds(pl.multiple_of(8 * i, 8), 8)
            for j in range(down_tiles):
                start = (PREV + 8 * i) * down_stride + 2 * j + l
                g = other_d[l, rows, pl.ds(j * LANES, LANES)].astype(F32) * factor
                moments(moments_d, start + 2 * down_tiles * (1 - core), down_stride, g)
            return 0

        lax.fori_loop(0, 9, down_other, 0)

    late = []
    for i, out in enumerate((m_out, v_out)):
        for c in range(2):

            @pl.when(core == c)
            def _(i=i, out=out, c=c):
                pltpu.make_async_copy(gate_rows(i, core), out[c], late_local.at[i]).start()
                put(gate_rows(i, 1 - core), out[c], late_send.at[i], late_recv.at[i], partner).start()

        pltpu.make_async_copy(down_rows(i, own_rows, DOWN_ROWS), out[2], late_local.at[2 + i]).start()
    gather.first_axis()
    gather.other_axes()
    for i, out in enumerate((m_out, v_out)):
        pltpu.make_async_copy(gate_rows(i, core), out[0], late_local.at[i]).wait()
        pltpu.make_async_copy(down_rows(i, own_rows, DOWN_ROWS), out[2], late_local.at[2 + i]).wait()
        copy = put(gate_rows(i, 1 - core), out[0], late_send.at[i], late_recv.at[i], partner)
        copy.wait_recv()
        copy.wait_send()
    for copy in sends:
        copy.wait_send()
    for i in range(2):
        for c in range(2):

            @pl.when(core == 1)
            def _(i=i, c=c):
                rows = down_rows(i, 0, PREV)
                put(rows, rows, early_send.at[4 + 2 * i + c], early_recv.at[4 + i], following[c]).wait_send()

    gather.drain()


def finish_call(count, collective_id, sums_gu, sums_d, m, v, w):
    gate_cols, down_half = sums_gu[0].shape[1], sums_d[0].shape[1]
    operands = [*sums_gu, *sums_d, *m, *v, *w]
    hbm, vmem = pl.BlockSpec(memory_space=pltpu.HBM), pl.BlockSpec(memory_space=pltpu.VMEM)
    dma = pltpu.SemaphoreType.DMA
    gate_stride, down_stride = gate_cols // 64, down_half // 32
    scratch = [
        pltpu.VMEM((2, 24 * gate_stride, LANES), F32),
        pltpu.VMEM((2, (PREV + 72) * down_stride, LANES), F32),
        pltpu.VMEM((2, 24, gate_cols), BF16),
        pltpu.VMEM((2, 72, down_half), BF16),
        pltpu.VMEM((2, 72, down_half), BF16),
        pltpu.VMEM((4, SIDE, 8, LANES), F32),
        dma((6,)), dma((10,)), dma((8,)), dma((12,)), dma((12,)), dma((4,)), dma((2,)), dma((2,)),
    ]
    return pl.pallas_call(
        functools.partial(finish_kernel, count),
        name="finish",
        out_shape=[jax.ShapeDtypeStruct(t.shape, t.dtype) for t in (*w, *m, *v)],
        in_specs=[vmem] * 4 + [hbm] * 9,
        out_specs=[hbm] * 9,
        scratch_shapes=scratch + Gather.scratch(gate_cols, down_half),
        compiler_params=pltpu.CompilerParams(collective_id=collective_id, has_side_effects=True, vmem_limit_bytes=VMEM_LIMIT),
        cost_estimate=pl.CostEstimate(flops=10**9, bytes_accessed=10**8, transcendentals=0),
    )(*operands)


TILE = 384
ROWS = 256
TIGHT = pl.Buffered(buffer_count=1)


def dot(a, b, dims):
    return lax.dot_general(a, b, (dims, ((), ())), preferred_element_type=F32)


NN, NT, TN = ((1,), (0,)), ((1,), (1,)), ((0,), (0,))


def norm_scale(wide):
    return lax.rsqrt(jnp.mean(wide * wide, -1, keepdims=True) + 1e-6)


def in_rows(total, step, body):
    def one(i, _):
        body(pl.ds(pl.multiple_of(i * step, step), step))
        return 0

    lax.fori_loop(0, total // step, one, 0)


def clear(acc):
    def rows(r):
        acc[r, :] = jnp.zeros((8, acc.shape[1]), F32)

    in_rows(acc.shape[0], 8, rows)


def spec(shape, index_map, tight=False):
    return pl.BlockSpec(shape, index_map, pipeline_mode=TIGHT) if tight else pl.BlockSpec(shape, index_map)


def whole(shape, tight=True):
    return spec(shape, lambda j: (0,) * len(shape), tight)


HBM = pl.BlockSpec(memory_space=pltpu.HBM)


def params(collective_id=None, semantics=("arbitrary",)):
    more = {} if collective_id is None else {"collective_id": collective_id, "has_side_effects": True}
    return pltpu.CompilerParams(dimension_semantics=semantics, vmem_limit_bytes=VMEM_LIMIT, **more)


def transpose_piece(j, last, src, dst):
    def piece(i):
        at = pl.ds(pl.multiple_of(i * LANES, LANES), LANES)
        dst[at, :] = src[:, at].T

    piece(j)
    pl.when(j == last)(lambda: piece(last + 1))


def side_by_side(a, b):
    return jnp.concatenate([a, b], axis=1)


def forward_kernel(tiles, x, wg, wu, wd, gate, up, h_out, a_out, at, a, acc, p):
    j = pl.program_id(0)

    @pl.when(j == 0)
    def _():
        def rows(r):
            wide = x[r, :].astype(F32)
            a[r, :] = (wide * norm_scale(wide)).astype(BF16)

        in_rows(x.shape[0], 32, rows)
        clear(acc)

    transpose_piece(j, tiles - 1, a, at)
    both = side_by_side(wg[0], wu[0])
    slot = lax.rem(j, 2)
    for m in range(x.shape[0] // ROWS):
        r = pl.ds(m * ROWS, ROWS)
        gu = dot(a[r, :], both, NN)
        g, u = gu[:, :TILE], gu[:, TILE:]
        gate[r, :] = g
        up[r, :] = u
        p[slot, r, :] = (g * lax.logistic(g) * u).astype(BF16)

    @pl.when(slot == 1)
    def _():
        for m in range(x.shape[0] // ROWS):
            r = pl.ds(m * ROWS, ROWS)
            acc[r, :] += dot(side_by_side(p[0, r, :], p[1, r, :]), wd[0], NN)

    @pl.when(j == tiles - 1)
    def _():
        def last_down(r):
            acc[r, :] += dot(p[0, r, :], wd[0, pl.ds(0, TILE), :], NN)

        in_rows(x.shape[0], ROWS, last_down)

        def rows(r):
            h = (x[r, :].astype(F32) + acc[r, :].astype(BF16).astype(F32)).astype(BF16)
            h_out[r, :] = h
            wide = h.astype(F32)
            a_out[r, :] = (wide * norm_scale(wide)).astype(BF16)

        in_rows(x.shape[0], 32, rows)


def forward_call(x, wg, wu, wd):
    tokens, d = x.shape
    ff = wg.shape[2]
    tiles = ff // TILE
    w_in = spec((1, d, TILE), lambda j: (0, 0, j))
    return pl.pallas_call(
        functools.partial(forward_kernel, tiles),
        name="forward_0",
        grid=(tiles,),
        in_specs=[whole((tokens, d)), w_in, w_in, spec((1, 2 * TILE, d), lambda j: (0, lax.div(j, 2), 0))],
        out_specs=[spec((tokens, TILE), lambda j: (0, j))] * 2 + [whole((tokens, d))] * 2 + [whole((d, tokens))],
        out_shape=[jax.ShapeDtypeStruct((tokens, ff), F32)] * 2
        + [jax.ShapeDtypeStruct((tokens, d), BF16)] * 2
        + [jax.ShapeDtypeStruct((d, tokens), BF16)],
        scratch_shapes=[pltpu.VMEM((tokens, d), BF16), pltpu.VMEM((tokens, d), F32), pltpu.VMEM((2, tokens, TILE), BF16)],
        compiler_params=params(),
    )(x, wg, wu, wd)


class PairSum:
    def __init__(self, place, tiles, landing, stage, send, recv):
        self.place, self.tiles, self.landing, self.stage, self.send, self.recv = place, tiles, landing, stage, send, recv

    @staticmethod
    def scratch(tiles, rows, cols):
        dma = pltpu.SemaphoreType.DMA
        return [pltpu.VMEM((tiles, rows, cols), BF16), pltpu.VMEM((2, rows, cols), BF16), dma((2,)), dma((tiles,))]

    def copy(self, i):
        slot = lax.rem(i, 2)
        return put(self.stage.at[slot], self.landing.at[i], self.send.at[slot], self.recv.at[i], self.place.partner())

    def reserve(self, i):
        pl.when(i >= 2)(lambda: self.copy(i - 2).wait_send())
        return self.stage.at[lax.rem(i, 2)]

    def drain(self):
        for i in (self.tiles - 2, self.tiles - 1):
            self.copy(i).wait_send()


def hidden_back(gate, up, dp):
    dp = dp.astype(F32)
    s = lax.logistic(gate)
    act = gate * s
    return (act * up).astype(BF16), (dp * up * (s + act * (1.0 - s))).astype(BF16), (dp * act).astype(BF16)


def down_gradient(j, tiles, pair, p, dy, half, out):
    core = pair.place.core

    def columns(c):
        return pl.ds(pl.multiple_of(c * half, LANES), half)

    @pl.when(j < tiles)
    def _():
        slot = pair.reserve(j)
        slot[...] = dot(p[lax.rem(j, 2)], dy[:, columns(1 - core)], TN).astype(BF16)
        pair.copy(j).start()

    @pl.when(j >= 1)
    def _():
        pair.copy(j - 1).wait_recv()
        own = dot(p[lax.rem(j - 1, 2)], dy[:, columns(core)], TN)
        out[...] = (own + pair.landing[j - 1].astype(F32)).astype(BF16)

    pl.when(j == tiles)(pair.drain)


def layer_kernel(tiles, a, dy, wg, wu, wd, dgu, at, out, p, dps, *rest):
    j = pl.program_id(0)
    place = Place()
    pair = PairSum(place, tiles, *rest)
    pl.when(j == 0)(lambda: signal_all([place.partner()]))
    two_tiles_of_dp(j, tiles, dy, wd, dps)

    @pl.when(j < tiles)
    def _():
        transpose_piece(j, tiles - 1, a, at)
        slot = lax.rem(j, 2)
        both = side_by_side(wg[0], wu[0])
        for m in range(a.shape[0] // ROWS):
            r = pl.ds(m * ROWS, ROWS)
            gu = dot(a[r, :], both, NN)
            p[slot, r, :], dgu[0, r, :], dgu[1, r, :] = hidden_back(gu[:, :TILE], gu[:, TILE:], dps[slot, r, :])

    down_gradient(j, tiles, pair, p, dy, dy.shape[1] // 2, out)


def two_tiles_of_dp(j, tiles, dy, wd, dps):
    @pl.when((lax.rem(j, 2) == 0) & (j < tiles - 1))
    def _():
        for m in range(dy.shape[0] // ROWS):
            r = pl.ds(m * ROWS, ROWS)
            dp = dot(dy[r, :], wd[0], NT).astype(BF16)
            dps[0, r, :] = dp[:, :TILE]
            dps[1, r, :] = dp[:, TILE:]

    @pl.when(j == tiles - 1)
    def _():
        def one_tile(r):
            dps[0, r, :] = dot(dy[r, :], wd[0, pl.ds(0, TILE), :], NT).astype(BF16)

        in_rows(dy.shape[0], ROWS, one_tile)


def clip(tiles, back=0):
    return lambda j: jnp.clip(j - back, 0, tiles - 1)


def layer_call(collective_id, a, dy, wg, wu, wd):
    tokens, d = a.shape
    ff = wg.shape[2]
    tiles, half = ff // TILE, d // 2
    now, before = clip(tiles), clip(tiles, 1)
    w_in = spec((1, d, TILE), lambda j: (1, 0, now(j)))
    return pl.pallas_call(
        functools.partial(layer_kernel, tiles),
        name="layer_1",
        grid=(tiles + 1,),
        in_specs=[whole((tokens, d))] * 2 + [w_in, w_in, spec((1, 2 * TILE, d), lambda j: (1, lax.div(now(j), 2), 0))],
        out_specs=[spec((2, tokens, TILE), lambda j: (0, 0, now(j))), whole((d, tokens)), spec((TILE, half), lambda j: (before(j), 0))],
        out_shape=[
            jax.ShapeDtypeStruct((2, tokens, ff), BF16),
            jax.ShapeDtypeStruct((d, tokens), BF16),
            jax.ShapeDtypeStruct((ff, half), BF16),
        ],
        scratch_shapes=[pltpu.VMEM((2, tokens, TILE), BF16)] * 2 + PairSum.scratch(tiles, TILE, half),
        compiler_params=params(collective_id),
    )(a, dy, wg, wu, wd)


GATE_ROWS, DOWN_WINDOW = 24, 72
RING = 6


def second(t, v, rest=ALL):
    return (rest, v) if t == 1 else (v, rest)


class Stream:
    def __init__(self, place, tiles, phases, refs):
        self.place, self.tiles, self.phases, self.rows = place, tiles, phases, GATE_ROWS // 3
        self.held, self.slots, self.send, self.recv = refs[0], refs[1 : 1 + 2 * phases], refs[-2], refs[-1]
        self.ways = ways_of(TILE)

    @staticmethod
    def scratch(tiles, phases):
        third, dma = GATE_ROWS // 3, pltpu.SemaphoreType.DMA
        leads = [(3, 3, tiles, SIDE, SIDE), (3, 3, tiles, SIDE), (3, 3, tiles)][:phases]
        slots = [pltpu.VMEM((*lead, third, width), BF16) for lead in leads for _, width in ways_of(TILE)]
        return [pltpu.VMEM((RING, SIDE, SIDE, SIDE, GATE_ROWS, TILE), BF16), *slots, dma((tiles, 7)), dma((tiles, 7))]

    def part(self, t, way):
        start, width = self.ways[way]
        return pl.ds(t * self.rows, self.rows), pl.ds(start, width)

    def own(self, c, t, way, hops, b=ALL, d=ALL):
        at = index(ORDERS[t], (self.place.block(ORDERS[t][0], way, hops), ALL, ALL))
        axes = [i for i in range(3) if i != ORDERS[t][0]]
        at = list(at)
        at[axes[0]], at[axes[1]] = b, d
        return self.held.at[(lax.rem(c, RING), *at, *self.part(t, way))]

    def copy(self, phase, t, way, n, c, first=False):
        axis = ORDERS[t][phase]
        slots = self.slots[2 * phase + way]
        if not first:
            src = slots.at[t, n - 1, c]
        elif phase == 0:
            src = self.own(c, t, way, 1)
        else:
            src = self.slots[way].at[(t, 2, c, *second(t, self.place.block(axis, way, 1)))]
        key = (c, 3 * phase + n)
        return put(src, slots.at[t, n, c], self.send.at[key], self.recv.at[key], self.place.device(axis, self.place.onward(way)))

    def direct(self, t, way, off, c):
        axis = ORDERS[t][2]
        v = lax.rem(self.place.at[axis] + off, SIDE)
        src, dst = self.slots[2 + way].at[t, 2, c, v], self.slots[4 + way].at[t, off - 1, c]
        return put(src, dst, self.send.at[c, 6], self.recv.at[c, 6], self.place.device(axis, off))

    def pairs(self):
        return [(t, way) for t in range(3) for way in range(2)]

    def all_of(self, phase):
        return self.held.at[(0,) * (phase + 2)] if phase < 2 else self.held.at[0, 0, 0, pl.ds(0, 3)]

    def begin(self, phase, c):
        for t, way in self.pairs():
            if phase < 2:
                self.copy(phase, t, way, 0, c, first=True).start()
            else:
                for off in range(1, SIDE):
                    self.direct(t, way, off, c).start()

    def add(self, phase, t, way, n, c):
        slots = self.slots[2 * phase + way]
        v = self.place.block(ORDERS[t][phase], way, n + 1)

        def one(at, other):
            at = (t, n - 1, c, *at)
            slots[at] = (slots[at].astype(F32) + other[...].astype(F32)).astype(BF16)

        if phase == 0:
            for b in range(SIDE):
                for d in range(SIDE):
                    one((b, d), self.own(c, t, way, n + 1, b, d))
        else:
            for d in range(SIDE):
                one((d,), self.slots[way].at[(t, 2, c, *second(t, v, d))])

    def stage(self, s, c, out):
        phase, n = (s - 1) // 3, (s - 1) % 3 + 1
        whole_stage = self.all_of(phase)
        pltpu.make_async_copy(whole_stage, whole_stage, self.recv.at[c, s - 1]).wait()
        if phase == 2:
            for t, way in self.pairs():
                total = self.slots[2 + way][t, 2, c, self.place.at[ORDERS[t][2]]].astype(F32)
                for i in range(3):
                    total += self.slots[4 + way][t, i, c].astype(F32)
                rows, _ = self.part(t, way)
                start, width = self.ways[way]
                out[rows, pl.ds(pl.multiple_of(c * TILE + start, LANES), width)] = total.astype(BF16)
            return
        for t, way in self.pairs():
            self.add(phase, t, way, n, c)
            if n < 3:
                self.copy(phase, t, way, n, c).start()
        if n == 3 and phase + 1 < self.phases:
            self.begin(phase + 1, c)

    def sent(self, phase, n, c):
        whole_stage = self.all_of(phase)
        pltpu.make_async_copy(whole_stage, whole_stage, self.send.at[c, 3 * phase + n]).wait()

    def count(self):
        return 3 if self.phases == 1 else 7

    def keep(self, c):
        pl.when(c >= RING)(lambda: self.sent(0, 0, c - RING))
        return self.held.at[lax.rem(c + RING, RING)]

    def run(self, s, c, out):
        act = (lambda: self.begin(0, c)) if s == 0 else (lambda: self.stage(s, c, out))
        pl.when((c >= 0) & (c < self.tiles))(act)

    def early(self, j, out=None):
        for s in range(self.count(), 1, -1):
            self.run(s, j - 3 - s, out)

    def late(self, j, out=None):
        self.run(0, j - 2, out)
        self.run(1, j - 3, out)

    def last_step(self):
        return self.tiles - 1 + 3 + self.count()

    def drain(self):
        def each(c, _):
            pl.when(c >= self.tiles - RING)(lambda: self.sent(0, 0, c))
            for i in range(1, self.count()):
                self.sent(i // 3, i % 3, c)
            return 0

        lax.fori_loop(0, self.tiles, each, 0)

    def results(self):
        return [self.slots[way].at[:, 2] for way in range(2)]


def stream_halves(tiles):
    return [(3, tiles, SIDE, SIDE, GATE_ROWS // 3, width) for _, width in ways_of(TILE)]


class StreamRest:
    def __init__(self, place, tiles, before, refs):
        self.place, self.tiles, self.before, self.slots, self.sems = place, tiles, before, refs[:4], refs[4:8]
        self.rows, self.ways = GATE_ROWS // 3, ways_of(TILE)

    @staticmethod
    def scratch(tiles):
        third, dma = GATE_ROWS // 3, pltpu.SemaphoreType.DMA
        shapes = [pltpu.VMEM((3, 3, *lead, third, width), BF16) for lead in ((tiles, SIDE), (tiles,)) for _, width in ways_of(TILE)]
        return shapes + [dma((3, 2, 3))] * 4

    def pairs(self):
        return [(t, way) for t in range(3) for way in range(2)]

    def message(self, phase, t, way, n, arriving=False):
        slots = self.slots[2 * phase - 2 + way]
        axis = ORDERS[t][phase]
        if arriving:
            src = slots.at[t, n]
        elif isinstance(n, int) and n == 0:
            v = self.place.block(axis, way, 1)
            src = self.before[way].at[(t, ALL, *second(t, v))] if phase == 1 else self.slots[way].at[t, 2, :, v]
        else:
            src = slots.at[t, n - 1]
        send, recv = self.sems[2 * phase - 2 : 2 * phase]
        key = (t, way, n)
        return put(src, slots.at[t, n], send.at[key], recv.at[key], self.place.device(axis, self.place.onward(way)))

    def start(self, phase):
        for t, way in self.pairs():
            self.message(phase, t, way, 0).start()

    def step(self, phase, n):
        for t, way in self.pairs():
            self.message(phase, t, way, n - 1, arriving=True).wait_recv()
            v = self.place.block(ORDERS[t][phase], way, n + 1)
            slots = self.slots[2 * phase - 2 + way]

            def add(c, _, t=t, way=way, v=v, slots=slots):
                for d in range(SIDE if phase == 1 else 1):
                    at = (t, n - 1, c, d) if phase == 1 else (t, n - 1, c)
                    other = self.before[way].at[(t, c, *second(t, v, d))] if phase == 1 else self.slots[way].at[t, 2, c, v]
                    slots[at] = (slots[at].astype(F32) + other[...].astype(F32)).astype(BF16)
                return 0

            lax.fori_loop(0, self.tiles, add, 0)
            pl.when(n < 3)(lambda t=t, way=way: self.message(phase, t, way, n).start())

    def tick(self, i):
        pl.when(i == 0)(lambda: self.start(1))
        pl.when((i >= 1) & (i <= 3))(lambda: self.step(1, i))
        pl.when(i == 3)(lambda: self.start(2))
        pl.when((i >= 4) & (i <= 6))(lambda: self.step(2, i - 3))

    def result(self, out):
        def one(c, _):
            for t, way in self.pairs():
                start, width = self.ways[way]
                lanes = pl.ds(pl.multiple_of(c * TILE + start, LANES), width)
                out[pl.ds(t * self.rows, self.rows), lanes] = self.slots[2 + way][t, 2, c]
            return 0

        lax.fori_loop(0, self.tiles, one, 0)

    def drain(self):
        for t, way in self.pairs():
            for phase in (1, 2):
                for n in range(3):
                    self.message(phase, t, way, n).wait_send()


BLOCK_ROWS = SIDE * SIDE * GATE_ROWS


def gate_up_kernel(tiles, phases, cols, at, ahead, behind, *rest):
    j = pl.program_id(0)
    place = Place()
    core = place.core
    if phases == 1:
        outs, out, rest = rest[:2], None, rest[2:]
    else:
        sum_down, out, out_down, rest = rest[0], rest[1], rest[2], rest[3:]
    pair = PairSum(place, tiles, *rest[:4])
    stream = Stream(place, tiles, phases, rest[4 : 4 + 3 + 2 * phases])
    rest = rest[4 + 3 + 2 * phases :]
    if phases == 3:
        first = First.of(place, DOWN_WINDOW, cols, rest[1:6])
        down = Rest.of(place, DOWN_WINDOW, cols, first.results(), rest[6:14])
        loads = loads_down(sum_down, first, rest[0])

    @pl.when(j == 0)
    def _():
        opposite = [place.device(axis, 2) for axis in range(3)] if phases == 3 else []
        signal_all(near(place) + opposite)
        if phases == 3:
            begin(loads)

    stream.early(j, out)

    pl.when((j >= 2) & (j <= tiles + 1))(lambda: pair.copy(j - 2).wait_recv())

    @pl.when(j <= tiles + 1)
    def _():
        slot, kept = pair.reserve(j), stream.keep(j - 2)
        both = side_by_side(ahead[1 - core], behind[core])
        landed = lax.rem(j + tiles - 2, tiles)
        for m in range(SIDE):
            r = pl.ds(m * BLOCK_ROWS, BLOCK_ROWS)
            tile = dot(at[r, :], both, NN)
            slot[r, :] = tile[:, :TILE].astype(BF16)
            total = (tile[:, TILE:] + pair.landing[landed, r, :].astype(F32)).astype(BF16)
            kept[m] = total.reshape(SIDE, SIDE, GATE_ROWS, TILE)

    pl.when(j < tiles)(lambda: pair.copy(j).start())
    stream.late(j, out)
    if phases == 3:
        pl.when(j == 0)(lambda: end(loads))
        pl.when(j < 8)(lambda: spread(j, 8, 16, first.tick))
        pl.when(j >= 8)(lambda: down.tick(j - 8))
        pl.when(j == 15)(lambda: down.result(out_down))

    @pl.when(j == stream.last_step())
    def _():
        if phases == 1:
            saves = copies(stream.results(), outs, rest[0])
            begin(saves)
            stream.drain()
            end(saves)
        else:
            stream.drain()
            first.drain()
            down.drain()


def gate_up_call(name, collective_id, phases, at, dgu, *sum_down):
    d, tokens = at.shape
    ff = dgu.shape[2]
    tiles, cols, dma = ff // TILE, d // 2, pltpu.SemaphoreType.DMA
    now, before = clip(tiles), clip(tiles, 2)
    if phases == 1:
        shapes = stream_halves(tiles)
        out_specs, more = [HBM] * 2, [dma((2,))]
    else:
        shapes = [(GATE_ROWS, ff), (DOWN_WINDOW, cols)]
        out_specs = [whole(s) for s in shapes]
        more = [dma((SIDE,)), *First.scratch(DOWN_WINDOW, cols), *Rest.scratch(DOWN_WINDOW, cols)]
    return pl.pallas_call(
        functools.partial(gate_up_kernel, tiles, phases, cols),
        name=name,
        grid=(tiles + (6 if phases == 1 else 10),),
        in_specs=[
            whole((d, tokens)),
            spec((2, tokens, TILE), lambda j: (0, 0, now(j))),
            spec((2, tokens, TILE), lambda j: (0, 0, before(j))),
            *[HBM] * len(sum_down),
        ],
        out_specs=out_specs,
        out_shape=[jax.ShapeDtypeStruct(s, BF16) for s in shapes],
        scratch_shapes=[*PairSum.scratch(tiles, d, TILE), *Stream.scratch(tiles, phases), *more],
        compiler_params=params(collective_id),
    )(at, dgu, dgu, *sum_down)


def middle_kernel(steps, down_cols, dgu, wg, wu, h, dy, sum_down, gate0, gate1, dh, out_gu, half0, half1, acc_g, acc_u, *rest):
    j = pl.program_id(0)
    place = Place()
    first = First.of(place, DOWN_WINDOW, down_cols, rest[:5])
    gate = StreamRest(place, gate0.shape[1], rest[5:7], rest[7:15])
    load_sem, gate_sem, save_sem = rest[15:18]
    loads = loads_down(sum_down, first, load_sem) + copies((gate0, gate1), rest[5:7], gate_sem)

    @pl.when(j == 0)
    def _():
        signal_all(near(place))
        begin(loads)
        clear(acc_g)
        clear(acc_u)

    def add_up(r, k):
        acc_g[r, :] += dot(dgu[0, r, pl.ds(0, k)], wg[0, :, pl.ds(0, k)], NT)
        acc_u[r, :] += dot(dgu[1, r, pl.ds(0, k)], wu[0, :, pl.ds(0, k)], NT)

    @pl.when(j < steps - 1)
    def _():
        for m in range(h.shape[0] // ROWS):
            add_up(pl.ds(m * ROWS, ROWS), 2 * TILE)

    pl.when(j == steps - 1)(lambda: in_rows(h.shape[0], ROWS, lambda r: add_up(r, TILE)))

    pl.when(j == 0)(lambda: end(loads))
    gate.tick(j)
    spread(j, steps, 16, first.tick)

    @pl.when(j == steps - 1)
    def _():
        lax.fori_loop(steps, 7, lambda i, _: (gate.tick(i), 0)[1], 0)
        saves = copies(first.results(), (half0, half1), save_sem)
        begin(saves)
        gate.result(out_gu)

        def rows(r):
            wide = h[r, :].astype(F32)
            scale = norm_scale(wide)
            da = (acc_g[r, :].astype(BF16).astype(F32) + acc_u[r, :].astype(BF16).astype(F32)).astype(BF16).astype(F32)
            back = scale * da - wide * (scale * scale * scale * jnp.mean(da * wide, -1, keepdims=True))
            dh[r, :] = (dy[r, :].astype(F32) + back.astype(BF16).astype(F32)).astype(BF16)

        in_rows(h.shape[0], 32, rows)
        first.drain()
        gate.drain()
        end(saves)


def middle_call(collective_id, dgu, wg, wu, h, dy, sum_down, gate_halves):
    tokens, d = h.shape
    ff = dgu.shape[2]
    tiles, dma, down_cols = ff // TILE, pltpu.SemaphoreType.DMA, d // 2
    steps = (tiles + 1) // 2
    w_in = spec((1, d, 2 * TILE), lambda j: (1, 0, j))
    return pl.pallas_call(
        functools.partial(middle_kernel, steps, down_cols),
        name="middle",
        grid=(steps,),
        in_specs=[spec((2, tokens, 2 * TILE), lambda j: (0, 0, j)), w_in, w_in, whole((tokens, d)), whole((tokens, d))] + [HBM] * 3,
        out_specs=[whole((tokens, d)), whole((GATE_ROWS, ff)), HBM, HBM],
        out_shape=[jax.ShapeDtypeStruct(s, BF16) for s in ((tokens, d), (GATE_ROWS, ff), *half_sums(DOWN_WINDOW, down_cols))],
        scratch_shapes=[pltpu.VMEM((tokens, d), F32)] * 2
        + First.scratch(DOWN_WINDOW, down_cols)
        + [pltpu.VMEM(t.shape, BF16) for t in gate_halves]
        + StreamRest.scratch(tiles)
        + [dma((SIDE,)), dma((2,)), dma((2,))],
        compiler_params=params(collective_id),
    )(dgu, wg, wu, h, dy, sum_down, *gate_halves)


def back_kernel(tiles, dh, gate, up, wd, down0, down1, dgu, out, out_down, p, dps, *rest):
    j = pl.program_id(0)
    place = Place()
    half = dh.shape[1] // 2
    pair = PairSum(place, tiles, *rest[:4])
    before = rest[4:6]
    down = Rest.of(place, DOWN_WINDOW, half, before, rest[6:14])
    loads = copies((down0, down1), before, rest[14])

    @pl.when(j == 0)
    def _():
        signal_all(near(place))
        begin(loads)

    two_tiles_of_dp(j, tiles, dh, wd, dps)

    @pl.when(j < tiles)
    def _():
        slot = lax.rem(j, 2)
        for m in range(dh.shape[0] // ROWS):
            r = pl.ds(m * ROWS, ROWS)
            p[slot, r, :], dgu[0, r, :], dgu[1, r, :] = hidden_back(gate[r, :], up[r, :], dps[slot, r, :])

    down_gradient(j, tiles, pair, p, dh, half, out)
    pl.when(j == 0)(lambda: end(loads))
    down.tick(j)
    pl.when(j == 7)(lambda: down.result(out_down))
    pl.when(j == tiles)(down.drain)


def back_call(collective_id, dh, gate, up, wd, down_halves):
    tokens, d = dh.shape
    ff = gate.shape[1]
    tiles, half = ff // TILE, d // 2
    now, before = clip(tiles), clip(tiles, 1)
    tile = spec((tokens, TILE), lambda j: (0, now(j)))
    return pl.pallas_call(
        functools.partial(back_kernel, tiles),
        name="back_0",
        grid=(tiles + 1,),
        in_specs=[whole((tokens, d)), tile, tile, spec((1, 2 * TILE, d), lambda j: (0, lax.div(now(j), 2), 0)), HBM, HBM],
        out_specs=[
            spec((2, tokens, TILE), lambda j: (0, 0, now(j))),
            spec((TILE, half), lambda j: (before(j), 0)),
            whole((DOWN_WINDOW, half)),
        ],
        out_shape=[jax.ShapeDtypeStruct(s, BF16) for s in ((2, tokens, ff), (ff, half), (DOWN_WINDOW, half))],
        scratch_shapes=[pltpu.VMEM((2, tokens, TILE), BF16)] * 2
        + PairSum.scratch(tiles, TILE, half)
        + [pltpu.VMEM(t.shape, BF16) for t in down_halves]
        + Rest.scratch(DOWN_WINDOW, half)
        + [pltpu.SemaphoreType.DMA((2,))],
        compiler_params=params(collective_id),
    )(dh, gate, up, wd, *down_halves)


def flat(m):
    layers, rows, cols = m.shape
    split = m.transpose(1, 0, 2).reshape(rows, layers, cols // LANES, LANES)
    return with_layout_constraint(split, Layout((0, 2, 1, 3))).transpose(0, 2, 1, 3).reshape(-1, LANES)


def unflat(f, shape):
    layers, rows, cols = shape
    split = f.reshape(rows, cols // LANES, layers, LANES).transpose(0, 2, 1, 3)
    return with_layout_constraint(split, Layout((0, 2, 1, 3))).reshape(rows, layers, cols).transpose(1, 0, 2)


def solution(mesh):
    def body(x, dy, wg, wu, wd, mg, mu, md, vg, vu, vd):
        layers, d, ff = wg.shape
        x, dy = x[0], dy[0]
        windows = (SIDE, SIDE, 4 * 66, d // 2)
        gate0, up0, h1, a1, a0t = forward_call(x, wg, wu, wd)
        dgu1, a1t, down1 = layer_call(1, a1, dy, wg, wu, wd)
        down1 = down1.reshape(windows)
        gate_halves = gate_up_call("gate_up_1", 2, 1, a1t, dgu1)
        dh1, sum_gu1, *down_halves = middle_call(3, dgu1, wg, wu, h1, dy, down1, gate_halves)
        dgu0, down0, sum_down1 = back_call(4, dh1, gate0, up0, wd, down_halves)
        sum_gu0, sum_down0 = gate_up_call("gate_up_0", 5, 3, a0t, dgu0, down0.reshape(windows))

        views = [(2, SIDE, SIDE, SIDE, GATE_ROWS, ff)] * 2 + [(2, SIDE, SIDE, 4 * 66, d)]
        w = [t.reshape(view) for t, view in zip((wg, wu, wd), views, strict=True)]
        m, v = [flat(t) for t in (mg, mu, md)], [flat(t) for t in (vg, vu, vd)]
        out = finish_call(3 * layers * d * ff, 7, [sum_gu0, sum_gu1], [sum_down0, sum_down1], m, v, w)
        new = [t.reshape(like.shape) for t, like in zip(out[:3], (wg, wu, wd), strict=True)]
        return (*new, *[unflat(t, like.shape) for t, like in zip(out[3:], (mg, mu, md, vg, vu, vd), strict=True)])

    shard = P(None, "dp", None)
    return jax.shard_map(
        body,
        mesh=mesh,
        in_specs=(P(("rep", "dp")), P(("rep", "dp")), P(), P(), P(), *[shard] * 6),
        out_specs=(P("rep"), P("rep"), P("rep"), *[P("rep", "dp", None)] * 6),
        check_vma=False,
    )
```

```python
import functools

import jax
import jax.numpy as jnp
from jax import lax
from jax.experimental import pallas as pl
from jax.experimental.layout import Layout, with_layout_constraint
from jax.experimental.pallas import tpu as pltpu
from jax.sharding import PartitionSpec as P

F32, BF16 = jnp.float32, jnp.bfloat16
CLIP_EPS = 1e-30
LANES = 128
SIDE = 4
ORDERS = ((0, 1, 2), (1, 2, 0), (2, 0, 1))
VMEM_LIMIT = 63 * 1024 * 1024


class Place:
    def __init__(self):
        me = lax.axis_index("dp")
        self.core = lax.rem(me, 2)
        chip = lax.div(me, 2)
        self.at = (lax.div(chip, SIDE * SIDE), lax.rem(lax.div(chip, SIDE), SIDE), lax.rem(chip, SIDE))

    def device(self, axis=None, off=0, core=None):
        at = list(self.at)
        if axis is not None:
            at[axis] = lax.rem(at[axis] + off, SIDE)
        core = self.core if core is None else core
        return {"dp": ((at[0] * SIDE + at[1]) * SIDE + at[2]) * 2 + core}

    def partner(self):
        return self.device(core=1 - self.core)

    def onward(self, way):
        return 1 + 2 * lax.rem(way + self.core, 2)

    def block(self, axis, way, hops):
        return lax.rem(self.at[axis] + hops * (SIDE - self.onward(way)), SIDE)


def signal_all(devices):
    barrier = pltpu.get_barrier_semaphore()
    for d in devices:
        pl.semaphore_signal(barrier, inc=1, device_id=d, device_id_type=pl.DeviceIdType.MESH)
    pl.semaphore_wait(barrier, len(devices))


def near(place):
    return [place.partner()] + [place.device(axis, off) for axis in range(3) for off in (1, SIDE - 1)]


def put(src, dst, send, recv, device):
    return pltpu.make_async_remote_copy(
        src_ref=src, dst_ref=dst, send_sem=send, recv_sem=recv, device_id=device, device_id_type=pl.DeviceIdType.MESH
    )


def ways_of(cols):
    tiles = cols // LANES
    first = (tiles + 1) // 2 * LANES
    return ((0, first), (first, cols - first))


def index(order, values):
    out = [None] * 3
    for axis, value in zip(order, values, strict=True):
        out[axis] = value
    return tuple(out)


ALL = slice(None)


class Rings:
    def __init__(self, place, rows, cols, slots, sems):
        self.place, self.rows, self.slots, self.sems = place, rows // 3, slots, sems
        self.ways = ways_of(cols)

    def part(self, t, way):
        start, width = self.ways[way]
        return pl.ds(t * self.rows, self.rows), pl.ds(start, width)

    @staticmethod
    def pairs():
        return [(t, way) for t in range(3) for way in range(2)]

    def send(self, axis, way, src, landing, key, sems):
        src = landing if src is None else src
        return put(src, landing, sems[0].at[key], sems[1].at[key], self.place.device(axis, self.place.onward(way)))


class First(Rings):
    @staticmethod
    def scratch(rows, cols):
        third, dma = rows // 3, pltpu.SemaphoreType.DMA
        slots = [pltpu.VMEM((3, 3, SIDE, SIDE, third, width), BF16) for _, width in ways_of(cols)]
        return [pltpu.VMEM((SIDE, SIDE, SIDE, rows, cols), BF16), *slots, dma((3, 2, 3, SIDE)), dma((3, 2, 3, SIDE))]

    @classmethod
    def of(cls, place, rows, cols, refs):
        one = cls(place, rows, cols, refs[1:3], refs[3:5])
        one.held = refs[0]
        return one

    def block(self, t, way, hops, k, c=ALL):
        order = ORDERS[t]
        return self.held.at[(*index(order, (self.place.block(order[0], way, hops), k, c)), *self.part(t, way))]

    def message(self, t, way, n, k, arriving=False):
        src = None
        if not arriving:
            src = self.block(t, way, 1, k) if isinstance(n, int) and n == 0 else self.slots[way].at[t, n - 1, k]
        return self.send(ORDERS[t][0], way, src, self.slots[way].at[t, n, k], (t, way, n, k), self.sems)

    def start(self, k):
        for t, way in self.pairs():
            self.message(t, way, 0, k).start()

    def step(self, n, k):
        for t, way in self.pairs():
            self.message(t, way, n - 1, k, arriving=True).wait_recv()
            slots = self.slots[way]
            for c in range(SIDE):
                own = self.block(t, way, n + 1, k, c)
                slots[t, n - 1, k, c] = (slots[t, n - 1, k, c].astype(F32) + own[...].astype(F32)).astype(BF16)
            pl.when(n < 3)(lambda t=t, way=way: self.message(t, way, n, k).start())

    def tick(self, i):
        pl.when(i < SIDE)(lambda: self.start(i))
        pl.when(i >= SIDE)(lambda: self.step(lax.div(i, SIDE), lax.rem(i, SIDE)))

    def results(self):
        return [slots.at[:, 2] for slots in self.slots]

    def drain(self):
        def sent(k, _):
            for t, way in self.pairs():
                self.message(t, way, 0, k).wait_send()
                lax.fori_loop(1, 3, lambda n, _: (self.message(t, way, n, k).wait_send(), 0)[1], 0)
            return 0

        lax.fori_loop(0, SIDE, sent, 0)


class Rest(Rings):
    @staticmethod
    def scratch(rows, cols):
        third, dma = rows // 3, pltpu.SemaphoreType.DMA
        shapes = [pltpu.VMEM((*lead, third, width), BF16) for lead in ((3, 3, SIDE), (3, 3)) for _, width in ways_of(cols)]
        return shapes + [dma((3, 2, 3))] * 4

    @classmethod
    def of(cls, place, rows, cols, before, refs):
        one = cls(place, rows, cols, refs[:4], refs[4:8])
        one.before = before
        return one

    def message(self, phase, t, way, n, arriving=False):
        slots = self.slots[2 * phase - 2 + way]
        axis = ORDERS[t][phase]
        if arriving:
            src = None
        elif isinstance(n, int) and n == 0:
            v = self.place.block(axis, way, 1)
            src = self.before[way].at[t, v] if phase == 1 else self.slots[way].at[t, 2, v]
        else:
            src = slots.at[t, n - 1]
        return self.send(axis, way, src, slots.at[t, n], (t, way, n), self.sems[2 * phase - 2 : 2 * phase])

    def start(self, phase):
        for t, way in self.pairs():
            self.message(phase, t, way, 0).start()

    def step1(self, n):
        for t, way in self.pairs():
            self.message(1, t, way, n - 1, arriving=True).wait_recv()
            v = self.place.block(ORDERS[t][1], way, n + 1)
            before, slots = self.before[way], self.slots[way]
            for c in range(SIDE):
                slots[t, n - 1, c] = (slots[t, n - 1, c].astype(F32) + before[t, v, c].astype(F32)).astype(BF16)
            pl.when(n < 3)(lambda t=t, way=way: self.message(1, t, way, n).start())

    def step2(self, n):
        for t, way in self.pairs():
            self.message(2, t, way, n - 1, arriving=True).wait_recv()
            v = self.place.block(ORDERS[t][2], way, n + 1)
            before, slots = self.slots[way], self.slots[2 + way]
            slots[t, n - 1] = (slots[t, n - 1].astype(F32) + before[t, 2, v].astype(F32)).astype(BF16)
            pl.when(n < 3)(lambda t=t, way=way: self.message(2, t, way, n).start())

    def tick(self, i):
        pl.when(i == 0)(lambda: self.start(1))
        pl.when((i >= 1) & (i <= 3))(lambda: self.step1(i))
        pl.when(i == 3)(lambda: self.start(2))
        pl.when((i >= 4) & (i <= 6))(lambda: self.step2(i - 3))

    def result(self, out):
        for t, way in self.pairs():
            out[self.part(t, way)] = self.slots[2 + way][t, 2]

    def drain(self):
        for t, way in self.pairs():
            for phase in (1, 2):
                for n in range(3):
                    self.message(phase, t, way, n).wait_send()


def loads_down(source, first, sems):
    return [pltpu.make_async_copy(source.at[:, :, pl.ds(64 * z, 72)], first.held.at[:, :, z], sems.at[z]) for z in range(SIDE)]


def spread(j, steps, count, tick):
    low, high = lax.div(count * j, steps), lax.div(count * (j + 1), steps)
    lax.fori_loop(low, high, lambda i, _: (tick(i), 0)[1], 0)


def copies(sources, targets, sems):
    return [pltpu.make_async_copy(s, t, sems.at[i]) for i, (s, t) in enumerate(zip(sources, targets, strict=True))]


def begin(all_copies):
    for copy in all_copies:
        copy.start()


def end(all_copies):
    for copy in all_copies:
        copy.wait()


def half_sums(rows, cols):
    return [(3, SIDE, SIDE, rows // 3, width) for _, width in ways_of(cols)]


PREV = 6
DOWN_ROWS = 33


class Gather:
    def __init__(self, place, bufs, sems, outs, copy_sems):
        self.place, self.bufs, self.sems, self.outs, self.copy_sems = place, bufs, sems, outs, copy_sems

    @staticmethod
    def scratch(gate_cols, down_cols):
        bufs = [pltpu.VMEM((2, SIDE, SIDE, SIDE, 24, gate_cols), BF16), pltpu.VMEM((2, SIDE, SIDE, SIDE, 72, down_cols), BF16)]
        return bufs + [pltpu.SemaphoreType.DMA((2, 3, 2, 6, 3))] * 4 + [pltpu.SemaphoreType.DMA((2,))] * 3

    def part(self, kind, t, way):
        rows, cols = self.bufs[kind].shape[-2:]
        start, width = ways_of(cols)[way]
        return pl.ds(t * (rows // 3), rows // 3), pl.ds(start, width)

    def behind(self, t, way, axis, hops):
        return self.place.block(ORDERS[t][axis], way, hops)

    def message(self, kind, l, t, way, line, n, hops):
        order, place = ORDERS[t], self.place
        if isinstance(line, int) and line == 0:
            axis, values = order[0], [self.behind(t, way, 0, hops), place.at[order[1]], place.at[order[2]]]
        elif isinstance(line, int) and line == 1:
            axis, values = order[1], [ALL, self.behind(t, way, 1, hops), place.at[order[2]]]
        else:
            axis, values = order[2], [ALL, self.behind(t, way, 1, line - 2), self.behind(t, way, 2, hops)]
        ref = self.bufs[kind].at[(l, *index(order, values), *self.part(kind, t, way))]
        key = (l, t, way, line, n)
        return put(ref, ref, self.sems[2 * kind].at[key], self.sems[2 * kind + 1].at[key], place.device(axis, place.onward(way)))

    def copies(self, kind, l, t, way, b, c):
        order = ORDERS[t]
        rows, cols = self.part(kind, t, way)
        at = index(order, (ALL, b, c))
        if kind == 0:
            return [lambda out: (self.bufs[0].at[(l, *at, rows, cols)], out.at[(l, *at, rows, cols)])]
        half = self.bufs[1].shape[-1]
        start, width = ways_of(half)[way]
        columns = pl.ds(pl.multiple_of(self.place.core * half + start, LANES), width)
        x, y, z = at

        def pair(out, z, count):
            src = self.bufs[1].at[l, x, y, z, pl.ds(24 * t, count), cols]
            return src, out.at[l, x, y, pl.ds(pl.multiple_of(64 * z + 24 * t, 8), count), columns]

        if t < 2:
            return [lambda out: pair(out, z, 24)]
        return [lambda out, z=z: pair(out, z, 16 if z < SIDE - 1 else 24) for z in range(SIDE)]

    def copy_out(self, kind, l, t, way, b, c):
        local, send, recv = self.copy_sems

        def both(out):
            for pair in self.copies(kind, l, t, way, b, c):
                src, dst = pair(out)
                pltpu.make_async_copy(src, dst, local.at[kind]).start()
                put(src, dst, send.at[kind], recv.at[kind], self.place.partner()).start()

        if kind:
            both(self.outs[2])
        else:
            for core in range(2):
                pl.when(self.place.core == core)(lambda core=core: both(self.outs[core]))

    def parts(self):
        return [(kind, t, way) for kind in range(2) for t in range(3) for way in range(2)]

    def own(self, l):
        for kind, t, way in self.parts():
            self.message(kind, l, t, way, 0, 0, 0).start()

    def start_third(self, kind, l, t, way, m):
        self.message(kind, l, t, way, 2 + m, 0, 0).start()
        self.copy_out(kind, l, t, way, self.behind(t, way, 1, m), self.place.at[ORDERS[t][2]])

    def first_axis(self):
        def step(i, _):
            n, l = 1 + lax.div(i, 2), lax.rem(i, 2)
            for kind, t, way in self.parts():
                self.message(kind, l, t, way, 0, n - 1, n).wait_recv()
                pl.when(n < 3)(lambda kind=kind, t=t, way=way: self.message(kind, l, t, way, 0, n, n).start())

                @pl.when(n == 3)
                def _(kind=kind, t=t, way=way):
                    self.message(kind, l, t, way, 1, 0, 0).start()
                    self.start_third(kind, l, t, way, 0)

            return 0

        lax.fori_loop(0, 6, step, 0)

    def other_axes(self):
        def step(i, _):
            r, l = 1 + lax.div(i, 2), lax.rem(i, 2)
            for kind, t, way in self.parts():

                @pl.when(r <= 3)
                def _(kind=kind, t=t, way=way):
                    self.message(kind, l, t, way, 1, r - 1, r).wait_recv()
                    pl.when(r < 3)(lambda: self.message(kind, l, t, way, 1, r, r).start())
                    self.start_third(kind, l, t, way, r)

                def third(m, _, kind=kind, t=t, way=way):
                    n = r - m
                    self.message(kind, l, t, way, 2 + m, n - 1, n).wait_recv()
                    pl.when(n < 3)(lambda: self.message(kind, l, t, way, 2 + m, n, n).start())
                    self.copy_out(kind, l, t, way, self.behind(t, way, 1, m), self.behind(t, way, 2, n))
                    return 0

                lax.fori_loop(jnp.maximum(r - 3, 0), jnp.minimum(r, SIDE), third, 0)
            return 0

        lax.fori_loop(0, 12, step, 0)

    def drain(self):
        local, send, recv = self.copy_sems
        half = self.bufs[1].shape[-1]
        columns = self.outs[2].at[:, :, :, :, pl.ds(0, half)]
        for kind, whole in ((0, self.outs[0]), (1, columns)):
            pltpu.make_async_copy(whole, whole, local.at[kind]).wait()
            copy = put(whole, whole, send.at[kind], recv.at[kind], self.place.partner())
            copy.wait_send()
            copy.wait_recv()

        def sent(i, _):
            l, n = lax.div(i, 3), lax.rem(i, 3)
            for kind, t, way in self.parts():
                for line in range(2):
                    self.message(kind, l, t, way, line, n, n).wait_send()
                lax.fori_loop(2, 6, lambda line, _: (self.message(kind, l, t, way, line, n, n).wait_send(), 0)[1], 0)
            return 0

        lax.fori_loop(0, 6, sent, 0)


def update_kernel(count, *refs):
    sums_gu, sums_d, m_in, v_in, w_in = refs[0:2], refs[2:4], refs[4:7], refs[7:10], refs[10:13]
    new_gu, new_d, m_out, v_out = refs[13], refs[14], refs[15:18], refs[18:21]
    moments_gu, moments_d, old_gu, old_d, other_d, tiles = refs[21:27]
    load_sem, early_send, early_recv, norm_send, norm_recv, late_local, late_send, late_recv = refs[27:35]
    place = Place()
    x, y, z = place.at
    core = place.core
    partner = place.partner()
    gate_tiles, down_tiles = sums_gu[0].shape[1] // LANES, sums_d[0].shape[1] // LANES
    gate_stride, down_stride = 2 * gate_tiles, 4 * down_tiles
    gate_size, down_size = 12 * gate_stride, DOWN_ROWS * down_stride

    def blank(i, _):
        for which in range(2):
            moments_d[which, pl.ds(pl.multiple_of(8 * i, 8), 8), :] = jnp.zeros((8, LANES), F32)
        return 0

    lax.fori_loop(0, moments_d.shape[1] // 8, blank, 0)
    following = [place.device(2, 1, core=c) for c in range(2)]
    others = [place.device(axis, 2) for axis in range(3)] + [place.device(2, off, core=1 - core) for off in (1, SIDE - 1)]
    signal_all(near(place) + others)

    def gate_rows(i, which):
        return moments_gu.at[i, pl.ds(pl.multiple_of(which * gate_size, 8), gate_size)]

    def down_rows(i, first, rows):
        return moments_d.at[i, pl.ds(pl.multiple_of(first * down_stride, 8), rows * down_stride)]

    def columns(ref):
        half = down_tiles * LANES
        return ref.at[:, x, y, pl.ds(pl.multiple_of(64 * z, 8), 72), pl.ds(pl.multiple_of(core * half, LANES), half)]

    own_rows = PREV + 2 * z + DOWN_ROWS * core
    loads, sends = [], []
    for i, moment in enumerate((m_in, v_in)):
        for c in range(2):

            @pl.when(core == c)
            def _(i=i, moment=moment, c=c):
                pltpu.make_async_copy(moment[c], gate_rows(i, core), load_sem.at[i]).start()
                put(moment[1 - c], gate_rows(i, core), early_send.at[i], early_recv.at[i], partner).start()

        loads.append(pltpu.make_async_copy(moment[0], gate_rows(i, core), load_sem.at[i]))
        sends.append(put(moment[0], gate_rows(i, core), early_send.at[i], early_recv.at[i], partner))
        loads.append(pltpu.make_async_copy(moment[2], down_rows(i, own_rows, DOWN_ROWS), load_sem.at[2 + i]))
        loads[-1].start()
        sends.append(put(moment[2], down_rows(i, own_rows, DOWN_ROWS), early_send.at[2 + i], early_recv.at[2 + i], partner))
        sends[-1].start()
        last = moment[2].at[pl.ds((DOWN_ROWS - PREV) * down_stride, PREV * down_stride)]
        landing = down_rows(i, 2 * lax.rem(z + 1, SIDE), PREV)

        @pl.when(core == 1)
        def _(i=i, last=last, landing=landing):
            for c in range(2):
                put(last, landing, early_send.at[4 + 2 * i + c], early_recv.at[4 + i], following[c]).start()

    for l in range(2):
        sends.append(put(sums_d[l], other_d.at[l], early_send.at[8 + l], early_recv.at[6 + l], partner))
        sends[-1].start()
    for c in range(2):

        @pl.when(core == c)
        def _(c=c):
            pltpu.make_async_copy(w_in[c].at[:, x, y, z], old_gu, load_sem.at[4]).start()

    loads.append(pltpu.make_async_copy(w_in[0].at[:, x, y, z], old_gu, load_sem.at[4]))
    loads.append(pltpu.make_async_copy(columns(w_in[2]), old_d, load_sem.at[5]))
    loads[-1].start()

    squares = jnp.zeros((8, LANES), F32)
    for l in range(2):

        def of_gate_up(j, total, l=l):
            for t in range(3):
                g = sums_gu[l][pl.ds(8 * t, 8), pl.ds(pl.multiple_of(j * LANES, LANES), LANES)].astype(F32)
                total += g * g
            return total

        squares = lax.fori_loop(0, gate_tiles, of_gate_up, squares)

        def of_down(i, total, l=l):
            row = 8 * i + lax.broadcasted_iota(jnp.int32, (8, LANES), 0)
            mine = (row >= 2 * z) & (row < 2 * z + 2 * DOWN_ROWS)
            for j in range(down_tiles):
                g = sums_d[l][pl.ds(pl.multiple_of(8 * i, 8), 8), pl.ds(j * LANES, LANES)].astype(F32)
                total += jnp.where(mine, g * g, 0.0)
            return total

        squares = lax.fori_loop(0, 9, of_down, squares)
    for stage, (coordinate, size) in enumerate(((core, 2), (x, SIDE), (y, SIDE), (z, SIDE))):
        tiles[stage, coordinate] = squares
        exchanges = []
        for off in range(1, size):
            target = partner if stage == 0 else place.device(stage - 1, off)
            key = 3 * stage + off - 1
            here = tiles.at[stage, coordinate]
            exchanges.append(put(here, here, norm_send.at[key], norm_recv.at[key], target))
            exchanges[-1].start()
        for exchange in exchanges:
            exchange.wait_recv()
        for exchange in exchanges:
            exchange.wait_send()
        squares = tiles[stage, 0]
        for other in range(1, size):
            squares += tiles[stage, other]
    total = jnp.sum(jnp.sum(squares, 0, keepdims=True), 1, keepdims=True)
    factor = jnp.minimum(1.0, 0.5 * lax.rsqrt(total / count + CLIP_EPS))

    for copy in loads:
        copy.wait()
    for copy in sends:
        copy.wait_recv()
    for i in range(2):
        put(down_rows(i, 0, PREV), down_rows(i, 0, PREV), early_send.at[0], early_recv.at[4 + i], partner).wait_recv()

    def moments(ref, start, stride, g):
        rows = pl.ds(start, 8, stride=stride)
        m = 0.9 * ref[0, rows, :] + 0.1 * g
        v = 0.95 * ref[1, rows, :] + 0.05 * g * g
        ref[0, rows, :] = m
        ref[1, rows, :] = v
        return m * lax.rsqrt(v + 1e-8)

    def weight(w, step):
        w = w.astype(F32)
        return (w - 0.02 * (step + 0.1 * w)).astype(BF16)

    for l in range(2):

        def gate_up(j, _, l=l):
            lanes = pl.ds(pl.multiple_of(j * LANES, LANES), LANES)
            for t in range(3):
                rows = pl.ds(8 * t, 8)
                g = sums_gu[l][rows, lanes].astype(F32) * factor
                step = moments(moments_gu, 8 * t * gate_stride + 2 * j + l, gate_stride, g)
                new_gu[l, rows, lanes] = weight(old_gu[l, rows, lanes], step)
            return 0

        lax.fori_loop(0, gate_tiles, gate_up, 0, unroll=3)

        def down(i, _, l=l):
            rows = pl.ds(pl.multiple_of(8 * i, 8), 8)
            for j in range(down_tiles):
                lanes = pl.ds(j * LANES, LANES)
                start = (PREV + 8 * i) * down_stride + 2 * j + l
                g = sums_d[l][rows, lanes].astype(F32) * factor
                step = moments(moments_d, start + 2 * down_tiles * core, down_stride, g)
                new_d[l, rows, lanes] = weight(old_d[l, rows, lanes], step)
            return 0

        lax.fori_loop(0, 9, down, 0)
    for l in range(2):

        def down_other(i, _, l=l):
            rows = pl.ds(pl.multiple_of(8 * i, 8), 8)
            for j in range(down_tiles):
                start = (PREV + 8 * i) * down_stride + 2 * j + l
                g = other_d[l, rows, pl.ds(j * LANES, LANES)].astype(F32) * factor
                moments(moments_d, start + 2 * down_tiles * (1 - core), down_stride, g)
            return 0

        lax.fori_loop(0, 9, down_other, 0)

    late = []
    for i, out in enumerate((m_out, v_out)):
        for c in range(2):

            @pl.when(core == c)
            def _(i=i, out=out, c=c):
                pltpu.make_async_copy(gate_rows(i, core), out[c], late_local.at[i]).start()
                put(gate_rows(i, 1 - core), out[c], late_send.at[i], late_recv.at[i], partner).start()

        pltpu.make_async_copy(down_rows(i, own_rows, DOWN_ROWS), out[2], late_local.at[2 + i]).start()
    for i, out in enumerate((m_out, v_out)):
        pltpu.make_async_copy(gate_rows(i, core), out[0], late_local.at[i]).wait()
        pltpu.make_async_copy(down_rows(i, own_rows, DOWN_ROWS), out[2], late_local.at[2 + i]).wait()
        copy = put(gate_rows(i, 1 - core), out[0], late_send.at[i], late_recv.at[i], partner)
        copy.wait_recv()
        copy.wait_send()
    for copy in sends:
        copy.wait_send()
    for i in range(2):
        for c in range(2):

            @pl.when(core == 1)
            def _(i=i, c=c):
                rows = down_rows(i, 0, PREV)
                put(rows, rows, early_send.at[4 + 2 * i + c], early_recv.at[4 + i], following[c]).wait_send()


def gather_kernel(new_gu, new_d, *refs):
    w_out, load_sem, rest = refs[:3], refs[3], refs[4:]
    place = Place()
    gather = Gather(place, rest[:2], rest[2:6], w_out, rest[6:9])
    loads = [pltpu.make_async_copy(new, buf.at[(ALL, *place.at)], load_sem.at[i]) for i, (new, buf) in enumerate(zip((new_gu, new_d), rest[:2]))]
    begin(loads)
    signal_all(near(place))
    end(loads)
    for l in range(2):
        gather.own(l)
    gather.first_axis()
    gather.other_axes()
    gather.drain()


def update_call(count, collective_id, sums_gu, sums_d, m, v, w):
    gate_cols, down_half = sums_gu[0].shape[1], sums_d[0].shape[1]
    operands = [*sums_gu, *sums_d, *m, *v, *w]
    hbm, vmem = pl.BlockSpec(memory_space=pltpu.HBM), pl.BlockSpec(memory_space=pltpu.VMEM)
    dma = pltpu.SemaphoreType.DMA
    gate_stride, down_stride = gate_cols // 64, down_half // 32
    scratch = [
        pltpu.VMEM((2, 24 * gate_stride, LANES), F32),
        pltpu.VMEM((2, (PREV + 72) * down_stride, LANES), F32),
        pltpu.VMEM((2, 24, gate_cols), BF16),
        pltpu.VMEM((2, 72, down_half), BF16),
        pltpu.VMEM((2, 72, down_half), BF16),
        pltpu.VMEM((4, SIDE, 8, LANES), F32),
        dma((6,)), dma((10,)), dma((8,)), dma((12,)), dma((12,)), dma((4,)), dma((2,)), dma((2,)),
    ]
    new = [jax.ShapeDtypeStruct((2, 24, gate_cols), BF16), jax.ShapeDtypeStruct((2, 72, down_half), BF16)]
    return pl.pallas_call(
        functools.partial(update_kernel, count),
        name="update",
        out_shape=[*new, *[jax.ShapeDtypeStruct(t.shape, t.dtype) for t in (*m, *v)]],
        in_specs=[vmem] * 4 + [hbm] * 9,
        out_specs=[vmem] * 2 + [hbm] * 6,
        scratch_shapes=scratch,
        compiler_params=pltpu.CompilerParams(collective_id=collective_id, has_side_effects=True, vmem_limit_bytes=VMEM_LIMIT),
    )(*operands)


def gather_call(collective_id, new_gu, new_d, w):
    hbm = pl.BlockSpec(memory_space=pltpu.HBM)
    return pl.pallas_call(
        gather_kernel,
        name="gather",
        out_shape=[jax.ShapeDtypeStruct(t.shape, t.dtype) for t in w],
        in_specs=[hbm] * 2,
        out_specs=[hbm] * 3,
        scratch_shapes=[pltpu.SemaphoreType.DMA((2,)), *Gather.scratch(new_gu.shape[2], new_d.shape[2])],
        compiler_params=pltpu.CompilerParams(collective_id=collective_id, has_side_effects=True, vmem_limit_bytes=VMEM_LIMIT),
    )(new_gu, new_d)


TILE = 384
ROWS = 256
TIGHT = pl.Buffered(buffer_count=1)


def dot(a, b, dims):
    return lax.dot_general(a, b, (dims, ((), ())), preferred_element_type=F32)


NN, NT, TN = ((1,), (0,)), ((1,), (1,)), ((0,), (0,))


def norm_scale(wide):
    return lax.rsqrt(jnp.mean(wide * wide, -1, keepdims=True) + 1e-6)


def in_rows(total, step, body):
    def one(i, _):
        body(pl.ds(pl.multiple_of(i * step, step), step))
        return 0

    lax.fori_loop(0, total // step, one, 0)


def clear(acc):
    def rows(r):
        acc[r, :] = jnp.zeros((8, acc.shape[1]), F32)

    in_rows(acc.shape[0], 8, rows)


def spec(shape, index_map, tight=False):
    return pl.BlockSpec(shape, index_map, pipeline_mode=TIGHT) if tight else pl.BlockSpec(shape, index_map)


def whole(shape, tight=True):
    return spec(shape, lambda j: (0,) * len(shape), tight)


HBM = pl.BlockSpec(memory_space=pltpu.HBM)


def params(collective_id=None, semantics=("arbitrary",)):
    more = {} if collective_id is None else {"collective_id": collective_id, "has_side_effects": True}
    return pltpu.CompilerParams(dimension_semantics=semantics, vmem_limit_bytes=VMEM_LIMIT, **more)


def transpose_piece(j, last, src, dst):
    def piece(i):
        at = pl.ds(pl.multiple_of(i * LANES, LANES), LANES)
        dst[at, :] = src[:, at].T

    piece(j)
    pl.when(j == last)(lambda: piece(last + 1))


def side_by_side(a, b):
    return jnp.concatenate([a, b], axis=1)


def forward_kernel(tiles, x, wg, wu, wd, gate, up, h_out, a_out, at, a, acc, p):
    j = pl.program_id(0)

    @pl.when(j == 0)
    def _():
        def rows(r):
            wide = x[r, :].astype(F32)
            a[r, :] = (wide * norm_scale(wide)).astype(BF16)

        in_rows(x.shape[0], 32, rows)
        clear(acc)

    transpose_piece(j, tiles - 1, a, at)
    both = side_by_side(wg[0], wu[0])
    slot = lax.rem(j, 2)
    for m in range(x.shape[0] // ROWS):
        r = pl.ds(m * ROWS, ROWS)
        gu = dot(a[r, :], both, NN)
        g, u = gu[:, :TILE], gu[:, TILE:]
        gate[0, r, :] = g
        up[0, r, :] = u
        p[slot, r, :] = (g * lax.logistic(g) * u).astype(BF16)

    @pl.when(slot == 1)
    def _():
        for m in range(x.shape[0] // ROWS):
            r = pl.ds(m * ROWS, ROWS)
            acc[r, :] += dot(side_by_side(p[0, r, :], p[1, r, :]), wd[0], NN)

    @pl.when(j == tiles - 1)
    def _():
        def last_down(r):
            acc[r, :] += dot(p[0, r, :], wd[0, pl.ds(0, TILE), :], NN)

        in_rows(x.shape[0], ROWS, last_down)

        def rows(r):
            h = (x[r, :].astype(F32) + acc[r, :].astype(BF16).astype(F32)).astype(BF16)
            h_out[r, :] = h
            wide = h.astype(F32)
            a_out[r, :] = (wide * norm_scale(wide)).astype(BF16)

        in_rows(x.shape[0], 32, rows)


def forward_call(x, wg, wu, wd):
    tokens, d = x.shape
    ff = wg.shape[2]
    tiles = ff // TILE
    w_in = spec((1, d, TILE), lambda j: (0, 0, j))
    return pl.pallas_call(
        functools.partial(forward_kernel, tiles),
        name="forward_0",
        grid=(tiles,),
        in_specs=[whole((tokens, d)), w_in, w_in, spec((1, 2 * TILE, d), lambda j: (0, lax.div(j, 2), 0))],
        out_specs=[spec((1, tokens, TILE), lambda j: (j, 0, 0))] * 2 + [whole((tokens, d))] * 2 + [whole((d, tokens))],
        out_shape=[jax.ShapeDtypeStruct((tiles, tokens, TILE), F32)] * 2
        + [jax.ShapeDtypeStruct((tokens, d), BF16)] * 2
        + [jax.ShapeDtypeStruct((d, tokens), BF16)],
        scratch_shapes=[pltpu.VMEM((tokens, d), BF16), pltpu.VMEM((tokens, d), F32), pltpu.VMEM((2, tokens, TILE), BF16)],
        compiler_params=params(),
    )(x, wg, wu, wd)


class PairSum:
    def __init__(self, place, tiles, landing, stage, send, recv):
        self.place, self.tiles, self.landing, self.stage, self.send, self.recv = place, tiles, landing, stage, send, recv

    @staticmethod
    def scratch(tiles, rows, cols):
        dma = pltpu.SemaphoreType.DMA
        return [pltpu.VMEM((tiles, rows, cols), BF16), pltpu.VMEM((2, rows, cols), BF16), dma((2,)), dma((tiles,))]

    def copy(self, i):
        slot = lax.rem(i, 2)
        return put(self.stage.at[slot], self.landing.at[i], self.send.at[slot], self.recv.at[i], self.place.partner())

    def reserve(self, i):
        pl.when(i >= 2)(lambda: self.copy(i - 2).wait_send())
        return self.stage.at[lax.rem(i, 2)]

    def drain(self):
        for i in (self.tiles - 2, self.tiles - 1):
            self.copy(i).wait_send()


def hidden_back(gate, up, dp):
    dp = dp.astype(F32)
    s = lax.logistic(gate)
    act = gate * s
    return (act * up).astype(BF16), (dp * up * (s + act * (1.0 - s))).astype(BF16), (dp * act).astype(BF16)


def down_gradient(j, tiles, pair, p, dy, half, out):
    core = pair.place.core

    def columns(c):
        return pl.ds(pl.multiple_of(c * half, LANES), half)

    @pl.when(j < tiles)
    def _():
        slot = pair.reserve(j)
        slot[...] = dot(p[lax.rem(j, 2)], dy[:, columns(1 - core)], TN).astype(BF16)
        pair.copy(j).start()

    @pl.when(j >= 1)
    def _():
        pair.copy(j - 1).wait_recv()
        own = dot(p[lax.rem(j - 1, 2)], dy[:, columns(core)], TN)
        out[...] = (own + pair.landing[j - 1].astype(F32)).astype(BF16)

    pl.when(j == tiles)(pair.drain)


def layer_kernel(tiles, a, dy, wg, wu, wd, dgu, at, out, p, dps, *rest):
    j = pl.program_id(0)
    place = Place()
    pair = PairSum(place, tiles, *rest)
    pl.when(j == 0)(lambda: signal_all([place.partner()]))
    two_tiles_of_dp(j, tiles, dy, wd, dps)

    @pl.when(j < tiles)
    def _():
        transpose_piece(j, tiles - 1, a, at)
        slot = lax.rem(j, 2)
        both = side_by_side(wg[0], wu[0])
        for m in range(a.shape[0] // ROWS):
            r = pl.ds(m * ROWS, ROWS)
            gu = dot(a[r, :], both, NN)
            p[slot, r, :], dgu[0, 0, r, :], dgu[0, 1, r, :] = hidden_back(gu[:, :TILE], gu[:, TILE:], dps[slot, r, :])

    down_gradient(j, tiles, pair, p, dy, dy.shape[1] // 2, out)


def two_tiles_of_dp(j, tiles, dy, wd, dps):
    @pl.when((lax.rem(j, 2) == 0) & (j < tiles - 1))
    def _():
        for m in range(dy.shape[0] // ROWS):
            r = pl.ds(m * ROWS, ROWS)
            dp = dot(dy[r, :], wd[0], NT).astype(BF16)
            dps[0, r, :] = dp[:, :TILE]
            dps[1, r, :] = dp[:, TILE:]

    @pl.when(j == tiles - 1)
    def _():
        def one_tile(r):
            dps[0, r, :] = dot(dy[r, :], wd[0, pl.ds(0, TILE), :], NT).astype(BF16)

        in_rows(dy.shape[0], ROWS, one_tile)


def clip(tiles, back=0):
    return lambda j: jnp.clip(j - back, 0, tiles - 1)


def layer_call(collective_id, a, dy, wg, wu, wd):
    tokens, d = a.shape
    ff = wg.shape[2]
    tiles, half = ff // TILE, d // 2
    now, before = clip(tiles), clip(tiles, 1)
    w_in = spec((1, d, TILE), lambda j: (1, 0, now(j)))
    return pl.pallas_call(
        functools.partial(layer_kernel, tiles),
        name="layer_1",
        grid=(tiles + 1,),
        in_specs=[whole((tokens, d))] * 2 + [w_in, w_in, spec((1, 2 * TILE, d), lambda j: (1, lax.div(now(j), 2), 0))],
        out_specs=[spec((1, 2, tokens, TILE), lambda j: (now(j), 0, 0, 0)), whole((d, tokens)), spec((TILE, half), lambda j: (before(j), 0))],
        out_shape=[
            jax.ShapeDtypeStruct((tiles, 2, tokens, TILE), BF16),
            jax.ShapeDtypeStruct((d, tokens), BF16),
            jax.ShapeDtypeStruct((ff, half), BF16),
        ],
        scratch_shapes=[pltpu.VMEM((2, tokens, TILE), BF16)] * 2 + PairSum.scratch(tiles, TILE, half),
        compiler_params=params(collective_id),
    )(a, dy, wg, wu, wd)


GATE_ROWS, DOWN_WINDOW = 24, 72
RING = 6


def second(t, v, rest=ALL):
    return (rest, v) if t == 1 else (v, rest)


class Stream:
    def __init__(self, place, tiles, phases, refs):
        self.place, self.tiles, self.phases, self.rows = place, tiles, phases, GATE_ROWS // 3
        self.held, self.slots, self.send, self.recv = refs[0], refs[1 : 1 + 2 * phases], refs[-2], refs[-1]
        self.ways = ways_of(TILE)

    @staticmethod
    def scratch(tiles, phases):
        third, dma = GATE_ROWS // 3, pltpu.SemaphoreType.DMA
        leads = [(3, 3, tiles, SIDE, SIDE), (3, 3, tiles, SIDE), (3, 3, tiles)][:phases]
        slots = [pltpu.VMEM((*lead, third, width), BF16) for lead in leads for _, width in ways_of(TILE)]
        return [pltpu.VMEM((RING, SIDE, SIDE, SIDE, GATE_ROWS, TILE), BF16), *slots, dma((tiles, 7)), dma((tiles, 7))]

    def part(self, t, way):
        start, width = self.ways[way]
        return pl.ds(t * self.rows, self.rows), pl.ds(start, width)

    def own(self, c, t, way, hops, b=ALL, d=ALL):
        at = index(ORDERS[t], (self.place.block(ORDERS[t][0], way, hops), ALL, ALL))
        axes = [i for i in range(3) if i != ORDERS[t][0]]
        at = list(at)
        at[axes[0]], at[axes[1]] = b, d
        return self.held.at[(lax.rem(c, RING), *at, *self.part(t, way))]

    def copy(self, phase, t, way, n, c, first=False):
        axis = ORDERS[t][phase]
        slots = self.slots[2 * phase + way]
        if not first:
            src = slots.at[t, n - 1, c]
        elif phase == 0:
            src = self.own(c, t, way, 1)
        else:
            src = self.slots[way].at[(t, 2, c, *second(t, self.place.block(axis, way, 1)))]
        key = (c, 3 * phase + n)
        return put(src, slots.at[t, n, c], self.send.at[key], self.recv.at[key], self.place.device(axis, self.place.onward(way)))

    def direct(self, t, way, off, c):
        axis = ORDERS[t][2]
        v = lax.rem(self.place.at[axis] + off, SIDE)
        src, dst = self.slots[2 + way].at[t, 2, c, v], self.slots[4 + way].at[t, off - 1, c]
        return put(src, dst, self.send.at[c, 6], self.recv.at[c, 6], self.place.device(axis, off))

    def pairs(self):
        return [(t, way) for t in range(3) for way in range(2)]

    def all_of(self, phase):
        return self.held.at[(0,) * (phase + 2)] if phase < 2 else self.held.at[0, 0, 0, pl.ds(0, 3)]

    def begin(self, phase, c):
        for t, way in self.pairs():
            if phase < 2:
                self.copy(phase, t, way, 0, c, first=True).start()
            else:
                for off in range(1, SIDE):
                    self.direct(t, way, off, c).start()

    def add(self, phase, t, way, n, c):
        slots = self.slots[2 * phase + way]
        v = self.place.block(ORDERS[t][phase], way, n + 1)

        def one(at, other):
            at = (t, n - 1, c, *at)
            slots[at] = (slots[at].astype(F32) + other[...].astype(F32)).astype(BF16)

        if phase == 0:
            for b in range(SIDE):
                for d in range(SIDE):
                    one((b, d), self.own(c, t, way, n + 1, b, d))
        else:
            for d in range(SIDE):
                one((d,), self.slots[way].at[(t, 2, c, *second(t, v, d))])

    def stage(self, s, c, out):
        phase, n = (s - 1) // 3, (s - 1) % 3 + 1
        whole_stage = self.all_of(phase)
        pltpu.make_async_copy(whole_stage, whole_stage, self.recv.at[c, s - 1]).wait()
        if phase == 2:
            for t, way in self.pairs():
                total = self.slots[2 + way][t, 2, c, self.place.at[ORDERS[t][2]]].astype(F32)
                for i in range(3):
                    total += self.slots[4 + way][t, i, c].astype(F32)
                rows, _ = self.part(t, way)
                start, width = self.ways[way]
                out[rows, pl.ds(pl.multiple_of(c * TILE + start, LANES), width)] = total.astype(BF16)
            return
        for t, way in self.pairs():
            self.add(phase, t, way, n, c)
            if n < 3:
                self.copy(phase, t, way, n, c).start()
        if n == 3 and phase + 1 < self.phases:
            self.begin(phase + 1, c)

    def sent(self, phase, n, c):
        whole_stage = self.all_of(phase)
        pltpu.make_async_copy(whole_stage, whole_stage, self.send.at[c, 3 * phase + n]).wait()

    def count(self):
        return 3 if self.phases == 1 else 7

    def keep(self, c):
        pl.when(c >= RING)(lambda: self.sent(0, 0, c - RING))
        return self.held.at[lax.rem(c + RING, RING)]

    def run(self, s, c, out):
        act = (lambda: self.begin(0, c)) if s == 0 else (lambda: self.stage(s, c, out))
        pl.when((c >= 0) & (c < self.tiles))(act)

    def early(self, j, out=None):
        for s in range(self.count(), 1, -1):
            self.run(s, j - 3 - s, out)

    def late(self, j, out=None):
        self.run(0, j - 2, out)
        self.run(1, j - 3, out)

    def last_step(self):
        return self.tiles - 1 + 3 + self.count()

    def drain(self):
        def each(c, _):
            pl.when(c >= self.tiles - RING)(lambda: self.sent(0, 0, c))
            for i in range(1, self.count()):
                self.sent(i // 3, i % 3, c)
            return 0

        lax.fori_loop(0, self.tiles, each, 0)

    def results(self):
        return [self.slots[way].at[:, 2] for way in range(2)]


def stream_halves(tiles):
    return [(3, tiles, SIDE, SIDE, GATE_ROWS // 3, width) for _, width in ways_of(TILE)]


class StreamRest:
    def __init__(self, place, tiles, before, refs):
        self.place, self.tiles, self.before, self.slots, self.sems = place, tiles, before, refs[:4], refs[4:8]
        self.rows, self.ways = GATE_ROWS // 3, ways_of(TILE)

    @staticmethod
    def scratch(tiles):
        third, dma = GATE_ROWS // 3, pltpu.SemaphoreType.DMA
        shapes = [pltpu.VMEM((3, 3, *lead, third, width), BF16) for lead in ((tiles, SIDE), (tiles,)) for _, width in ways_of(TILE)]
        return shapes + [dma((3, 2, 3))] * 4

    def pairs(self):
        return [(t, way) for t in range(3) for way in range(2)]

    def message(self, phase, t, way, n, arriving=False):
        slots = self.slots[2 * phase - 2 + way]
        axis = ORDERS[t][phase]
        if arriving:
            src = slots.at[t, n]
        elif isinstance(n, int) and n == 0:
            v = self.place.block(axis, way, 1)
            src = self.before[way].at[(t, ALL, *second(t, v))] if phase == 1 else self.slots[way].at[t, 2, :, v]
        else:
            src = slots.at[t, n - 1]
        send, recv = self.sems[2 * phase - 2 : 2 * phase]
        key = (t, way, n)
        return put(src, slots.at[t, n], send.at[key], recv.at[key], self.place.device(axis, self.place.onward(way)))

    def start(self, phase):
        for t, way in self.pairs():
            self.message(phase, t, way, 0).start()

    def step(self, phase, n):
        for t, way in self.pairs():
            self.message(phase, t, way, n - 1, arriving=True).wait_recv()
            v = self.place.block(ORDERS[t][phase], way, n + 1)
            slots = self.slots[2 * phase - 2 + way]

            def add(c, _, t=t, way=way, v=v, slots=slots):
                for d in range(SIDE if phase == 1 else 1):
                    at = (t, n - 1, c, d) if phase == 1 else (t, n - 1, c)
                    other = self.before[way].at[(t, c, *second(t, v, d))] if phase == 1 else self.slots[way].at[t, 2, c, v]
                    slots[at] = (slots[at].astype(F32) + other[...].astype(F32)).astype(BF16)
                return 0

            lax.fori_loop(0, self.tiles, add, 0)
            pl.when(n < 3)(lambda t=t, way=way: self.message(phase, t, way, n).start())

    def tick(self, i):
        pl.when(i == 0)(lambda: self.start(1))
        pl.when((i >= 1) & (i <= 3))(lambda: self.step(1, i))
        pl.when(i == 3)(lambda: self.start(2))
        pl.when((i >= 4) & (i <= 6))(lambda: self.step(2, i - 3))

    def result(self, out):
        def one(c, _):
            for t, way in self.pairs():
                start, width = self.ways[way]
                lanes = pl.ds(pl.multiple_of(c * TILE + start, LANES), width)
                out[pl.ds(t * self.rows, self.rows), lanes] = self.slots[2 + way][t, 2, c]
            return 0

        lax.fori_loop(0, self.tiles, one, 0)

    def drain(self):
        for t, way in self.pairs():
            for phase in (1, 2):
                for n in range(3):
                    self.message(phase, t, way, n).wait_send()


BLOCK_ROWS = SIDE * SIDE * GATE_ROWS


def gate_up_kernel(tiles, phases, cols, at, ahead, behind, *rest):
    j = pl.program_id(0)
    place = Place()
    core = place.core
    if phases == 1:
        outs, out, rest = rest[:2], None, rest[2:]
    else:
        sum_down, out, out_down, rest = rest[0], rest[1], rest[2], rest[3:]
    pair = PairSum(place, tiles, *rest[:4])
    stream = Stream(place, tiles, phases, rest[4 : 4 + 3 + 2 * phases])
    rest = rest[4 + 3 + 2 * phases :]
    if phases == 3:
        first = First.of(place, DOWN_WINDOW, cols, rest[1:6])
        down = Rest.of(place, DOWN_WINDOW, cols, first.results(), rest[6:14])
        loads = loads_down(sum_down, first, rest[0])

    @pl.when(j == 0)
    def _():
        opposite = [place.device(axis, 2) for axis in range(3)] if phases == 3 else []
        signal_all(near(place) + opposite)
        if phases == 3:
            begin(loads)

    stream.early(j, out)

    pl.when((j >= 2) & (j <= tiles + 1))(lambda: pair.copy(j - 2).wait_recv())

    @pl.when(j <= tiles + 1)
    def _():
        slot, kept = pair.reserve(j), stream.keep(j - 2)
        both = side_by_side(ahead[0, 1 - core], behind[0, core])
        landed = lax.rem(j + tiles - 2, tiles)
        for m in range(SIDE):
            r = pl.ds(m * BLOCK_ROWS, BLOCK_ROWS)
            tile = dot(at[r, :], both, NN)
            slot[r, :] = tile[:, :TILE].astype(BF16)
            total = (tile[:, TILE:] + pair.landing[landed, r, :].astype(F32)).astype(BF16)
            kept[m] = total.reshape(SIDE, SIDE, GATE_ROWS, TILE)

    pl.when(j < tiles)(lambda: pair.copy(j).start())
    stream.late(j, out)
    if phases == 3:
        pl.when(j == 0)(lambda: end(loads))
        pl.when(j < 8)(lambda: spread(j, 8, 16, first.tick))
        pl.when(j >= 8)(lambda: down.tick(j - 8))
        pl.when(j == 15)(lambda: down.result(out_down))

    @pl.when(j == stream.last_step())
    def _():
        if phases == 1:
            saves = copies(stream.results(), outs, rest[0])
            begin(saves)
            stream.drain()
            end(saves)
        else:
            stream.drain()
            first.drain()
            down.drain()


def gate_up_call(name, collective_id, phases, at, dgu, *sum_down):
    d, tokens = at.shape
    tiles, cols, dma = dgu.shape[0], d // 2, pltpu.SemaphoreType.DMA
    ff = tiles * TILE
    now, before = clip(tiles), clip(tiles, 2)
    if phases == 1:
        shapes = stream_halves(tiles)
        out_specs, more = [HBM] * 2, [dma((2,))]
    else:
        shapes = [(GATE_ROWS, ff), (DOWN_WINDOW, cols)]
        out_specs = [whole(s) for s in shapes]
        more = [dma((SIDE,)), *First.scratch(DOWN_WINDOW, cols), *Rest.scratch(DOWN_WINDOW, cols)]
    return pl.pallas_call(
        functools.partial(gate_up_kernel, tiles, phases, cols),
        name=name,
        grid=(tiles + (6 if phases == 1 else 10),),
        in_specs=[
            whole((d, tokens)),
            spec((1, 2, tokens, TILE), lambda j: (now(j), 0, 0, 0)),
            spec((1, 2, tokens, TILE), lambda j: (before(j), 0, 0, 0)),
            *[HBM] * len(sum_down),
        ],
        out_specs=out_specs,
        out_shape=[jax.ShapeDtypeStruct(s, BF16) for s in shapes],
        scratch_shapes=[*PairSum.scratch(tiles, d, TILE), *Stream.scratch(tiles, phases), *more],
        compiler_params=params(collective_id),
    )(at, dgu, dgu, *sum_down)


def gate_up_first_kernel(tiles, cols, at, ahead, behind, sum_down, out, half0, half1, *rest):
    j = pl.program_id(0)
    place = Place()
    core = place.core
    pair = PairSum(place, tiles, *rest[:4])
    first = First.of(place, DOWN_WINDOW, cols, rest[4:9])
    load_sem, save_sem = rest[9:11]
    loads = loads_down(sum_down, first, load_sem)

    @pl.when(j == 0)
    def _():
        signal_all(near(place))
        begin(loads)

    pl.when(j >= 2)(lambda: pair.copy(j - 2).wait_recv())
    slot = pair.reserve(j)
    both = side_by_side(ahead[0, 1 - core], behind[0, core])
    landed = lax.rem(j + tiles - 2, tiles)
    for m in range(at.shape[0] // ROWS):
        r = pl.ds(m * ROWS, ROWS)
        tile = dot(at[r, :], both, NN)
        slot[r, :] = tile[:, :TILE].astype(BF16)
        out[r, :] = (tile[:, TILE:] + pair.landing[landed, r, :].astype(F32)).astype(BF16)
    pl.when(j < tiles)(lambda: pair.copy(j).start())

    pl.when(j == 0)(lambda: end(loads))
    spread(j, tiles + 2, 16, first.tick)

    @pl.when(j == tiles + 1)
    def _():
        saves = copies(first.results(), (half0, half1), save_sem)
        begin(saves)
        first.drain()
        end(saves)


def gate_up_first_call(name, collective_id, at, dgu, sum_down):
    d, tokens = at.shape
    tiles, cols, dma = dgu.shape[0], sum_down.shape[-1], pltpu.SemaphoreType.DMA
    now, before = clip(tiles), clip(tiles, 2)
    return pl.pallas_call(
        functools.partial(gate_up_first_kernel, tiles, cols),
        name=name,
        grid=(tiles + 2,),
        in_specs=[
            whole((d, tokens)),
            spec((1, 2, tokens, TILE), lambda j: (now(j), 0, 0, 0)),
            spec((1, 2, tokens, TILE), lambda j: (before(j), 0, 0, 0)),
            HBM,
        ],
        out_specs=[spec((d, TILE), lambda j: (0, before(j))), HBM, HBM],
        out_shape=[jax.ShapeDtypeStruct((d, tiles * TILE), BF16)]
        + [jax.ShapeDtypeStruct(s, BF16) for s in half_sums(DOWN_WINDOW, cols)],
        scratch_shapes=[*PairSum.scratch(tiles, d, TILE), *First.scratch(DOWN_WINDOW, cols), dma((SIDE,)), dma((2,))],
        compiler_params=params(collective_id),
    )(at, dgu, dgu, sum_down)


def column_halves(cols):
    return ways_of(cols)


def load_columns(source, first, part, sem):
    start, width = part
    return [pltpu.make_async_copy(source.at[:, :, :, :, pl.ds(start, width)], first.held, sem)]


def middle_kernel(steps, ff, down_cols, dgu, wg, wu, h, dy, sum_gu, down0, down1, dh, out_down, half0, half1, acc_g, acc_u, *rest):
    j = pl.program_id(0)
    place = Place()
    part = column_halves(ff)[0]
    first = First.of(place, GATE_ROWS, part[1], rest[:5])
    before = rest[5:7]
    down = Rest.of(place, DOWN_WINDOW, down_cols, before, rest[7:15])
    load_sem, save_sem = rest[15:17]
    loads = copies((down0, down1), before, load_sem) + load_columns(sum_gu, first, part, load_sem.at[2])

    @pl.when(j == 0)
    def _():
        signal_all(near(place))
        begin(loads)
        clear(acc_g)
        clear(acc_u)

    def add_up(r, two):
        for which, (acc, w) in enumerate(((acc_g, wg), (acc_u, wu))):
            if two:
                acc[r, :] += dot(side_by_side(dgu[0, which, r, :], dgu[1, which, r, :]), w[0], NT)
            else:
                acc[r, :] += dot(dgu[0, which, r, :], w[0, :, pl.ds(0, TILE)], NT)

    pl.when(j < steps - 1)(lambda: in_rows(h.shape[0], 2 * ROWS, lambda r: add_up(r, True)))
    pl.when(j == steps - 1)(lambda: in_rows(h.shape[0], ROWS, lambda r: add_up(r, False)))

    pl.when(j == 0)(lambda: end(loads))
    down.tick(j)
    spread(j, steps, 16, first.tick)

    @pl.when(j == steps - 1)
    def _():
        lax.fori_loop(steps, 7, lambda i, _: (down.tick(i), 0)[1], 0)
        saves = copies(first.results(), (half0, half1), save_sem)
        begin(saves)
        down.result(out_down)

        def rows(r):
            wide = h[r, :].astype(F32)
            scale = norm_scale(wide)
            da = (acc_g[r, :].astype(BF16).astype(F32) + acc_u[r, :].astype(BF16).astype(F32)).astype(BF16).astype(F32)
            back = scale * da - wide * (scale * scale * scale * jnp.mean(da * wide, -1, keepdims=True))
            dh[r, :] = (dy[r, :].astype(F32) + back.astype(BF16).astype(F32)).astype(BF16)

        in_rows(h.shape[0], 32, rows)
        first.drain()
        down.drain()
        end(saves)


def middle_call(collective_id, dgu, wg, wu, h, dy, sum_gu, down_halves):
    tokens, d = h.shape
    tiles, dma, down_cols = dgu.shape[0], pltpu.SemaphoreType.DMA, d // 2
    ff = tiles * TILE
    steps = (tiles + 1) // 2
    width = column_halves(ff)[0][1]
    w_in = spec((1, d, 2 * TILE), lambda j: (1, 0, j))
    return pl.pallas_call(
        functools.partial(middle_kernel, steps, ff, down_cols),
        name="middle",
        grid=(steps,),
        in_specs=[spec((2, 2, tokens, TILE), lambda j: (j, 0, 0, 0)), w_in, w_in, whole((tokens, d)), whole((tokens, d))] + [HBM] * 3,
        out_specs=[whole((tokens, d)), whole((DOWN_WINDOW, down_cols)), HBM, HBM],
        out_shape=[jax.ShapeDtypeStruct(s, BF16) for s in ((tokens, d), (DOWN_WINDOW, down_cols), *half_sums(GATE_ROWS, width))],
        scratch_shapes=[pltpu.VMEM((tokens, d), F32)] * 2
        + First.scratch(GATE_ROWS, width)
        + [pltpu.VMEM(t.shape, BF16) for t in down_halves]
        + Rest.scratch(DOWN_WINDOW, down_cols)
        + [dma((3,)), dma((2,))],
        compiler_params=params(collective_id),
    )(dgu, wg, wu, h, dy, sum_gu, *down_halves)


def back_kernel(tiles, ff, dh, gate, up, wd, gate0, gate1, sum_gu, dgu, out, out_gu, p, dps, *rest):
    j = pl.program_id(0)
    place = Place()
    core, half = place.core, dh.shape[1] // 2
    parts = column_halves(ff)
    pair = PairSum(place, tiles, *rest[:4])
    before = rest[4:6]
    rest_a = Rest.of(place, GATE_ROWS, parts[0][1], before, rest[6:14])
    first = First.of(place, GATE_ROWS, parts[1][1], rest[14:19])
    rest_b = Rest.of(place, GATE_ROWS, parts[1][1], first.results(), rest[19:27])
    load_sem = rest[27]
    loads = copies((gate0, gate1), before, load_sem) + load_columns(sum_gu, first, parts[1], load_sem.at[2])

    @pl.when(j == 0)
    def _():
        signal_all(near(place))
        begin(loads)

    two_tiles_of_dp(j, tiles, dh, wd, dps)
    pl.when(j >= 2)(lambda: pair.copy(j - 2).wait_recv())
    tile = jnp.minimum(j, tiles - 1)
    ours = p[lax.rem(j + 1, 3)]
    for m in range(dh.shape[0] // ROWS):
        r = pl.ds(m * ROWS, ROWS)
        p[lax.rem(tile, 3), r, :], dgu[0, 0, r, :], dgu[0, 1, r, :] = hidden_back(gate[0, r, :], up[0, r, :], dps[lax.rem(tile, 2), r, :])
    own = dot(ours, dh[:, pl.ds(pl.multiple_of(core * half, LANES), half)], TN)
    out[...] = (own + pair.landing[lax.rem(j + tiles - 2, tiles)].astype(F32)).astype(BF16)

    @pl.when(j < tiles)
    def _():
        slot = pair.reserve(j)
        slot[...] = dot(p[lax.rem(j, 3)], dh[:, pl.ds(pl.multiple_of((1 - core) * half, LANES), half)], TN).astype(BF16)
        pair.copy(j).start()

    pl.when(j == 0)(lambda: end(loads))
    rest_a.tick(j)
    pl.when(j < 6)(lambda: spread(j, 6, 16, first.tick))
    pl.when(j >= 5)(lambda: rest_b.tick(j - 5))

    @pl.when(j == tiles + 1)
    def _():
        for sums, (start, width) in ((rest_a, parts[0]), (rest_b, parts[1])):
            sums.result(out_gu.at[:, pl.ds(start, width)])
        pair.drain()
        for sums in (rest_a, first, rest_b):
            sums.drain()


def back_call(collective_id, dh, gate, up, wd, sum_gu, gate_halves):
    tokens, d = dh.shape
    tiles, half, dma = gate.shape[0], d // 2, pltpu.SemaphoreType.DMA
    ff = tiles * TILE
    now, before = clip(tiles), clip(tiles, 2)
    tile = spec((1, tokens, TILE), lambda j: (now(j), 0, 0))
    parts = column_halves(ff)
    return pl.pallas_call(
        functools.partial(back_kernel, tiles, ff),
        name="back_0",
        grid=(tiles + 2,),
        in_specs=[whole((tokens, d)), tile, tile, spec((1, 2 * TILE, d), lambda j: (0, lax.div(now(j), 2), 0)), HBM, HBM, HBM],
        out_specs=[
            spec((1, 2, tokens, TILE), lambda j: (now(j), 0, 0, 0)),
            spec((TILE, half), lambda j: (before(j), 0)),
            whole((GATE_ROWS, ff)),
        ],
        out_shape=[jax.ShapeDtypeStruct(s, BF16) for s in ((tiles, 2, tokens, TILE), (ff, half), (GATE_ROWS, ff))],
        scratch_shapes=[pltpu.VMEM((3, tokens, TILE), BF16), pltpu.VMEM((2, tokens, TILE), BF16)]
        + PairSum.scratch(tiles, TILE, half)
        + [pltpu.VMEM(t.shape, BF16) for t in gate_halves]
        + Rest.scratch(GATE_ROWS, parts[0][1])
        + First.scratch(GATE_ROWS, parts[1][1])
        + Rest.scratch(GATE_ROWS, parts[1][1])
        + [dma((3,))],
        compiler_params=params(collective_id),
    )(dh, gate, up, wd, *gate_halves, sum_gu)


def flat(m):
    layers, rows, cols = m.shape
    split = m.transpose(1, 0, 2).reshape(rows, layers, cols // LANES, LANES)
    return with_layout_constraint(split, Layout((0, 2, 1, 3))).transpose(0, 2, 1, 3).reshape(-1, LANES)


def unflat(f, shape):
    layers, rows, cols = shape
    split = f.reshape(rows, cols // LANES, layers, LANES).transpose(0, 2, 1, 3)
    return with_layout_constraint(split, Layout((0, 2, 1, 3))).reshape(rows, layers, cols).transpose(1, 0, 2)


def solution(mesh):
    def body(x, dy, wg, wu, wd, mg, mu, md, vg, vu, vd):
        layers, d, ff = wg.shape
        x, dy = x[0], dy[0]
        windows = (SIDE, SIDE, 4 * 66, d // 2)
        gate0, up0, h1, a1, a0t = forward_call(x, wg, wu, wd)
        dgu1, a1t, down1 = layer_call(1, a1, dy, wg, wu, wd)
        blocks = (SIDE, SIDE, SIDE, GATE_ROWS, ff)
        gu1, *down_halves = gate_up_first_call("gate_up_1", 2, a1t, dgu1, down1.reshape(windows))
        gu1 = gu1.reshape(blocks)
        dh1, sum_down1, *gate_halves = middle_call(3, dgu1, wg, wu, h1, dy, gu1, down_halves)
        dgu0, down0, sum_gu1 = back_call(4, dh1, gate0, up0, wd, gu1, gate_halves)
        sum_gu0, sum_down0 = gate_up_call("gate_up_0", 5, 3, a0t, dgu0, down0.reshape(windows))

        views = [(2, SIDE, SIDE, SIDE, GATE_ROWS, ff)] * 2 + [(2, SIDE, SIDE, 4 * 66, d)]
        w = [t.reshape(view) for t, view in zip((wg, wu, wd), views, strict=True)]
        m, v = [flat(t) for t in (mg, mu, md)], [flat(t) for t in (vg, vu, vd)]
        new_gu, new_d, *moments = update_call(3 * layers * d * ff, 6, [sum_gu0, sum_gu1], [sum_down0, sum_down1], m, v, w)
        out = [*gather_call(7, new_gu, new_d, w), *moments]
        new = [t.reshape(like.shape) for t, like in zip(out[:3], (wg, wu, wd), strict=True)]
        return (*new, *[unflat(t, like.shape) for t, like in zip(out[3:], (mg, mu, md, vg, vu, vd), strict=True)])

    shard = P(None, "dp", None)
    return jax.shard_map(
        body,
        mesh=mesh,
        in_specs=(P(("rep", "dp")), P(("rep", "dp")), P(), P(), P(), *[shard] * 6),
        out_specs=(P("rep"), P("rep"), P("rep"), *[P("rep", "dp", None)] * 6),
        check_vma=False,
    )
```

```python
import functools

import jax
import jax.numpy as jnp
from jax import lax
from jax.experimental import pallas as pl
from jax.experimental.layout import Layout, with_layout_constraint
from jax.experimental.pallas import tpu as pltpu
from jax.sharding import PartitionSpec as P

F32, BF16 = jnp.float32, jnp.bfloat16
CLIP_EPS = 1e-30
LANES = 128
SIDE = 4
ORDERS = ((0, 1, 2), (1, 2, 0), (2, 0, 1))
VMEM_LIMIT = 63 * 1024 * 1024


class Place:
    def __init__(self):
        me = lax.axis_index("dp")
        self.core = lax.rem(me, 2)
        chip = lax.div(me, 2)
        self.at = (lax.div(chip, SIDE * SIDE), lax.rem(lax.div(chip, SIDE), SIDE), lax.rem(chip, SIDE))
        self.ways = [1 + 2 * lax.rem(way + self.core, 2) for way in range(2)]
        self.onwards = {(axis, way): self.device(axis, self.ways[way]) for axis in range(3) for way in range(2)}
        self.blocks = {
            (axis, way, hops): lax.rem(self.at[axis] + hops * (SIDE - self.ways[way]), SIDE)
            for axis in range(3)
            for way in range(2)
            for hops in range(1, 5)
        }

    def device(self, axis=None, off=0, core=None):
        at = list(self.at)
        if axis is not None:
            at[axis] = lax.rem(at[axis] + off, SIDE)
        core = self.core if core is None else core
        return {"dp": ((at[0] * SIDE + at[1]) * SIDE + at[2]) * 2 + core}

    def partner(self):
        return self.device(core=1 - self.core)

    def onward(self, way):
        return self.ways[way]

    def block(self, axis, way, hops):
        if isinstance(hops, int) and hops:
            return self.blocks[axis, way, hops]
        return lax.rem(self.at[axis] + hops * (SIDE - self.ways[way]), SIDE)


def signal_all(devices):
    barrier = pltpu.get_barrier_semaphore()
    for d in devices:
        pl.semaphore_signal(barrier, inc=1, device_id=d, device_id_type=pl.DeviceIdType.MESH)
    pl.semaphore_wait(barrier, len(devices))


def near(place):
    return [place.partner()] + [place.device(axis, off) for axis in range(3) for off in (1, SIDE - 1)]


def put(src, dst, send, recv, device):
    return pltpu.make_async_remote_copy(
        src_ref=src, dst_ref=dst, send_sem=send, recv_sem=recv, device_id=device, device_id_type=pl.DeviceIdType.MESH
    )


def ways_of(cols):
    tiles = cols // LANES
    first = (tiles + 1) // 2 * LANES
    return ((0, first), (first, cols - first))


def index(order, values):
    out = [None] * 3
    for axis, value in zip(order, values, strict=True):
        out[axis] = value
    return tuple(out)


ALL = slice(None)


class Rings:
    def __init__(self, place, rows, cols, slots, sems):
        self.place, self.rows, self.slots, self.sems = place, rows // 3, slots, sems
        self.ways = ways_of(cols)

    def part(self, t, way):
        start, width = self.ways[way]
        return pl.ds(t * self.rows, self.rows), pl.ds(start, width)

    @staticmethod
    def pairs():
        return [(t, way) for t in range(3) for way in range(2)]

    def send(self, axis, way, src, landing, key, sems):
        src = landing if src is None else src
        return put(src, landing, sems[0].at[key], sems[1].at[key], self.place.onwards[axis, way])


class First(Rings):
    @staticmethod
    def scratch(rows, cols):
        third, dma = rows // 3, pltpu.SemaphoreType.DMA
        slots = [pltpu.VMEM((3, 3, SIDE, SIDE, third, width), BF16) for _, width in ways_of(cols)]
        return [pltpu.VMEM((SIDE, SIDE, SIDE, rows, cols), BF16), *slots, dma((3, 2, 3, SIDE)), dma((3, 2, 3, SIDE))]

    @classmethod
    def of(cls, place, rows, cols, refs):
        one = cls(place, rows, cols, refs[1:3], refs[3:5])
        one.held = refs[0]
        return one

    def block(self, t, way, hops, k, c=ALL):
        order = ORDERS[t]
        return self.held.at[(*index(order, (self.place.block(order[0], way, hops), k, c)), *self.part(t, way))]

    def message(self, t, way, n, k, arriving=False):
        src = None
        if not arriving:
            src = self.block(t, way, 1, k) if isinstance(n, int) and n == 0 else self.slots[way].at[t, n - 1, k]
        return self.send(ORDERS[t][0], way, src, self.slots[way].at[t, n, k], (t, way, n, k), self.sems)

    def start(self, k):
        for t, way in self.pairs():
            self.message(t, way, 0, k).start()

    def step(self, n, k):
        for t, way in self.pairs():
            self.message(t, way, n - 1, k, arriving=True).wait_recv()
            slots = self.slots[way]
            for c in range(SIDE):
                own = self.block(t, way, n + 1, k, c)
                slots[t, n - 1, k, c] = (slots[t, n - 1, k, c].astype(F32) + own[...].astype(F32)).astype(BF16)
            pl.when(n < 3)(lambda t=t, way=way: self.message(t, way, n, k).start())

    def tick(self, i):
        pl.when(i < SIDE)(lambda: self.start(i))
        pl.when(i >= SIDE)(lambda: self.step(lax.div(i, SIDE), lax.rem(i, SIDE)))

    def results(self):
        return [slots.at[:, 2] for slots in self.slots]

    def drain(self):
        def sent(k, _):
            for t, way in self.pairs():
                self.message(t, way, 0, k).wait_send()
                lax.fori_loop(1, 3, lambda n, _: (self.message(t, way, n, k).wait_send(), 0)[1], 0)
            return 0

        lax.fori_loop(0, SIDE, sent, 0)


class Rest(Rings):
    @staticmethod
    def scratch(rows, cols):
        third, dma = rows // 3, pltpu.SemaphoreType.DMA
        shapes = [pltpu.VMEM((*lead, third, width), BF16) for lead in ((3, 3, SIDE), (3, 3)) for _, width in ways_of(cols)]
        return shapes + [dma((3, 2, 3))] * 4

    @classmethod
    def of(cls, place, rows, cols, before, refs):
        one = cls(place, rows, cols, refs[:4], refs[4:8])
        one.before = before
        return one

    def message(self, phase, t, way, n, arriving=False):
        slots = self.slots[2 * phase - 2 + way]
        axis = ORDERS[t][phase]
        if arriving:
            src = None
        elif isinstance(n, int) and n == 0:
            v = self.place.block(axis, way, 1)
            src = self.before[way].at[t, v] if phase == 1 else self.slots[way].at[t, 2, v]
        else:
            src = slots.at[t, n - 1]
        return self.send(axis, way, src, slots.at[t, n], (t, way, n), self.sems[2 * phase - 2 : 2 * phase])

    def start(self, phase):
        for t, way in self.pairs():
            self.message(phase, t, way, 0).start()

    def step1(self, n):
        for t, way in self.pairs():
            self.message(1, t, way, n - 1, arriving=True).wait_recv()
            v = self.place.block(ORDERS[t][1], way, n + 1)
            before, slots = self.before[way], self.slots[way]
            for c in range(SIDE):
                slots[t, n - 1, c] = (slots[t, n - 1, c].astype(F32) + before[t, v, c].astype(F32)).astype(BF16)
            pl.when(n < 3)(lambda t=t, way=way: self.message(1, t, way, n).start())

    def step2(self, n):
        for t, way in self.pairs():
            self.message(2, t, way, n - 1, arriving=True).wait_recv()
            v = self.place.block(ORDERS[t][2], way, n + 1)
            before, slots = self.slots[way], self.slots[2 + way]
            slots[t, n - 1] = (slots[t, n - 1].astype(F32) + before[t, 2, v].astype(F32)).astype(BF16)
            pl.when(n < 3)(lambda t=t, way=way: self.message(2, t, way, n).start())

    def tick(self, i):
        pl.when(i == 0)(lambda: self.start(1))
        pl.when((i >= 1) & (i <= 3))(lambda: self.step1(i))
        pl.when(i == 3)(lambda: self.start(2))
        pl.when((i >= 4) & (i <= 6))(lambda: self.step2(i - 3))

    def result(self, out):
        for t, way in self.pairs():
            out[self.part(t, way)] = self.slots[2 + way][t, 2]

    def drain(self):
        for t, way in self.pairs():
            for phase in (1, 2):
                for n in range(3):
                    self.message(phase, t, way, n).wait_send()


def loads_down(source, first, sems):
    return [pltpu.make_async_copy(source.at[:, :, pl.ds(64 * z, 72)], first.held.at[:, :, z], sems.at[z]) for z in range(SIDE)]


def spread(j, steps, count, tick):
    low, high = lax.div(count * j, steps), lax.div(count * (j + 1), steps)
    lax.fori_loop(low, high, lambda i, _: (tick(i), 0)[1], 0)


def copies(sources, targets, sems):
    return [pltpu.make_async_copy(s, t, sems.at[i]) for i, (s, t) in enumerate(zip(sources, targets, strict=True))]


def begin(all_copies):
    for copy in all_copies:
        copy.start()


def end(all_copies):
    for copy in all_copies:
        copy.wait()


def half_sums(rows, cols):
    return [(3, SIDE, SIDE, rows // 3, width) for _, width in ways_of(cols)]


PREV = 6
DOWN_ROWS = 33


class Gather:
    def __init__(self, place, bufs, sems, outs, copy_sems):
        self.place, self.bufs, self.sems, self.outs, self.copy_sems = place, bufs, sems, outs, copy_sems

    @staticmethod
    def scratch(down_cols):
        buf = pltpu.VMEM((2, SIDE, SIDE, SIDE, 72, down_cols), BF16)
        return [buf] + [pltpu.SemaphoreType.DMA((2, 3, 2, 6, 3))] * 4 + [pltpu.SemaphoreType.DMA((2,))] * 3

    def part(self, kind, t, way):
        rows, cols = self.bufs[kind].shape[-2:]
        start, width = ways_of(cols)[way]
        return pl.ds(t * (rows // 3), rows // 3), pl.ds(start, width)

    def behind(self, t, way, axis, hops):
        return self.place.block(ORDERS[t][axis], way, hops)

    def message(self, kind, l, t, way, line, n, hops):
        order, place = ORDERS[t], self.place
        if isinstance(line, int) and line == 0:
            axis, values = order[0], [self.behind(t, way, 0, hops), place.at[order[1]], place.at[order[2]]]
        elif isinstance(line, int) and line == 1:
            axis, values = order[1], [ALL, self.behind(t, way, 1, hops), place.at[order[2]]]
        else:
            axis, values = order[2], [ALL, self.behind(t, way, 1, line - 2), self.behind(t, way, 2, hops)]
        ref = self.bufs[kind].at[(l, *index(order, values), *self.part(kind, t, way))]
        key = (l, t, way, line, n)
        return put(ref, ref, self.sems[2 * kind].at[key], self.sems[2 * kind + 1].at[key], place.onwards[axis, way])

    def copies(self, kind, l, t, way, b, c):
        order = ORDERS[t]
        rows, cols = self.part(kind, t, way)
        at = index(order, (ALL, b, c))
        if kind == 0:
            return [lambda out: (self.bufs[0].at[(l, *at, rows, cols)], out.at[(l, *at, rows, cols)])]
        half = self.bufs[1].shape[-1]
        start, width = ways_of(half)[way]
        columns = pl.ds(pl.multiple_of(self.place.core * half + start, LANES), width)
        x, y, z = at

        def pair(out, z, count):
            src = self.bufs[1].at[l, x, y, z, pl.ds(24 * t, count), cols]
            return src, out.at[l, x, y, pl.ds(pl.multiple_of(64 * z + 24 * t, 8), count), columns]

        if t < 2:
            return [lambda out: pair(out, z, 24)]
        return [lambda out, z=z: pair(out, z, 16 if z < SIDE - 1 else 24) for z in range(SIDE)]

    def copy_out(self, kind, l, t, way, b, c):
        local, send, recv = self.copy_sems
        for pair in self.copies(kind, l, t, way, b, c):
            src, dst = pair(self.outs[kind])
            if kind:
                pltpu.make_async_copy(src, dst, local.at[kind]).start()
            put(src, dst, send.at[kind], recv.at[kind], self.place.partner()).start()

    def parts(self):
        return [(kind, t, way) for kind in range(2) for t in range(3) for way in range(2)]

    def own(self, l):
        for kind, t, way in self.parts():
            self.message(kind, l, t, way, 0, 0, 0).start()

    def start_third(self, kind, l, t, way, m):
        self.message(kind, l, t, way, 2 + m, 0, 0).start()
        self.copy_out(kind, l, t, way, self.behind(t, way, 1, m), self.place.at[ORDERS[t][2]])

    def first_axis(self):
        def step(i, _):
            n, l = 1 + lax.div(i, 2), lax.rem(i, 2)
            for kind, t, way in self.parts():
                self.message(kind, l, t, way, 0, n - 1, n).wait_recv()
                pl.when(n < 3)(lambda kind=kind, t=t, way=way: self.message(kind, l, t, way, 0, n, n).start())

                @pl.when(n == 3)
                def _(kind=kind, t=t, way=way):
                    self.message(kind, l, t, way, 1, 0, 0).start()
                    self.start_third(kind, l, t, way, 0)

            return 0

        lax.fori_loop(0, 6, step, 0)

    def other_axes(self):
        def step(i, _):
            r, l = 1 + lax.div(i, 2), lax.rem(i, 2)
            for kind, t, way in self.parts():

                @pl.when(r <= 3)
                def _(kind=kind, t=t, way=way):
                    self.message(kind, l, t, way, 1, r - 1, r).wait_recv()
                    pl.when(r < 3)(lambda: self.message(kind, l, t, way, 1, r, r).start())
                    self.start_third(kind, l, t, way, r)

                def third(m, _, kind=kind, t=t, way=way):
                    n = r - m
                    self.message(kind, l, t, way, 2 + m, n - 1, n).wait_recv()
                    pl.when(n < 3)(lambda: self.message(kind, l, t, way, 2 + m, n, n).start())
                    self.copy_out(kind, l, t, way, self.behind(t, way, 1, m), self.behind(t, way, 2, n))
                    return 0

                lax.fori_loop(jnp.maximum(r - 3, 0), jnp.minimum(r, SIDE), third, 0)
            return 0

        lax.fori_loop(0, 12, step, 0)

    def drain(self):
        local, send, recv = self.copy_sems
        half = self.bufs[1].shape[-1]
        columns = self.outs[1].at[:, :, :, :, pl.ds(0, half)]
        for kind, whole in ((0, self.outs[0]), (1, columns)):
            if kind:
                pltpu.make_async_copy(whole, whole, local.at[kind]).wait()
            copy = put(whole, whole, send.at[kind], recv.at[kind], self.place.partner())
            copy.wait_send()
            copy.wait_recv()

        def sent(i, _):
            l, n = lax.div(i, 3), lax.rem(i, 3)
            for kind, t, way in self.parts():
                for line in range(2):
                    self.message(kind, l, t, way, line, n, n).wait_send()
                lax.fori_loop(2, 6, lambda line, _: (self.message(kind, l, t, way, line, n, n).wait_send(), 0)[1], 0)
            return 0

        lax.fori_loop(0, 6, sent, 0)


def finish_kernel(count, *refs):
    sums_gu, sums_d, m_in, v_in, w_in = refs[0:2], refs[2:4], refs[4:7], refs[7:10], refs[10:13]
    own_gu, w_out, m_out, v_out = refs[13], refs[14:16], refs[16:19], refs[19:22]
    moments_gu, moments_d, old_gu, old_d, other_d, tiles = refs[22:28]
    load_sem, early_send, early_recv, norm_send, norm_recv, late_local, late_send, late_recv = refs[28:36]
    gather_refs = refs[36:]
    place = Place()
    x, y, z = place.at
    core = place.core
    gather = Gather(place, (own_gu, gather_refs[0]), gather_refs[1:5], w_out, gather_refs[5:8])
    partner = place.partner()
    gate_tiles, down_tiles = sums_gu[0].shape[1] // LANES, sums_d[0].shape[1] // LANES
    gate_stride, down_stride = 2 * gate_tiles, 4 * down_tiles
    gate_size, down_size = 12 * gate_stride, DOWN_ROWS * down_stride

    def blank(i, _):
        for which in range(2):
            moments_d[which, pl.ds(pl.multiple_of(8 * i, 8), 8), :] = jnp.zeros((8, LANES), F32)
        return 0

    lax.fori_loop(0, moments_d.shape[1] // 8, blank, 0)
    following = [place.device(2, 1, core=c) for c in range(2)]
    others = [place.device(axis, 2) for axis in range(3)] + [place.device(2, off, core=1 - core) for off in (1, SIDE - 1)]
    signal_all(near(place) + others)

    def gate_rows(i, which):
        return moments_gu.at[i, pl.ds(pl.multiple_of(which * gate_size, 8), gate_size)]

    def down_rows(i, first, rows):
        return moments_d.at[i, pl.ds(pl.multiple_of(first * down_stride, 8), rows * down_stride)]

    def columns(ref):
        half = down_tiles * LANES
        return ref.at[:, x, y, pl.ds(pl.multiple_of(64 * z, 8), 72), pl.ds(pl.multiple_of(core * half, LANES), half)]

    own_rows = PREV + 2 * z + DOWN_ROWS * core
    loads, sends = [], []
    for i, moment in enumerate((m_in, v_in)):
        for c in range(2):

            @pl.when(core == c)
            def _(i=i, moment=moment, c=c):
                pltpu.make_async_copy(moment[c], gate_rows(i, core), load_sem.at[i]).start()
                put(moment[1 - c], gate_rows(i, core), early_send.at[i], early_recv.at[i], partner).start()

        loads.append(pltpu.make_async_copy(moment[0], gate_rows(i, core), load_sem.at[i]))
        sends.append(put(moment[0], gate_rows(i, core), early_send.at[i], early_recv.at[i], partner))
        loads.append(pltpu.make_async_copy(moment[2], down_rows(i, own_rows, DOWN_ROWS), load_sem.at[2 + i]))
        loads[-1].start()
        sends.append(put(moment[2], down_rows(i, own_rows, DOWN_ROWS), early_send.at[2 + i], early_recv.at[2 + i], partner))
        sends[-1].start()
        last = moment[2].at[pl.ds((DOWN_ROWS - PREV) * down_stride, PREV * down_stride)]
        landing = down_rows(i, 2 * lax.rem(z + 1, SIDE), PREV)

        @pl.when(core == 1)
        def _(i=i, last=last, landing=landing):
            for c in range(2):
                put(last, landing, early_send.at[4 + 2 * i + c], early_recv.at[4 + i], following[c]).start()

    for l in range(2):
        sends.append(put(sums_d[l], other_d.at[l], early_send.at[8 + l], early_recv.at[6 + l], partner))
        sends[-1].start()
    for c in range(2):

        @pl.when(core == c)
        def _(c=c):
            pltpu.make_async_copy(w_in[c].at[:, x, y, z], old_gu, load_sem.at[4]).start()

    loads.append(pltpu.make_async_copy(w_in[0].at[:, x, y, z], old_gu, load_sem.at[4]))
    loads.append(pltpu.make_async_copy(columns(w_in[2]), old_d, load_sem.at[5]))
    loads[-1].start()

    squares = jnp.zeros((8, LANES), F32)
    for l in range(2):

        def of_gate_up(j, total, l=l):
            for t in range(3):
                g = sums_gu[l][pl.ds(8 * t, 8), pl.ds(pl.multiple_of(j * LANES, LANES), LANES)].astype(F32)
                total += g * g
            return total

        squares = lax.fori_loop(0, gate_tiles, of_gate_up, squares)

        def of_down(i, total, l=l):
            row = 8 * i + lax.broadcasted_iota(jnp.int32, (8, LANES), 0)
            mine = (row >= 2 * z) & (row < 2 * z + 2 * DOWN_ROWS)
            for j in range(down_tiles):
                g = sums_d[l][pl.ds(pl.multiple_of(8 * i, 8), 8), pl.ds(j * LANES, LANES)].astype(F32)
                total += jnp.where(mine, g * g, 0.0)
            return total

        squares = lax.fori_loop(0, 9, of_down, squares)
    for stage, (coordinate, size) in enumerate(((core, 2), (x, SIDE), (y, SIDE), (z, SIDE))):
        tiles[stage, coordinate] = squares
        exchanges = []
        for off in range(1, size):
            target = partner if stage == 0 else place.device(stage - 1, off)
            key = 3 * stage + off - 1
            here = tiles.at[stage, coordinate]
            exchanges.append(put(here, here, norm_send.at[key], norm_recv.at[key], target))
            exchanges[-1].start()
        for exchange in exchanges:
            exchange.wait_recv()
        for exchange in exchanges:
            exchange.wait_send()
        squares = tiles[stage, 0]
        for other in range(1, size):
            squares += tiles[stage, other]
    total = jnp.sum(jnp.sum(squares, 0, keepdims=True), 1, keepdims=True)
    factor = jnp.minimum(1.0, 0.5 * lax.rsqrt(total / count + CLIP_EPS))

    for copy in loads:
        copy.wait()
    for copy in sends:
        copy.wait_recv()
    for i in range(2):
        put(down_rows(i, 0, PREV), down_rows(i, 0, PREV), early_send.at[0], early_recv.at[4 + i], partner).wait_recv()

    def moments(ref, start, stride, g):
        rows = pl.ds(start, 8, stride=stride)
        m = 0.9 * ref[0, rows, :] + 0.1 * g
        v = 0.95 * ref[1, rows, :] + 0.05 * g * g
        ref[0, rows, :] = m
        ref[1, rows, :] = v
        return m * lax.rsqrt(v + 1e-8)

    def weight(w, step):
        w = w.astype(F32)
        return (w - 0.02 * (step + 0.1 * w)).astype(BF16)

    for l in range(2):

        def gate_up(j, _, l=l):
            lanes = pl.ds(pl.multiple_of(j * LANES, LANES), LANES)
            for t in range(3):
                rows = pl.ds(8 * t, 8)
                g = sums_gu[l][rows, lanes].astype(F32) * factor
                step = moments(moments_gu, 8 * t * gate_stride + 2 * j + l, gate_stride, g)
                gather.bufs[0][l, x, y, z, rows, lanes] = weight(old_gu[l, rows, lanes], step)
            return 0

        lax.fori_loop(0, gate_tiles, gate_up, 0, unroll=3)

        def down(i, _, l=l):
            rows = pl.ds(pl.multiple_of(8 * i, 8), 8)
            for j in range(down_tiles):
                lanes = pl.ds(j * LANES, LANES)
                start = (PREV + 8 * i) * down_stride + 2 * j + l
                g = sums_d[l][rows, lanes].astype(F32) * factor
                step = moments(moments_d, start + 2 * down_tiles * core, down_stride, g)
                gather.bufs[1][l, x, y, z, rows, lanes] = weight(old_d[l, rows, lanes], step)
            return 0

        lax.fori_loop(0, 9, down, 0)
        gather.own(l)
    for l in range(2):

        def down_other(i, _, l=l):
            rows = pl.ds(pl.multiple_of(8 * i, 8), 8)
            for j in range(down_tiles):
                start = (PREV + 8 * i) * down_stride + 2 * j + l
                g = other_d[l, rows, pl.ds(j * LANES, LANES)].astype(F32) * factor
                moments(moments_d, start + 2 * down_tiles * (1 - core), down_stride, g)
            return 0

        lax.fori_loop(0, 9, down_other, 0)

    late = []
    for i, out in enumerate((m_out, v_out)):
        for c in range(2):

            @pl.when(core == c)
            def _(i=i, out=out, c=c):
                pltpu.make_async_copy(gate_rows(i, core), out[c], late_local.at[i]).start()
                put(gate_rows(i, 1 - core), out[c], late_send.at[i], late_recv.at[i], partner).start()

        pltpu.make_async_copy(down_rows(i, own_rows, DOWN_ROWS), out[2], late_local.at[2 + i]).start()
    gather.first_axis()
    gather.other_axes()
    for i, out in enumerate((m_out, v_out)):
        pltpu.make_async_copy(gate_rows(i, core), out[0], late_local.at[i]).wait()
        pltpu.make_async_copy(down_rows(i, own_rows, DOWN_ROWS), out[2], late_local.at[2 + i]).wait()
        copy = put(gate_rows(i, 1 - core), out[0], late_send.at[i], late_recv.at[i], partner)
        copy.wait_recv()
        copy.wait_send()
    for copy in sends:
        copy.wait_send()
    for i in range(2):
        for c in range(2):

            @pl.when(core == 1)
            def _(i=i, c=c):
                rows = down_rows(i, 0, PREV)
                put(rows, rows, early_send.at[4 + 2 * i + c], early_recv.at[4 + i], following[c]).wait_send()

    gather.drain()


def finish_call(count, collective_id, sums_gu, sums_d, m, v, w):
    gate_cols, down_half = sums_gu[0].shape[1], sums_d[0].shape[1]
    operands = [*sums_gu, *sums_d, *m, *v, *w]
    hbm, vmem = pl.BlockSpec(memory_space=pltpu.HBM), pl.BlockSpec(memory_space=pltpu.VMEM)
    dma = pltpu.SemaphoreType.DMA
    gate_stride, down_stride = gate_cols // 64, down_half // 32
    scratch = [
        pltpu.VMEM((2, 24 * gate_stride, LANES), F32),
        pltpu.VMEM((2, (PREV + 72) * down_stride, LANES), F32),
        pltpu.VMEM((2, 24, gate_cols), BF16),
        pltpu.VMEM((2, 72, down_half), BF16),
        pltpu.VMEM((2, 72, down_half), BF16),
        pltpu.VMEM((4, SIDE, 8, LANES), F32),
        dma((6,)), dma((10,)), dma((8,)), dma((12,)), dma((12,)), dma((4,)), dma((2,)), dma((2,)),
    ]
    return pl.pallas_call(
        functools.partial(finish_kernel, count),
        name="finish",
        out_shape=[pltpu.VMEM(w[0].shape, BF16), *[jax.ShapeDtypeStruct(t.shape, t.dtype) for t in (w[0], w[2], *m, *v)]],
        in_specs=[vmem] * 4 + [hbm] * 9,
        out_specs=[vmem] + [hbm] * 8,
        scratch_shapes=scratch + Gather.scratch(down_half),
        compiler_params=pltpu.CompilerParams(collective_id=collective_id, has_side_effects=True, vmem_limit_bytes=26 * 1024 * 1024),
        cost_estimate=pl.CostEstimate(flops=10**9, bytes_accessed=10**8, transcendentals=0),
    )(*operands)


def write_kernel(bounces, own, other, down, gate_out, up_out, down_out, bounce, own_sem, in_sem, out_sem):
    core = lax.rem(lax.axis_index("dp"), 2)
    places = [(l, x, y) for l in range(2) for x in range(SIDE) for y in range(SIDE)]
    pieces = [(other, None, at) for at in places] + [(down, down_out, at) for at in places]

    def slot(i):
        source = pieces[i][0]
        return bounce[0 if source is other else 1].at[i % bounces]

    def read(i):
        source, _, at = pieces[i]
        return pltpu.make_async_copy(source.at[at], slot(i), in_sem.at[i % bounces])

    def write(i, out=None):
        _, to, at = pieces[i]
        return pltpu.make_async_copy(slot(i), (out if to is None else to).at[at], out_sem.at[i % bounces])

    for i in range(bounces):
        read(i).start()
    for c, (mine, others) in enumerate(((gate_out, up_out), (up_out, gate_out))):

        @pl.when(core == c)
        def _(mine=mine, others=others):
            pltpu.make_async_copy(own, mine, own_sem).start()
            for i in range(len(pieces)):
                read(i).wait()
                write(i, others).start()
                done = i - bounces // 2
                if done >= 0 and done + bounces < len(pieces):
                    write(done, others).wait()
                    read(done + bounces).start()

    for i in range(len(pieces) - bounces, len(pieces)):
        write(i, gate_out).wait()
    pltpu.make_async_copy(own, gate_out, own_sem).wait()


def write_call(own, other, down):
    hbm = pl.BlockSpec(memory_space=pltpu.HBM)
    bounces, dma = 8, pltpu.SemaphoreType.DMA
    return pl.pallas_call(
        lambda *refs: write_kernel(bounces, *refs[:6], refs[6:8], *refs[8:]),
        name="write",
        out_shape=[jax.ShapeDtypeStruct(t.shape, BF16) for t in (other, other, down)],
        in_specs=[pl.BlockSpec(memory_space=pl.ANY), hbm, hbm],
        out_specs=[hbm] * 3,
        scratch_shapes=[pltpu.VMEM((bounces, *t.shape[3:]), BF16) for t in (other, down)] + [dma, dma((bounces,)), dma((bounces,))],
        compiler_params=pltpu.CompilerParams(vmem_limit_bytes=14 * 1024 * 1024),
    )(own, other, down)


TILE = 384
ROWS = 256
TIGHT = pl.Buffered(buffer_count=1)


def dot(a, b, dims):
    return lax.dot_general(a, b, (dims, ((), ())), preferred_element_type=F32)


NN, NT, TN = ((1,), (0,)), ((1,), (1,)), ((0,), (0,))


def norm_scale(wide):
    return lax.rsqrt(jnp.mean(wide * wide, -1, keepdims=True) + 1e-6)


def in_rows(total, step, body):
    def one(i, _):
        body(pl.ds(pl.multiple_of(i * step, step), step))
        return 0

    lax.fori_loop(0, total // step, one, 0)


def clear(acc):
    def rows(r):
        acc[r, :] = jnp.zeros((8, acc.shape[1]), F32)

    in_rows(acc.shape[0], 8, rows)


def spec(shape, index_map, tight=False):
    return pl.BlockSpec(shape, index_map, pipeline_mode=TIGHT) if tight else pl.BlockSpec(shape, index_map)


def whole(shape, tight=True):
    return spec(shape, lambda j: (0,) * len(shape), tight)


HBM = pl.BlockSpec(memory_space=pltpu.HBM)


def params(collective_id=None, semantics=("arbitrary",)):
    more = {} if collective_id is None else {"collective_id": collective_id, "has_side_effects": True}
    return pltpu.CompilerParams(dimension_semantics=semantics, vmem_limit_bytes=VMEM_LIMIT, **more)


def transpose_piece(j, last, src, dst):
    def piece(i):
        at = pl.ds(pl.multiple_of(i * LANES, LANES), LANES)
        dst[at, :] = src[:, at].T

    piece(j)
    pl.when(j == last)(lambda: piece(last + 1))


def side_by_side(a, b):
    return jnp.concatenate([a, b], axis=1)


def forward_kernel(tiles, x, wg, wu, wd, gate, up, h_out, a_out, at, a, acc, p):
    j = pl.program_id(0)

    @pl.when(j == 0)
    def _():
        def rows(r):
            wide = x[r, :].astype(F32)
            a[r, :] = (wide * norm_scale(wide)).astype(BF16)

        in_rows(x.shape[0], 32, rows)
        clear(acc)

    transpose_piece(j, tiles - 1, a, at)
    both = side_by_side(wg[0], wu[0])
    slot = lax.rem(j, 2)
    for m in range(x.shape[0] // ROWS):
        r = pl.ds(m * ROWS, ROWS)
        gu = dot(a[r, :], both, NN)
        g, u = gu[:, :TILE], gu[:, TILE:]
        gate[0, r, :] = g
        up[0, r, :] = u
        p[slot, r, :] = (g * lax.logistic(g) * u).astype(BF16)

    @pl.when(slot == 1)
    def _():
        for m in range(x.shape[0] // ROWS):
            r = pl.ds(m * ROWS, ROWS)
            acc[r, :] += dot(side_by_side(p[0, r, :], p[1, r, :]), wd[0], NN)

    @pl.when(j == tiles - 1)
    def _():
        def last_down(r):
            acc[r, :] += dot(p[0, r, :], wd[0, pl.ds(0, TILE), :], NN)

        in_rows(x.shape[0], ROWS, last_down)

        def rows(r):
            h = (x[r, :].astype(F32) + acc[r, :].astype(BF16).astype(F32)).astype(BF16)
            h_out[r, :] = h
            wide = h.astype(F32)
            a_out[r, :] = (wide * norm_scale(wide)).astype(BF16)

        in_rows(x.shape[0], 32, rows)


def forward_call(x, wg, wu, wd):
    tokens, d = x.shape
    ff = wg.shape[2]
    tiles = ff // TILE
    w_in = spec((1, d, TILE), lambda j: (0, 0, j))
    return pl.pallas_call(
        functools.partial(forward_kernel, tiles),
        name="forward_0",
        grid=(tiles,),
        in_specs=[whole((tokens, d)), w_in, w_in, spec((1, 2 * TILE, d), lambda j: (0, lax.div(j, 2), 0))],
        out_specs=[spec((1, tokens, TILE), lambda j: (j, 0, 0))] * 2 + [whole((tokens, d))] * 2 + [whole((d, tokens))],
        out_shape=[jax.ShapeDtypeStruct((tiles, tokens, TILE), F32)] * 2
        + [jax.ShapeDtypeStruct((tokens, d), BF16)] * 2
        + [jax.ShapeDtypeStruct((d, tokens), BF16)],
        scratch_shapes=[pltpu.VMEM((tokens, d), BF16), pltpu.VMEM((tokens, d), F32), pltpu.VMEM((2, tokens, TILE), BF16)],
        compiler_params=params(),
    )(x, wg, wu, wd)


class PairSum:
    def __init__(self, place, tiles, landing, stage, send, recv):
        self.place, self.tiles, self.landing, self.stage, self.send, self.recv = place, tiles, landing, stage, send, recv

    @staticmethod
    def scratch(tiles, rows, cols):
        dma = pltpu.SemaphoreType.DMA
        return [pltpu.VMEM((tiles, rows, cols), BF16), pltpu.VMEM((2, rows, cols), BF16), dma((2,)), dma((tiles,))]

    def copy(self, i):
        slot = lax.rem(i, 2)
        return put(self.stage.at[slot], self.landing.at[i], self.send.at[slot], self.recv.at[i], self.place.partner())

    def reserve(self, i):
        pl.when(i >= 2)(lambda: self.copy(i - 2).wait_send())
        return self.stage.at[lax.rem(i, 2)]

    def drain(self):
        for i in (self.tiles - 2, self.tiles - 1):
            self.copy(i).wait_send()


def hidden_back(gate, up, dp):
    dp = dp.astype(F32)
    s = lax.logistic(gate)
    act = gate * s
    return (act * up).astype(BF16), (dp * up * (s + act * (1.0 - s))).astype(BF16), (dp * act).astype(BF16)


def down_gradient(j, tiles, pair, p, dy, half, out):
    core = pair.place.core

    def columns(c):
        return pl.ds(pl.multiple_of(c * half, LANES), half)

    @pl.when(j < tiles)
    def _():
        slot = pair.reserve(j)
        slot[...] = dot(p[lax.rem(j, 2)], dy[:, columns(1 - core)], TN).astype(BF16)
        pair.copy(j).start()

    @pl.when(j >= 1)
    def _():
        pair.copy(j - 1).wait_recv()
        own = dot(p[lax.rem(j - 1, 2)], dy[:, columns(core)], TN)
        out[...] = (own + pair.landing[j - 1].astype(F32)).astype(BF16)

    pl.when(j == tiles)(pair.drain)


def layer_kernel(tiles, a, dy, wg, wu, wd, dgu, at, out, p, dps, *rest):
    j = pl.program_id(0)
    place = Place()
    pair = PairSum(place, tiles, *rest)
    pl.when(j == 0)(lambda: signal_all([place.partner()]))
    two_tiles_of_dp(j, tiles, dy, wd, dps)

    @pl.when(j < tiles)
    def _():
        transpose_piece(j, tiles - 1, a, at)
        slot = lax.rem(j, 2)
        both = side_by_side(wg[0], wu[0])
        for m in range(a.shape[0] // ROWS):
            r = pl.ds(m * ROWS, ROWS)
            gu = dot(a[r, :], both, NN)
            p[slot, r, :], dgu[0, 0, r, :], dgu[0, 1, r, :] = hidden_back(gu[:, :TILE], gu[:, TILE:], dps[slot, r, :])

    down_gradient(j, tiles, pair, p, dy, dy.shape[1] // 2, out)


def two_tiles_of_dp(j, tiles, dy, wd, dps):
    @pl.when((lax.rem(j, 2) == 0) & (j < tiles - 1))
    def _():
        for m in range(dy.shape[0] // ROWS):
            r = pl.ds(m * ROWS, ROWS)
            dp = dot(dy[r, :], wd[0], NT).astype(BF16)
            dps[0, r, :] = dp[:, :TILE]
            dps[1, r, :] = dp[:, TILE:]

    @pl.when(j == tiles - 1)
    def _():
        def one_tile(r):
            dps[0, r, :] = dot(dy[r, :], wd[0, pl.ds(0, TILE), :], NT).astype(BF16)

        in_rows(dy.shape[0], ROWS, one_tile)


def clip(tiles, back=0):
    return lambda j: jnp.clip(j - back, 0, tiles - 1)


def layer_call(collective_id, a, dy, wg, wu, wd):
    tokens, d = a.shape
    ff = wg.shape[2]
    tiles, half = ff // TILE, d // 2
    now, before = clip(tiles), clip(tiles, 1)
    w_in = spec((1, d, TILE), lambda j: (1, 0, now(j)))
    return pl.pallas_call(
        functools.partial(layer_kernel, tiles),
        name="layer_1",
        grid=(tiles + 1,),
        in_specs=[whole((tokens, d))] * 2 + [w_in, w_in, spec((1, 2 * TILE, d), lambda j: (1, lax.div(now(j), 2), 0))],
        out_specs=[spec((1, 2, tokens, TILE), lambda j: (now(j), 0, 0, 0)), whole((d, tokens)), spec((TILE, half), lambda j: (before(j), 0))],
        out_shape=[
            jax.ShapeDtypeStruct((tiles, 2, tokens, TILE), BF16),
            jax.ShapeDtypeStruct((d, tokens), BF16),
            jax.ShapeDtypeStruct((ff, half), BF16),
        ],
        scratch_shapes=[pltpu.VMEM((2, tokens, TILE), BF16)] * 2 + PairSum.scratch(tiles, TILE, half),
        compiler_params=params(collective_id),
    )(a, dy, wg, wu, wd)


GATE_ROWS, DOWN_WINDOW = 24, 72
RING = 6


def second(t, v, rest=ALL):
    return (rest, v) if t == 1 else (v, rest)


class Stream:
    def __init__(self, place, tiles, phases, refs):
        self.place, self.tiles, self.phases, self.rows = place, tiles, phases, GATE_ROWS // 3
        self.held, self.slots, self.send, self.recv = refs[0], refs[1 : 1 + 2 * phases], refs[-2], refs[-1]
        self.ways = ways_of(TILE)

    @staticmethod
    def scratch(tiles, phases):
        third, dma = GATE_ROWS // 3, pltpu.SemaphoreType.DMA
        leads = [(3, 3, tiles, SIDE, SIDE), (3, 3, tiles, SIDE), (3, 3, tiles)][:phases]
        slots = [pltpu.VMEM((*lead, third, width), BF16) for lead in leads for _, width in ways_of(TILE)]
        return [pltpu.VMEM((RING, SIDE, SIDE, SIDE, GATE_ROWS, TILE), BF16), *slots, dma((tiles, 7)), dma((tiles, 7))]

    def part(self, t, way):
        start, width = self.ways[way]
        return pl.ds(t * self.rows, self.rows), pl.ds(start, width)

    def own(self, c, t, way, hops, b=ALL, d=ALL):
        at = index(ORDERS[t], (self.place.block(ORDERS[t][0], way, hops), ALL, ALL))
        axes = [i for i in range(3) if i != ORDERS[t][0]]
        at = list(at)
        at[axes[0]], at[axes[1]] = b, d
        return self.held.at[(lax.rem(c, RING), *at, *self.part(t, way))]

    def copy(self, phase, t, way, n, c, first=False):
        axis = ORDERS[t][phase]
        slots = self.slots[2 * phase + way]
        if not first:
            src = slots.at[t, n - 1, c]
        elif phase == 0:
            src = self.own(c, t, way, 1)
        else:
            src = self.slots[way].at[(t, 2, c, *second(t, self.place.block(axis, way, 1)))]
        key = (c, 3 * phase + n)
        return put(src, slots.at[t, n, c], self.send.at[key], self.recv.at[key], self.place.onwards[axis, way])

    def direct(self, t, way, off, c):
        axis = ORDERS[t][2]
        v = lax.rem(self.place.at[axis] + off, SIDE)
        src, dst = self.slots[2 + way].at[t, 2, c, v], self.slots[4 + way].at[t, off - 1, c]
        return put(src, dst, self.send.at[c, 6], self.recv.at[c, 6], self.place.device(axis, off))

    def pairs(self):
        return [(t, way) for t in range(3) for way in range(2)]

    def all_of(self, phase):
        return self.held.at[(0,) * (phase + 2)] if phase < 2 else self.held.at[0, 0, 0, pl.ds(0, 3)]

    def begin(self, phase, c):
        for t, way in self.pairs():
            if phase < 2:
                self.copy(phase, t, way, 0, c, first=True).start()
            else:
                for off in range(1, SIDE):
                    self.direct(t, way, off, c).start()

    def add(self, phase, t, way, n, c):
        slots = self.slots[2 * phase + way]
        v = self.place.block(ORDERS[t][phase], way, n + 1)

        def one(at, other):
            at = (t, n - 1, c, *at)
            slots[at] = (slots[at].astype(F32) + other[...].astype(F32)).astype(BF16)

        if phase == 0:
            for b in range(SIDE):
                for d in range(SIDE):
                    one((b, d), self.own(c, t, way, n + 1, b, d))
        else:
            for d in range(SIDE):
                one((d,), self.slots[way].at[(t, 2, c, *second(t, v, d))])

    def stage(self, s, c, out):
        phase, n = (s - 1) // 3, (s - 1) % 3 + 1
        whole_stage = self.all_of(phase)
        pltpu.make_async_copy(whole_stage, whole_stage, self.recv.at[c, s - 1]).wait()
        if phase == 2:
            for t, way in self.pairs():
                total = self.slots[2 + way][t, 2, c, self.place.at[ORDERS[t][2]]].astype(F32)
                for i in range(3):
                    total += self.slots[4 + way][t, i, c].astype(F32)
                rows, _ = self.part(t, way)
                start, width = self.ways[way]
                out[rows, pl.ds(pl.multiple_of(c * TILE + start, LANES), width)] = total.astype(BF16)
            return
        for t, way in self.pairs():
            self.add(phase, t, way, n, c)
            if n < 3:
                self.copy(phase, t, way, n, c).start()
        if n == 3 and phase + 1 < self.phases:
            self.begin(phase + 1, c)

    def sent(self, phase, n, c):
        whole_stage = self.all_of(phase)
        pltpu.make_async_copy(whole_stage, whole_stage, self.send.at[c, 3 * phase + n]).wait()

    def count(self):
        return 3 if self.phases == 1 else 7

    def keep(self, c):
        pl.when(c >= RING)(lambda: self.sent(0, 0, c - RING))
        return self.held.at[lax.rem(c + RING, RING)]

    def run(self, s, c, out):
        act = (lambda: self.begin(0, c)) if s == 0 else (lambda: self.stage(s, c, out))
        pl.when((c >= 0) & (c < self.tiles))(act)

    def early(self, j, out=None):
        for s in range(self.count(), 1, -1):
            self.run(s, j - 3 - s, out)

    def late(self, j, out=None):
        self.run(0, j - 2, out)
        self.run(1, j - 3, out)

    def last_step(self):
        return self.tiles - 1 + 3 + self.count()

    def drain(self):
        def each(c, _):
            pl.when(c >= self.tiles - RING)(lambda: self.sent(0, 0, c))
            for i in range(1, self.count()):
                self.sent(i // 3, i % 3, c)
            return 0

        lax.fori_loop(0, self.tiles, each, 0)

    def results(self):
        return [self.slots[way].at[:, 2] for way in range(2)]


def stream_halves(tiles):
    return [(3, tiles, SIDE, SIDE, GATE_ROWS // 3, width) for _, width in ways_of(TILE)]


class StreamRest:
    def __init__(self, place, tiles, before, refs):
        self.place, self.tiles, self.before, self.slots, self.sems = place, tiles, before, refs[:4], refs[4:8]
        self.rows, self.ways = GATE_ROWS // 3, ways_of(TILE)

    @staticmethod
    def scratch(tiles):
        third, dma = GATE_ROWS // 3, pltpu.SemaphoreType.DMA
        shapes = [pltpu.VMEM((3, 3, *lead, third, width), BF16) for lead in ((tiles, SIDE), (tiles,)) for _, width in ways_of(TILE)]
        return shapes + [dma((3, 2, 3))] * 4

    def pairs(self):
        return [(t, way) for t in range(3) for way in range(2)]

    def message(self, phase, t, way, n, arriving=False):
        slots = self.slots[2 * phase - 2 + way]
        axis = ORDERS[t][phase]
        if arriving:
            src = slots.at[t, n]
        elif isinstance(n, int) and n == 0:
            v = self.place.block(axis, way, 1)
            src = self.before[way].at[(t, ALL, *second(t, v))] if phase == 1 else self.slots[way].at[t, 2, :, v]
        else:
            src = slots.at[t, n - 1]
        send, recv = self.sems[2 * phase - 2 : 2 * phase]
        key = (t, way, n)
        return put(src, slots.at[t, n], send.at[key], recv.at[key], self.place.onwards[axis, way])

    def start(self, phase):
        for t, way in self.pairs():
            self.message(phase, t, way, 0).start()

    def step(self, phase, n):
        for t, way in self.pairs():
            self.message(phase, t, way, n - 1, arriving=True).wait_recv()
            v = self.place.block(ORDERS[t][phase], way, n + 1)
            slots = self.slots[2 * phase - 2 + way]

            def add(c, _, t=t, way=way, v=v, slots=slots):
                for d in range(SIDE if phase == 1 else 1):
                    at = (t, n - 1, c, d) if phase == 1 else (t, n - 1, c)
                    other = self.before[way].at[(t, c, *second(t, v, d))] if phase == 1 else self.slots[way].at[t, 2, c, v]
                    slots[at] = (slots[at].astype(F32) + other[...].astype(F32)).astype(BF16)
                return 0

            lax.fori_loop(0, self.tiles, add, 0)
            pl.when(n < 3)(lambda t=t, way=way: self.message(phase, t, way, n).start())

    def tick(self, i):
        pl.when(i == 0)(lambda: self.start(1))
        pl.when((i >= 1) & (i <= 3))(lambda: self.step(1, i))
        pl.when(i == 3)(lambda: self.start(2))
        pl.when((i >= 4) & (i <= 6))(lambda: self.step(2, i - 3))

    def result(self, out):
        def one(c, _):
            for t, way in self.pairs():
                start, width = self.ways[way]
                lanes = pl.ds(pl.multiple_of(c * TILE + start, LANES), width)
                out[pl.ds(t * self.rows, self.rows), lanes] = self.slots[2 + way][t, 2, c]
            return 0

        lax.fori_loop(0, self.tiles, one, 0)

    def drain(self):
        for t, way in self.pairs():
            for phase in (1, 2):
                for n in range(3):
                    self.message(phase, t, way, n).wait_send()


BLOCK_ROWS = SIDE * SIDE * GATE_ROWS


def gate_up_kernel(tiles, phases, cols, at, ahead, behind, *rest):
    j = pl.program_id(0)
    place = Place()
    core = place.core
    if phases == 1:
        outs, out, rest = rest[:2], None, rest[2:]
    else:
        sum_down, out, out_down, rest = rest[0], rest[1], rest[2], rest[3:]
    pair = PairSum(place, tiles, *rest[:4])
    stream = Stream(place, tiles, phases, rest[4 : 4 + 3 + 2 * phases])
    rest = rest[4 + 3 + 2 * phases :]
    if phases == 3:
        first = First.of(place, DOWN_WINDOW, cols, rest[1:6])
        down = Rest.of(place, DOWN_WINDOW, cols, first.results(), rest[6:14])
        loads = loads_down(sum_down, first, rest[0])

    @pl.when(j == 0)
    def _():
        opposite = [place.device(axis, 2) for axis in range(3)] if phases == 3 else []
        signal_all(near(place) + opposite)
        if phases == 3:
            begin(loads)

    stream.early(j, out)

    pl.when((j >= 2) & (j <= tiles + 1))(lambda: pair.copy(j - 2).wait_recv())

    @pl.when(j <= tiles + 1)
    def _():
        slot, kept = pair.reserve(j), stream.keep(j - 2)
        both = side_by_side(ahead[0, 1 - core], behind[0, core])
        landed = lax.rem(j + tiles - 2, tiles)
        for m in range(SIDE):
            r = pl.ds(m * BLOCK_ROWS, BLOCK_ROWS)
            tile = dot(at[r, :], both, NN)
            slot[r, :] = tile[:, :TILE].astype(BF16)
            total = (tile[:, TILE:] + pair.landing[landed, r, :].astype(F32)).astype(BF16)
            kept[m] = total.reshape(SIDE, SIDE, GATE_ROWS, TILE)

    pl.when(j < tiles)(lambda: pair.copy(j).start())
    stream.late(j, out)
    if phases == 3:
        pl.when(j == 0)(lambda: end(loads))
        pl.when(j < 8)(lambda: spread(j, 8, 16, first.tick))
        pl.when(j >= 8)(lambda: down.tick(j - 8))
        pl.when(j == 15)(lambda: down.result(out_down))

    @pl.when(j == stream.last_step())
    def _():
        if phases == 1:
            saves = copies(stream.results(), outs, rest[0])
            begin(saves)
            stream.drain()
            end(saves)
        else:
            stream.drain()
            first.drain()
            down.drain()


def gate_up_call(name, collective_id, phases, at, dgu, *sum_down):
    d, tokens = at.shape
    tiles, cols, dma = dgu.shape[0], d // 2, pltpu.SemaphoreType.DMA
    ff = tiles * TILE
    now, before = clip(tiles), clip(tiles, 2)
    if phases == 1:
        shapes = stream_halves(tiles)
        out_specs, more = [HBM] * 2, [dma((2,))]
    else:
        shapes = [(GATE_ROWS, ff), (DOWN_WINDOW, cols)]
        out_specs = [whole(s) for s in shapes]
        more = [dma((SIDE,)), *First.scratch(DOWN_WINDOW, cols), *Rest.scratch(DOWN_WINDOW, cols)]
    return pl.pallas_call(
        functools.partial(gate_up_kernel, tiles, phases, cols),
        name=name,
        grid=(tiles + (6 if phases == 1 else 10),),
        in_specs=[
            whole((d, tokens)),
            spec((1, 2, tokens, TILE), lambda j: (now(j), 0, 0, 0)),
            spec((1, 2, tokens, TILE), lambda j: (before(j), 0, 0, 0)),
            *[HBM] * len(sum_down),
        ],
        out_specs=out_specs,
        out_shape=[jax.ShapeDtypeStruct(s, BF16) for s in shapes],
        scratch_shapes=[*PairSum.scratch(tiles, d, TILE), *Stream.scratch(tiles, phases), *more],
        compiler_params=params(collective_id),
    )(at, dgu, dgu, *sum_down)


def gate_up_first_kernel(tiles, cols, at, ahead, behind, sum_down, out, half0, half1, *rest):
    j = pl.program_id(0)
    place = Place()
    core = place.core
    pair = PairSum(place, tiles, *rest[:4])
    first = First.of(place, DOWN_WINDOW, cols, rest[4:9])
    load_sem, save_sem = rest[9:11]
    loads = loads_down(sum_down, first, load_sem)

    @pl.when(j == 0)
    def _():
        signal_all(near(place))
        begin(loads)

    pl.when(j >= 2)(lambda: pair.copy(j - 2).wait_recv())
    slot = pair.reserve(j)
    both = side_by_side(ahead[0, 1 - core], behind[0, core])
    landed = lax.rem(j + tiles - 2, tiles)
    for m in range(at.shape[0] // ROWS):
        r = pl.ds(m * ROWS, ROWS)
        tile = dot(at[r, :], both, NN)
        slot[r, :] = tile[:, :TILE].astype(BF16)
        out[r, :] = (tile[:, TILE:] + pair.landing[landed, r, :].astype(F32)).astype(BF16)
    pl.when(j < tiles)(lambda: pair.copy(j).start())

    pl.when(j == 0)(lambda: end(loads))
    spread(j, tiles + 2, 16, first.tick)

    @pl.when(j == tiles + 1)
    def _():
        saves = copies(first.results(), (half0, half1), save_sem)
        begin(saves)
        first.drain()
        end(saves)


def gate_up_first_call(name, collective_id, at, dgu, sum_down):
    d, tokens = at.shape
    tiles, cols, dma = dgu.shape[0], sum_down.shape[-1], pltpu.SemaphoreType.DMA
    now, before = clip(tiles), clip(tiles, 2)
    return pl.pallas_call(
        functools.partial(gate_up_first_kernel, tiles, cols),
        name=name,
        grid=(tiles + 2,),
        in_specs=[
            whole((d, tokens)),
            spec((1, 2, tokens, TILE), lambda j: (now(j), 0, 0, 0)),
            spec((1, 2, tokens, TILE), lambda j: (before(j), 0, 0, 0)),
            HBM,
        ],
        out_specs=[spec((d, TILE), lambda j: (0, before(j))), HBM, HBM],
        out_shape=[jax.ShapeDtypeStruct((d, tiles * TILE), BF16)]
        + [jax.ShapeDtypeStruct(s, BF16) for s in half_sums(DOWN_WINDOW, cols)],
        scratch_shapes=[*PairSum.scratch(tiles, d, TILE), *First.scratch(DOWN_WINDOW, cols), dma((SIDE,)), dma((2,))],
        compiler_params=params(collective_id),
    )(at, dgu, dgu, sum_down)


def column_halves(cols):
    return ways_of(cols)


def load_columns(source, first, part, sem):
    start, width = part
    return [pltpu.make_async_copy(source.at[:, :, :, :, pl.ds(start, width)], first.held, sem)]


def middle_kernel(steps, ff, down_cols, dgu, wg, wu, h, dy, sum_gu, down0, down1, dh, out_down, half0, half1, acc_g, acc_u, *rest):
    j = pl.program_id(0)
    place = Place()
    part = column_halves(ff)[0]
    first = First.of(place, GATE_ROWS, part[1], rest[:5])
    before = rest[5:7]
    down = Rest.of(place, DOWN_WINDOW, down_cols, before, rest[7:15])
    load_sem, save_sem = rest[15:17]
    loads = copies((down0, down1), before, load_sem) + load_columns(sum_gu, first, part, load_sem.at[2])

    @pl.when(j == 0)
    def _():
        signal_all(near(place))
        begin(loads)
        clear(acc_g)
        clear(acc_u)

    def add_up(r, two):
        for which, (acc, w) in enumerate(((acc_g, wg), (acc_u, wu))):
            if two:
                acc[r, :] += dot(side_by_side(dgu[0, which, r, :], dgu[1, which, r, :]), w[0], NT)
            else:
                acc[r, :] += dot(dgu[0, which, r, :], w[0, :, pl.ds(0, TILE)], NT)

    pl.when(j < steps - 1)(lambda: in_rows(h.shape[0], 2 * ROWS, lambda r: add_up(r, True)))
    pl.when(j == steps - 1)(lambda: in_rows(h.shape[0], ROWS, lambda r: add_up(r, False)))

    pl.when(j == 0)(lambda: end(loads))
    down.tick(j)
    spread(j, steps, 16, first.tick)

    @pl.when(j == steps - 1)
    def _():
        lax.fori_loop(steps, 7, lambda i, _: (down.tick(i), 0)[1], 0)
        saves = copies(first.results(), (half0, half1), save_sem)
        begin(saves)
        down.result(out_down)

        def rows(r):
            wide = h[r, :].astype(F32)
            scale = norm_scale(wide)
            da = (acc_g[r, :].astype(BF16).astype(F32) + acc_u[r, :].astype(BF16).astype(F32)).astype(BF16).astype(F32)
            back = scale * da - wide * (scale * scale * scale * jnp.mean(da * wide, -1, keepdims=True))
            dh[r, :] = (dy[r, :].astype(F32) + back.astype(BF16).astype(F32)).astype(BF16)

        in_rows(h.shape[0], 32, rows)
        first.drain()
        down.drain()
        end(saves)


def middle_call(collective_id, dgu, wg, wu, h, dy, sum_gu, down_halves):
    tokens, d = h.shape
    tiles, dma, down_cols = dgu.shape[0], pltpu.SemaphoreType.DMA, d // 2
    ff = tiles * TILE
    steps = (tiles + 1) // 2
    width = column_halves(ff)[0][1]
    w_in = spec((1, d, 2 * TILE), lambda j: (1, 0, j))
    return pl.pallas_call(
        functools.partial(middle_kernel, steps, ff, down_cols),
        name="middle",
        grid=(steps,),
        in_specs=[spec((2, 2, tokens, TILE), lambda j: (j, 0, 0, 0)), w_in, w_in, whole((tokens, d)), whole((tokens, d))] + [HBM] * 3,
        out_specs=[whole((tokens, d)), whole((DOWN_WINDOW, down_cols)), HBM, HBM],
        out_shape=[jax.ShapeDtypeStruct(s, BF16) for s in ((tokens, d), (DOWN_WINDOW, down_cols), *half_sums(GATE_ROWS, width))],
        scratch_shapes=[pltpu.VMEM((tokens, d), F32)] * 2
        + First.scratch(GATE_ROWS, width)
        + [pltpu.VMEM(t.shape, BF16) for t in down_halves]
        + Rest.scratch(DOWN_WINDOW, down_cols)
        + [dma((3,)), dma((2,))],
        compiler_params=params(collective_id),
    )(dgu, wg, wu, h, dy, sum_gu, *down_halves)


def back_kernel(tiles, ff, dh, gate, up, wd, gate0, gate1, sum_gu, dgu, out, out_gu, p, dps, *rest):
    j = pl.program_id(0)
    place = Place()
    core, half = place.core, dh.shape[1] // 2
    parts = column_halves(ff)
    pair = PairSum(place, tiles, *rest[:4])
    before = rest[4:6]
    rest_a = Rest.of(place, GATE_ROWS, parts[0][1], before, rest[6:14])
    first = First.of(place, GATE_ROWS, parts[1][1], rest[14:19])
    rest_b = Rest.of(place, GATE_ROWS, parts[1][1], first.results(), rest[19:27])
    load_sem = rest[27]
    loads = copies((gate0, gate1), before, load_sem) + load_columns(sum_gu, first, parts[1], load_sem.at[2])

    @pl.when(j == 0)
    def _():
        signal_all(near(place))
        begin(loads)

    two_tiles_of_dp(j, tiles, dh, wd, dps)
    pl.when(j >= 2)(lambda: pair.copy(j - 2).wait_recv())
    tile = jnp.minimum(j, tiles - 1)
    ours = p[lax.rem(j + 1, 3)]
    for m in range(dh.shape[0] // ROWS):
        r = pl.ds(m * ROWS, ROWS)
        p[lax.rem(tile, 3), r, :], dgu[0, 0, r, :], dgu[0, 1, r, :] = hidden_back(gate[0, r, :], up[0, r, :], dps[lax.rem(tile, 2), r, :])
    own = dot(ours, dh[:, pl.ds(pl.multiple_of(core * half, LANES), half)], TN)
    out[...] = (own + pair.landing[lax.rem(j + tiles - 2, tiles)].astype(F32)).astype(BF16)

    @pl.when(j < tiles)
    def _():
        slot = pair.reserve(j)
        slot[...] = dot(p[lax.rem(j, 3)], dh[:, pl.ds(pl.multiple_of((1 - core) * half, LANES), half)], TN).astype(BF16)
        pair.copy(j).start()

    pl.when(j == 0)(lambda: end(loads))
    rest_a.tick(j)
    pl.when(j < 6)(lambda: spread(j, 6, 16, first.tick))
    pl.when(j >= 5)(lambda: rest_b.tick(j - 5))

    @pl.when(j == tiles + 1)
    def _():
        for sums, (start, width) in ((rest_a, parts[0]), (rest_b, parts[1])):
            sums.result(out_gu.at[:, pl.ds(start, width)])
        pair.drain()
        for sums in (rest_a, first, rest_b):
            sums.drain()


def back_call(collective_id, dh, gate, up, wd, sum_gu, gate_halves):
    tokens, d = dh.shape
    tiles, half, dma = gate.shape[0], d // 2, pltpu.SemaphoreType.DMA
    ff = tiles * TILE
    now, before = clip(tiles), clip(tiles, 2)
    tile = spec((1, tokens, TILE), lambda j: (now(j), 0, 0))
    parts = column_halves(ff)
    return pl.pallas_call(
        functools.partial(back_kernel, tiles, ff),
        name="back_0",
        grid=(tiles + 2,),
        in_specs=[whole((tokens, d)), tile, tile, spec((1, 2 * TILE, d), lambda j: (0, lax.div(now(j), 2), 0)), HBM, HBM, HBM],
        out_specs=[
            spec((1, 2, tokens, TILE), lambda j: (now(j), 0, 0, 0)),
            spec((TILE, half), lambda j: (before(j), 0)),
            whole((GATE_ROWS, ff)),
        ],
        out_shape=[jax.ShapeDtypeStruct(s, BF16) for s in ((tiles, 2, tokens, TILE), (ff, half), (GATE_ROWS, ff))],
        scratch_shapes=[pltpu.VMEM((3, tokens, TILE), BF16), pltpu.VMEM((2, tokens, TILE), BF16)]
        + PairSum.scratch(tiles, TILE, half)
        + [pltpu.VMEM(t.shape, BF16) for t in gate_halves]
        + Rest.scratch(GATE_ROWS, parts[0][1])
        + First.scratch(GATE_ROWS, parts[1][1])
        + Rest.scratch(GATE_ROWS, parts[1][1])
        + [dma((3,))],
        compiler_params=params(collective_id),
    )(dh, gate, up, wd, *gate_halves, sum_gu)


def flat(m):
    layers, rows, cols = m.shape
    split = m.transpose(1, 0, 2).reshape(rows, layers, cols // LANES, LANES)
    return with_layout_constraint(split, Layout((0, 2, 1, 3))).transpose(0, 2, 1, 3).reshape(-1, LANES)


def unflat(f, shape):
    layers, rows, cols = shape
    split = f.reshape(rows, cols // LANES, layers, LANES).transpose(0, 2, 1, 3)
    return with_layout_constraint(split, Layout((0, 2, 1, 3))).reshape(rows, layers, cols).transpose(1, 0, 2)


def solution(mesh):
    def body(x, dy, wg, wu, wd, mg, mu, md, vg, vu, vd):
        layers, d, ff = wg.shape
        x, dy = x[0], dy[0]
        windows = (SIDE, SIDE, 4 * 66, d // 2)
        gate0, up0, h1, a1, a0t = forward_call(x, wg, wu, wd)
        dgu1, a1t, down1 = layer_call(1, a1, dy, wg, wu, wd)
        blocks = (SIDE, SIDE, SIDE, GATE_ROWS, ff)
        gu1, *down_halves = gate_up_first_call("gate_up_1", 2, a1t, dgu1, down1.reshape(windows))
        gu1 = gu1.reshape(blocks)
        dh1, sum_down1, *gate_halves = middle_call(3, dgu1, wg, wu, h1, dy, gu1, down_halves)
        dgu0, down0, sum_gu1 = back_call(4, dh1, gate0, up0, wd, gu1, gate_halves)
        sum_gu0, sum_down0 = gate_up_call("gate_up_0", 5, 3, a0t, dgu0, down0.reshape(windows))

        views = [(2, SIDE, SIDE, SIDE, GATE_ROWS, ff)] * 2 + [(2, SIDE, SIDE, 4 * 66, d)]
        w = [t.reshape(view) for t, view in zip((wg, wu, wd), views, strict=True)]
        m, v = [flat(t) for t in (mg, mu, md)], [flat(t) for t in (vg, vu, vd)]
        own, other, down, *moments = finish_call(3 * layers * d * ff, 6, [sum_gu0, sum_gu1], [sum_down0, sum_down1], m, v, w)
        out = [*write_call(own, other, down), *moments]
        new = [t.reshape(like.shape) for t, like in zip(out[:3], (wg, wu, wd), strict=True)]
        return (*new, *[unflat(t, like.shape) for t, like in zip(out[3:], (mg, mu, md, vg, vu, vd), strict=True)])

    shard = P(None, "dp", None)
    return jax.shard_map(
        body,
        mesh=mesh,
        in_specs=(P(("rep", "dp")), P(("rep", "dp")), P(), P(), P(), *[shard] * 6),
        out_specs=(P("rep"), P("rep"), P("rep"), *[P("rep", "dp", None)] * 6),
        check_vma=False,
    )
```

```python
import functools

import jax
import jax.numpy as jnp
from jax import lax
from jax.experimental import pallas as pl
from jax.experimental.layout import Layout, with_layout_constraint
from jax.experimental.pallas import tpu as pltpu
from jax.sharding import PartitionSpec as P

F32, BF16 = jnp.float32, jnp.bfloat16
CLIP_EPS = 1e-30
LANES = 128
SIDE = 4
ORDERS = ((0, 1, 2), (1, 2, 0), (2, 0, 1))
VMEM_LIMIT = 63 * 1024 * 1024


class Place:
    def __init__(self):
        me = lax.axis_index("dp")
        self.core = lax.rem(me, 2)
        chip = lax.div(me, 2)
        self.at = (lax.div(chip, SIDE * SIDE), lax.rem(lax.div(chip, SIDE), SIDE), lax.rem(chip, SIDE))
        self.ways = [1 + 2 * lax.rem(way + self.core, 2) for way in range(2)]
        self.onwards = {(axis, way): self.device(axis, self.ways[way]) for axis in range(3) for way in range(2)}
        self.blocks = {
            (axis, way, hops): lax.rem(self.at[axis] + hops * (SIDE - self.ways[way]), SIDE)
            for axis in range(3)
            for way in range(2)
            for hops in range(1, 5)
        }

    def device(self, axis=None, off=0, core=None):
        at = list(self.at)
        if axis is not None:
            at[axis] = lax.rem(at[axis] + off, SIDE)
        core = self.core if core is None else core
        return {"dp": ((at[0] * SIDE + at[1]) * SIDE + at[2]) * 2 + core}

    def partner(self):
        return self.device(core=1 - self.core)

    def onward(self, way):
        return self.ways[way]

    def block(self, axis, way, hops):
        if isinstance(hops, int) and hops:
            return self.blocks[axis, way, hops]
        return lax.rem(self.at[axis] + hops * (SIDE - self.ways[way]), SIDE)


def signal_all(devices):
    barrier = pltpu.get_barrier_semaphore()
    for d in devices:
        pl.semaphore_signal(barrier, inc=1, device_id=d, device_id_type=pl.DeviceIdType.MESH)
    pl.semaphore_wait(barrier, len(devices))


def near(place):
    return [place.partner()] + [place.device(axis, off) for axis in range(3) for off in (1, SIDE - 1)]


def put(src, dst, send, recv, device):
    return pltpu.make_async_remote_copy(
        src_ref=src, dst_ref=dst, send_sem=send, recv_sem=recv, device_id=device, device_id_type=pl.DeviceIdType.MESH
    )


def ways_of(cols):
    tiles = cols // LANES
    first = (tiles + 1) // 2 * LANES
    return ((0, first), (first, cols - first))


def index(order, values):
    out = [None] * 3
    for axis, value in zip(order, values, strict=True):
        out[axis] = value
    return tuple(out)


ALL = slice(None)


class Rings:
    def __init__(self, place, rows, cols, slots, sems):
        self.place, self.rows, self.slots, self.sems = place, rows // 3, slots, sems
        self.ways = ways_of(cols)

    def part(self, t, way):
        start, width = self.ways[way]
        return pl.ds(t * self.rows, self.rows), pl.ds(start, width)

    @staticmethod
    def pairs():
        return [(t, way) for t in range(3) for way in range(2)]

    def send(self, axis, way, src, landing, key, sems):
        src = landing if src is None else src
        return put(src, landing, sems[0].at[key], sems[1].at[key], self.place.onwards[axis, way])


class First(Rings):
    @staticmethod
    def scratch(rows, cols):
        third, dma = rows // 3, pltpu.SemaphoreType.DMA
        slots = [pltpu.VMEM((3, 3, SIDE, SIDE, third, width), BF16) for _, width in ways_of(cols)]
        return [pltpu.VMEM((SIDE, SIDE, SIDE, rows, cols), BF16), *slots, dma((3, 2, 3, SIDE)), dma((3, 2, 3, SIDE))]

    @classmethod
    def of(cls, place, rows, cols, refs):
        one = cls(place, rows, cols, refs[1:3], refs[3:5])
        one.held = refs[0]
        return one

    def block(self, t, way, hops, k, c=ALL):
        order = ORDERS[t]
        return self.held.at[(*index(order, (self.place.block(order[0], way, hops), k, c)), *self.part(t, way))]

    def message(self, t, way, n, k, arriving=False):
        src = None
        if not arriving:
            src = self.block(t, way, 1, k) if isinstance(n, int) and n == 0 else self.slots[way].at[t, n - 1, k]
        return self.send(ORDERS[t][0], way, src, self.slots[way].at[t, n, k], (t, way, n, k), self.sems)

    def start(self, k):
        for t, way in self.pairs():
            self.message(t, way, 0, k).start()

    def step(self, n, k):
        for t, way in self.pairs():
            self.message(t, way, n - 1, k, arriving=True).wait_recv()
            slots = self.slots[way]
            for c in range(SIDE):
                own = self.block(t, way, n + 1, k, c)
                slots[t, n - 1, k, c] = (slots[t, n - 1, k, c].astype(F32) + own[...].astype(F32)).astype(BF16)
            pl.when(n < 3)(lambda t=t, way=way: self.message(t, way, n, k).start())

    def tick(self, i):
        pl.when(i < SIDE)(lambda: self.start(i))
        pl.when(i >= SIDE)(lambda: self.step(lax.div(i, SIDE), lax.rem(i, SIDE)))

    def results(self):
        return [slots.at[:, 2] for slots in self.slots]

    def drain(self):
        def sent(k, _):
            for t, way in self.pairs():
                self.message(t, way, 0, k).wait_send()
                lax.fori_loop(1, 3, lambda n, _: (self.message(t, way, n, k).wait_send(), 0)[1], 0)
            return 0

        lax.fori_loop(0, SIDE, sent, 0)


class Rest(Rings):
    @staticmethod
    def scratch(rows, cols):
        third, dma = rows // 3, pltpu.SemaphoreType.DMA
        shapes = [pltpu.VMEM((*lead, third, width), BF16) for lead in ((3, 3, SIDE), (3, 3)) for _, width in ways_of(cols)]
        return shapes + [dma((3, 2, 3))] * 4

    @classmethod
    def of(cls, place, rows, cols, before, refs):
        one = cls(place, rows, cols, refs[:4], refs[4:8])
        one.before = before
        return one

    def message(self, phase, t, way, n, arriving=False):
        slots = self.slots[2 * phase - 2 + way]
        axis = ORDERS[t][phase]
        if arriving:
            src = None
        elif isinstance(n, int) and n == 0:
            v = self.place.block(axis, way, 1)
            src = self.before[way].at[t, v] if phase == 1 else self.slots[way].at[t, 2, v]
        else:
            src = slots.at[t, n - 1]
        return self.send(axis, way, src, slots.at[t, n], (t, way, n), self.sems[2 * phase - 2 : 2 * phase])

    def start(self, phase):
        for t, way in self.pairs():
            self.message(phase, t, way, 0).start()

    def step1(self, n):
        for t, way in self.pairs():
            self.message(1, t, way, n - 1, arriving=True).wait_recv()
            v = self.place.block(ORDERS[t][1], way, n + 1)
            before, slots = self.before[way], self.slots[way]
            for c in range(SIDE):
                slots[t, n - 1, c] = (slots[t, n - 1, c].astype(F32) + before[t, v, c].astype(F32)).astype(BF16)
            pl.when(n < 3)(lambda t=t, way=way: self.message(1, t, way, n).start())

    def step2(self, n):
        for t, way in self.pairs():
            self.message(2, t, way, n - 1, arriving=True).wait_recv()
            v = self.place.block(ORDERS[t][2], way, n + 1)
            before, slots = self.slots[way], self.slots[2 + way]
            slots[t, n - 1] = (slots[t, n - 1].astype(F32) + before[t, 2, v].astype(F32)).astype(BF16)
            pl.when(n < 3)(lambda t=t, way=way: self.message(2, t, way, n).start())

    def tick(self, i):
        pl.when(i == 0)(lambda: self.start(1))
        pl.when((i >= 1) & (i <= 3))(lambda: self.step1(i))
        pl.when(i == 3)(lambda: self.start(2))
        pl.when((i >= 4) & (i <= 6))(lambda: self.step2(i - 3))

    def result(self, out):
        for t, way in self.pairs():
            out[self.part(t, way)] = self.slots[2 + way][t, 2]

    def drain(self):
        for t, way in self.pairs():
            for phase in (1, 2):
                for n in range(3):
                    self.message(phase, t, way, n).wait_send()


def loads_down(source, first, sems):
    return [pltpu.make_async_copy(source.at[:, :, pl.ds(64 * z, 72)], first.held.at[:, :, z], sems.at[z]) for z in range(SIDE)]


def spread(j, steps, count, tick):
    low, high = lax.div(count * j, steps), lax.div(count * (j + 1), steps)
    lax.fori_loop(low, high, lambda i, _: (tick(i), 0)[1], 0)


def copies(sources, targets, sems):
    return [pltpu.make_async_copy(s, t, sems.at[i]) for i, (s, t) in enumerate(zip(sources, targets, strict=True))]


def begin(all_copies):
    for copy in all_copies:
        copy.start()


def end(all_copies):
    for copy in all_copies:
        copy.wait()


def half_sums(rows, cols):
    return [(3, SIDE, SIDE, rows // 3, width) for _, width in ways_of(cols)]


PREV = 6
DOWN_ROWS = 33


class Gather:
    def __init__(self, place, bufs, sems, outs, copy_sems):
        self.place, self.bufs, self.sems, self.outs, self.copy_sems = place, bufs, sems, outs, copy_sems

    @staticmethod
    def scratch(down_cols):
        buf = pltpu.VMEM((2, SIDE, SIDE, SIDE, 72, down_cols), BF16)
        return [buf] + [pltpu.SemaphoreType.DMA((2, 3, 2, 6, 3))] * 4 + [pltpu.SemaphoreType.DMA((2,))] * 3

    def part(self, kind, t, way):
        rows, cols = self.bufs[kind].shape[-2:]
        start, width = ways_of(cols)[way]
        return pl.ds(t * (rows // 3), rows // 3), pl.ds(start, width)

    def behind(self, t, way, axis, hops):
        return self.place.block(ORDERS[t][axis], way, hops)

    def message(self, kind, l, t, way, line, n, hops):
        order, place = ORDERS[t], self.place
        if isinstance(line, int) and line == 0:
            axis, values = order[0], [self.behind(t, way, 0, hops), place.at[order[1]], place.at[order[2]]]
        elif isinstance(line, int) and line == 1:
            axis, values = order[1], [ALL, self.behind(t, way, 1, hops), place.at[order[2]]]
        else:
            axis, values = order[2], [ALL, self.behind(t, way, 1, line - 2), self.behind(t, way, 2, hops)]
        ref = self.bufs[kind].at[(l, *index(order, values), *self.part(kind, t, way))]
        key = (l, t, way, line, n)
        return put(ref, ref, self.sems[2 * kind].at[key], self.sems[2 * kind + 1].at[key], place.onwards[axis, way])

    def copies(self, kind, l, t, way, b, c):
        order = ORDERS[t]
        rows, cols = self.part(kind, t, way)
        at = index(order, (ALL, b, c))
        if kind == 0:
            return [lambda out: (self.bufs[0].at[(l, *at, rows, cols)], out.at[(l, *at, rows, cols)])]
        half = self.bufs[1].shape[-1]
        start, width = ways_of(half)[way]
        columns = pl.ds(pl.multiple_of(self.place.core * half + start, LANES), width)
        x, y, z = at

        def pair(out, z, count):
            src = self.bufs[1].at[l, x, y, z, pl.ds(24 * t, count), cols]
            return src, out.at[l, x, y, pl.ds(pl.multiple_of(64 * z + 24 * t, 8), count), columns]

        if t < 2:
            return [lambda out: pair(out, z, 24)]
        return [lambda out, z=z: pair(out, z, 16 if z < SIDE - 1 else 24) for z in range(SIDE)]

    def copy_out(self, kind, l, t, way, b, c):
        local, send, recv = self.copy_sems
        for pair in self.copies(kind, l, t, way, b, c):
            src, dst = pair(self.outs[kind])
            if kind:
                pltpu.make_async_copy(src, dst, local.at[kind]).start()
            put(src, dst, send.at[kind], recv.at[kind], self.place.partner()).start()

    def parts(self):
        return [(kind, t, way) for kind in range(2) for t in range(3) for way in range(2)]

    def own(self, l):
        for kind, t, way in self.parts():
            self.message(kind, l, t, way, 0, 0, 0).start()

    def start_third(self, kind, l, t, way, m):
        self.message(kind, l, t, way, 2 + m, 0, 0).start()
        self.copy_out(kind, l, t, way, self.behind(t, way, 1, m), self.place.at[ORDERS[t][2]])

    def first_axis(self):
        def step(i, _):
            n, l = 1 + lax.div(i, 2), lax.rem(i, 2)
            for kind, t, way in self.parts():
                self.message(kind, l, t, way, 0, n - 1, n).wait_recv()
                pl.when(n < 3)(lambda kind=kind, t=t, way=way: self.message(kind, l, t, way, 0, n, n).start())

                @pl.when(n == 3)
                def _(kind=kind, t=t, way=way):
                    self.message(kind, l, t, way, 1, 0, 0).start()
                    self.start_third(kind, l, t, way, 0)

            return 0

        lax.fori_loop(0, 6, step, 0)

    def other_axes(self):
        def step(i, _):
            r, l = 1 + lax.div(i, 2), lax.rem(i, 2)
            for kind, t, way in self.parts():

                @pl.when(r <= 3)
                def _(kind=kind, t=t, way=way):
                    self.message(kind, l, t, way, 1, r - 1, r).wait_recv()
                    pl.when(r < 3)(lambda: self.message(kind, l, t, way, 1, r, r).start())
                    self.start_third(kind, l, t, way, r)

                def third(m, _, kind=kind, t=t, way=way):
                    n = r - m
                    self.message(kind, l, t, way, 2 + m, n - 1, n).wait_recv()
                    pl.when(n < 3)(lambda: self.message(kind, l, t, way, 2 + m, n, n).start())
                    self.copy_out(kind, l, t, way, self.behind(t, way, 1, m), self.behind(t, way, 2, n))
                    return 0

                lax.fori_loop(jnp.maximum(r - 3, 0), jnp.minimum(r, SIDE), third, 0)
            return 0

        lax.fori_loop(0, 12, step, 0)

    def drain(self):
        local, send, recv = self.copy_sems
        half = self.bufs[1].shape[-1]
        columns = self.outs[1].at[:, :, :, :, pl.ds(0, half)]
        for kind, whole in ((0, self.outs[0]), (1, columns)):
            if kind:
                pltpu.make_async_copy(whole, whole, local.at[kind]).wait()
            copy = put(whole, whole, send.at[kind], recv.at[kind], self.place.partner())
            copy.wait_send()
            copy.wait_recv()

        def sent(i, _):
            l, n = lax.div(i, 3), lax.rem(i, 3)
            for kind, t, way in self.parts():
                for line in range(2):
                    self.message(kind, l, t, way, line, n, n).wait_send()
                lax.fori_loop(2, 6, lambda line, _: (self.message(kind, l, t, way, line, n, n).wait_send(), 0)[1], 0)
            return 0

        lax.fori_loop(0, 6, sent, 0)


def finish_kernel(count, *refs):
    sums_gu, sums_d, m_in, v_in, w_in = refs[0:2], refs[2:4], refs[4:7], refs[7:10], refs[10:13]
    own_gu, w_out, m_out, v_out = refs[13], refs[14:16], refs[16:19], refs[19:22]
    moments_gu, moments_d, old_gu, old_d, other_d, tiles = refs[22:28]
    load_sem, early_send, early_recv, norm_send, norm_recv, late_local, late_send, late_recv = refs[28:36]
    gather_refs = refs[36:]
    place = Place()
    x, y, z = place.at
    core = place.core
    gather = Gather(place, (own_gu, gather_refs[0]), gather_refs[1:5], w_out, gather_refs[5:8])
    partner = place.partner()
    gate_tiles, down_tiles = sums_gu[0].shape[1] // LANES, sums_d[0].shape[1] // LANES
    gate_stride, down_stride = 2 * gate_tiles, 4 * down_tiles
    gate_size, down_size = 12 * gate_stride, DOWN_ROWS * down_stride

    def blank(i, _):
        for which in range(2):
            moments_d[which, pl.ds(pl.multiple_of(8 * i, 8), 8), :] = jnp.zeros((8, LANES), F32)
        return 0

    lax.fori_loop(0, moments_d.shape[1] // 8, blank, 0)
    following = [place.device(2, 1, core=c) for c in range(2)]
    others = [place.device(axis, 2) for axis in range(3)] + [place.device(2, off, core=1 - core) for off in (1, SIDE - 1)]
    signal_all(near(place) + others)

    def gate_rows(i, which):
        return moments_gu.at[i, pl.ds(pl.multiple_of(which * gate_size, 8), gate_size)]

    def down_rows(i, first, rows):
        return moments_d.at[i, pl.ds(pl.multiple_of(first * down_stride, 8), rows * down_stride)]

    def columns(ref):
        half = down_tiles * LANES
        return ref.at[:, x, y, pl.ds(pl.multiple_of(64 * z, 8), 72), pl.ds(pl.multiple_of(core * half, LANES), half)]

    own_rows = PREV + 2 * z + DOWN_ROWS * core
    loads, sends = [], []
    for i, moment in enumerate((m_in, v_in)):
        for c in range(2):

            @pl.when(core == c)
            def _(i=i, moment=moment, c=c):
                pltpu.make_async_copy(moment[c], gate_rows(i, core), load_sem.at[i]).start()
                put(moment[1 - c], gate_rows(i, core), early_send.at[i], early_recv.at[i], partner).start()

        loads.append(pltpu.make_async_copy(moment[0], gate_rows(i, core), load_sem.at[i]))
        sends.append(put(moment[0], gate_rows(i, core), early_send.at[i], early_recv.at[i], partner))
        loads.append(pltpu.make_async_copy(moment[2], down_rows(i, own_rows, DOWN_ROWS), load_sem.at[2 + i]))
        loads[-1].start()
        sends.append(put(moment[2], down_rows(i, own_rows, DOWN_ROWS), early_send.at[2 + i], early_recv.at[2 + i], partner))
        sends[-1].start()
        last = moment[2].at[pl.ds((DOWN_ROWS - PREV) * down_stride, PREV * down_stride)]
        landing = down_rows(i, 2 * lax.rem(z + 1, SIDE), PREV)

        @pl.when(core == 1)
        def _(i=i, last=last, landing=landing):
            for c in range(2):
                put(last, landing, early_send.at[4 + 2 * i + c], early_recv.at[4 + i], following[c]).start()

    for l in range(2):
        sends.append(put(sums_d[l], other_d.at[l], early_send.at[8 + l], early_recv.at[6 + l], partner))
        sends[-1].start()
    for c in range(2):

        @pl.when(core == c)
        def _(c=c):
            pltpu.make_async_copy(w_in[c].at[:, x, y, z], old_gu, load_sem.at[4]).start()

    loads.append(pltpu.make_async_copy(w_in[0].at[:, x, y, z], old_gu, load_sem.at[4]))
    loads.append(pltpu.make_async_copy(columns(w_in[2]), old_d, load_sem.at[5]))
    loads[-1].start()

    squares = jnp.zeros((8, LANES), F32)
    for l in range(2):

        def of_gate_up(j, total, l=l):
            for t in range(3):
                g = sums_gu[l][pl.ds(8 * t, 8), pl.ds(pl.multiple_of(j * LANES, LANES), LANES)].astype(F32)
                total += g * g
            return total

        squares = lax.fori_loop(0, gate_tiles, of_gate_up, squares)

        def of_down(i, total, l=l):
            row = 8 * i + lax.broadcasted_iota(jnp.int32, (8, LANES), 0)
            mine = (row >= 2 * z) & (row < 2 * z + 2 * DOWN_ROWS)
            for j in range(down_tiles):
                g = sums_d[l][pl.ds(pl.multiple_of(8 * i, 8), 8), pl.ds(j * LANES, LANES)].astype(F32)
                total += jnp.where(mine, g * g, 0.0)
            return total

        squares = lax.fori_loop(0, 9, of_down, squares)
    for stage, (coordinate, size) in enumerate(((core, 2), (x, SIDE), (y, SIDE), (z, SIDE))):
        tiles[stage, coordinate] = squares
        exchanges = []
        for off in range(1, size):
            target = partner if stage == 0 else place.device(stage - 1, off)
            key = 3 * stage + off - 1
            here = tiles.at[stage, coordinate]
            exchanges.append(put(here, here, norm_send.at[key], norm_recv.at[key], target))
            exchanges[-1].start()
        for exchange in exchanges:
            exchange.wait_recv()
        for exchange in exchanges:
            exchange.wait_send()
        squares = tiles[stage, 0]
        for other in range(1, size):
            squares += tiles[stage, other]
    total = jnp.sum(jnp.sum(squares, 0, keepdims=True), 1, keepdims=True)
    factor = jnp.minimum(1.0, 0.5 * lax.rsqrt(total / count + CLIP_EPS))

    for copy in loads:
        copy.wait()
    for copy in sends:
        copy.wait_recv()
    for i in range(2):
        put(down_rows(i, 0, PREV), down_rows(i, 0, PREV), early_send.at[0], early_recv.at[4 + i], partner).wait_recv()

    def moments(ref, start, stride, g):
        rows = pl.ds(start, 8, stride=stride)
        m = 0.9 * ref[0, rows, :] + 0.1 * g
        v = 0.95 * ref[1, rows, :] + 0.05 * g * g
        ref[0, rows, :] = m
        ref[1, rows, :] = v
        return m * lax.rsqrt(v + 1e-8)

    def weight(w, step):
        w = w.astype(F32)
        return (w - 0.02 * (step + 0.1 * w)).astype(BF16)

    for l in range(2):

        def gate_up(j, _, l=l):
            lanes = pl.ds(pl.multiple_of(j * LANES, LANES), LANES)
            for t in range(3):
                rows = pl.ds(8 * t, 8)
                g = sums_gu[l][rows, lanes].astype(F32) * factor
                step = moments(moments_gu, 8 * t * gate_stride + 2 * j + l, gate_stride, g)
                gather.bufs[0][l, x, y, z, rows, lanes] = weight(old_gu[l, rows, lanes], step)
            return 0

        lax.fori_loop(0, gate_tiles, gate_up, 0, unroll=3)

        def down(i, _, l=l):
            rows = pl.ds(pl.multiple_of(8 * i, 8), 8)
            for j in range(down_tiles):
                lanes = pl.ds(j * LANES, LANES)
                start = (PREV + 8 * i) * down_stride + 2 * j + l
                g = sums_d[l][rows, lanes].astype(F32) * factor
                step = moments(moments_d, start + 2 * down_tiles * core, down_stride, g)
                gather.bufs[1][l, x, y, z, rows, lanes] = weight(old_d[l, rows, lanes], step)
            return 0

        lax.fori_loop(0, 9, down, 0)
        gather.own(l)
    for l in range(2):

        def down_other(i, _, l=l):
            rows = pl.ds(pl.multiple_of(8 * i, 8), 8)
            for j in range(down_tiles):
                start = (PREV + 8 * i) * down_stride + 2 * j + l
                g = other_d[l, rows, pl.ds(j * LANES, LANES)].astype(F32) * factor
                moments(moments_d, start + 2 * down_tiles * (1 - core), down_stride, g)
            return 0

        lax.fori_loop(0, 9, down_other, 0)

    late = []
    for i, out in enumerate((m_out, v_out)):
        for c in range(2):

            @pl.when(core == c)
            def _(i=i, out=out, c=c):
                pltpu.make_async_copy(gate_rows(i, core), out[c], late_local.at[i]).start()
                put(gate_rows(i, 1 - core), out[c], late_send.at[i], late_recv.at[i], partner).start()

        pltpu.make_async_copy(down_rows(i, own_rows, DOWN_ROWS), out[2], late_local.at[2 + i]).start()
    gather.first_axis()
    gather.other_axes()
    for i, out in enumerate((m_out, v_out)):
        pltpu.make_async_copy(gate_rows(i, core), out[0], late_local.at[i]).wait()
        pltpu.make_async_copy(down_rows(i, own_rows, DOWN_ROWS), out[2], late_local.at[2 + i]).wait()
        copy = put(gate_rows(i, 1 - core), out[0], late_send.at[i], late_recv.at[i], partner)
        copy.wait_recv()
        copy.wait_send()
    for copy in sends:
        copy.wait_send()
    for i in range(2):
        for c in range(2):

            @pl.when(core == 1)
            def _(i=i, c=c):
                rows = down_rows(i, 0, PREV)
                put(rows, rows, early_send.at[4 + 2 * i + c], early_recv.at[4 + i], following[c]).wait_send()

    gather.drain()


def finish_call(count, collective_id, sums_gu, sums_d, m, v, w):
    gate_cols, down_half = sums_gu[0].shape[1], sums_d[0].shape[1]
    operands = [*sums_gu, *sums_d, *m, *v, *w]
    hbm, vmem = pl.BlockSpec(memory_space=pltpu.HBM), pl.BlockSpec(memory_space=pltpu.VMEM)
    dma = pltpu.SemaphoreType.DMA
    gate_stride, down_stride = gate_cols // 64, down_half // 32
    scratch = [
        pltpu.VMEM((2, 24 * gate_stride, LANES), F32),
        pltpu.VMEM((2, (PREV + 72) * down_stride, LANES), F32),
        pltpu.VMEM((2, 24, gate_cols), BF16),
        pltpu.VMEM((2, 72, down_half), BF16),
        pltpu.VMEM((2, 72, down_half), BF16),
        pltpu.VMEM((4, SIDE, 8, LANES), F32),
        dma((6,)), dma((10,)), dma((8,)), dma((12,)), dma((12,)), dma((4,)), dma((2,)), dma((2,)),
    ]
    return pl.pallas_call(
        functools.partial(finish_kernel, count),
        name="finish",
        out_shape=[pltpu.VMEM(w[0].shape, BF16), *[jax.ShapeDtypeStruct(t.shape, t.dtype) for t in (w[0], w[2], *m, *v)]],
        in_specs=[vmem] * 4 + [hbm] * 9,
        out_specs=[vmem] + [hbm] * 8,
        scratch_shapes=scratch + Gather.scratch(down_half),
        compiler_params=pltpu.CompilerParams(collective_id=collective_id, has_side_effects=True, vmem_limit_bytes=26 * 1024 * 1024),
        cost_estimate=pl.CostEstimate(flops=10**9, bytes_accessed=10**8, transcendentals=0),
    )(*operands)


def write_kernel(bounces, own, other, down, gate_out, up_out, down_out, bounce, own_sem, in_sem, out_sem):
    core = lax.rem(lax.axis_index("dp"), 2)
    places = [(l, x, y) for l in range(2) for x in range(SIDE) for y in range(SIDE)]
    pieces = [(other, None, at) for at in places] + [(down, down_out, at) for at in places]

    def slot(i):
        source = pieces[i][0]
        return bounce[0 if source is other else 1].at[i % bounces]

    def read(i):
        source, _, at = pieces[i]
        return pltpu.make_async_copy(source.at[at], slot(i), in_sem.at[i % bounces])

    def write(i, out=None):
        _, to, at = pieces[i]
        return pltpu.make_async_copy(slot(i), (out if to is None else to).at[at], out_sem.at[i % bounces])

    for i in range(bounces):
        read(i).start()
    for c, (mine, others) in enumerate(((gate_out, up_out), (up_out, gate_out))):

        @pl.when(core == c)
        def _(mine=mine, others=others):
            pltpu.make_async_copy(own, mine, own_sem).start()
            for i in range(len(pieces)):
                read(i).wait()
                write(i, others).start()
                done = i - bounces // 2
                if done >= 0 and done + bounces < len(pieces):
                    write(done, others).wait()
                    read(done + bounces).start()

    for i in range(len(pieces) - bounces, len(pieces)):
        write(i, gate_out).wait()
    pltpu.make_async_copy(own, gate_out, own_sem).wait()


def write_call(own, other, down):
    hbm = pl.BlockSpec(memory_space=pltpu.HBM)
    bounces, dma = 8, pltpu.SemaphoreType.DMA
    return pl.pallas_call(
        lambda *refs: write_kernel(bounces, *refs[:6], refs[6:8], *refs[8:]),
        name="write",
        out_shape=[jax.ShapeDtypeStruct(t.shape, BF16) for t in (other, other, down)],
        in_specs=[pl.BlockSpec(memory_space=pl.ANY), hbm, hbm],
        out_specs=[hbm] * 3,
        scratch_shapes=[pltpu.VMEM((bounces, *t.shape[3:]), BF16) for t in (other, down)] + [dma, dma((bounces,)), dma((bounces,))],
        compiler_params=pltpu.CompilerParams(vmem_limit_bytes=14 * 1024 * 1024),
    )(own, other, down)


TILE = 384
ROWS = 256
TIGHT = pl.Buffered(buffer_count=1)


def dot(a, b, dims):
    return lax.dot_general(a, b, (dims, ((), ())), preferred_element_type=F32)


NN, NT, TN = ((1,), (0,)), ((1,), (1,)), ((0,), (0,))


def norm_scale(wide):
    return lax.rsqrt(jnp.mean(wide * wide, -1, keepdims=True) + 1e-6)


def in_rows(total, step, body):
    def one(i, _):
        body(pl.ds(pl.multiple_of(i * step, step), step))
        return 0

    lax.fori_loop(0, total // step, one, 0)


def clear(acc):
    def rows(r):
        acc[r, :] = jnp.zeros((8, acc.shape[1]), F32)

    in_rows(acc.shape[0], 8, rows)


def spec(shape, index_map, tight=False):
    return pl.BlockSpec(shape, index_map, pipeline_mode=TIGHT) if tight else pl.BlockSpec(shape, index_map)


def whole(shape, tight=True):
    return spec(shape, lambda j: (0,) * len(shape), tight)


HBM = pl.BlockSpec(memory_space=pltpu.HBM)


def params(collective_id=None, semantics=("arbitrary",)):
    more = {} if collective_id is None else {"collective_id": collective_id, "has_side_effects": True}
    return pltpu.CompilerParams(dimension_semantics=semantics, vmem_limit_bytes=VMEM_LIMIT, **more)


def transpose_piece(j, last, src, dst):
    def piece(i):
        at = pl.ds(pl.multiple_of(i * LANES, LANES), LANES)
        dst[at, :] = src[:, at].T

    piece(j)
    pl.when(j == last)(lambda: piece(last + 1))


def side_by_side(a, b):
    return jnp.concatenate([a, b], axis=1)


def forward_kernel(tiles, x, wg, wu, wd, gate, up, h_out, a_out, at, a, acc, p):
    j = pl.program_id(0)

    @pl.when(j == 0)
    def _():
        def rows(r):
            wide = x[r, :].astype(F32)
            a[r, :] = (wide * norm_scale(wide)).astype(BF16)

        in_rows(x.shape[0], 32, rows)
        clear(acc)

    transpose_piece(j, tiles - 1, a, at)
    both = side_by_side(wg[0], wu[0])
    slot = lax.rem(j, 2)
    for m in range(x.shape[0] // ROWS):
        r = pl.ds(m * ROWS, ROWS)
        gu = dot(a[r, :], both, NN)
        g, u = gu[:, :TILE], gu[:, TILE:]
        gate[0, r, :] = g
        up[0, r, :] = u
        p[slot, r, :] = (g * lax.logistic(g) * u).astype(BF16)

    @pl.when(slot == 1)
    def _():
        for m in range(x.shape[0] // ROWS):
            r = pl.ds(m * ROWS, ROWS)
            acc[r, :] += dot(side_by_side(p[0, r, :], p[1, r, :]), wd[0], NN)

    @pl.when(j == tiles - 1)
    def _():
        def last_down(r):
            acc[r, :] += dot(p[0, r, :], wd[0, pl.ds(0, TILE), :], NN)

        in_rows(x.shape[0], ROWS, last_down)

        def rows(r):
            h = (x[r, :].astype(F32) + acc[r, :].astype(BF16).astype(F32)).astype(BF16)
            h_out[r, :] = h
            wide = h.astype(F32)
            a_out[r, :] = (wide * norm_scale(wide)).astype(BF16)

        in_rows(x.shape[0], 32, rows)


def forward_call(x, wg, wu, wd):
    tokens, d = x.shape
    ff = wg.shape[2]
    tiles = ff // TILE
    w_in = spec((1, d, TILE), lambda j: (0, 0, j))
    return pl.pallas_call(
        functools.partial(forward_kernel, tiles),
        name="forward_0",
        grid=(tiles,),
        in_specs=[whole((tokens, d)), w_in, w_in, spec((1, 2 * TILE, d), lambda j: (0, lax.div(j, 2), 0))],
        out_specs=[spec((1, tokens, TILE), lambda j: (j, 0, 0))] * 2 + [whole((tokens, d))] * 2 + [whole((d, tokens))],
        out_shape=[jax.ShapeDtypeStruct((tiles, tokens, TILE), F32)] * 2
        + [jax.ShapeDtypeStruct((tokens, d), BF16)] * 2
        + [jax.ShapeDtypeStruct((d, tokens), BF16)],
        scratch_shapes=[pltpu.VMEM((tokens, d), BF16), pltpu.VMEM((tokens, d), F32), pltpu.VMEM((2, tokens, TILE), BF16)],
        compiler_params=params(),
    )(x, wg, wu, wd)


class PairSum:
    def __init__(self, place, tiles, landing, stage, send, recv):
        self.place, self.tiles, self.landing, self.stage, self.send, self.recv = place, tiles, landing, stage, send, recv

    @staticmethod
    def scratch(tiles, rows, cols):
        dma = pltpu.SemaphoreType.DMA
        return [pltpu.VMEM((tiles, rows, cols), BF16), pltpu.VMEM((2, rows, cols), BF16), dma((2,)), dma((tiles,))]

    def copy(self, i):
        slot = lax.rem(i, 2)
        return put(self.stage.at[slot], self.landing.at[i], self.send.at[slot], self.recv.at[i], self.place.partner())

    def reserve(self, i):
        pl.when(i >= 2)(lambda: self.copy(i - 2).wait_send())
        return self.stage.at[lax.rem(i, 2)]

    def drain(self):
        for i in (self.tiles - 2, self.tiles - 1):
            self.copy(i).wait_send()


def hidden_back(gate, up, dp):
    dp = dp.astype(F32)
    s = lax.logistic(gate)
    act = gate * s
    return (act * up).astype(BF16), (dp * up * (s + act * (1.0 - s))).astype(BF16), (dp * act).astype(BF16)


def down_gradient(j, tiles, pair, p, dy, half, out):
    core = pair.place.core

    def columns(c):
        return pl.ds(pl.multiple_of(c * half, LANES), half)

    @pl.when(j < tiles)
    def _():
        slot = pair.reserve(j)
        slot[...] = dot(p[lax.rem(j, 2)], dy[:, columns(1 - core)], TN).astype(BF16)
        pair.copy(j).start()

    @pl.when(j >= 1)
    def _():
        pair.copy(j - 1).wait_recv()
        own = dot(p[lax.rem(j - 1, 2)], dy[:, columns(core)], TN)
        out[...] = (own + pair.landing[j - 1].astype(F32)).astype(BF16)

    pl.when(j == tiles)(pair.drain)


def layer_kernel(tiles, a, dy, wg, wu, wd, dgu, at, out, p, dps, *rest):
    j = pl.program_id(0)
    place = Place()
    pair = PairSum(place, tiles, *rest)
    pl.when(j == 0)(lambda: signal_all([place.partner()]))
    two_tiles_of_dp(j, tiles, dy, wd, dps)

    @pl.when(j < tiles)
    def _():
        transpose_piece(j, tiles - 1, a, at)
        slot = lax.rem(j, 2)
        both = side_by_side(wg[0], wu[0])
        for m in range(a.shape[0] // ROWS):
            r = pl.ds(m * ROWS, ROWS)
            gu = dot(a[r, :], both, NN)
            p[slot, r, :], dgu[0, 0, r, :], dgu[0, 1, r, :] = hidden_back(gu[:, :TILE], gu[:, TILE:], dps[slot, r, :])

    down_gradient(j, tiles, pair, p, dy, dy.shape[1] // 2, out)


def two_tiles_of_dp(j, tiles, dy, wd, dps):
    @pl.when((lax.rem(j, 2) == 0) & (j < tiles - 1))
    def _():
        for m in range(dy.shape[0] // ROWS):
            r = pl.ds(m * ROWS, ROWS)
            dp = dot(dy[r, :], wd[0], NT).astype(BF16)
            dps[0, r, :] = dp[:, :TILE]
            dps[1, r, :] = dp[:, TILE:]

    @pl.when(j == tiles - 1)
    def _():
        def one_tile(r):
            dps[0, r, :] = dot(dy[r, :], wd[0, pl.ds(0, TILE), :], NT).astype(BF16)

        in_rows(dy.shape[0], ROWS, one_tile)


def clip(tiles, back=0):
    return lambda j: jnp.clip(j - back, 0, tiles - 1)


def layer_call(collective_id, a, dy, wg, wu, wd):
    tokens, d = a.shape
    ff = wg.shape[2]
    tiles, half = ff // TILE, d // 2
    now, before = clip(tiles), clip(tiles, 1)
    w_in = spec((1, d, TILE), lambda j: (1, 0, now(j)))
    return pl.pallas_call(
        functools.partial(layer_kernel, tiles),
        name="layer_1",
        grid=(tiles + 1,),
        in_specs=[whole((tokens, d))] * 2 + [w_in, w_in, spec((1, 2 * TILE, d), lambda j: (1, lax.div(now(j), 2), 0))],
        out_specs=[spec((1, 2, tokens, TILE), lambda j: (now(j), 0, 0, 0)), whole((d, tokens)), spec((TILE, half), lambda j: (before(j), 0))],
        out_shape=[
            jax.ShapeDtypeStruct((tiles, 2, tokens, TILE), BF16),
            jax.ShapeDtypeStruct((d, tokens), BF16),
            jax.ShapeDtypeStruct((ff, half), BF16),
        ],
        scratch_shapes=[pltpu.VMEM((2, tokens, TILE), BF16)] * 2 + PairSum.scratch(tiles, TILE, half),
        compiler_params=params(collective_id),
    )(a, dy, wg, wu, wd)


GATE_ROWS, DOWN_WINDOW = 24, 72
RING = 6


def second(t, v, rest=ALL):
    return (rest, v) if t == 1 else (v, rest)


class Stream:
    def __init__(self, place, tiles, phases, refs):
        self.place, self.tiles, self.phases, self.rows = place, tiles, phases, GATE_ROWS // 3
        self.held, self.slots, self.send, self.recv = refs[0], refs[1 : 1 + 2 * phases], refs[-2], refs[-1]
        self.ways = ways_of(TILE)

    @staticmethod
    def scratch(tiles, phases):
        third, dma = GATE_ROWS // 3, pltpu.SemaphoreType.DMA
        leads = [(3, 3, tiles, SIDE, SIDE), (3, 3, tiles, SIDE), (3, 3, tiles)][:phases]
        slots = [pltpu.VMEM((*lead, third, width), BF16) for lead in leads for _, width in ways_of(TILE)]
        return [pltpu.VMEM((RING, SIDE, SIDE, SIDE, GATE_ROWS, TILE), BF16), *slots, dma((tiles, 7)), dma((tiles, 7))]

    def part(self, t, way):
        start, width = self.ways[way]
        return pl.ds(t * self.rows, self.rows), pl.ds(start, width)

    def own(self, c, t, way, hops, b=ALL, d=ALL):
        at = index(ORDERS[t], (self.place.block(ORDERS[t][0], way, hops), ALL, ALL))
        axes = [i for i in range(3) if i != ORDERS[t][0]]
        at = list(at)
        at[axes[0]], at[axes[1]] = b, d
        return self.held.at[(lax.rem(c, RING), *at, *self.part(t, way))]

    def copy(self, phase, t, way, n, c, first=False):
        axis = ORDERS[t][phase]
        slots = self.slots[2 * phase + way]
        if not first:
            src = slots.at[t, n - 1, c]
        elif phase == 0:
            src = self.own(c, t, way, 1)
        else:
            src = self.slots[way].at[(t, 2, c, *second(t, self.place.block(axis, way, 1)))]
        key = (c, 3 * phase + n)
        return put(src, slots.at[t, n, c], self.send.at[key], self.recv.at[key], self.place.onwards[axis, way])

    def direct(self, t, way, off, c):
        axis = ORDERS[t][2]
        v = lax.rem(self.place.at[axis] + off, SIDE)
        src, dst = self.slots[2 + way].at[t, 2, c, v], self.slots[4 + way].at[t, off - 1, c]
        return put(src, dst, self.send.at[c, 6], self.recv.at[c, 6], self.place.device(axis, off))

    def pairs(self):
        return [(t, way) for t in range(3) for way in range(2)]

    def all_of(self, phase):
        return self.held.at[(0,) * (phase + 2)] if phase < 2 else self.held.at[0, 0, 0, pl.ds(0, 3)]

    def begin(self, phase, c):
        for t, way in self.pairs():
            if phase < 2:
                self.copy(phase, t, way, 0, c, first=True).start()
            else:
                for off in range(1, SIDE):
                    self.direct(t, way, off, c).start()

    def add(self, phase, t, way, n, c):
        slots = self.slots[2 * phase + way]
        v = self.place.block(ORDERS[t][phase], way, n + 1)

        def one(at, other):
            at = (t, n - 1, c, *at)
            slots[at] = (slots[at].astype(F32) + other[...].astype(F32)).astype(BF16)

        if phase == 0:
            for b in range(SIDE):
                for d in range(SIDE):
                    one((b, d), self.own(c, t, way, n + 1, b, d))
        else:
            for d in range(SIDE):
                one((d,), self.slots[way].at[(t, 2, c, *second(t, v, d))])

    def stage(self, s, c, out):
        phase, n = (s - 1) // 3, (s - 1) % 3 + 1
        whole_stage = self.all_of(phase)
        pltpu.make_async_copy(whole_stage, whole_stage, self.recv.at[c, s - 1]).wait()
        if phase == 2:
            for t, way in self.pairs():
                total = self.slots[2 + way][t, 2, c, self.place.at[ORDERS[t][2]]].astype(F32)
                for i in range(3):
                    total += self.slots[4 + way][t, i, c].astype(F32)
                rows, _ = self.part(t, way)
                start, width = self.ways[way]
                out[rows, pl.ds(pl.multiple_of(c * TILE + start, LANES), width)] = total.astype(BF16)
            return
        for t, way in self.pairs():
            self.add(phase, t, way, n, c)
            if n < 3:
                self.copy(phase, t, way, n, c).start()
        if n == 3 and phase + 1 < self.phases:
            self.begin(phase + 1, c)

    def sent(self, phase, n, c):
        whole_stage = self.all_of(phase)
        pltpu.make_async_copy(whole_stage, whole_stage, self.send.at[c, 3 * phase + n]).wait()

    def count(self):
        return 3 if self.phases == 1 else 7

    def keep(self, c):
        pl.when(c >= RING)(lambda: self.sent(0, 0, c - RING))
        return self.held.at[lax.rem(c + RING, RING)]

    def run(self, s, c, out):
        act = (lambda: self.begin(0, c)) if s == 0 else (lambda: self.stage(s, c, out))
        pl.when((c >= 0) & (c < self.tiles))(act)

    def early(self, j, out=None):
        for s in range(self.count(), 1, -1):
            self.run(s, j - 3 - s, out)

    def late(self, j, out=None):
        self.run(0, j - 2, out)
        self.run(1, j - 3, out)

    def last_step(self):
        return self.tiles - 1 + 3 + self.count()

    def drain(self):
        def each(c, _):
            pl.when(c >= self.tiles - RING)(lambda: self.sent(0, 0, c))
            for i in range(1, self.count()):
                self.sent(i // 3, i % 3, c)
            return 0

        lax.fori_loop(0, self.tiles, each, 0)

    def results(self):
        return [self.slots[way].at[:, 2] for way in range(2)]


def stream_halves(tiles):
    return [(3, tiles, SIDE, SIDE, GATE_ROWS // 3, width) for _, width in ways_of(TILE)]


class StreamRest:
    def __init__(self, place, tiles, before, refs):
        self.place, self.tiles, self.before, self.slots, self.sems = place, tiles, before, refs[:4], refs[4:8]
        self.rows, self.ways = GATE_ROWS // 3, ways_of(TILE)

    @staticmethod
    def scratch(tiles):
        third, dma = GATE_ROWS // 3, pltpu.SemaphoreType.DMA
        shapes = [pltpu.VMEM((3, 3, *lead, third, width), BF16) for lead in ((tiles, SIDE), (tiles,)) for _, width in ways_of(TILE)]
        return shapes + [dma((3, 2, 3))] * 4

    def pairs(self):
        return [(t, way) for t in range(3) for way in range(2)]

    def message(self, phase, t, way, n, arriving=False):
        slots = self.slots[2 * phase - 2 + way]
        axis = ORDERS[t][phase]
        if arriving:
            src = slots.at[t, n]
        elif isinstance(n, int) and n == 0:
            v = self.place.block(axis, way, 1)
            src = self.before[way].at[(t, ALL, *second(t, v))] if phase == 1 else self.slots[way].at[t, 2, :, v]
        else:
            src = slots.at[t, n - 1]
        send, recv = self.sems[2 * phase - 2 : 2 * phase]
        key = (t, way, n)
        return put(src, slots.at[t, n], send.at[key], recv.at[key], self.place.onwards[axis, way])

    def start(self, phase):
        for t, way in self.pairs():
            self.message(phase, t, way, 0).start()

    def step(self, phase, n):
        for t, way in self.pairs():
            self.message(phase, t, way, n - 1, arriving=True).wait_recv()
            v = self.place.block(ORDERS[t][phase], way, n + 1)
            slots = self.slots[2 * phase - 2 + way]

            def add(c, _, t=t, way=way, v=v, slots=slots):
                for d in range(SIDE if phase == 1 else 1):
                    at = (t, n - 1, c, d) if phase == 1 else (t, n - 1, c)
                    other = self.before[way].at[(t, c, *second(t, v, d))] if phase == 1 else self.slots[way].at[t, 2, c, v]
                    slots[at] = (slots[at].astype(F32) + other[...].astype(F32)).astype(BF16)
                return 0

            lax.fori_loop(0, self.tiles, add, 0)
            pl.when(n < 3)(lambda t=t, way=way: self.message(phase, t, way, n).start())

    def tick(self, i):
        pl.when(i == 0)(lambda: self.start(1))
        pl.when((i >= 1) & (i <= 3))(lambda: self.step(1, i))
        pl.when(i == 3)(lambda: self.start(2))
        pl.when((i >= 4) & (i <= 6))(lambda: self.step(2, i - 3))

    def result(self, out):
        def one(c, _):
            for t, way in self.pairs():
                start, width = self.ways[way]
                lanes = pl.ds(pl.multiple_of(c * TILE + start, LANES), width)
                out[pl.ds(t * self.rows, self.rows), lanes] = self.slots[2 + way][t, 2, c]
            return 0

        lax.fori_loop(0, self.tiles, one, 0)

    def drain(self):
        for t, way in self.pairs():
            for phase in (1, 2):
                for n in range(3):
                    self.message(phase, t, way, n).wait_send()


BLOCK_ROWS = SIDE * SIDE * GATE_ROWS


def gate_up_kernel(tiles, phases, cols, at, ahead, behind, *rest):
    j = pl.program_id(0)
    place = Place()
    core = place.core
    if phases == 1:
        outs, out, rest = rest[:2], None, rest[2:]
    else:
        sum_down, out, out_down, rest = rest[0], rest[1], rest[2], rest[3:]
    pair = PairSum(place, tiles, *rest[:4])
    stream = Stream(place, tiles, phases, rest[4 : 4 + 3 + 2 * phases])
    rest = rest[4 + 3 + 2 * phases :]
    if phases == 3:
        first = First.of(place, DOWN_WINDOW, cols, rest[1:6])
        down = Rest.of(place, DOWN_WINDOW, cols, first.results(), rest[6:14])
        loads = loads_down(sum_down, first, rest[0])

    @pl.when(j == 0)
    def _():
        opposite = [place.device(axis, 2) for axis in range(3)] if phases == 3 else []
        signal_all(near(place) + opposite)
        if phases == 3:
            begin(loads)

    stream.early(j, out)

    pl.when((j >= 2) & (j <= tiles + 1))(lambda: pair.copy(j - 2).wait_recv())

    @pl.when(j <= tiles + 1)
    def _():
        slot, kept = pair.reserve(j), stream.keep(j - 2)
        both = side_by_side(ahead[0, 1 - core], behind[0, core])
        landed = lax.rem(j + tiles - 2, tiles)
        for m in range(SIDE):
            r = pl.ds(m * BLOCK_ROWS, BLOCK_ROWS)
            tile = dot(at[r, :], both, NN)
            slot[r, :] = tile[:, :TILE].astype(BF16)
            total = (tile[:, TILE:] + pair.landing[landed, r, :].astype(F32)).astype(BF16)
            kept[m] = total.reshape(SIDE, SIDE, GATE_ROWS, TILE)

    pl.when(j < tiles)(lambda: pair.copy(j).start())
    stream.late(j, out)
    if phases == 3:
        pl.when(j == 0)(lambda: end(loads))
        pl.when(j <= tiles + 1)(lambda: spread(j, tiles + 2, 16, first.tick))
        pl.when(j > tiles + 1)(lambda: down.tick(j - tiles - 2))

    @pl.when(j == stream.last_step())
    def _():
        if phases == 1:
            saves = copies(stream.results(), outs, rest[0])
            begin(saves)
            stream.drain()
            end(saves)
        else:
            down.result(out_down)
            stream.drain()
            first.drain()
            down.drain()


def gate_up_call(name, collective_id, phases, at, dgu, *sum_down):
    d, tokens = at.shape
    tiles, cols, dma = dgu.shape[0], d // 2, pltpu.SemaphoreType.DMA
    ff = tiles * TILE
    now, before = clip(tiles), clip(tiles, 2)
    if phases == 1:
        shapes = stream_halves(tiles)
        out_specs, more = [HBM] * 2, [dma((2,))]
    else:
        shapes = [(GATE_ROWS, ff), (DOWN_WINDOW, cols)]
        out_specs = [whole(s) for s in shapes]
        more = [dma((SIDE,)), *First.scratch(DOWN_WINDOW, cols), *Rest.scratch(DOWN_WINDOW, cols)]
    return pl.pallas_call(
        functools.partial(gate_up_kernel, tiles, phases, cols),
        name=name,
        grid=(tiles + (6 if phases == 1 else 10),),
        in_specs=[
            whole((d, tokens)),
            spec((1, 2, tokens, TILE), lambda j: (now(j), 0, 0, 0)),
            spec((1, 2, tokens, TILE), lambda j: (before(j), 0, 0, 0)),
            *[HBM] * len(sum_down),
        ],
        out_specs=out_specs,
        out_shape=[jax.ShapeDtypeStruct(s, BF16) for s in shapes],
        scratch_shapes=[*PairSum.scratch(tiles, d, TILE), *Stream.scratch(tiles, phases), *more],
        compiler_params=params(collective_id),
    )(at, dgu, dgu, *sum_down)


def gate_up_first_kernel(tiles, cols, at, ahead, behind, sum_down, out, out_down, *rest):
    j = pl.program_id(0)
    place = Place()
    core = place.core
    pair = PairSum(place, tiles, *rest[:4])
    first = First.of(place, DOWN_WINDOW, cols, rest[4:9])
    down = Rest.of(place, DOWN_WINDOW, cols, first.results(), rest[9:17])
    loads = loads_down(sum_down, first, rest[17])

    @pl.when(j == 0)
    def _():
        signal_all(near(place))
        begin(loads)

    pl.when(j >= 2)(lambda: pair.copy(j - 2).wait_recv())
    slot = pair.reserve(j)
    both = side_by_side(ahead[0, 1 - core], behind[0, core])
    landed = lax.rem(j + tiles - 2, tiles)
    for m in range(at.shape[0] // ROWS):
        r = pl.ds(m * ROWS, ROWS)
        tile = dot(at[r, :], both, NN)
        slot[r, :] = tile[:, :TILE].astype(BF16)
        out[r, :] = (tile[:, TILE:] + pair.landing[landed, r, :].astype(F32)).astype(BF16)
    pl.when(j < tiles)(lambda: pair.copy(j).start())

    pl.when(j == 0)(lambda: end(loads))
    pl.when(j <= tiles - 5)(lambda: spread(j, tiles - 4, 16, first.tick))
    pl.when(j >= tiles - 5)(lambda: down.tick(j - tiles + 5))

    @pl.when(j == tiles + 1)
    def _():
        down.result(out_down)
        first.drain()
        down.drain()


def gate_up_first_call(name, collective_id, at, dgu, sum_down):
    d, tokens = at.shape
    tiles, cols, dma = dgu.shape[0], sum_down.shape[-1], pltpu.SemaphoreType.DMA
    now, before = clip(tiles), clip(tiles, 2)
    return pl.pallas_call(
        functools.partial(gate_up_first_kernel, tiles, cols),
        name=name,
        grid=(tiles + 2,),
        in_specs=[
            whole((d, tokens)),
            spec((1, 2, tokens, TILE), lambda j: (now(j), 0, 0, 0)),
            spec((1, 2, tokens, TILE), lambda j: (before(j), 0, 0, 0)),
            HBM,
        ],
        out_specs=[spec((d, TILE), lambda j: (0, before(j))), whole((DOWN_WINDOW, cols))],
        out_shape=[jax.ShapeDtypeStruct(s, BF16) for s in ((d, tiles * TILE), (DOWN_WINDOW, cols))],
        scratch_shapes=[
            *PairSum.scratch(tiles, d, TILE),
            *First.scratch(DOWN_WINDOW, cols),
            *Rest.scratch(DOWN_WINDOW, cols),
            dma((SIDE,)),
        ],
        compiler_params=params(collective_id),
    )(at, dgu, dgu, sum_down)


def middle_kernel(steps, ff, dgu, wg, wu, h, dy, sum_gu, dh, half0, half1, acc_g, acc_u, *rest):
    j = pl.program_id(0)
    place = Place()
    first = First.of(place, GATE_ROWS, ff, rest[:5])
    load_sem, save_sem = rest[5:7]
    loads = [pltpu.make_async_copy(sum_gu.at[x], first.held.at[x], load_sem.at[x]) for x in range(SIDE)]

    @pl.when(j == 0)
    def _():
        signal_all(near(place))
        begin(loads)
        clear(acc_g)
        clear(acc_u)

    def add_up(r, two):
        for which, (acc, w) in enumerate(((acc_g, wg), (acc_u, wu))):
            if two:
                acc[r, :] += dot(side_by_side(dgu[0, which, r, :], dgu[1, which, r, :]), w[0], NT)
            else:
                acc[r, :] += dot(dgu[0, which, r, :], w[0, :, pl.ds(0, TILE)], NT)

    pl.when(j < steps - 1)(lambda: in_rows(h.shape[0], 2 * ROWS, lambda r: add_up(r, True)))
    pl.when(j == steps - 1)(lambda: in_rows(h.shape[0], ROWS, lambda r: add_up(r, False)))

    pl.when(j == 0)(lambda: end(loads))
    spread(j, steps, 16, first.tick)

    @pl.when(j == steps - 1)
    def _():
        saves = copies(first.results(), (half0, half1), save_sem)
        begin(saves)

        def rows(r):
            wide = h[r, :].astype(F32)
            scale = norm_scale(wide)
            da = (acc_g[r, :].astype(BF16).astype(F32) + acc_u[r, :].astype(BF16).astype(F32)).astype(BF16).astype(F32)
            back = scale * da - wide * (scale * scale * scale * jnp.mean(da * wide, -1, keepdims=True))
            dh[r, :] = (dy[r, :].astype(F32) + back.astype(BF16).astype(F32)).astype(BF16)

        in_rows(h.shape[0], 32, rows)
        first.drain()
        end(saves)


def middle_call(collective_id, dgu, wg, wu, h, dy, sum_gu):
    tokens, d = h.shape
    tiles, dma = dgu.shape[0], pltpu.SemaphoreType.DMA
    ff = tiles * TILE
    steps = (tiles + 1) // 2
    w_in = spec((1, d, 2 * TILE), lambda j: (1, 0, j))
    return pl.pallas_call(
        functools.partial(middle_kernel, steps, ff),
        name="middle",
        grid=(steps,),
        in_specs=[spec((2, 2, tokens, TILE), lambda j: (j, 0, 0, 0)), w_in, w_in, whole((tokens, d)), whole((tokens, d)), HBM],
        out_specs=[whole((tokens, d)), HBM, HBM],
        out_shape=[jax.ShapeDtypeStruct(s, BF16) for s in ((tokens, d), *half_sums(GATE_ROWS, ff))],
        scratch_shapes=[pltpu.VMEM((tokens, d), F32)] * 2 + First.scratch(GATE_ROWS, ff) + [dma((SIDE,)), dma((2,))],
        compiler_params=params(collective_id),
    )(dgu, wg, wu, h, dy, sum_gu)


def back_kernel(tiles, ff, dh, gate, up, wd, gate0, gate1, dgu, out, out_gu, p, dps, *rest):
    j = pl.program_id(0)
    place = Place()
    core, half = place.core, dh.shape[1] // 2
    pair = PairSum(place, tiles, *rest[:4])
    before = rest[4:6]
    sums = Rest.of(place, GATE_ROWS, ff, before, rest[6:14])
    loads = copies((gate0, gate1), before, rest[14])

    @pl.when(j == 0)
    def _():
        signal_all(near(place))
        begin(loads)

    two_tiles_of_dp(j, tiles, dh, wd, dps)
    pl.when(j >= 2)(lambda: pair.copy(j - 2).wait_recv())
    tile = jnp.minimum(j, tiles - 1)
    ours = p[lax.rem(j + 1, 3)]
    for m in range(dh.shape[0] // ROWS):
        r = pl.ds(m * ROWS, ROWS)
        p[lax.rem(tile, 3), r, :], dgu[0, 0, r, :], dgu[0, 1, r, :] = hidden_back(gate[0, r, :], up[0, r, :], dps[lax.rem(tile, 2), r, :])
    own = dot(ours, dh[:, pl.ds(pl.multiple_of(core * half, LANES), half)], TN)
    out[...] = (own + pair.landing[lax.rem(j + tiles - 2, tiles)].astype(F32)).astype(BF16)

    @pl.when(j < tiles)
    def _():
        slot = pair.reserve(j)
        slot[...] = dot(p[lax.rem(j, 3)], dh[:, pl.ds(pl.multiple_of((1 - core) * half, LANES), half)], TN).astype(BF16)
        pair.copy(j).start()

    pl.when(j == 0)(lambda: end(loads))
    sums.tick(j)

    @pl.when(j == tiles + 1)
    def _():
        sums.result(out_gu)
        pair.drain()
        sums.drain()


def back_call(collective_id, dh, gate, up, wd, gate_halves):
    tokens, d = dh.shape
    tiles, half, dma = gate.shape[0], d // 2, pltpu.SemaphoreType.DMA
    ff = tiles * TILE
    now, before = clip(tiles), clip(tiles, 2)
    tile = spec((1, tokens, TILE), lambda j: (now(j), 0, 0))
    return pl.pallas_call(
        functools.partial(back_kernel, tiles, ff),
        name="back_0",
        grid=(tiles + 2,),
        in_specs=[whole((tokens, d)), tile, tile, spec((1, 2 * TILE, d), lambda j: (0, lax.div(now(j), 2), 0)), HBM, HBM],
        out_specs=[
            spec((1, 2, tokens, TILE), lambda j: (now(j), 0, 0, 0)),
            spec((TILE, half), lambda j: (before(j), 0)),
            whole((GATE_ROWS, ff)),
        ],
        out_shape=[jax.ShapeDtypeStruct(s, BF16) for s in ((tiles, 2, tokens, TILE), (ff, half), (GATE_ROWS, ff))],
        scratch_shapes=[pltpu.VMEM((3, tokens, TILE), BF16), pltpu.VMEM((2, tokens, TILE), BF16)]
        + PairSum.scratch(tiles, TILE, half)
        + [pltpu.VMEM(t.shape, BF16) for t in gate_halves]
        + Rest.scratch(GATE_ROWS, ff)
        + [dma((2,))],
        compiler_params=params(collective_id),
    )(dh, gate, up, wd, *gate_halves)


def flat(m):
    layers, rows, cols = m.shape
    split = m.transpose(1, 0, 2).reshape(rows, layers, cols // LANES, LANES)
    return with_layout_constraint(split, Layout((0, 2, 1, 3))).transpose(0, 2, 1, 3).reshape(-1, LANES)


def unflat(f, shape):
    layers, rows, cols = shape
    split = f.reshape(rows, cols // LANES, layers, LANES).transpose(0, 2, 1, 3)
    return with_layout_constraint(split, Layout((0, 2, 1, 3))).reshape(rows, layers, cols).transpose(1, 0, 2)


def solution(mesh):
    def body(x, dy, wg, wu, wd, mg, mu, md, vg, vu, vd):
        layers, d, ff = wg.shape
        x, dy = x[0], dy[0]
        windows = (SIDE, SIDE, 4 * 66, d // 2)
        gate0, up0, h1, a1, a0t = forward_call(x, wg, wu, wd)
        dgu1, a1t, down1 = layer_call(1, a1, dy, wg, wu, wd)
        blocks = (SIDE, SIDE, SIDE, GATE_ROWS, ff)
        gu1, sum_down1 = gate_up_first_call("gate_up_1", 2, a1t, dgu1, down1.reshape(windows))
        dh1, *gate_halves = middle_call(3, dgu1, wg, wu, h1, dy, gu1.reshape(blocks))
        dgu0, down0, sum_gu1 = back_call(4, dh1, gate0, up0, wd, gate_halves)
        sum_gu0, sum_down0 = gate_up_call("gate_up_0", 5, 3, a0t, dgu0, down0.reshape(windows))

        views = [(2, SIDE, SIDE, SIDE, GATE_ROWS, ff)] * 2 + [(2, SIDE, SIDE, 4 * 66, d)]
        w = [t.reshape(view) for t, view in zip((wg, wu, wd), views, strict=True)]
        m, v = [flat(t) for t in (mg, mu, md)], [flat(t) for t in (vg, vu, vd)]
        own, other, down, *moments = finish_call(3 * layers * d * ff, 6, [sum_gu0, sum_gu1], [sum_down0, sum_down1], m, v, w)
        out = [*write_call(own, other, down), *moments]
        new = [t.reshape(like.shape) for t, like in zip(out[:3], (wg, wu, wd), strict=True)]
        return (*new, *[unflat(t, like.shape) for t, like in zip(out[3:], (mg, mu, md, vg, vu, vd), strict=True)])

    shard = P(None, "dp", None)
    return jax.shard_map(
        body,
        mesh=mesh,
        in_specs=(P(("rep", "dp")), P(("rep", "dp")), P(), P(), P(), *[shard] * 6),
        out_specs=(P("rep"), P("rep"), P("rep"), *[P("rep", "dp", None)] * 6),
        check_vma=False,
    )
```

```python
import functools

import jax
import jax.numpy as jnp
from jax import lax
from jax.experimental import pallas as pl
from jax.experimental.layout import Layout, with_layout_constraint
from jax.experimental.pallas import tpu as pltpu
from jax.sharding import PartitionSpec as P

F32, BF16 = jnp.float32, jnp.bfloat16
CLIP_EPS = 1e-30
LANES = 128
SIDE = 4
ORDERS = ((0, 1, 2), (1, 2, 0), (2, 0, 1))
VMEM_LIMIT = 63 * 1024 * 1024


class Place:
    def __init__(self):
        me = lax.axis_index("dp")
        self.core = lax.rem(me, 2)
        chip = lax.div(me, 2)
        self.at = (lax.div(chip, SIDE * SIDE), lax.rem(lax.div(chip, SIDE), SIDE), lax.rem(chip, SIDE))
        self.ways = [1 + 2 * lax.rem(way + self.core, 2) for way in range(2)]
        self.onwards = {(axis, way): self.device(axis, self.ways[way]) for axis in range(3) for way in range(2)}
        self.blocks = {
            (axis, way, hops): lax.rem(self.at[axis] + hops * (SIDE - self.ways[way]), SIDE)
            for axis in range(3)
            for way in range(2)
            for hops in range(1, 5)
        }

    def device(self, axis=None, off=0, core=None):
        at = list(self.at)
        if axis is not None:
            at[axis] = lax.rem(at[axis] + off, SIDE)
        core = self.core if core is None else core
        return {"dp": ((at[0] * SIDE + at[1]) * SIDE + at[2]) * 2 + core}

    def partner(self):
        return self.device(core=1 - self.core)

    def onward(self, way):
        return self.ways[way]

    def block(self, axis, way, hops):
        if isinstance(hops, int) and hops:
            return self.blocks[axis, way, hops]
        return lax.rem(self.at[axis] + hops * (SIDE - self.ways[way]), SIDE)


def signal_all(devices):
    barrier = pltpu.get_barrier_semaphore()
    for d in devices:
        pl.semaphore_signal(barrier, inc=1, device_id=d, device_id_type=pl.DeviceIdType.MESH)
    pl.semaphore_wait(barrier, len(devices))


def near(place):
    return [place.partner()] + [place.device(axis, off) for axis in range(3) for off in (1, SIDE - 1)]


def put(src, dst, send, recv, device):
    return pltpu.make_async_remote_copy(
        src_ref=src, dst_ref=dst, send_sem=send, recv_sem=recv, device_id=device, device_id_type=pl.DeviceIdType.MESH
    )


def ways_of(cols):
    tiles = cols // LANES
    first = (tiles + 1) // 2 * LANES
    return ((0, first), (first, cols - first))


def index(order, values):
    out = [None] * 3
    for axis, value in zip(order, values, strict=True):
        out[axis] = value
    return tuple(out)


ALL = slice(None)


class Rings:
    def __init__(self, place, rows, cols, slots, sems):
        self.place, self.rows, self.slots, self.sems = place, rows // 3, slots, sems
        self.ways = ways_of(cols)

    def part(self, t, way):
        start, width = self.ways[way]
        return pl.ds(t * self.rows, self.rows), pl.ds(start, width)

    @staticmethod
    def pairs():
        return [(t, way) for t in range(3) for way in range(2)]

    def send(self, axis, way, src, landing, key, sems):
        src = landing if src is None else src
        return put(src, landing, sems[0].at[key], sems[1].at[key], self.place.onwards[axis, way])


class First(Rings):
    @staticmethod
    def scratch(rows, cols):
        third, dma = rows // 3, pltpu.SemaphoreType.DMA
        slots = [pltpu.VMEM((3, 3, SIDE, SIDE, third, width), BF16) for _, width in ways_of(cols)]
        return [pltpu.VMEM((SIDE, SIDE, SIDE, rows, cols), BF16), *slots, dma((3, 2, 3, SIDE)), dma((3, 2, 3, SIDE))]

    @classmethod
    def of(cls, place, rows, cols, refs):
        one = cls(place, rows, cols, refs[1:3], refs[3:5])
        one.held = refs[0]
        return one

    def block(self, t, way, hops, k, c=ALL):
        order = ORDERS[t]
        return self.held.at[(*index(order, (self.place.block(order[0], way, hops), k, c)), *self.part(t, way))]

    def message(self, t, way, n, k, arriving=False):
        src = None
        if not arriving:
            src = self.block(t, way, 1, k) if isinstance(n, int) and n == 0 else self.slots[way].at[t, n - 1, k]
        return self.send(ORDERS[t][0], way, src, self.slots[way].at[t, n, k], (t, way, n, k), self.sems)

    def start(self, k):
        for t, way in self.pairs():
            self.message(t, way, 0, k).start()

    def step(self, n, k):
        for t, way in self.pairs():
            self.message(t, way, n - 1, k, arriving=True).wait_recv()
            slots = self.slots[way]
            for c in range(SIDE):
                own = self.block(t, way, n + 1, k, c)
                slots[t, n - 1, k, c] = (slots[t, n - 1, k, c].astype(F32) + own[...].astype(F32)).astype(BF16)
            pl.when(n < 3)(lambda t=t, way=way: self.message(t, way, n, k).start())

    def tick(self, i):
        pl.when(i < SIDE)(lambda: self.start(i))
        pl.when(i >= SIDE)(lambda: self.step(lax.div(i, SIDE), lax.rem(i, SIDE)))

    def results(self):
        return [slots.at[:, 2] for slots in self.slots]

    def drain(self):
        def sent(k, _):
            for t, way in self.pairs():
                self.message(t, way, 0, k).wait_send()
                lax.fori_loop(1, 3, lambda n, _: (self.message(t, way, n, k).wait_send(), 0)[1], 0)
            return 0

        lax.fori_loop(0, SIDE, sent, 0)


class Rest(Rings):
    @staticmethod
    def scratch(rows, cols):
        third, dma = rows // 3, pltpu.SemaphoreType.DMA
        shapes = [pltpu.VMEM((*lead, third, width), BF16) for lead in ((3, 3, SIDE), (3, 3)) for _, width in ways_of(cols)]
        return shapes + [dma((3, 2, 3))] * 4

    @classmethod
    def of(cls, place, rows, cols, before, refs):
        one = cls(place, rows, cols, refs[:4], refs[4:8])
        one.before = before
        return one

    def message(self, phase, t, way, n, arriving=False):
        slots = self.slots[2 * phase - 2 + way]
        axis = ORDERS[t][phase]
        if arriving:
            src = None
        elif isinstance(n, int) and n == 0:
            v = self.place.block(axis, way, 1)
            src = self.before[way].at[t, v] if phase == 1 else self.slots[way].at[t, 2, v]
        else:
            src = slots.at[t, n - 1]
        return self.send(axis, way, src, slots.at[t, n], (t, way, n), self.sems[2 * phase - 2 : 2 * phase])

    def start(self, phase):
        for t, way in self.pairs():
            self.message(phase, t, way, 0).start()

    def step1(self, n):
        for t, way in self.pairs():
            self.message(1, t, way, n - 1, arriving=True).wait_recv()
            v = self.place.block(ORDERS[t][1], way, n + 1)
            before, slots = self.before[way], self.slots[way]
            for c in range(SIDE):
                slots[t, n - 1, c] = (slots[t, n - 1, c].astype(F32) + before[t, v, c].astype(F32)).astype(BF16)
            pl.when(n < 3)(lambda t=t, way=way: self.message(1, t, way, n).start())

    def step2(self, n):
        for t, way in self.pairs():
            self.message(2, t, way, n - 1, arriving=True).wait_recv()
            v = self.place.block(ORDERS[t][2], way, n + 1)
            before, slots = self.slots[way], self.slots[2 + way]
            slots[t, n - 1] = (slots[t, n - 1].astype(F32) + before[t, 2, v].astype(F32)).astype(BF16)
            pl.when(n < 3)(lambda t=t, way=way: self.message(2, t, way, n).start())

    def tick(self, i):
        pl.when(i == 0)(lambda: self.start(1))
        pl.when((i >= 1) & (i <= 3))(lambda: self.step1(i))
        pl.when(i == 3)(lambda: self.start(2))
        pl.when((i >= 4) & (i <= 6))(lambda: self.step2(i - 3))

    def result(self, out):
        for t, way in self.pairs():
            out[self.part(t, way)] = self.slots[2 + way][t, 2]

    def drain(self):
        for t, way in self.pairs():
            for phase in (1, 2):
                for n in range(3):
                    self.message(phase, t, way, n).wait_send()


def loads_down(source, first, sems):
    return [pltpu.make_async_copy(source.at[:, :, pl.ds(64 * z, 72)], first.held.at[:, :, z], sems.at[z]) for z in range(SIDE)]


def spread(j, steps, count, tick):
    low, high = lax.div(count * j, steps), lax.div(count * (j + 1), steps)
    lax.fori_loop(low, high, lambda i, _: (tick(i), 0)[1], 0)


def copies(sources, targets, sems):
    return [pltpu.make_async_copy(s, t, sems.at[i]) for i, (s, t) in enumerate(zip(sources, targets, strict=True))]


def begin(all_copies):
    for copy in all_copies:
        copy.start()


def end(all_copies):
    for copy in all_copies:
        copy.wait()


def half_sums(rows, cols):
    return [(3, SIDE, SIDE, rows // 3, width) for _, width in ways_of(cols)]


PREV = 6
DOWN_ROWS = 33


class Gather:
    def __init__(self, place, bufs, sems, outs, copy_sems):
        self.place, self.bufs, self.sems, self.outs, self.copy_sems = place, bufs, sems, outs, copy_sems

    @staticmethod
    def scratch(down_cols):
        buf = pltpu.VMEM((2, SIDE, SIDE, SIDE, 72, down_cols), BF16)
        return [buf] + [pltpu.SemaphoreType.DMA((2, 3, 2, 6, 3))] * 4 + [pltpu.SemaphoreType.DMA((2,))] * 3

    def part(self, kind, t, way):
        rows, cols = self.bufs[kind].shape[-2:]
        start, width = ways_of(cols)[way]
        return pl.ds(t * (rows // 3), rows // 3), pl.ds(start, width)

    def behind(self, t, way, axis, hops):
        return self.place.block(ORDERS[t][axis], way, hops)

    def message(self, kind, l, t, way, line, n, hops):
        order, place = ORDERS[t], self.place
        if isinstance(line, int) and line == 0:
            axis, values = order[0], [self.behind(t, way, 0, hops), place.at[order[1]], place.at[order[2]]]
        elif isinstance(line, int) and line == 1:
            axis, values = order[1], [ALL, self.behind(t, way, 1, hops), place.at[order[2]]]
        else:
            axis, values = order[2], [ALL, self.behind(t, way, 1, line - 2), self.behind(t, way, 2, hops)]
        ref = self.bufs[kind].at[(l, *index(order, values), *self.part(kind, t, way))]
        key = (l, t, way, line, n)
        return put(ref, ref, self.sems[2 * kind].at[key], self.sems[2 * kind + 1].at[key], place.onwards[axis, way])

    def copies(self, kind, l, t, way, b, c):
        order = ORDERS[t]
        rows, cols = self.part(kind, t, way)
        at = index(order, (ALL, b, c))
        if kind == 0:
            return [lambda out: (self.bufs[0].at[(l, *at, rows, cols)], out.at[(l, *at, rows, cols)])]
        half = self.bufs[1].shape[-1]
        start, width = ways_of(half)[way]
        columns = pl.ds(pl.multiple_of(self.place.core * half + start, LANES), width)
        x, y, z = at

        def pair(out, z, count):
            src = self.bufs[1].at[l, x, y, z, pl.ds(24 * t, count), cols]
            return src, out.at[l, x, y, pl.ds(pl.multiple_of(64 * z + 24 * t, 8), count), columns]

        if t < 2:
            return [lambda out: pair(out, z, 24)]
        return [lambda out, z=z: pair(out, z, 16 if z < SIDE - 1 else 24) for z in range(SIDE)]

    def copy_out(self, kind, l, t, way, b, c):
        local, send, recv = self.copy_sems
        for pair in self.copies(kind, l, t, way, b, c):
            src, dst = pair(self.outs[kind])
            if kind:
                pltpu.make_async_copy(src, dst, local.at[kind]).start()
            put(src, dst, send.at[kind], recv.at[kind], self.place.partner()).start()

    def parts(self):
        return [(kind, t, way) for kind in range(2) for t in range(3) for way in range(2)]

    def own(self, l):
        for kind, t, way in self.parts():
            self.message(kind, l, t, way, 0, 0, 0).start()

    def start_third(self, kind, l, t, way, m):
        self.message(kind, l, t, way, 2 + m, 0, 0).start()
        self.copy_out(kind, l, t, way, self.behind(t, way, 1, m), self.place.at[ORDERS[t][2]])

    def first_axis(self):
        def step(i, _):
            n, l = 1 + lax.div(i, 2), lax.rem(i, 2)
            for kind, t, way in self.parts():
                self.message(kind, l, t, way, 0, n - 1, n).wait_recv()
                pl.when(n < 3)(lambda kind=kind, t=t, way=way: self.message(kind, l, t, way, 0, n, n).start())

                @pl.when(n == 3)
                def _(kind=kind, t=t, way=way):
                    self.message(kind, l, t, way, 1, 0, 0).start()
                    self.start_third(kind, l, t, way, 0)

            return 0

        lax.fori_loop(0, 6, step, 0)

    def other_axes(self):
        def step(i, _):
            r, l = 1 + lax.div(i, 2), lax.rem(i, 2)
            for kind, t, way in self.parts():

                @pl.when(r <= 3)
                def _(kind=kind, t=t, way=way):
                    self.message(kind, l, t, way, 1, r - 1, r).wait_recv()
                    pl.when(r < 3)(lambda: self.message(kind, l, t, way, 1, r, r).start())
                    self.start_third(kind, l, t, way, r)

                def third(m, _, kind=kind, t=t, way=way):
                    n = r - m
                    self.message(kind, l, t, way, 2 + m, n - 1, n).wait_recv()
                    pl.when(n < 3)(lambda: self.message(kind, l, t, way, 2 + m, n, n).start())
                    self.copy_out(kind, l, t, way, self.behind(t, way, 1, m), self.behind(t, way, 2, n))
                    return 0

                lax.fori_loop(jnp.maximum(r - 3, 0), jnp.minimum(r, SIDE), third, 0)
            return 0

        lax.fori_loop(0, 12, step, 0)

    def drain(self):
        local, send, recv = self.copy_sems
        half = self.bufs[1].shape[-1]
        columns = self.outs[1].at[:, :, :, :, pl.ds(0, half)]
        for kind, whole in ((0, self.outs[0]), (1, columns)):
            if kind:
                pltpu.make_async_copy(whole, whole, local.at[kind]).wait()
            copy = put(whole, whole, send.at[kind], recv.at[kind], self.place.partner())
            copy.wait_send()
            copy.wait_recv()

        def sent(i, _):
            l, n = lax.div(i, 3), lax.rem(i, 3)
            for kind, t, way in self.parts():
                for line in range(2):
                    self.message(kind, l, t, way, line, n, n).wait_send()
                lax.fori_loop(2, 6, lambda line, _: (self.message(kind, l, t, way, line, n, n).wait_send(), 0)[1], 0)
            return 0

        lax.fori_loop(0, 6, sent, 0)


def finish_kernel(count, *refs):
    sums_gu, sums_d, m_in, v_in, w_in = refs[0:2], refs[2:4], refs[4:7], refs[7:10], refs[10:13]
    own_gu, w_out, m_out, v_out = refs[13], refs[14:16], refs[16:19], refs[19:22]
    moments_gu, moments_d, old_gu, old_d, other_d, tiles = refs[22:28]
    load_sem, early_send, early_recv, norm_send, norm_recv, late_local, late_send, late_recv = refs[28:36]
    gather_refs = refs[36:]
    place = Place()
    x, y, z = place.at
    core = place.core
    gather = Gather(place, (own_gu, gather_refs[0]), gather_refs[1:5], w_out, gather_refs[5:8])
    partner = place.partner()
    gate_tiles, down_tiles = sums_gu[0].shape[1] // LANES, sums_d[0].shape[1] // LANES
    gate_stride, down_stride = 2 * gate_tiles, 4 * down_tiles
    gate_size, down_size = 12 * gate_stride, DOWN_ROWS * down_stride

    def blank(i, _):
        for which in range(2):
            moments_d[which, pl.ds(pl.multiple_of(8 * i, 8), 8), :] = jnp.zeros((8, LANES), F32)
        return 0

    lax.fori_loop(0, moments_d.shape[1] // 8, blank, 0)
    following = [place.device(2, 1, core=c) for c in range(2)]
    others = [place.device(axis, 2) for axis in range(3)] + [place.device(2, off, core=1 - core) for off in (1, SIDE - 1)]
    signal_all(near(place) + others)

    def gate_rows(i, which):
        return moments_gu.at[i, pl.ds(pl.multiple_of(which * gate_size, 8), gate_size)]

    def down_rows(i, first, rows):
        return moments_d.at[i, pl.ds(pl.multiple_of(first * down_stride, 8), rows * down_stride)]

    def columns(ref):
        half = down_tiles * LANES
        return ref.at[:, x, y, pl.ds(pl.multiple_of(64 * z, 8), 72), pl.ds(pl.multiple_of(core * half, LANES), half)]

    own_rows = PREV + 2 * z + DOWN_ROWS * core
    loads, sends = [], []
    for i, moment in enumerate((m_in, v_in)):
        for c in range(2):

            @pl.when(core == c)
            def _(i=i, moment=moment, c=c):
                pltpu.make_async_copy(moment[c], gate_rows(i, core), load_sem.at[i]).start()
                put(moment[1 - c], gate_rows(i, core), early_send.at[i], early_recv.at[i], partner).start()

        loads.append(pltpu.make_async_copy(moment[0], gate_rows(i, core), load_sem.at[i]))
        sends.append(put(moment[0], gate_rows(i, core), early_send.at[i], early_recv.at[i], partner))
        loads.append(pltpu.make_async_copy(moment[2], down_rows(i, own_rows, DOWN_ROWS), load_sem.at[2 + i]))
        loads[-1].start()
        sends.append(put(moment[2], down_rows(i, own_rows, DOWN_ROWS), early_send.at[2 + i], early_recv.at[2 + i], partner))
        sends[-1].start()
        last = moment[2].at[pl.ds((DOWN_ROWS - PREV) * down_stride, PREV * down_stride)]
        landing = down_rows(i, 2 * lax.rem(z + 1, SIDE), PREV)

        @pl.when(core == 1)
        def _(i=i, last=last, landing=landing):
            for c in range(2):
                put(last, landing, early_send.at[4 + 2 * i + c], early_recv.at[4 + i], following[c]).start()

    for l in range(2):
        sends.append(put(sums_d[l], other_d.at[l], early_send.at[8 + l], early_recv.at[6 + l], partner))
        sends[-1].start()
    for c in range(2):

        @pl.when(core == c)
        def _(c=c):
            pltpu.make_async_copy(w_in[c].at[:, x, y, z], old_gu, load_sem.at[4]).start()

    loads.append(pltpu.make_async_copy(w_in[0].at[:, x, y, z], old_gu, load_sem.at[4]))
    loads.append(pltpu.make_async_copy(columns(w_in[2]), old_d, load_sem.at[5]))
    loads[-1].start()

    squares = jnp.zeros((8, LANES), F32)
    for l in range(2):

        def of_gate_up(j, total, l=l):
            for t in range(3):
                g = sums_gu[l][pl.ds(8 * t, 8), pl.ds(pl.multiple_of(j * LANES, LANES), LANES)].astype(F32)
                total += g * g
            return total

        squares = lax.fori_loop(0, gate_tiles, of_gate_up, squares)

        def of_down(i, total, l=l):
            row = 8 * i + lax.broadcasted_iota(jnp.int32, (8, LANES), 0)
            mine = (row >= 2 * z) & (row < 2 * z + 2 * DOWN_ROWS)
            for j in range(down_tiles):
                g = sums_d[l][pl.ds(pl.multiple_of(8 * i, 8), 8), pl.ds(j * LANES, LANES)].astype(F32)
                total += jnp.where(mine, g * g, 0.0)
            return total

        squares = lax.fori_loop(0, 9, of_down, squares)
    for stage, (coordinate, size) in enumerate(((core, 2), (x, SIDE), (y, SIDE), (z, SIDE))):
        tiles[stage, coordinate] = squares
        exchanges = []
        for off in range(1, size):
            target = partner if stage == 0 else place.device(stage - 1, off)
            key = 3 * stage + off - 1
            here = tiles.at[stage, coordinate]
            exchanges.append(put(here, here, norm_send.at[key], norm_recv.at[key], target))
            exchanges[-1].start()
        for exchange in exchanges:
            exchange.wait_recv()
        for exchange in exchanges:
            exchange.wait_send()
        squares = tiles[stage, 0]
        for other in range(1, size):
            squares += tiles[stage, other]
    total = jnp.sum(jnp.sum(squares, 0, keepdims=True), 1, keepdims=True)
    factor = jnp.minimum(1.0, 0.5 * lax.rsqrt(total / count + CLIP_EPS))

    for copy in loads:
        copy.wait()
    for copy in sends:
        copy.wait_recv()
    for i in range(2):
        put(down_rows(i, 0, PREV), down_rows(i, 0, PREV), early_send.at[0], early_recv.at[4 + i], partner).wait_recv()

    def moments(ref, start, stride, g):
        rows = pl.ds(start, 8, stride=stride)
        m = 0.9 * ref[0, rows, :] + 0.1 * g
        v = 0.95 * ref[1, rows, :] + 0.05 * g * g
        ref[0, rows, :] = m
        ref[1, rows, :] = v
        return m * lax.rsqrt(v + 1e-8)

    def weight(w, step):
        w = w.astype(F32)
        return (w - 0.02 * (step + 0.1 * w)).astype(BF16)

    for l in range(2):

        def gate_up(j, _, l=l):
            lanes = pl.ds(pl.multiple_of(j * LANES, LANES), LANES)
            for t in range(3):
                rows = pl.ds(8 * t, 8)
                g = sums_gu[l][rows, lanes].astype(F32) * factor
                step = moments(moments_gu, 8 * t * gate_stride + 2 * j + l, gate_stride, g)
                gather.bufs[0][l, x, y, z, rows, lanes] = weight(old_gu[l, rows, lanes], step)
            return 0

        lax.fori_loop(0, gate_tiles, gate_up, 0, unroll=3)

        def down(i, _, l=l):
            rows = pl.ds(pl.multiple_of(8 * i, 8), 8)
            for j in range(down_tiles):
                lanes = pl.ds(j * LANES, LANES)
                start = (PREV + 8 * i) * down_stride + 2 * j + l
                g = sums_d[l][rows, lanes].astype(F32) * factor
                step = moments(moments_d, start + 2 * down_tiles * core, down_stride, g)
                gather.bufs[1][l, x, y, z, rows, lanes] = weight(old_d[l, rows, lanes], step)
            return 0

        lax.fori_loop(0, 9, down, 0)
        gather.own(l)
    for l in range(2):

        def down_other(i, _, l=l):
            rows = pl.ds(pl.multiple_of(8 * i, 8), 8)
            for j in range(down_tiles):
                start = (PREV + 8 * i) * down_stride + 2 * j + l
                g = other_d[l, rows, pl.ds(j * LANES, LANES)].astype(F32) * factor
                moments(moments_d, start + 2 * down_tiles * (1 - core), down_stride, g)
            return 0

        lax.fori_loop(0, 9, down_other, 0)

    late = []
    for i, out in enumerate((m_out, v_out)):
        for c in range(2):

            @pl.when(core == c)
            def _(i=i, out=out, c=c):
                pltpu.make_async_copy(gate_rows(i, core), out[c], late_local.at[i]).start()
                put(gate_rows(i, 1 - core), out[c], late_send.at[i], late_recv.at[i], partner).start()

        pltpu.make_async_copy(down_rows(i, own_rows, DOWN_ROWS), out[2], late_local.at[2 + i]).start()
    gather.first_axis()
    gather.other_axes()
    for i, out in enumerate((m_out, v_out)):
        pltpu.make_async_copy(gate_rows(i, core), out[0], late_local.at[i]).wait()
        pltpu.make_async_copy(down_rows(i, own_rows, DOWN_ROWS), out[2], late_local.at[2 + i]).wait()
        copy = put(gate_rows(i, 1 - core), out[0], late_send.at[i], late_recv.at[i], partner)
        copy.wait_recv()
        copy.wait_send()
    for copy in sends:
        copy.wait_send()
    for i in range(2):
        for c in range(2):

            @pl.when(core == 1)
            def _(i=i, c=c):
                rows = down_rows(i, 0, PREV)
                put(rows, rows, early_send.at[4 + 2 * i + c], early_recv.at[4 + i], following[c]).wait_send()

    gather.drain()


def finish_call(count, collective_id, sums_gu, sums_d, m, v, w):
    gate_cols, down_half = sums_gu[0].shape[1], sums_d[0].shape[1]
    operands = [*sums_gu, *sums_d, *m, *v, *w]
    hbm, vmem = pl.BlockSpec(memory_space=pltpu.HBM), pl.BlockSpec(memory_space=pltpu.VMEM)
    dma = pltpu.SemaphoreType.DMA
    gate_stride, down_stride = gate_cols // 64, down_half // 32
    scratch = [
        pltpu.VMEM((2, 24 * gate_stride, LANES), F32),
        pltpu.VMEM((2, (PREV + 72) * down_stride, LANES), F32),
        pltpu.VMEM((2, 24, gate_cols), BF16),
        pltpu.VMEM((2, 72, down_half), BF16),
        pltpu.VMEM((2, 72, down_half), BF16),
        pltpu.VMEM((4, SIDE, 8, LANES), F32),
        dma((6,)), dma((10,)), dma((8,)), dma((12,)), dma((12,)), dma((4,)), dma((2,)), dma((2,)),
    ]
    return pl.pallas_call(
        functools.partial(finish_kernel, count),
        name="finish",
        out_shape=[pltpu.VMEM(w[0].shape, BF16), *[jax.ShapeDtypeStruct(t.shape, t.dtype) for t in (w[0], w[2], *m, *v)]],
        in_specs=[vmem] * 4 + [hbm] * 9,
        out_specs=[vmem] + [hbm] * 8,
        scratch_shapes=scratch + Gather.scratch(down_half),
        compiler_params=pltpu.CompilerParams(collective_id=collective_id, has_side_effects=True, vmem_limit_bytes=26 * 1024 * 1024),
        cost_estimate=pl.CostEstimate(flops=10**9, bytes_accessed=10**8, transcendentals=0),
    )(*operands)


def write_kernel(bounces, own, other, down, gate_out, up_out, down_out, bounce, own_sem, in_sem, out_sem):
    core = lax.rem(lax.axis_index("dp"), 2)
    places = [(l, x, y) for l in range(2) for x in range(SIDE) for y in range(SIDE)]
    pieces = [(other, None, at) for at in places] + [(down, down_out, at) for at in places]

    def slot(i):
        source = pieces[i][0]
        return bounce[0 if source is other else 1].at[i % bounces]

    def read(i):
        source, _, at = pieces[i]
        return pltpu.make_async_copy(source.at[at], slot(i), in_sem.at[i % bounces])

    def write(i, out=None):
        _, to, at = pieces[i]
        return pltpu.make_async_copy(slot(i), (out if to is None else to).at[at], out_sem.at[i % bounces])

    for i in range(bounces):
        read(i).start()
    for c, (mine, others) in enumerate(((gate_out, up_out), (up_out, gate_out))):

        @pl.when(core == c)
        def _(mine=mine, others=others):
            pltpu.make_async_copy(own, mine, own_sem).start()
            for i in range(len(pieces)):
                read(i).wait()
                write(i, others).start()
                done = i - bounces // 2
                if done >= 0 and done + bounces < len(pieces):
                    write(done, others).wait()
                    read(done + bounces).start()

    for i in range(len(pieces) - bounces, len(pieces)):
        write(i, gate_out).wait()
    pltpu.make_async_copy(own, gate_out, own_sem).wait()


def write_call(own, other, down):
    hbm = pl.BlockSpec(memory_space=pltpu.HBM)
    bounces, dma = 8, pltpu.SemaphoreType.DMA
    return pl.pallas_call(
        lambda *refs: write_kernel(bounces, *refs[:6], refs[6:8], *refs[8:]),
        name="write",
        out_shape=[jax.ShapeDtypeStruct(t.shape, BF16) for t in (other, other, down)],
        in_specs=[pl.BlockSpec(memory_space=pl.ANY), hbm, hbm],
        out_specs=[hbm] * 3,
        scratch_shapes=[pltpu.VMEM((bounces, *t.shape[3:]), BF16) for t in (other, down)] + [dma, dma((bounces,)), dma((bounces,))],
        compiler_params=pltpu.CompilerParams(vmem_limit_bytes=14 * 1024 * 1024),
    )(own, other, down)


TILE = 384
ROWS = 256
TIGHT = pl.Buffered(buffer_count=1)


def dot(a, b, dims):
    return lax.dot_general(a, b, (dims, ((), ())), preferred_element_type=F32)


NN, NT, TN = ((1,), (0,)), ((1,), (1,)), ((0,), (0,))


def norm_scale(wide):
    return lax.rsqrt(jnp.mean(wide * wide, -1, keepdims=True) + 1e-6)


def in_rows(total, step, body):
    def one(i, _):
        body(pl.ds(pl.multiple_of(i * step, step), step))
        return 0

    lax.fori_loop(0, total // step, one, 0)


def clear(acc):
    def rows(r):
        acc[r, :] = jnp.zeros((8, acc.shape[1]), F32)

    in_rows(acc.shape[0], 8, rows)


def spec(shape, index_map, tight=False):
    return pl.BlockSpec(shape, index_map, pipeline_mode=TIGHT) if tight else pl.BlockSpec(shape, index_map)


def whole(shape, tight=True):
    return spec(shape, lambda j: (0,) * len(shape), tight)


HBM = pl.BlockSpec(memory_space=pltpu.HBM)


def params(collective_id=None, semantics=("arbitrary",)):
    more = {} if collective_id is None else {"collective_id": collective_id, "has_side_effects": True}
    return pltpu.CompilerParams(dimension_semantics=semantics, vmem_limit_bytes=VMEM_LIMIT, **more)


def transpose_piece(j, last, src, dst):
    def piece(i):
        at = pl.ds(pl.multiple_of(i * LANES, LANES), LANES)
        dst[at, :] = src[:, at].T

    piece(j)
    pl.when(j == last)(lambda: piece(last + 1))


def side_by_side(a, b):
    return jnp.concatenate([a, b], axis=1)


def forward_kernel(tiles, x, wg, wu, wd, gate, up, h_out, a_out, at, a, acc, p):
    j = pl.program_id(0)

    @pl.when(j == 0)
    def _():
        def rows(r):
            wide = x[r, :].astype(F32)
            a[r, :] = (wide * norm_scale(wide)).astype(BF16)

        in_rows(x.shape[0], 32, rows)
        clear(acc)

    transpose_piece(j, tiles - 1, a, at)
    both = side_by_side(wg[0], wu[0])
    slot = lax.rem(j, 2)
    for m in range(x.shape[0] // ROWS):
        r = pl.ds(m * ROWS, ROWS)
        gu = dot(a[r, :], both, NN)
        g, u = gu[:, :TILE], gu[:, TILE:]
        gate[0, r, :] = g
        up[0, r, :] = u
        p[slot, r, :] = (g * lax.logistic(g) * u).astype(BF16)

    @pl.when(slot == 1)
    def _():
        for m in range(x.shape[0] // ROWS):
            r = pl.ds(m * ROWS, ROWS)
            acc[r, :] += dot(side_by_side(p[0, r, :], p[1, r, :]), wd[0], NN)

    @pl.when(j == tiles - 1)
    def _():
        def last_down(r):
            acc[r, :] += dot(p[0, r, :], wd[0, pl.ds(0, TILE), :], NN)

        in_rows(x.shape[0], ROWS, last_down)

        def rows(r):
            h = (x[r, :].astype(F32) + acc[r, :].astype(BF16).astype(F32)).astype(BF16)
            h_out[r, :] = h
            wide = h.astype(F32)
            a_out[r, :] = (wide * norm_scale(wide)).astype(BF16)

        in_rows(x.shape[0], 32, rows)


def forward_call(x, wg, wu, wd):
    tokens, d = x.shape
    ff = wg.shape[2]
    tiles = ff // TILE
    w_in = spec((1, d, TILE), lambda j: (0, 0, j))
    return pl.pallas_call(
        functools.partial(forward_kernel, tiles),
        name="forward_0",
        grid=(tiles,),
        in_specs=[whole((tokens, d)), w_in, w_in, spec((1, 2 * TILE, d), lambda j: (0, lax.div(j, 2), 0))],
        out_specs=[spec((1, tokens, TILE), lambda j: (j, 0, 0))] * 2 + [whole((tokens, d))] * 2 + [whole((d, tokens))],
        out_shape=[jax.ShapeDtypeStruct((tiles, tokens, TILE), F32)] * 2
        + [jax.ShapeDtypeStruct((tokens, d), BF16)] * 2
        + [jax.ShapeDtypeStruct((d, tokens), BF16)],
        scratch_shapes=[pltpu.VMEM((tokens, d), BF16), pltpu.VMEM((tokens, d), F32), pltpu.VMEM((2, tokens, TILE), BF16)],
        compiler_params=params(),
    )(x, wg, wu, wd)


class PairSum:
    def __init__(self, place, tiles, landing, stage, send, recv):
        self.place, self.tiles, self.landing, self.stage, self.send, self.recv = place, tiles, landing, stage, send, recv

    @staticmethod
    def scratch(tiles, rows, cols):
        dma = pltpu.SemaphoreType.DMA
        return [pltpu.VMEM((tiles, rows, cols), BF16), pltpu.VMEM((2, rows, cols), BF16), dma((2,)), dma((tiles,))]

    def copy(self, i):
        slot = lax.rem(i, 2)
        return put(self.stage.at[slot], self.landing.at[i], self.send.at[slot], self.recv.at[i], self.place.partner())

    def reserve(self, i):
        pl.when(i >= 2)(lambda: self.copy(i - 2).wait_send())
        return self.stage.at[lax.rem(i, 2)]

    def drain(self):
        for i in (self.tiles - 2, self.tiles - 1):
            self.copy(i).wait_send()


def hidden_back(gate, up, dp):
    dp = dp.astype(F32)
    s = lax.logistic(gate)
    act = gate * s
    return (act * up).astype(BF16), (dp * up * (s + act * (1.0 - s))).astype(BF16), (dp * act).astype(BF16)


def down_gradient(j, tiles, pair, p, dy, half, out):
    core = pair.place.core

    def columns(c):
        return pl.ds(pl.multiple_of(c * half, LANES), half)

    @pl.when(j < tiles)
    def _():
        slot = pair.reserve(j)
        slot[...] = dot(p[lax.rem(j, 2)], dy[:, columns(1 - core)], TN).astype(BF16)
        pair.copy(j).start()

    @pl.when(j >= 1)
    def _():
        pair.copy(j - 1).wait_recv()
        own = dot(p[lax.rem(j - 1, 2)], dy[:, columns(core)], TN)
        out[...] = (own + pair.landing[j - 1].astype(F32)).astype(BF16)

    pl.when(j == tiles)(pair.drain)


def layer_kernel(tiles, a, dy, wg, wu, wd, dgu, at, out, p, dps, *rest):
    j = pl.program_id(0)
    place = Place()
    pair = PairSum(place, tiles, *rest)
    pl.when(j == 0)(lambda: signal_all([place.partner()]))
    two_tiles_of_dp(j, tiles, dy, wd, dps)

    @pl.when(j < tiles)
    def _():
        transpose_piece(j, tiles - 1, a, at)
        slot = lax.rem(j, 2)
        both = side_by_side(wg[0], wu[0])
        for m in range(a.shape[0] // ROWS):
            r = pl.ds(m * ROWS, ROWS)
            gu = dot(a[r, :], both, NN)
            p[slot, r, :], dgu[0, 0, r, :], dgu[0, 1, r, :] = hidden_back(gu[:, :TILE], gu[:, TILE:], dps[slot, r, :])

    down_gradient(j, tiles, pair, p, dy, dy.shape[1] // 2, out)


def two_tiles_of_dp(j, tiles, dy, wd, dps):
    @pl.when((lax.rem(j, 2) == 0) & (j < tiles - 1))
    def _():
        for m in range(dy.shape[0] // ROWS):
            r = pl.ds(m * ROWS, ROWS)
            dp = dot(dy[r, :], wd[0], NT).astype(BF16)
            dps[0, r, :] = dp[:, :TILE]
            dps[1, r, :] = dp[:, TILE:]

    @pl.when(j == tiles - 1)
    def _():
        def one_tile(r):
            dps[0, r, :] = dot(dy[r, :], wd[0, pl.ds(0, TILE), :], NT).astype(BF16)

        in_rows(dy.shape[0], ROWS, one_tile)


def clip(tiles, back=0):
    return lambda j: jnp.clip(j - back, 0, tiles - 1)


def layer_call(collective_id, a, dy, wg, wu, wd):
    tokens, d = a.shape
    ff = wg.shape[2]
    tiles, half = ff // TILE, d // 2
    now, before = clip(tiles), clip(tiles, 1)
    w_in = spec((1, d, TILE), lambda j: (1, 0, now(j)))
    return pl.pallas_call(
        functools.partial(layer_kernel, tiles),
        name="layer_1",
        grid=(tiles + 1,),
        in_specs=[whole((tokens, d))] * 2 + [w_in, w_in, spec((1, 2 * TILE, d), lambda j: (1, lax.div(now(j), 2), 0))],
        out_specs=[spec((1, 2, tokens, TILE), lambda j: (now(j), 0, 0, 0)), whole((d, tokens)), spec((TILE, half), lambda j: (before(j), 0))],
        out_shape=[
            jax.ShapeDtypeStruct((tiles, 2, tokens, TILE), BF16),
            jax.ShapeDtypeStruct((d, tokens), BF16),
            jax.ShapeDtypeStruct((ff, half), BF16),
        ],
        scratch_shapes=[pltpu.VMEM((2, tokens, TILE), BF16)] * 2 + PairSum.scratch(tiles, TILE, half),
        compiler_params=params(collective_id),
    )(a, dy, wg, wu, wd)


GATE_ROWS, DOWN_WINDOW = 24, 72
RING = 6


def second(t, v, rest=ALL):
    return (rest, v) if t == 1 else (v, rest)


class Stream:
    def __init__(self, place, tiles, phases, refs):
        self.place, self.tiles, self.phases, self.rows = place, tiles, phases, GATE_ROWS // 3
        self.held, self.slots, self.send, self.recv = refs[0], refs[1 : 1 + 2 * phases], refs[-2], refs[-1]
        self.ways = ways_of(TILE)

    @staticmethod
    def scratch(tiles, phases):
        third, dma = GATE_ROWS // 3, pltpu.SemaphoreType.DMA
        leads = [(3, 3, tiles, SIDE, SIDE), (3, 3, tiles, SIDE), (3, 3, tiles)][:phases]
        slots = [pltpu.VMEM((*lead, third, width), BF16) for lead in leads for _, width in ways_of(TILE)]
        return [pltpu.VMEM((RING, SIDE, SIDE, SIDE, GATE_ROWS, TILE), BF16), *slots, dma((tiles, 7)), dma((tiles, 7))]

    def part(self, t, way):
        start, width = self.ways[way]
        return pl.ds(t * self.rows, self.rows), pl.ds(start, width)

    def own(self, c, t, way, hops, b=ALL, d=ALL):
        at = index(ORDERS[t], (self.place.block(ORDERS[t][0], way, hops), ALL, ALL))
        axes = [i for i in range(3) if i != ORDERS[t][0]]
        at = list(at)
        at[axes[0]], at[axes[1]] = b, d
        return self.held.at[(lax.rem(c, RING), *at, *self.part(t, way))]

    def copy(self, phase, t, way, n, c, first=False):
        axis = ORDERS[t][phase]
        slots = self.slots[2 * phase + way]
        if not first:
            src = slots.at[t, n - 1, c]
        elif phase == 0:
            src = self.own(c, t, way, 1)
        else:
            src = self.slots[way].at[(t, 2, c, *second(t, self.place.block(axis, way, 1)))]
        key = (c, 3 * phase + n)
        return put(src, slots.at[t, n, c], self.send.at[key], self.recv.at[key], self.place.onwards[axis, way])

    def direct(self, t, way, off, c):
        axis = ORDERS[t][2]
        v = lax.rem(self.place.at[axis] + off, SIDE)
        src, dst = self.slots[2 + way].at[t, 2, c, v], self.slots[4 + way].at[t, off - 1, c]
        return put(src, dst, self.send.at[c, 6], self.recv.at[c, 6], self.place.device(axis, off))

    def pairs(self):
        return [(t, way) for t in range(3) for way in range(2)]

    def all_of(self, phase):
        return self.held.at[(0,) * (phase + 2)] if phase < 2 else self.held.at[0, 0, 0, pl.ds(0, 3)]

    def begin(self, phase, c):
        for t, way in self.pairs():
            if phase < 2:
                self.copy(phase, t, way, 0, c, first=True).start()
            else:
                for off in range(1, SIDE):
                    self.direct(t, way, off, c).start()

    def add(self, phase, t, way, n, c):
        slots = self.slots[2 * phase + way]
        v = self.place.block(ORDERS[t][phase], way, n + 1)

        def one(at, other):
            at = (t, n - 1, c, *at)
            slots[at] = (slots[at].astype(F32) + other[...].astype(F32)).astype(BF16)

        if phase == 0:
            for b in range(SIDE):
                for d in range(SIDE):
                    one((b, d), self.own(c, t, way, n + 1, b, d))
        else:
            for d in range(SIDE):
                one((d,), self.slots[way].at[(t, 2, c, *second(t, v, d))])

    def stage(self, s, c, out):
        phase, n = (s - 1) // 3, (s - 1) % 3 + 1
        whole_stage = self.all_of(phase)
        pltpu.make_async_copy(whole_stage, whole_stage, self.recv.at[c, s - 1]).wait()
        if phase == 2:
            for t, way in self.pairs():
                total = self.slots[2 + way][t, 2, c, self.place.at[ORDERS[t][2]]].astype(F32)
                for i in range(3):
                    total += self.slots[4 + way][t, i, c].astype(F32)
                rows, _ = self.part(t, way)
                start, width = self.ways[way]
                out[rows, pl.ds(pl.multiple_of(c * TILE + start, LANES), width)] = total.astype(BF16)
            return
        for t, way in self.pairs():
            self.add(phase, t, way, n, c)
            if n < 3:
                self.copy(phase, t, way, n, c).start()
        if n == 3 and phase + 1 < self.phases:
            self.begin(phase + 1, c)

    def sent(self, phase, n, c):
        whole_stage = self.all_of(phase)
        pltpu.make_async_copy(whole_stage, whole_stage, self.send.at[c, 3 * phase + n]).wait()

    def count(self):
        return 3 if self.phases == 1 else 7

    def keep(self, c):
        pl.when(c >= RING)(lambda: self.sent(0, 0, c - RING))
        return self.held.at[lax.rem(c + RING, RING)]

    def run(self, s, c, out):
        act = (lambda: self.begin(0, c)) if s == 0 else (lambda: self.stage(s, c, out))
        pl.when((c >= 0) & (c < self.tiles))(act)

    def early(self, j, out=None):
        for s in range(self.count(), 1, -1):
            self.run(s, j - 3 - s, out)

    def late(self, j, out=None):
        self.run(0, j - 2, out)
        self.run(1, j - 3, out)

    def last_step(self):
        return self.tiles - 1 + 3 + self.count()

    def drain(self):
        def each(c, _):
            pl.when(c >= self.tiles - RING)(lambda: self.sent(0, 0, c))
            for i in range(1, self.count()):
                self.sent(i // 3, i % 3, c)
            return 0

        lax.fori_loop(0, self.tiles, each, 0)

    def results(self):
        return [self.slots[way].at[:, 2] for way in range(2)]


def stream_halves(tiles):
    return [(3, tiles, SIDE, SIDE, GATE_ROWS // 3, width) for _, width in ways_of(TILE)]


class StreamRest:
    def __init__(self, place, tiles, before, refs):
        self.place, self.tiles, self.before, self.slots, self.sems = place, tiles, before, refs[:4], refs[4:8]
        self.rows, self.ways = GATE_ROWS // 3, ways_of(TILE)

    @staticmethod
    def scratch(tiles):
        third, dma = GATE_ROWS // 3, pltpu.SemaphoreType.DMA
        shapes = [pltpu.VMEM((3, 3, *lead, third, width), BF16) for lead in ((tiles, SIDE), (tiles,)) for _, width in ways_of(TILE)]
        return shapes + [dma((3, 2, 3))] * 4

    def pairs(self):
        return [(t, way) for t in range(3) for way in range(2)]

    def message(self, phase, t, way, n, arriving=False):
        slots = self.slots[2 * phase - 2 + way]
        axis = ORDERS[t][phase]
        if arriving:
            src = slots.at[t, n]
        elif isinstance(n, int) and n == 0:
            v = self.place.block(axis, way, 1)
            src = self.before[way].at[(t, ALL, *second(t, v))] if phase == 1 else self.slots[way].at[t, 2, :, v]
        else:
            src = slots.at[t, n - 1]
        send, recv = self.sems[2 * phase - 2 : 2 * phase]
        key = (t, way, n)
        return put(src, slots.at[t, n], send.at[key], recv.at[key], self.place.onwards[axis, way])

    def start(self, phase):
        for t, way in self.pairs():
            self.message(phase, t, way, 0).start()

    def step(self, phase, n):
        for t, way in self.pairs():
            self.message(phase, t, way, n - 1, arriving=True).wait_recv()
            v = self.place.block(ORDERS[t][phase], way, n + 1)
            slots = self.slots[2 * phase - 2 + way]

            def add(c, _, t=t, way=way, v=v, slots=slots):
                for d in range(SIDE if phase == 1 else 1):
                    at = (t, n - 1, c, d) if phase == 1 else (t, n - 1, c)
                    other = self.before[way].at[(t, c, *second(t, v, d))] if phase == 1 else self.slots[way].at[t, 2, c, v]
                    slots[at] = (slots[at].astype(F32) + other[...].astype(F32)).astype(BF16)
                return 0

            lax.fori_loop(0, self.tiles, add, 0)
            pl.when(n < 3)(lambda t=t, way=way: self.message(phase, t, way, n).start())

    def tick(self, i):
        pl.when(i == 0)(lambda: self.start(1))
        pl.when((i >= 1) & (i <= 3))(lambda: self.step(1, i))
        pl.when(i == 3)(lambda: self.start(2))
        pl.when((i >= 4) & (i <= 6))(lambda: self.step(2, i - 3))

    def result(self, out):
        def one(c, _):
            for t, way in self.pairs():
                start, width = self.ways[way]
                lanes = pl.ds(pl.multiple_of(c * TILE + start, LANES), width)
                out[pl.ds(t * self.rows, self.rows), lanes] = self.slots[2 + way][t, 2, c]
            return 0

        lax.fori_loop(0, self.tiles, one, 0)

    def drain(self):
        for t, way in self.pairs():
            for phase in (1, 2):
                for n in range(3):
                    self.message(phase, t, way, n).wait_send()


BLOCK_ROWS = SIDE * SIDE * GATE_ROWS


def gate_up_kernel(tiles, phases, cols, at, ahead, behind, *rest):
    j = pl.program_id(0)
    place = Place()
    core = place.core
    if phases == 1:
        outs, out, rest = rest[:2], None, rest[2:]
    else:
        sum_down, out, out_down, rest = rest[0], rest[1], rest[2], rest[3:]
    pair = PairSum(place, tiles, *rest[:4])
    stream = Stream(place, tiles, phases, rest[4 : 4 + 3 + 2 * phases])
    rest = rest[4 + 3 + 2 * phases :]
    if phases == 3:
        first = First.of(place, DOWN_WINDOW, cols, rest[1:6])
        down = Rest.of(place, DOWN_WINDOW, cols, first.results(), rest[6:14])
        loads = loads_down(sum_down, first, rest[0])

    @pl.when(j == 0)
    def _():
        opposite = [place.device(axis, 2) for axis in range(3)] if phases == 3 else []
        signal_all(near(place) + opposite)
        if phases == 3:
            begin(loads)

    stream.early(j, out)

    pl.when((j >= 2) & (j <= tiles + 1))(lambda: pair.copy(j - 2).wait_recv())

    @pl.when(j <= tiles + 1)
    def _():
        slot, kept = pair.reserve(j), stream.keep(j - 2)
        both = side_by_side(ahead[0, 1 - core], behind[0, core])
        landed = lax.rem(j + tiles - 2, tiles)
        for m in range(SIDE):
            r = pl.ds(m * BLOCK_ROWS, BLOCK_ROWS)
            tile = dot(at[r, :], both, NN)
            slot[r, :] = tile[:, :TILE].astype(BF16)
            total = (tile[:, TILE:] + pair.landing[landed, r, :].astype(F32)).astype(BF16)
            kept[m] = total.reshape(SIDE, SIDE, GATE_ROWS, TILE)

    pl.when(j < tiles)(lambda: pair.copy(j).start())
    stream.late(j, out)
    if phases == 3:
        pl.when(j == 0)(lambda: end(loads))
        pl.when(j <= tiles + 1)(lambda: spread(j, tiles + 2, 16, first.tick))
        pl.when(j > tiles + 1)(lambda: down.tick(j - tiles - 2))

    @pl.when(j == stream.last_step())
    def _():
        if phases == 1:
            saves = copies(stream.results(), outs, rest[0])
            begin(saves)
            stream.drain()
            end(saves)
        else:
            down.result(out_down)
            stream.drain()
            first.drain()
            down.drain()


def gate_up_call(name, collective_id, phases, at, dgu, *sum_down):
    d, tokens = at.shape
    tiles, cols, dma = dgu.shape[0], d // 2, pltpu.SemaphoreType.DMA
    ff = tiles * TILE
    now, before = clip(tiles), clip(tiles, 2)
    if phases == 1:
        shapes = stream_halves(tiles)
        out_specs, more = [HBM] * 2, [dma((2,))]
    else:
        shapes = [(GATE_ROWS, ff), (DOWN_WINDOW, cols)]
        out_specs = [whole(s) for s in shapes]
        more = [dma((SIDE,)), *First.scratch(DOWN_WINDOW, cols), *Rest.scratch(DOWN_WINDOW, cols)]
    return pl.pallas_call(
        functools.partial(gate_up_kernel, tiles, phases, cols),
        name=name,
        grid=(tiles + (6 if phases == 1 else 10),),
        in_specs=[
            whole((d, tokens)),
            spec((1, 2, tokens, TILE), lambda j: (now(j), 0, 0, 0)),
            spec((1, 2, tokens, TILE), lambda j: (before(j), 0, 0, 0)),
            *[HBM] * len(sum_down),
        ],
        out_specs=out_specs,
        out_shape=[jax.ShapeDtypeStruct(s, BF16) for s in shapes],
        scratch_shapes=[*PairSum.scratch(tiles, d, TILE), *Stream.scratch(tiles, phases), *more],
        compiler_params=params(collective_id),
    )(at, dgu, dgu, *sum_down)


def gate_up_first_kernel(tiles, cols, at, ahead, behind, sum_down, out, half0, half1, *rest):
    j = pl.program_id(0)
    place = Place()
    core = place.core
    pair = PairSum(place, tiles, *rest[:4])
    first = First.of(place, DOWN_WINDOW, cols, rest[4:9])
    load_sem, save_sem = rest[9:11]
    loads = loads_down(sum_down, first, load_sem)

    @pl.when(j == 0)
    def _():
        signal_all(near(place))
        begin(loads)

    pl.when(j >= 2)(lambda: pair.copy(j - 2).wait_recv())
    slot = pair.reserve(j)
    both = side_by_side(ahead[0, 1 - core], behind[0, core])
    landed = lax.rem(j + tiles - 2, tiles)
    for m in range(at.shape[0] // ROWS):
        r = pl.ds(m * ROWS, ROWS)
        tile = dot(at[r, :], both, NN)
        slot[r, :] = tile[:, :TILE].astype(BF16)
        out[r, :] = (tile[:, TILE:] + pair.landing[landed, r, :].astype(F32)).astype(BF16)
    pl.when(j < tiles)(lambda: pair.copy(j).start())

    pl.when(j == 0)(lambda: end(loads))
    spread(j, tiles + 2, 16, first.tick)

    @pl.when(j == tiles + 1)
    def _():
        saves = copies(first.results(), (half0, half1), save_sem)
        begin(saves)
        first.drain()
        end(saves)


def gate_up_first_call(name, collective_id, at, dgu, sum_down):
    d, tokens = at.shape
    tiles, cols, dma = dgu.shape[0], sum_down.shape[-1], pltpu.SemaphoreType.DMA
    now, before = clip(tiles), clip(tiles, 2)
    return pl.pallas_call(
        functools.partial(gate_up_first_kernel, tiles, cols),
        name=name,
        grid=(tiles + 2,),
        in_specs=[
            whole((d, tokens)),
            spec((1, 2, tokens, TILE), lambda j: (now(j), 0, 0, 0)),
            spec((1, 2, tokens, TILE), lambda j: (before(j), 0, 0, 0)),
            HBM,
        ],
        out_specs=[spec((d, TILE), lambda j: (0, before(j))), HBM, HBM],
        out_shape=[jax.ShapeDtypeStruct((d, tiles * TILE), BF16)]
        + [jax.ShapeDtypeStruct(s, BF16) for s in half_sums(DOWN_WINDOW, cols)],
        scratch_shapes=[*PairSum.scratch(tiles, d, TILE), *First.scratch(DOWN_WINDOW, cols), dma((SIDE,)), dma((2,))],
        compiler_params=params(collective_id),
    )(at, dgu, dgu, sum_down)


def middle_kernel(steps, ff, dgu, wg, wu, h, dy, sum_gu, dh, half0, half1, acc_g, acc_u, *rest):
    j = pl.program_id(0)
    place = Place()
    first = First.of(place, GATE_ROWS, ff, rest[:5])
    load_sem, save_sem = rest[5:7]
    loads = [pltpu.make_async_copy(sum_gu.at[x], first.held.at[x], load_sem.at[x]) for x in range(SIDE)]

    @pl.when(j == 0)
    def _():
        signal_all(near(place))
        begin(loads)
        clear(acc_g)
        clear(acc_u)

    def add_up(r, two):
        for which, (acc, w) in enumerate(((acc_g, wg), (acc_u, wu))):
            if two:
                acc[r, :] += dot(side_by_side(dgu[0, which, r, :], dgu[1, which, r, :]), w[0], NT)
            else:
                acc[r, :] += dot(dgu[0, which, r, :], w[0, :, pl.ds(0, TILE)], NT)

    pl.when(j < steps - 1)(lambda: in_rows(h.shape[0], 2 * ROWS, lambda r: add_up(r, True)))
    pl.when(j == steps - 1)(lambda: in_rows(h.shape[0], ROWS, lambda r: add_up(r, False)))

    pl.when(j == 0)(lambda: end(loads))
    spread(j, steps, 16, first.tick)

    @pl.when(j == steps - 1)
    def _():
        saves = copies(first.results(), (half0, half1), save_sem)
        begin(saves)

        def rows(r):
            wide = h[r, :].astype(F32)
            scale = norm_scale(wide)
            da = (acc_g[r, :].astype(BF16).astype(F32) + acc_u[r, :].astype(BF16).astype(F32)).astype(BF16).astype(F32)
            back = scale * da - wide * (scale * scale * scale * jnp.mean(da * wide, -1, keepdims=True))
            dh[r, :] = (dy[r, :].astype(F32) + back.astype(BF16).astype(F32)).astype(BF16)

        in_rows(h.shape[0], 32, rows)
        first.drain()
        end(saves)


def middle_call(collective_id, dgu, wg, wu, h, dy, sum_gu):
    tokens, d = h.shape
    tiles, dma = dgu.shape[0], pltpu.SemaphoreType.DMA
    ff = tiles * TILE
    steps = (tiles + 1) // 2
    w_in = spec((1, d, 2 * TILE), lambda j: (1, 0, j))
    return pl.pallas_call(
        functools.partial(middle_kernel, steps, ff),
        name="middle",
        grid=(steps,),
        in_specs=[spec((2, 2, tokens, TILE), lambda j: (j, 0, 0, 0)), w_in, w_in, whole((tokens, d)), whole((tokens, d)), HBM],
        out_specs=[whole((tokens, d)), HBM, HBM],
        out_shape=[jax.ShapeDtypeStruct(s, BF16) for s in ((tokens, d), *half_sums(GATE_ROWS, ff))],
        scratch_shapes=[pltpu.VMEM((tokens, d), F32)] * 2 + First.scratch(GATE_ROWS, ff) + [dma((SIDE,)), dma((2,))],
        compiler_params=params(collective_id),
    )(dgu, wg, wu, h, dy, sum_gu)


def back_kernel(tiles, ff, dh, gate, up, wd, gate0, gate1, down0, down1, dgu, out, out_gu, out_down, p, *rest):
    j = pl.program_id(0)
    place = Place()
    half = dh.shape[1] // 2
    pair = PairSum(place, tiles, *rest[:4])
    before = rest[4:8]
    gate_up = Rest.of(place, GATE_ROWS, ff, before[:2], rest[8:16])
    down = Rest.of(place, DOWN_WINDOW, half, before[2:], rest[16:24])
    loads = copies((gate0, gate1, down0, down1), before, rest[24])

    @pl.when(j == 0)
    def _():
        signal_all(near(place))
        begin(loads)

    @pl.when(j < tiles)
    def _():
        slot = lax.rem(j, 2)
        for m in range(dh.shape[0] // ROWS):
            r = pl.ds(m * ROWS, ROWS)
            dp = dot(dh[r, :], wd[0], NT).astype(BF16)
            p[slot, r, :], dgu[0, 0, r, :], dgu[0, 1, r, :] = hidden_back(gate[0, r, :], up[0, r, :], dp)

    down_gradient(j, tiles, pair, p, dh, half, out)
    pl.when(j == 0)(lambda: end(loads))
    gate_up.tick(j)
    pl.when(j >= tiles - 6)(lambda: down.tick(j - tiles + 6))

    @pl.when(j == tiles)
    def _():
        gate_up.result(out_gu)
        down.result(out_down)
        gate_up.drain()
        down.drain()


def back_call(collective_id, dh, gate, up, wd, gate_halves, down_halves):
    tokens, d = dh.shape
    tiles, half, dma = gate.shape[0], d // 2, pltpu.SemaphoreType.DMA
    ff = tiles * TILE
    now, before = clip(tiles), clip(tiles, 1)
    tile = spec((1, tokens, TILE), lambda j: (now(j), 0, 0))
    sums = [(GATE_ROWS, ff), (DOWN_WINDOW, half)]
    return pl.pallas_call(
        functools.partial(back_kernel, tiles, ff),
        name="back_0",
        grid=(tiles + 1,),
        in_specs=[whole((tokens, d)), tile, tile, spec((1, TILE, d), lambda j: (0, now(j), 0))] + [HBM] * 4,
        out_specs=[
            spec((1, 2, tokens, TILE), lambda j: (now(j), 0, 0, 0)),
            spec((TILE, half), lambda j: (before(j), 0)),
            *[whole(s) for s in sums],
        ],
        out_shape=[jax.ShapeDtypeStruct(s, BF16) for s in ((tiles, 2, tokens, TILE), (ff, half), *sums)],
        scratch_shapes=[pltpu.VMEM((2, tokens, TILE), BF16), *PairSum.scratch(tiles, TILE, half)]
        + [pltpu.VMEM(t.shape, BF16) for t in (*gate_halves, *down_halves)]
        + Rest.scratch(GATE_ROWS, ff)
        + Rest.scratch(DOWN_WINDOW, half)
        + [dma((4,))],
        compiler_params=params(collective_id),
    )(dh, gate, up, wd, *gate_halves, *down_halves)


def flat(m):
    layers, rows, cols = m.shape
    split = m.transpose(1, 0, 2).reshape(rows, layers, cols // LANES, LANES)
    return with_layout_constraint(split, Layout((0, 2, 1, 3))).transpose(0, 2, 1, 3).reshape(-1, LANES)


def unflat(f, shape):
    layers, rows, cols = shape
    split = f.reshape(rows, cols // LANES, layers, LANES).transpose(0, 2, 1, 3)
    return with_layout_constraint(split, Layout((0, 2, 1, 3))).reshape(rows, layers, cols).transpose(1, 0, 2)


def solution(mesh):
    def body(x, dy, wg, wu, wd, mg, mu, md, vg, vu, vd):
        layers, d, ff = wg.shape
        x, dy = x[0], dy[0]
        windows = (SIDE, SIDE, 4 * 66, d // 2)
        gate0, up0, h1, a1, a0t = forward_call(x, wg, wu, wd)
        dgu1, a1t, down1 = layer_call(1, a1, dy, wg, wu, wd)
        blocks = (SIDE, SIDE, SIDE, GATE_ROWS, ff)
        gu1, *down_halves = gate_up_first_call("gate_up_1", 2, a1t, dgu1, down1.reshape(windows))
        dh1, *gate_halves = middle_call(3, dgu1, wg, wu, h1, dy, gu1.reshape(blocks))
        dgu0, down0, sum_gu1, sum_down1 = back_call(4, dh1, gate0, up0, wd, gate_halves, down_halves)
        sum_gu0, sum_down0 = gate_up_call("gate_up_0", 5, 3, a0t, dgu0, down0.reshape(windows))

        views = [(2, SIDE, SIDE, SIDE, GATE_ROWS, ff)] * 2 + [(2, SIDE, SIDE, 4 * 66, d)]
        w = [t.reshape(view) for t, view in zip((wg, wu, wd), views, strict=True)]
        m, v = [flat(t) for t in (mg, mu, md)], [flat(t) for t in (vg, vu, vd)]
        own, other, down, *moments = finish_call(3 * layers * d * ff, 6, [sum_gu0, sum_gu1], [sum_down0, sum_down1], m, v, w)
        out = [*write_call(own, other, down), *moments]
        new = [t.reshape(like.shape) for t, like in zip(out[:3], (wg, wu, wd), strict=True)]
        return (*new, *[unflat(t, like.shape) for t, like in zip(out[3:], (mg, mu, md, vg, vu, vd), strict=True)])

    shard = P(None, "dp", None)
    return jax.shard_map(
        body,
        mesh=mesh,
        in_specs=(P(("rep", "dp")), P(("rep", "dp")), P(), P(), P(), *[shard] * 6),
        out_specs=(P("rep"), P("rep"), P("rep"), *[P("rep", "dp", None)] * 6),
        check_vma=False,
    )
```
